32 devices in a mesh: dp: 1 (over z), tp: 32 (over y, x, core).
Axes of the slice: x: 4, y: 4, z: 1, core: 2. Of those that a mesh axis runs over, the one named last changes fastest.
The devices are a block of a 4x4x8 slice.
Arguments:
- x_in: bfloat16 [2048, 8192], P(('dp', 'tp'))
- dy_in: bfloat16 [2048, 8192], P(('dp', 'tp'))
- w_q: bfloat16 [8192, 128, 64], P(None, 'tp')
- w_k: bfloat16 [8192, 8, 64], replicated
- w_v: bfloat16 [8192, 8, 64], replicated
- w_o: bfloat16 [128, 64, 8192], P('tp')
Outputs:
- output 1: bfloat16 [2048, 8192], P(('dp', 'tp'))
- output 2: float32 [8192, 128, 64], P('dp', 'tp')
- output 3: float32 [128, 64, 8192], P(('dp', 'tp'))
- output 4: float32 [65536, 64], P(('dp', 'tp'))
- output 5: float32 [65536, 64], P(('dp', 'tp'))
All inputs are finite; a program needn't handle non-finite values.
Results may differ from the reference program's by a relative error of at most 0.00953466.
Values are sent between devices in bfloat16 or wider.
A program may use at most 768 MiB of HBM per device.

```python
import jax
import jax.numpy as jnp
from jax import lax

D = 8192
HEADS = 128
KV_HEADS = 8
HEAD = 64
TOKENS = 2048
MODEL = 32

HEADS_DEV = HEADS // MODEL
REPL = MODEL // KV_HEADS
SCALE = HEAD ** -0.5


def setup_inputs(seed: int = 0, part: int = 0) -> dict:
    part_key = jax.random.fold_in(jax.random.key(seed), part)
    key_x, key_dy = jax.random.split(part_key)
    key_q, key_k, key_v, key_o = jax.random.split(jax.random.key(seed + 1), 4)
    fan_scale = D ** -0.5
    x_in = jax.random.normal(key_x, (TOKENS, D), jnp.float32).astype(jnp.bfloat16)
    dy_in = jax.random.normal(key_dy, (TOKENS, D), jnp.float32).astype(jnp.bfloat16)
    w_q = (jax.random.normal(key_q, (D, HEADS, HEAD), jnp.float32) * fan_scale).astype(jnp.bfloat16)
    w_k = (jax.random.normal(key_k, (D, KV_HEADS, HEAD), jnp.float32) * fan_scale).astype(jnp.bfloat16)
    w_v = (jax.random.normal(key_v, (D, KV_HEADS, HEAD), jnp.float32) * fan_scale).astype(jnp.bfloat16)
    w_o = (jax.random.normal(key_o, (HEADS, HEAD, D), jnp.float32) * fan_scale).astype(jnp.bfloat16)
    return dict(x_in=x_in, dy_in=dy_in, w_q=w_q, w_k=w_k, w_v=w_v, w_o=w_o)


def reference(x_in, dy_in, w_q, w_k, w_v, w_o):
    f32 = jnp.float32
    bf16 = jnp.bfloat16
    x_wide = x_in.astype(f32)
    dy_wide = dy_in.astype(f32)
    causal = lax.broadcasted_iota(jnp.int32, (TOKENS, TOKENS), 0) >= lax.broadcasted_iota(jnp.int32, (TOKENS, TOKENS), 1)
    wq_dev = jnp.transpose(w_q.reshape(D, MODEL, HEADS_DEV, HEAD), (1, 0, 2, 3))
    wo_dev = w_o.reshape(MODEL, HEADS_DEV, HEAD, D)
    wk_dev = jnp.repeat(jnp.transpose(w_k, (1, 0, 2)), REPL, axis=0)
    wv_dev = jnp.repeat(jnp.transpose(w_v, (1, 0, 2)), REPL, axis=0)

    def device_step(dx_acc, weights):
        wq_loc, wo_loc, wk_loc, wv_loc = weights
        wq_wide = wq_loc.astype(f32)
        wk_wide = wk_loc.astype(f32)
        wv_wide = wv_loc.astype(f32)
        queries = jnp.einsum("tc,che->hte", x_wide, wq_wide).astype(bf16)
        key_rows = jnp.dot(x_in, wk_loc, preferred_element_type=f32).astype(bf16)
        val_rows = jnp.dot(x_in, wv_loc, preferred_element_type=f32).astype(bf16)
        scores = jnp.einsum("hqe,ke->hqk", queries.astype(f32), key_rows.astype(f32)) * SCALE
        scores = jnp.where(causal, scores, -jnp.inf)
        attn_prob = jax.nn.softmax(scores, axis=-1)
        prob_bf = attn_prob.astype(bf16)
        attn_out = jnp.einsum("hqk,ke->hqe", prob_bf.astype(f32), val_rows.astype(f32)).astype(bf16)
        d_out = jnp.einsum("tc,hec->hte", dy_wide, wo_loc.astype(f32)).astype(bf16)
        grad_wo = jnp.einsum("hte,tc->hec", attn_out.astype(f32), dy_wide)
        d_prob = jnp.einsum("hqe,ke->hqk", d_out.astype(f32), val_rows.astype(f32))
        delta_row = jnp.sum(d_out.astype(f32) * attn_out.astype(f32), axis=-1, keepdims=True)
        d_score = (attn_prob * (d_prob - delta_row)).astype(bf16)
        d_query = (jnp.einsum("hqk,ke->hqe", d_score.astype(f32), key_rows.astype(f32)) * SCALE).astype(bf16)
        d_key = (jnp.einsum("hqk,hqe->ke", d_score.astype(f32), queries.astype(f32)) * SCALE).astype(bf16)
        d_val = jnp.einsum("hqk,hqe->ke", prob_bf.astype(f32), d_out.astype(f32)).astype(bf16)
        grad_wq = jnp.einsum("tc,hte->che", x_wide, d_query.astype(f32))
        dx_part = (jnp.einsum("hte,che->tc", d_query.astype(f32), wq_wide)
                   + jnp.dot(d_key.astype(f32), wk_wide.T)
                   + jnp.dot(d_val.astype(f32), wv_wide.T))
        return dx_acc + dx_part, (grad_wq, grad_wo, d_key, d_val)

    dx_sum, stacked = lax.scan(device_step, jnp.zeros((TOKENS, D), f32), (wq_dev, wo_dev, wk_dev, wv_dev))
    grad_wq, grad_wo, d_key, d_val = stacked
    dx_out = dx_sum.astype(bf16)
    dw_q = jnp.transpose(grad_wq, (1, 0, 2, 3)).reshape(D, HEADS, HEAD)
    dw_o = grad_wo.reshape(HEADS, HEAD, D)
    key_grp = d_key.reshape(KV_HEADS, REPL, TOKENS, HEAD).astype(f32)
    val_grp = d_val.reshape(KV_HEADS, REPL, TOKENS, HEAD).astype(f32)
    dw_k = jnp.einsum("tc,jrte->jce", x_wide, key_grp).reshape(KV_HEADS * D, HEAD)
    dw_v = jnp.einsum("tc,jrte->jce", x_wide, val_grp).reshape(KV_HEADS * D, HEAD)
    return dx_out, dw_q, dw_o, dw_k, dw_v
```

```python
import functools
import math

import jax
import jax.numpy as jnp
from jax import lax
from jax.experimental import pallas as pl
from jax.experimental.pallas import tpu as pltpu
from jax.sharding import PartitionSpec as P

F32 = jnp.float32
BF16 = jnp.bfloat16
MESH = pl.DeviceIdType.MESH
ANY = pl.BlockSpec(memory_space=pl.ANY)
VMEM = pl.BlockSpec(memory_space=pltpu.VMEM)
LOG2E = math.log2(math.e)
ORDER = (2, 1, 3, 0)


def _dot(a, b, dims):
    return lax.dot_general(a, b, (dims, ((), ())), preferred_element_type=F32)


def _nn(a, b):
    return _dot(a, b, ((1,), (0,)))


def _nt(a, b):
    return _dot(a, b, ((1,), (1,)))


class Place:
    def __init__(self, ring, cores):
        me = lax.axis_index("tp")
        self.ring, self.cores = ring, cores
        self.c = lax.rem(me, cores)
        self.x = lax.rem(me // cores, ring)
        self.y = me // (cores * ring)
        self.r = self.x * cores + self.c
        self.n_row = ring * cores

    def dev(self, y, x, c):
        y = lax.rem(y + self.ring, self.ring)
        x = lax.rem(x + self.ring, self.ring)
        return {"tp": (y * self.ring + x) * self.cores + c}

    def row_dev(self, r):
        return {"tp": self.y * self.n_row + r}

    def slot(self, x, c):
        return lax.rem(x + self.ring, self.ring) * self.cores + c


def _remote(src, dst, send, recv, dev):
    return pltpu.make_async_remote_copy(
        src_ref=src, dst_ref=dst, send_sem=send, recv_sem=recv, device_id=dev, device_id_type=MESH
    )


def _enter(devices):
    barrier = pltpu.get_barrier_semaphore()
    for dev in devices:
        pl.semaphore_signal(barrier, inc=1, device_id=dev, device_id_type=MESH)
    pl.semaphore_wait(barrier, len(devices))


def _proj_kernel(w_ref, x_ref, o_ref):
    o_ref[...] = _nt(w_ref[...], x_ref[...]).astype(BF16)


def _proj(w, x, block):
    n, width = w.shape
    tokens = x.shape[0]
    return pl.pallas_call(
        _proj_kernel,
        name="proj",
        grid=(tokens // block,),
        in_specs=[pl.BlockSpec((n, width), lambda i: (0, 0)), pl.BlockSpec((block, width), lambda i: (i, 0))],
        out_specs=pl.BlockSpec((n, block), lambda i: (0, i)),
        out_shape=jax.ShapeDtypeStruct((n, tokens), BF16),
        compiler_params=pltpu.CompilerParams(vmem_limit_bytes=48 << 20),
        cost_estimate=pl.CostEstimate(flops=2 * n * width * tokens, bytes_accessed=2 * (n + tokens) * width, transcendentals=0),
    )(w, x)


def _attn_kernel(ring, cores, heads, scale, bq, qkvt_ref, dot_ref, wq_ref, g_ref, dqt_ref, ot_ref, wrow_ref,
                 s_ref, dk_ref, dv_ref, w_buf, send, recv, local):
    at = Place(ring, cores)
    n_row = at.n_row
    e = qkvt_ref.shape[0] // (heads + 2)
    tokens = qkvt_ref.shape[1]
    cw = wrow_ref.shape[2]
    peers = [lax.rem(at.r + d, n_row) for d in range(n_row)]
    _enter([at.row_dev(r) for r in peers[1:]])
    copies = []
    for d in range(1, n_row):
        cols = pl.ds(pl.multiple_of(peers[d] * cw, cw), cw)
        cp = _remote(wq_ref.at[:, cols], wrow_ref.at[at.r], send.at[d], recv.at[d], at.row_dev(peers[d]))
        cp.start()
        copies.append(cp)
    own_in = pltpu.make_async_copy(wq_ref.at[:, pl.ds(pl.multiple_of(at.r * cw, cw), cw)], w_buf, local.at[0])
    own_in.start()
    own_in.wait()
    own_out = pltpu.make_async_copy(w_buf, wrow_ref.at[at.r], local.at[1])
    own_out.start()

    dk_ref[...] = jnp.zeros_like(dk_ref)
    dv_ref[...] = jnp.zeros_like(dv_ref)
    krow, vrow = heads * e, (heads + 1) * e
    row = lax.broadcasted_iota(jnp.int32, (bq, bq), 0)
    col = lax.broadcasted_iota(jnp.int32, (bq, bq), 1)
    for i in range(tokens // bq):
        q0 = i * bq
        chunks = [slice(k, k + bq) for k in range(0, q0 + bq, bq)]
        qs = slice(q0, q0 + bq)

        def head(h, _, q0=q0, chunks=chunks, qs=qs):
            hs = pl.ds(pl.multiple_of(h * e, e), e)
            qt = qkvt_ref[hs, qs]
            dot = dot_ref[hs, qs]
            q = qt.T
            do = dot.T
            m = None
            for ks in chunks:
                s = _nn(q, qkvt_ref[krow:krow + e, ks])
                if ks.start == q0:
                    s = jnp.where(row >= col, s, -jnp.inf)
                s_ref[:, ks] = s
                part = s[:, :128]
                for t in range(128, bq, 128):
                    part = jnp.maximum(part, s[:, t:t + 128])
                m = part if m is None else jnp.maximum(m, part)
            m = jnp.max(m, axis=1, keepdims=True)
            total = None
            for ks in chunks:
                p = jnp.exp2((s_ref[:, ks] - m) * (scale * LOG2E))
                s_ref[:, ks] = p
                part = p[:, :128]
                for t in range(128, bq, 128):
                    part = part + p[:, t:t + 128]
                total = part if total is None else total + part
            inv = 1.0 / jnp.sum(total, axis=1, keepdims=True)
            out = None
            for ks in chunks:
                p = s_ref[:, ks] * inv
                s_ref[:, ks] = p
                pb = p.astype(BF16)
                part = _nt(pb, qkvt_ref[vrow:vrow + e, ks])
                out = part if out is None else out + part
                dv_ref[:, ks] += _nn(dot, pb)
            out = out.astype(BF16)
            ot_ref[hs, qs] = out.T
            delta = jnp.sum(do.astype(F32) * out.astype(F32), axis=1, keepdims=True)
            dq = None
            for ks in chunks:
                dp = _nn(do, qkvt_ref[vrow:vrow + e, ks])
                ds = (s_ref[:, ks] * (dp - delta)).astype(BF16)
                part = _nt(ds, qkvt_ref[krow:krow + e, ks])
                dq = part if dq is None else dq + part
                dk_ref[:, ks] += _nn(qt, ds)
            dqt_ref[hs, qs] = (dq * scale).astype(BF16).T
            return 0

        lax.fori_loop(0, heads, head, 0)
        g_ref[qs, 0:heads * e] = dqt_ref[:, qs].T
    for k in range(0, tokens, bq):
        ks = slice(k, k + bq)
        g_ref[ks, heads * e:(heads + 1) * e] = (dk_ref[:, ks] * scale).astype(BF16).T
        g_ref[ks, (heads + 1) * e:(heads + 2) * e] = dv_ref[:, ks].astype(BF16).T
    own_out.wait()
    for cp in copies:
        cp.wait()


def _attention(ring, cores, heads, scale, qkvt, dot, wq):
    tokens = qkvt.shape[1]
    e = qkvt.shape[0] // (heads + 2)
    n_row = ring * cores
    cw = wq.shape[1] // n_row
    bq = min(256, tokens)
    return pl.pallas_call(
        functools.partial(_attn_kernel, ring, cores, heads, scale, bq),
        name="attn",
        in_specs=[VMEM, VMEM, ANY],
        out_specs=[VMEM, VMEM, VMEM, ANY],
        out_shape=[
            jax.ShapeDtypeStruct((tokens, (heads + 2) * e), BF16),
            jax.ShapeDtypeStruct((heads * e, tokens), BF16),
            jax.ShapeDtypeStruct((heads * e, tokens), BF16),
            jax.ShapeDtypeStruct((n_row, heads * e, cw), BF16),
        ],
        scratch_shapes=[
            pltpu.VMEM((bq, tokens), F32),
            pltpu.VMEM((e, tokens), F32),
            pltpu.VMEM((e, tokens), F32),
            pltpu.VMEM((heads * e, cw), BF16),
            pltpu.SemaphoreType.DMA((n_row,)),
            pltpu.SemaphoreType.DMA((n_row,)),
            pltpu.SemaphoreType.DMA((2,)),
        ],
        compiler_params=pltpu.CompilerParams(collective_id=0, has_side_effects=True, vmem_limit_bytes=40 << 20),
        cost_estimate=pl.CostEstimate(flops=12 * heads * tokens * tokens * e, bytes_accessed=8 << 20, transcendentals=heads * tokens * tokens // 2),
    )(qkvt, dot, wq)


def _grads_kernel(ring, cores, heads, g_ref, wrow_ref, wkv_ref, dqt_ref, ot_ref, x_ref, dy_ref,
                  dx_ref, dwq_ref, dwo_ref, dwk_ref, dwv_ref,
                  gq, w_all, part, rs_half, rs_full, stage, xbuf, obuf, kvt,
                  ag_send, ag_recv, rs_send, rs_recv, out_send, out_recv, in_sem, o_sem, ld_sem):
    at = Place(ring, cores)
    n_row = at.n_row
    tokens, width = x_ref.shape
    gw = g_ref.shape[1]
    hd = dqt_ref.shape[0]
    e = hd // heads
    tb = tokens // ring
    th = tb // 2
    tl = tb // n_row
    cw = w_all.shape[1]
    hw = cw // 2
    half_a, half_b = pl.ds(0, hw), pl.ds(hw, hw)
    n_ld = 2 * n_row + 1

    def gcols(slot):
        return pl.ds(pl.multiple_of(slot * gw, gw), gw)

    loads = [pltpu.make_async_copy(g_ref, gq.at[:, gcols(at.r)], ld_sem.at[0])]
    per_kv = n_row // wkv_ref.shape[0]
    for r in range(n_row):
        loads.append(pltpu.make_async_copy(wrow_ref.at[r], w_all.at[pl.ds(r * gw, hd), :], ld_sem.at[1 + r]))
        loads.append(pltpu.make_async_copy(wkv_ref.at[r // per_kv], w_all.at[pl.ds(r * gw + hd, gw - hd), :], ld_sem.at[1 + n_row + r]))
    for cp in loads:
        cp.start()

    up, down = at.dev(at.y + 1, at.x, at.c), at.dev(at.y - 1, at.x, at.c)
    right, left = at.dev(at.y, at.x + 1, at.c), at.dev(at.y, at.x - 1, at.c)
    mate = at.dev(at.y, at.x, 1 - at.c)
    peers = [lax.rem(at.r + d, n_row) for d in range(n_row)]
    _enter([up, down] + [at.row_dev(r) for r in peers[1:]])
    loads[0].wait()

    s_own, s_left, s_right, s_far = at.r, at.slot(at.x - 1, at.c), at.slot(at.x + 1, at.c), at.slot(at.x + 2, at.c)
    m_own, m_left, m_right, m_far = at.slot(at.x, 1 - at.c), at.slot(at.x - 1, 1 - at.c), at.slot(at.x + 1, 1 - at.c), at.slot(at.x + 2, 1 - at.c)
    blocks = [lax.rem(at.y + o, ring) for o in ORDER]
    sends = []

    def piece(k, slot, half=None):
        r0 = pl.multiple_of(blocks[k] * tb, tb)
        rows = pl.ds(r0, tb) if half is None else pl.ds(pl.multiple_of(r0 + half * th, th), th)
        return gq.at[rows, gcols(slot)]

    def ag_send_piece(k, n, slot, dev, half=None):
        ref = piece(k, slot, half)
        cp = _remote(ref, ref, ag_send.at[k, n], ag_recv.at[k, n], dev)
        cp.start()
        sends.append(cp)

    def ag_wait(k, n, slot, half=None):
        ref = piece(k, slot, half)
        _remote(ref, ref, ag_send.at[k, n], ag_recv.at[k, n], mate).wait_recv()

    def ag_own(k):
        ag_send_piece(k, 0, s_own, right)
        ag_send_piece(k, 1, s_own, left)
        ag_send_piece(k, 2, s_own, mate)

    def ag_relay(k):
        ag_wait(k, 0, s_left)
        ag_send_piece(k, 3, s_left, right, 0)
        ag_send_piece(k, 4, s_left, mate)
        ag_wait(k, 1, s_right)
        ag_send_piece(k, 5, s_right, left, 1)
        ag_send_piece(k, 6, s_right, mate)

    def ag_finish(k):
        ag_wait(k, 3, s_far, 0)
        ag_send_piece(k, 7, s_far, mate, 0)
        ag_wait(k, 5, s_far, 1)
        ag_send_piece(k, 8, s_far, mate, 1)
        ag_wait(k, 2, m_own)
        ag_wait(k, 4, m_left)
        ag_wait(k, 6, m_right)
        ag_wait(k, 7, m_far, 0)
        ag_wait(k, 8, m_far, 1)

    nt = min(256, cw)

    def partial(k):
        rows = pl.ds(pl.multiple_of(blocks[k] * tb, tb), tb)

        def tile(j, _):
            cs = pl.ds(pl.multiple_of(j * nt, nt), nt)
            part[k, :, cs] = _nn(gq[rows, :], w_all[:, cs])
            return 0

        lax.fori_loop(0, cw // nt, tile, 0)

    def rs_send_piece(n, src, dst, dev):
        cp = _remote(src, dst, rs_send.at[n], rs_recv.at[n], dev)
        cp.start()
        sends.append(cp)

    def rs_wait(n, ref):
        _remote(ref, ref, rs_send.at[n], rs_recv.at[n], mate).wait_recv()

    bc = xbuf.shape[2]
    n_steps = width // bc

    def stream(src, lhs, out, j0, j1):
        def load(j, slot):
            return pltpu.make_async_copy(src.at[:, pl.ds(pl.multiple_of(j * bc, bc), bc)], xbuf.at[slot], in_sem.at[slot])

        def store(j, slot):
            return pltpu.make_async_copy(obuf.at[slot], out.at[:, pl.ds(pl.multiple_of(j * bc, bc), bc)], o_sem.at[slot])

        if j0 == 0:
            load(0, 0).start()

        def step(j, _):
            slot = lax.rem(j, 2)

            @pl.when(j + 1 < n_steps)
            def _():
                load(j + 1, 1 - slot).start()

            load(j, slot).wait()

            @pl.when(j >= 2)
            def _():
                store(j - 2, slot).wait()

            obuf[slot] = _nn(lhs[...], xbuf[slot])
            store(j, slot).start()
            return 0

        lax.fori_loop(j0, j1, step, 0)
        if j1 == n_steps:
            for j in range(max(n_steps - 2, 0), n_steps):
                store(j, j % 2).wait()

    cut = [n_steps * q // 4 for q in range(5)]

    ag_own(0)
    stream(dy_ref, ot_ref, dwo_ref, cut[0], cut[2])
    ag_relay(0)
    ag_own(1)
    stream(dy_ref, ot_ref, dwo_ref, cut[2], cut[3])
    ag_finish(0)
    for cp in loads[1:]:
        cp.wait()
    partial(0)
    rs_send_piece(0, part.at[0, :, half_a], rs_half.at[0], up)
    rs_send_piece(1, part.at[0, :, half_b], rs_half.at[1], down)
    stream(dy_ref, ot_ref, dwo_ref, cut[3], cut[4])
    ag_relay(1)
    ag_own(2)
    stream(x_ref, dqt_ref, dwq_ref, cut[0], cut[1])
    ag_finish(1)
    partial(1)
    rs_send_piece(2, part.at[1, :, half_b], rs_full.at[0, :, half_b], up)
    ag_relay(2)
    ag_own(3)
    stream(x_ref, dqt_ref, dwq_ref, cut[1], cut[2])
    ag_finish(2)
    partial(2)
    rs_send_piece(4, part.at[2, :, half_a], rs_full.at[1, :, half_a], down)
    ag_relay(3)
    rs_wait(0, rs_half.at[0])
    part[1, :, half_a] += rs_half[0]
    rs_wait(1, rs_half.at[1])
    part[2, :, half_b] += rs_half[1]
    rs_send_piece(3, part.at[1, :, half_a], rs_full.at[0, :, half_a], up)
    rs_send_piece(5, part.at[2, :, half_b], rs_full.at[1, :, half_b], down)
    ag_finish(3)
    partial(3)
    stream(x_ref, dqt_ref, dwq_ref, cut[2], cut[4])

    n_kv = wkv_ref.shape[0]
    first = (at.r // per_kv) * per_kv
    for q in range(per_kv):
        cols = pl.ds(pl.multiple_of((first + q) * gw + hd, 128), gw - hd)
        for t in range(0, tokens, th):
            kvt[q * (gw - hd):(q + 1) * (gw - hd), t:t + th] = gq[t:t + th, cols].T
    share = width // per_kv
    col0 = lax.rem(at.r, per_kv) * share

    def kv_load(j, slot):
        cs = pl.ds(pl.multiple_of(col0 + j * bc, bc), bc)
        return pltpu.make_async_copy(x_ref.at[:, cs], xbuf.at[slot], in_sem.at[slot])

    def kv_step(j, _):
        slot = lax.rem(j, 2)

        @pl.when(j + 1 < share // bc)
        def _():
            kv_load(j + 1, 1 - slot).start()

        kv_load(j, slot).wait()
        prod = _nn(kvt[...], xbuf[slot])
        dk = dv = None
        for q in range(per_kv):
            a = prod[q * 2 * e:q * 2 * e + e]
            b = prod[q * 2 * e + e:(q + 1) * 2 * e]
            dk = a if dk is None else dk + a
            dv = b if dv is None else dv + b
        cs = pl.ds(pl.multiple_of(j * bc, bc), bc)
        dwk_ref[:, cs] = dk
        dwv_ref[:, cs] = dv
        return 0

    kv_load(0, 0).start()
    lax.fori_loop(0, share // bc, kv_step, 0)

    rs_wait(4, rs_full.at[1, :, half_a])
    rs_wait(3, rs_full.at[0, :, half_a])
    rs_wait(2, rs_full.at[0, :, half_b])
    rs_wait(5, rs_full.at[1, :, half_b])
    stage[...] = (part[3] + rs_full[0] + rs_full[1]).astype(BF16)
    my_cols = pl.ds(pl.multiple_of(at.r * cw, cw), cw)
    for d in range(1, n_row):
        rows = pl.ds(pl.multiple_of(peers[d] * tl, tl), tl)
        cp = _remote(stage.at[rows, :], dx_ref.at[:, my_cols], out_send.at[d], out_recv.at[d], at.row_dev(peers[d]))
        cp.start()
        sends.append(cp)
    keep = pltpu.make_async_copy(stage.at[pl.ds(pl.multiple_of(at.r * tl, tl), tl), :], dx_ref.at[:, my_cols], ld_sem.at[0])
    keep.start()
    for d in range(1, n_row):
        src = lax.rem(at.r + n_row - d, n_row)
        ref = dx_ref.at[:, pl.ds(pl.multiple_of(src * cw, cw), cw)]
        _remote(ref, ref, out_send.at[d], out_recv.at[d], mate).wait_recv()
    keep.wait()
    for cp in sends:
        cp.wait_send()


def _grads(ring, cores, heads, g, wrow, wkv, dqt, ot, x, dy):
    tokens, width = x.shape
    n_row = ring * cores
    hd = dqt.shape[0]
    e = hd // heads
    gw = g.shape[1]
    tb = tokens // ring
    cw = width // n_row
    per_kv = n_row // wkv.shape[0]
    bc = min(512, cw // 2)
    dma = pltpu.SemaphoreType.DMA
    return pl.pallas_call(
        functools.partial(_grads_kernel, ring, cores, heads),
        name="grads",
        in_specs=[ANY, ANY, ANY, VMEM, VMEM, ANY, ANY],
        out_specs=[ANY, ANY, ANY, VMEM, VMEM],
        out_shape=[
            jax.ShapeDtypeStruct((tb // n_row, width), BF16),
            jax.ShapeDtypeStruct((hd, width), F32),
            jax.ShapeDtypeStruct((hd, width), F32),
            jax.ShapeDtypeStruct((e, width // per_kv), F32),
            jax.ShapeDtypeStruct((e, width // per_kv), F32),
        ],
        scratch_shapes=[
            pltpu.VMEM((tokens, n_row * gw), BF16),
            pltpu.VMEM((n_row * gw, cw), BF16),
            pltpu.VMEM((ring, tb, cw), F32),
            pltpu.VMEM((2, tb, cw // 2), F32),
            pltpu.VMEM((2, tb, cw), F32),
            pltpu.VMEM((tb, cw), BF16),
            pltpu.VMEM((2, tokens, bc), BF16),
            pltpu.VMEM((2, hd, bc), F32),
            pltpu.VMEM((per_kv * (gw - hd), tokens), BF16),
            dma((ring, 9)),
            dma((ring, 9)),
            dma((6,)),
            dma((6,)),
            dma((n_row,)),
            dma((n_row,)),
            dma((2,)),
            dma((2,)),
            dma((2 * n_row + 1,)),
        ],
        compiler_params=pltpu.CompilerParams(collective_id=1, has_side_effects=True, vmem_limit_bytes=60 << 20),
        cost_estimate=pl.CostEstimate(flops=2 * tokens * width * (n_row * gw // n_row + 3 * hd), bytes_accessed=100 << 20, transcendentals=0),
    )(g, wrow, wkv, dqt, ot, x, dy)


def solution(mesh):
    n = mesh.shape["tp"]
    ring = math.isqrt(n // 2)
    cores = n // (ring * ring)
    if ring != 4 or cores != 2:
        raise ValueError("needs a 4x4 torus")

    def local_grads(x_blk, dy_blk, wq_loc, w_k, w_v, wo_loc):
        model_dim, kv_heads, e = w_k.shape
        heads = wq_loc.shape[1]
        hd = heads * e
        n_row = ring * cores
        scale = e ** -0.5
        me = lax.axis_index("tp")
        wq = jnp.transpose(wq_loc, (1, 2, 0)).reshape(hd, model_dim)
        wk = jnp.transpose(w_k, (1, 2, 0))
        wv = jnp.transpose(w_v, (1, 2, 0))
        wo = wo_loc.reshape(hd, model_dim)
        j = me // (n // kv_heads)
        w_in = jnp.concatenate([wq, lax.dynamic_index_in_dim(wk, j, 0, False), lax.dynamic_index_in_dim(wv, j, 0, False)])
        kv_row = kv_heads // ring
        cw = model_dim // n_row
        start = ((me // n_row) * kv_row, 0, lax.rem(me, n_row) * cw)
        wkv = jnp.concatenate([lax.dynamic_slice(w, start, (kv_row, e, cw)) for w in (wk, wv)], axis=1)

        x_full = lax.all_gather(x_blk, "tp", axis=0, tiled=True)
        dy_full = lax.all_gather(dy_blk, "tp", axis=0, tiled=True)
        tokens = x_full.shape[0]
        block = min(512, tokens)
        qkvt = _proj(w_in, x_full, block)
        dot = _proj(wo, dy_full, block)
        g, dqt, ot, wrow = _attention(ring, cores, heads, scale, qkvt, dot, wq)
        dx, dwq, dwo, dwk, dwv = _grads(ring, cores, heads, g, wrow, wkv, dqt, ot, x_full, dy_full)
        return (dx, jnp.transpose(dwq.reshape(heads, e, model_dim), (2, 0, 1)), dwo.reshape(heads, e, model_dim), dwk.T, dwv.T)

    tok = P(("dp", "tp"))
    return jax.shard_map(
        local_grads,
        mesh=mesh,
        in_specs=(tok, tok, P(None, "tp", None), P(), P(), P("tp")),
        out_specs=(tok, P("dp", "tp", None), tok, tok, tok),
        check_vma=False,
    )
```

```python
import functools
import math

import jax
import jax.numpy as jnp
from jax import lax
from jax.experimental import pallas as pl
from jax.experimental.pallas import tpu as pltpu
from jax.sharding import PartitionSpec as P

F32 = jnp.float32
BF16 = jnp.bfloat16
MESH = pl.DeviceIdType.MESH
ANY = pl.BlockSpec(memory_space=pl.ANY)
VMEM = pl.BlockSpec(memory_space=pltpu.VMEM)
LOG2E = math.log2(math.e)
ORDER = (2, 1, 3, 0)


def _dot(a, b, dims):
    return lax.dot_general(a, b, (dims, ((), ())), preferred_element_type=F32)


def _nn(a, b):
    return _dot(a, b, ((1,), (0,)))


def _nt(a, b):
    return _dot(a, b, ((1,), (1,)))


class Place:
    def __init__(self, ring, cores):
        me = lax.axis_index("tp")
        self.ring, self.cores = ring, cores
        self.c = lax.rem(me, cores)
        self.x = lax.rem(me // cores, ring)
        self.y = me // (cores * ring)
        self.r = self.x * cores + self.c
        self.n_row = ring * cores

    def dev(self, y, x, c):
        y = lax.rem(y + self.ring, self.ring)
        x = lax.rem(x + self.ring, self.ring)
        return {"tp": (y * self.ring + x) * self.cores + c}

    def row_dev(self, r):
        return {"tp": self.y * self.n_row + r}

    def slot(self, x, c):
        return lax.rem(x + self.ring, self.ring) * self.cores + c


def _remote(src, dst, send, recv, dev):
    return pltpu.make_async_remote_copy(
        src_ref=src, dst_ref=dst, send_sem=send, recv_sem=recv, device_id=dev, device_id_type=MESH
    )


def _enter(devices):
    barrier = pltpu.get_barrier_semaphore()
    for dev in devices:
        pl.semaphore_signal(barrier, inc=1, device_id=dev, device_id_type=MESH)
    pl.semaphore_wait(barrier, len(devices))


OWN, MINUS, PLUS, FAR = range(4)
STEP = (0, -1, 1, 2)


class Gather:
    def __init__(self, at, src, full, send, recv, mate_recv):
        self.at, self.src, self.full = at, src, full
        self.send, self.recv, self.mate_recv = send, recv, mate_recv
        self.rows = src.shape[0]
        self.next_send = 0
        self.sent = []
        c = at.c
        self.first = {s: at.dev(at.y + c * s, at.x + (1 - c) * s, c) for s in (1, -1)}
        self.second = {s: at.dev(at.y + (1 - c) * s, at.x + c * s, c) for s in (1, -1)}
        self.mate = at.dev(at.y, at.x, 1 - c)

    def ref(self, d1, d2, core, half=None):
        at = self.at
        o1, o2 = STEP[d1], STEP[d2]
        x = at.x + (1 - core) * o1 + core * o2
        y = at.y + core * o1 + (1 - core) * o2
        n = self.rows if half is None else self.rows // 2
        r0 = at.dev(y, x, core)["tp"] * self.rows + (0 if half is None else half * n)
        return self.full.at[pl.ds(pl.multiple_of(r0, n), n), :]

    def push(self, src, dst, recv, dev):
        k = self.next_send
        self.next_send += 1
        self.sent.append(dst.shape[0])
        return _remote(src, dst, self.send.at[k], recv, dev)

    def out(self, d1, d2, half=None):
        if d1 == OWN and d2 == OWN:
            n = self.rows if half is None else self.rows // 2
            return self.src.at[pl.ds(0 if half is None else half * n, n), :]
        return self.ref(d1, d2, self.at.c, half)

    def to_mate(self, d1, d2):
        ref = self.ref(d1, d2, self.at.c)
        self.push(self.out(d1, d2), ref, self.mate_recv.at[d1, d2], self.mate).start()

    def arrived(self, d1, d2, half=None):
        ref = self.ref(d1, d2, self.at.c, half)
        _remote(ref, ref, self.send.at[0], self.recv.at[d1, d2, half or 0], self.mate).wait_recv()

    def second_full(self, d1):
        ref = self.ref(d1, OWN, self.at.c)
        return [self.push(self.out(d1, OWN), ref, self.recv.at[d1, to, 0], self.second[s]) for s, to in ((1, MINUS), (-1, PLUS))]

    def prepare(self):
        self.fulls = {d: self.second_full(d) for d in range(4)}

    def start(self):
        ref = self.ref(OWN, OWN, self.at.c)
        for s, to in ((1, MINUS), (-1, PLUS)):
            self.push(self.src, ref, self.recv.at[to, OWN, 0], self.first[s]).start()
        self.go(OWN)
        self.to_mate(OWN, OWN)

    def go(self, d1):
        for cp in self.fulls[d1]:
            cp.start()

    def relay_first(self):
        for d, s, half in ((MINUS, 1, 0), (PLUS, -1, 1)):
            self.arrived(d, OWN)
            ref = self.ref(d, OWN, self.at.c, half)
            self.push(ref, ref, self.recv.at[FAR, OWN, half], self.first[s]).start()
            self.to_mate(d, OWN)

    def far_first(self):
        for half in (0, 1):
            self.arrived(FAR, OWN, half)
        self.to_mate(FAR, OWN)

    def relay_second(self, d1):
        for d, s, half in ((MINUS, 1, 0), (PLUS, -1, 1)):
            self.arrived(d1, d)
            ref = self.ref(d1, d, self.at.c, half)
            self.push(ref, ref, self.recv.at[d1, FAR, half], self.second[s]).start()
            self.to_mate(d1, d)

    def far_second(self, d1):
        for half in (0, 1):
            self.arrived(d1, FAR, half)
        self.to_mate(d1, FAR)

    def await_mate_row(self, t):
        at = self.at
        for j in range(4):
            i1 = (1 - at.c) * t + at.c * j
            i2 = at.c * t + (1 - at.c) * j
            ref = self.full.at[pl.ds(0, self.rows), :]
            _remote(ref, ref, self.send.at[0], self.mate_recv.at[i1, i2], self.mate).wait_recv()

    def drain(self):
        for k, n in enumerate(self.sent):
            ref = self.full.at[pl.ds(0, n), :]
            _remote(ref, ref, self.send.at[k], self.send.at[k], self.mate).wait_send()


def _front_kernel(ring, cores, heads, scale, bq, x_ref, dy_ref, w_ref, wo_ref,
                  xf_ref, dyf_ref, g_ref, dqt_ref, ot_ref, wrow_ref, hop_ref,
                  w_v, wo_v, xblk, qkvt_ref, dot_ref, s_ref, dk_ref, dv_ref, w_buf,
                  send, recv, mate_recv, w_send, w_recv, hop_recv, ld_sem, blk_sem):
    at = Place(ring, cores)
    n_row = at.n_row
    hd = wo_ref.shape[0]
    e = hd // heads
    tokens, width = xf_ref.shape
    tb = tokens // ring
    cw = width // n_row
    c = at.c
    gx = Gather(at, x_ref, xf_ref, send.at[0], recv.at[0], mate_recv.at[0])
    gy = Gather(at, dy_ref, dyf_ref, send.at[1], recv.at[1], mate_recv.at[1])

    loads = [pltpu.make_async_copy(w_ref, w_v, ld_sem.at[0]), pltpu.make_async_copy(wo_ref, wo_v, ld_sem.at[1])]
    rows = x_ref.shape[0]
    own_rows = pl.ds(pl.multiple_of((at.y * n_row + at.r) * rows, rows), rows)
    ins = [pltpu.make_async_copy(src, xblk.at[i, pl.ds(0, rows), :], ld_sem.at[2 + i]) for i, src in enumerate((x_ref, dy_ref))]
    outs = [pltpu.make_async_copy(xblk.at[i, pl.ds(0, rows), :], dst.at[own_rows, :], ld_sem.at[4 + i]) for i, dst in enumerate((xf_ref, dyf_ref))]
    for cp in ins:
        cp.start()
    row_peers = [lax.rem(at.r + d, n_row) for d in range(1, n_row)]
    up, down = at.dev(at.y + 1, at.x, c), at.dev(at.y - 1, at.x, c)
    _enter([up, down] + [at.row_dev(r) for r in row_peers])
    gx.prepare()
    gx.start()
    for cp in loads:
        cp.start()
    for cp in ins:
        cp.wait()
    for cp in outs:
        cp.start()

    dk_ref[...] = jnp.zeros_like(dk_ref)
    dv_ref[...] = jnp.zeros_like(dv_ref)

    def project(full, w, out, b):
        def load(i):
            r0 = pl.multiple_of(b * tb + i * bq, bq)
            return pltpu.make_async_copy(full.at[pl.ds(r0, bq), :], xblk.at[i], blk_sem.at[i])

        for i in range(tb // bq):
            load(i).start()

        def block(i, _):
            load(i).wait()
            out[:, pl.ds(pl.multiple_of(b * tb + i * bq, bq), bq)] = _nt(w[...], xblk[i]).astype(BF16)
            return 0

        lax.fori_loop(0, tb // bq, block, 0)

    def row_at(t):
        off = jnp.where(t == 1, ring - 1, jnp.where(t == 2, 1, jnp.where(t == 3, 2, 0)))
        return lax.rem(at.y + off, ring)

    for cp in loads + outs:
        cp.wait()

    def x_turn(t, _):
        @pl.when(t == 0)
        def _():
            gx.relay_first()
            gx.go(MINUS)

            @pl.when(c == 0)
            def _():
                gx.go(PLUS)

            gx.far_first()

            @pl.when(c == 0)
            def _():
                gx.go(FAR)

            gx.relay_second(OWN)

            @pl.when(c == 1)
            def _():
                gx.go(PLUS)

            gx.relay_second(MINUS)

            @pl.when(c == 1)
            def _():
                gx.go(FAR)

            gx.relay_second(PLUS)
            gx.far_second(OWN)

        @pl.when(t == 1)
        def _():
            gx.relay_second(FAR)
            gy.start()
            gx.far_second(MINUS)

        @pl.when(t == 2)
        def _():
            gx.far_second(PLUS)
            gx.far_second(FAR)

        gx.await_mate_row(t)
        project(xf_ref, w_v, qkvt_ref, row_at(t))
        return 0

    gy.prepare()
    lax.fori_loop(0, ring, x_turn, 0)

    krow, vrow = heads * e, (heads + 1) * e
    row = lax.broadcasted_iota(jnp.int32, (bq, bq), 0)
    col = lax.broadcasted_iota(jnp.int32, (bq, bq), 1)

    def attend(i):
        q0 = i * bq
        chunks = [slice(k, k + bq) for k in range(0, q0 + bq, bq)]
        qs = slice(q0, q0 + bq)

        def head(h, _):
            hs = pl.ds(pl.multiple_of(h * e, e), e)
            qt = qkvt_ref[hs, qs]
            dot = dot_ref[hs, qs]
            q = qt.T
            do = dot.T
            m = None
            for ks in chunks:
                s = _nn(q, qkvt_ref[krow:krow + e, ks])
                if ks.start == q0:
                    s = jnp.where(row >= col, s, -jnp.inf)
                s_ref[:, ks] = s
                part = s[:, :128]
                for t in range(128, bq, 128):
                    part = jnp.maximum(part, s[:, t:t + 128])
                m = part if m is None else jnp.maximum(m, part)
            m = jnp.max(m, axis=1, keepdims=True)
            total = None
            for ks in chunks:
                p = jnp.exp2((s_ref[:, ks] - m) * (scale * LOG2E))
                s_ref[:, ks] = p
                part = p[:, :128]
                for t in range(128, bq, 128):
                    part = part + p[:, t:t + 128]
                total = part if total is None else total + part
            inv = 1.0 / jnp.sum(total, axis=1, keepdims=True)
            out = None
            for ks in chunks:
                p = s_ref[:, ks] * inv
                s_ref[:, ks] = p
                pb = p.astype(BF16)
                part = _nt(pb, qkvt_ref[vrow:vrow + e, ks])
                out = part if out is None else out + part
                dv_ref[:, ks] += _nn(dot, pb)
            out = out.astype(BF16)
            ot_ref[hs, qs] = out.T
            delta = jnp.sum(do.astype(F32) * out.astype(F32), axis=1, keepdims=True)
            dq = None
            for ks in chunks:
                dp = _nn(do, qkvt_ref[vrow:vrow + e, ks])
                ds = (s_ref[:, ks] * (dp - delta)).astype(BF16)
                part = _nt(ds, qkvt_ref[krow:krow + e, ks])
                dq = part if dq is None else dq + part
                dk_ref[:, ks] += _nn(qt, ds)
            dqt_ref[hs, qs] = (dq * scale).astype(BF16).T
            return 0

        lax.fori_loop(0, heads, head, 0)
        g_ref[qs, 0:heads * e] = dqt_ref[:, qs].T

    hh = hd // 2

    def w_push(k, src, dst, rsem, dev):
        _remote(src, dst, w_send.at[k], rsem, dev).start()

    def wcols(slot):
        return pl.ds(pl.multiple_of(slot * cw, cw), cw)

    right, left, mate = at.dev(at.y, at.x + 1, c), at.dev(at.y, at.x - 1, c), at.dev(at.y, at.x, 1 - c)

    def w_start():
        for half, dev in ((0, right), (1, left)):
            for k in range(cores):
                w_push(half * 2 + k, w_ref.at[pl.ds(half * hh, hh), wcols(at.slot(at.x + 2, k))], hop_ref.at[half * 2 + k], hop_recv.at[half * 2 + k], dev)
        w_push(4, w_ref.at[pl.ds(0, hd), wcols(at.slot(at.x, 1 - c))], wrow_ref.at[at.r], w_recv.at[0], mate)
        for i, s in enumerate((1, -1)):
            for k in range(cores):
                dst_core = c if k == 0 else 1 - c
                w_push(5 + 2 * i + k, w_ref.at[pl.ds(0, hd), wcols(at.slot(at.x + s, dst_core))], wrow_ref.at[at.r], w_recv.at[1 + 2 * i + k], at.dev(at.y, at.x + s, dst_core))

    def w_relay():
        for half, s in ((0, 1), (1, -1)):
            for n in (half * 2, half * 2 + 1):
                _remote(hop_ref.at[n], hop_ref.at[n], w_send.at[0], hop_recv.at[n], mate).wait_recv()
            for k in range(cores):
                n = half * 2 + k
                src_slot = at.slot(at.x - s, c)
                same = k == 0
                dst_core = c if same else 1 - c
                w_push(9 + n, hop_ref.at[half * 2 + dst_core], wrow_ref.at[src_slot, pl.ds(half * hh, hh), :], w_recv.at[5 + n], at.dev(at.y, at.x + s, dst_core))

    def w_finish():
        whole = wrow_ref.at[0]
        part = wrow_ref.at[0, pl.ds(0, hh), :]
        for n in range(9):
            ref = whole if n < 5 else part
            _remote(ref, ref, w_send.at[0], w_recv.at[n], mate).wait_recv()
        for k in range(13):
            ref = whole if 4 <= k < 9 else part
            _remote(ref, ref, w_send.at[k], w_send.at[k], mate).wait_send()

    own_in = pltpu.make_async_copy(w_ref.at[pl.ds(0, hd), wcols(at.r)], w_buf, ld_sem.at[0])
    own_in.start()
    own_in.wait()
    own_out = pltpu.make_async_copy(w_buf, wrow_ref.at[at.r], ld_sem.at[1])
    own_out.start()

    def turn(t, _):
        @pl.when(t == 0)
        def _():
            gy.relay_first()
            gy.go(MINUS)

            @pl.when(c == 0)
            def _():
                gy.go(PLUS)

            gy.far_first()

            @pl.when(c == 0)
            def _():
                gy.go(FAR)

            gy.relay_second(OWN)

            @pl.when(c == 1)
            def _():
                gy.go(PLUS)

            gy.relay_second(MINUS)

            @pl.when(c == 1)
            def _():
                gy.go(FAR)
                far_step(OWN)

        @pl.when(t == 1)
        def _():
            gy.relay_second(PLUS)

            @pl.when(c == 1)
            def _():
                far_step(MINUS)

            gy.relay_second(FAR)

        @pl.when(t == 2)
        def _():
            w_start()

            @pl.when(c == 1)
            def _():
                far_step(PLUS)

            @pl.when(c == 0)
            def _():
                far_step(OWN)
                far_step(MINUS)

        @pl.when(t == 3)
        def _():
            @pl.when(c == 0)
            def _():
                far_step(PLUS)

            far_step(FAR)
            w_relay()

        gy.await_mate_row(t)
        b = row_at(t)
        project(dyf_ref, wo_v, dot_ref, b)
        for k in range(ring):
            @pl.when(b == k)
            def _(k=k):
                for i in range(k * tb // bq, (k + 1) * tb // bq):
                    attend(i)
        return 0

    far_cp = {d: gy.push(gy.ref(d, FAR, c), gy.ref(d, FAR, c), gy.mate_recv.at[d, FAR], gy.mate) for d in range(4)}

    def far_step(d):
        for half in (0, 1):
            gy.arrived(d, FAR, half)
        far_cp[d].start()

    lax.fori_loop(0, ring, turn, 0)

    for k in range(0, tokens, bq):
        ks = slice(k, k + bq)
        g_ref[ks, heads * e:(heads + 1) * e] = (dk_ref[:, ks] * scale).astype(BF16).T
        g_ref[ks, (heads + 1) * e:(heads + 2) * e] = dv_ref[:, ks].astype(BF16).T
    own_out.wait()
    w_finish()
    gx.drain()
    gy.drain()


def _front(ring, cores, heads, scale, x, dy, w_in, wo):
    rows, width = x.shape
    tokens = rows * ring * ring * cores
    hd = wo.shape[0]
    e = hd // heads
    n_row = ring * cores
    cw = width // n_row
    bq = min(256, tokens // ring)
    dma = pltpu.SemaphoreType.DMA
    return pl.pallas_call(
        functools.partial(_front_kernel, ring, cores, heads, scale, bq),
        name="front",
        in_specs=[ANY, ANY, ANY, ANY],
        out_specs=[ANY, ANY, VMEM, VMEM, VMEM, ANY, ANY],
        out_shape=[
            jax.ShapeDtypeStruct((tokens, width), BF16),
            jax.ShapeDtypeStruct((tokens, width), BF16),
            jax.ShapeDtypeStruct((tokens, (heads + 2) * e), BF16),
            jax.ShapeDtypeStruct((hd, tokens), BF16),
            jax.ShapeDtypeStruct((hd, tokens), BF16),
            jax.ShapeDtypeStruct((n_row, hd, cw), BF16),
            jax.ShapeDtypeStruct((4, hd // 2, cw), BF16),
        ],
        scratch_shapes=[
            pltpu.VMEM(w_in.shape, BF16),
            pltpu.VMEM(wo.shape, BF16),
            pltpu.VMEM((2, bq, width), BF16),
            pltpu.VMEM((w_in.shape[0], tokens), BF16),
            pltpu.VMEM((hd, tokens), BF16),
            pltpu.VMEM((bq, tokens), F32),
            pltpu.VMEM((e, tokens), F32),
            pltpu.VMEM((e, tokens), F32),
            pltpu.VMEM((hd, cw), BF16),
            dma((2, 40)),
            dma((2, 4, 4, 2)),
            dma((2, 4, 4)),
            dma((13,)),
            dma((9,)),
            dma((4,)),
            dma((6,)),
            dma((2,)),
        ],
        compiler_params=pltpu.CompilerParams(collective_id=0, has_side_effects=True, vmem_limit_bytes=56 << 20),
        cost_estimate=pl.CostEstimate(flops=12 * heads * tokens * tokens * e, bytes_accessed=200 << 20, transcendentals=heads * tokens * tokens // 2),
    )(x, dy, w_in, wo)


def _grads_kernel(ring, cores, heads, g_ref, wrow_ref, wkv_ref, dqt_ref, ot_ref, x_ref, dy_ref,
                  dx_ref, dwq_ref, dwo_ref, dwk_ref, dwv_ref,
                  gq, w_all, part, rs_half, rs_full, stage, xbuf, obuf, kvt,
                  ag_send, ag_recv, rs_send, rs_recv, out_send, out_recv, in_sem, o_sem, ld_sem):
    at = Place(ring, cores)
    n_row = at.n_row
    tokens, width = x_ref.shape
    gw = g_ref.shape[1]
    hd = dqt_ref.shape[0]
    e = hd // heads
    tb = tokens // ring
    th = tb // 2
    tl = tb // n_row
    cw = w_all.shape[1]
    hw = cw // 2
    half_a, half_b = pl.ds(0, hw), pl.ds(hw, hw)
    n_ld = 2 * n_row + 1

    def gcols(slot):
        return pl.ds(pl.multiple_of(slot * gw, gw), gw)

    loads = [pltpu.make_async_copy(g_ref, gq.at[:, gcols(at.r)], ld_sem.at[0])]
    per_kv = n_row // wkv_ref.shape[0]
    for r in range(n_row):
        loads.append(pltpu.make_async_copy(wrow_ref.at[r], w_all.at[pl.ds(r * gw, hd), :], ld_sem.at[1 + r]))
        loads.append(pltpu.make_async_copy(wkv_ref.at[r // per_kv], w_all.at[pl.ds(r * gw + hd, gw - hd), :], ld_sem.at[1 + n_row + r]))
    for cp in loads:
        cp.start()

    up, down = at.dev(at.y + 1, at.x, at.c), at.dev(at.y - 1, at.x, at.c)
    right, left = at.dev(at.y, at.x + 1, at.c), at.dev(at.y, at.x - 1, at.c)
    mate = at.dev(at.y, at.x, 1 - at.c)
    peers = [lax.rem(at.r + d, n_row) for d in range(n_row)]
    _enter([up, down] + [at.row_dev(r) for r in peers[1:]])
    loads[0].wait()

    s_own, s_left, s_right, s_far = at.r, at.slot(at.x - 1, at.c), at.slot(at.x + 1, at.c), at.slot(at.x + 2, at.c)
    m_own, m_left, m_right, m_far = at.slot(at.x, 1 - at.c), at.slot(at.x - 1, 1 - at.c), at.slot(at.x + 1, 1 - at.c), at.slot(at.x + 2, 1 - at.c)
    blocks = [lax.rem(at.y + o, ring) for o in ORDER]
    sends = []

    def piece(k, slot, half=None):
        r0 = pl.multiple_of(blocks[k] * tb, tb)
        rows = pl.ds(r0, tb) if half is None else pl.ds(pl.multiple_of(r0 + half * th, th), th)
        return gq.at[rows, gcols(slot)]

    def ag_send_piece(k, n, slot, dev, half=None):
        ref = piece(k, slot, half)
        cp = _remote(ref, ref, ag_send.at[k, n], ag_recv.at[k, n], dev)
        cp.start()
        sends.append(cp)

    def ag_wait(k, n, slot, half=None):
        ref = piece(k, slot, half)
        _remote(ref, ref, ag_send.at[k, n], ag_recv.at[k, n], mate).wait_recv()

    def ag_own(k):
        ag_send_piece(k, 0, s_own, right)
        ag_send_piece(k, 1, s_own, left)
        ag_send_piece(k, 2, s_own, mate)

    def ag_relay(k):
        ag_wait(k, 0, s_left)
        ag_send_piece(k, 3, s_left, right, 0)
        ag_send_piece(k, 4, s_left, mate)
        ag_wait(k, 1, s_right)
        ag_send_piece(k, 5, s_right, left, 1)
        ag_send_piece(k, 6, s_right, mate)

    def ag_finish(k):
        ag_wait(k, 3, s_far, 0)
        ag_send_piece(k, 7, s_far, mate, 0)
        ag_wait(k, 5, s_far, 1)
        ag_send_piece(k, 8, s_far, mate, 1)
        ag_wait(k, 2, m_own)
        ag_wait(k, 4, m_left)
        ag_wait(k, 6, m_right)
        ag_wait(k, 7, m_far, 0)
        ag_wait(k, 8, m_far, 1)

    nt = min(256, cw)

    def partial(k):
        rows = pl.ds(pl.multiple_of(blocks[k] * tb, tb), tb)

        def tile(j, _):
            cs = pl.ds(pl.multiple_of(j * nt, nt), nt)
            part[k, :, cs] = _nn(gq[rows, :], w_all[:, cs])
            return 0

        lax.fori_loop(0, cw // nt, tile, 0)

    def rs_send_piece(n, src, dst, dev):
        cp = _remote(src, dst, rs_send.at[n], rs_recv.at[n], dev)
        cp.start()
        sends.append(cp)

    def rs_wait(n, ref):
        _remote(ref, ref, rs_send.at[n], rs_recv.at[n], mate).wait_recv()

    bc = xbuf.shape[2]
    n_steps = width // bc

    def stream(src, lhs, out, j0, j1):
        def load(j, slot):
            return pltpu.make_async_copy(src.at[:, pl.ds(pl.multiple_of(j * bc, bc), bc)], xbuf.at[slot], in_sem.at[slot])

        def store(j, slot):
            return pltpu.make_async_copy(obuf.at[slot], out.at[:, pl.ds(pl.multiple_of(j * bc, bc), bc)], o_sem.at[slot])

        if j0 == 0:
            load(0, 0).start()

        def step(j, _):
            slot = lax.rem(j, 2)

            @pl.when(j + 1 < n_steps)
            def _():
                load(j + 1, 1 - slot).start()

            load(j, slot).wait()

            @pl.when(j >= 2)
            def _():
                store(j - 2, slot).wait()

            obuf[slot] = _nn(lhs[...], xbuf[slot])
            store(j, slot).start()
            return 0

        lax.fori_loop(j0, j1, step, 0)
        if j1 == n_steps:
            for j in range(max(n_steps - 2, 0), n_steps):
                store(j, j % 2).wait()

    cut = [n_steps * q // 4 for q in range(5)]

    ag_own(0)
    stream(dy_ref, ot_ref, dwo_ref, cut[0], cut[2])
    ag_relay(0)
    ag_own(1)
    stream(dy_ref, ot_ref, dwo_ref, cut[2], cut[3])
    ag_finish(0)
    for cp in loads[1:]:
        cp.wait()
    partial(0)
    rs_send_piece(0, part.at[0, :, half_a], rs_half.at[0], up)
    rs_send_piece(1, part.at[0, :, half_b], rs_half.at[1], down)
    stream(dy_ref, ot_ref, dwo_ref, cut[3], cut[4])
    ag_relay(1)
    ag_own(2)
    stream(x_ref, dqt_ref, dwq_ref, cut[0], cut[1])
    ag_finish(1)
    partial(1)
    rs_send_piece(2, part.at[1, :, half_b], rs_full.at[0, :, half_b], up)
    ag_relay(2)
    ag_own(3)
    stream(x_ref, dqt_ref, dwq_ref, cut[1], cut[2])
    ag_finish(2)
    partial(2)
    rs_send_piece(4, part.at[2, :, half_a], rs_full.at[1, :, half_a], down)
    ag_relay(3)
    rs_wait(0, rs_half.at[0])
    part[1, :, half_a] += rs_half[0]
    rs_wait(1, rs_half.at[1])
    part[2, :, half_b] += rs_half[1]
    rs_send_piece(3, part.at[1, :, half_a], rs_full.at[0, :, half_a], up)
    rs_send_piece(5, part.at[2, :, half_b], rs_full.at[1, :, half_b], down)
    ag_finish(3)
    partial(3)
    stream(x_ref, dqt_ref, dwq_ref, cut[2], cut[4])

    n_kv = wkv_ref.shape[0]
    first = (at.r // per_kv) * per_kv
    for q in range(per_kv):
        cols = pl.ds(pl.multiple_of((first + q) * gw + hd, 128), gw - hd)
        for t in range(0, tokens, th):
            kvt[q * (gw - hd):(q + 1) * (gw - hd), t:t + th] = gq[t:t + th, cols].T
    share = width // per_kv
    col0 = lax.rem(at.r, per_kv) * share

    def kv_load(j, slot):
        cs = pl.ds(pl.multiple_of(col0 + j * bc, bc), bc)
        return pltpu.make_async_copy(x_ref.at[:, cs], xbuf.at[slot], in_sem.at[slot])

    def kv_step(j, _):
        slot = lax.rem(j, 2)

        @pl.when(j + 1 < share // bc)
        def _():
            kv_load(j + 1, 1 - slot).start()

        kv_load(j, slot).wait()
        prod = _nn(kvt[...], xbuf[slot])
        dk = dv = None
        for q in range(per_kv):
            a = prod[q * 2 * e:q * 2 * e + e]
            b = prod[q * 2 * e + e:(q + 1) * 2 * e]
            dk = a if dk is None else dk + a
            dv = b if dv is None else dv + b
        cs = pl.ds(pl.multiple_of(j * bc, bc), bc)
        dwk_ref[:, cs] = dk
        dwv_ref[:, cs] = dv
        return 0

    kv_load(0, 0).start()
    lax.fori_loop(0, share // bc, kv_step, 0)

    rs_wait(4, rs_full.at[1, :, half_a])
    rs_wait(3, rs_full.at[0, :, half_a])
    rs_wait(2, rs_full.at[0, :, half_b])
    rs_wait(5, rs_full.at[1, :, half_b])
    stage[...] = (part[3] + rs_full[0] + rs_full[1]).astype(BF16)
    my_cols = pl.ds(pl.multiple_of(at.r * cw, cw), cw)
    for d in range(1, n_row):
        rows = pl.ds(pl.multiple_of(peers[d] * tl, tl), tl)
        cp = _remote(stage.at[rows, :], dx_ref.at[:, my_cols], out_send.at[d], out_recv.at[d], at.row_dev(peers[d]))
        cp.start()
        sends.append(cp)
    keep = pltpu.make_async_copy(stage.at[pl.ds(pl.multiple_of(at.r * tl, tl), tl), :], dx_ref.at[:, my_cols], ld_sem.at[0])
    keep.start()
    for d in range(1, n_row):
        src = lax.rem(at.r + n_row - d, n_row)
        ref = dx_ref.at[:, pl.ds(pl.multiple_of(src * cw, cw), cw)]
        _remote(ref, ref, out_send.at[d], out_recv.at[d], mate).wait_recv()
    keep.wait()
    for cp in sends:
        cp.wait_send()


def _grads(ring, cores, heads, g, wrow, wkv, dqt, ot, x, dy):
    tokens, width = x.shape
    n_row = ring * cores
    hd = dqt.shape[0]
    e = hd // heads
    gw = g.shape[1]
    tb = tokens // ring
    cw = width // n_row
    per_kv = n_row // wkv.shape[0]
    bc = min(512, cw // 2)
    dma = pltpu.SemaphoreType.DMA
    return pl.pallas_call(
        functools.partial(_grads_kernel, ring, cores, heads),
        name="grads",
        in_specs=[ANY, ANY, ANY, VMEM, VMEM, ANY, ANY],
        out_specs=[ANY, ANY, ANY, VMEM, VMEM],
        out_shape=[
            jax.ShapeDtypeStruct((tb // n_row, width), BF16),
            jax.ShapeDtypeStruct((hd, width), F32),
            jax.ShapeDtypeStruct((hd, width), F32),
            jax.ShapeDtypeStruct((e, width // per_kv), F32),
            jax.ShapeDtypeStruct((e, width // per_kv), F32),
        ],
        scratch_shapes=[
            pltpu.VMEM((tokens, n_row * gw), BF16),
            pltpu.VMEM((n_row * gw, cw), BF16),
            pltpu.VMEM((ring, tb, cw), F32),
            pltpu.VMEM((2, tb, cw // 2), F32),
            pltpu.VMEM((2, tb, cw), F32),
            pltpu.VMEM((tb, cw), BF16),
            pltpu.VMEM((2, tokens, bc), BF16),
            pltpu.VMEM((2, hd, bc), F32),
            pltpu.VMEM((per_kv * (gw - hd), tokens), BF16),
            dma((ring, 9)),
            dma((ring, 9)),
            dma((6,)),
            dma((6,)),
            dma((n_row,)),
            dma((n_row,)),
            dma((2,)),
            dma((2,)),
            dma((2 * n_row + 1,)),
        ],
        compiler_params=pltpu.CompilerParams(collective_id=1, has_side_effects=True, vmem_limit_bytes=60 << 20),
        cost_estimate=pl.CostEstimate(flops=2 * tokens * width * (n_row * gw // n_row + 3 * hd), bytes_accessed=100 << 20, transcendentals=0),
    )(g, wrow, wkv, dqt, ot, x, dy)


def solution(mesh):
    n = mesh.shape["tp"]
    ring = math.isqrt(n // 2)
    cores = n // (ring * ring)
    if ring != 4 or cores != 2:
        raise ValueError("needs a 4x4 torus")

    def local_grads(x_blk, dy_blk, wq_loc, w_k, w_v, wo_loc):
        model_dim, kv_heads, e = w_k.shape
        heads = wq_loc.shape[1]
        hd = heads * e
        n_row = ring * cores
        scale = e ** -0.5
        me = lax.axis_index("tp")
        wq = jnp.transpose(wq_loc, (1, 2, 0)).reshape(hd, model_dim)
        wk = jnp.transpose(w_k, (1, 2, 0))
        wv = jnp.transpose(w_v, (1, 2, 0))
        wo = wo_loc.reshape(hd, model_dim)
        j = me // (n // kv_heads)
        w_in = jnp.concatenate([wq, lax.dynamic_index_in_dim(wk, j, 0, False), lax.dynamic_index_in_dim(wv, j, 0, False)])
        kv_row = kv_heads // ring
        cw = model_dim // n_row
        start = ((me // n_row) * kv_row, 0, lax.rem(me, n_row) * cw)
        wkv = jnp.concatenate([lax.dynamic_slice(w, start, (kv_row, e, cw)) for w in (wk, wv)], axis=1)

        x_full, dy_full, g, dqt, ot, wrow, _ = _front(ring, cores, heads, scale, x_blk, dy_blk, w_in, wo)
        dx, dwq, dwo, dwk, dwv = _grads(ring, cores, heads, g, wrow, wkv, dqt, ot, x_full, dy_full)
        return (dx, jnp.transpose(dwq.reshape(heads, e, model_dim), (2, 0, 1)), dwo.reshape(heads, e, model_dim), dwk.T, dwv.T)

    tok = P(("dp", "tp"))
    return jax.shard_map(
        local_grads,
        mesh=mesh,
        in_specs=(tok, tok, P(None, "tp", None), P(), P(), P("tp")),
        out_specs=(tok, P("dp", "tp", None), tok, tok, tok),
        check_vma=False,
    )
```

```python
import functools
import math

import jax
import jax.numpy as jnp
from jax import lax
from jax.experimental import pallas as pl
from jax.experimental.pallas import tpu as pltpu
from jax.sharding import PartitionSpec as P

F32 = jnp.float32
BF16 = jnp.bfloat16
MESH = pl.DeviceIdType.MESH
ANY = pl.BlockSpec(memory_space=pl.ANY)
VMEM = pl.BlockSpec(memory_space=pltpu.VMEM)
LOG2E = math.log2(math.e)
ORDER = (2, 1, 3, 0)


def _dot(a, b, dims):
    return lax.dot_general(a, b, (dims, ((), ())), preferred_element_type=F32)


def _nn(a, b):
    return _dot(a, b, ((1,), (0,)))


def _nt(a, b):
    return _dot(a, b, ((1,), (1,)))


class Place:
    def __init__(self, ring, cores):
        me = lax.axis_index("tp")
        self.ring, self.cores = ring, cores
        self.c = lax.rem(me, cores)
        self.x = lax.rem(me // cores, ring)
        self.y = me // (cores * ring)
        self.r = self.x * cores + self.c
        self.n_row = ring * cores

    def dev(self, y, x, c):
        y = lax.rem(y + self.ring, self.ring)
        x = lax.rem(x + self.ring, self.ring)
        return {"tp": (y * self.ring + x) * self.cores + c}

    def row_dev(self, r):
        return {"tp": self.y * self.n_row + r}

    def slot(self, x, c):
        return lax.rem(x + self.ring, self.ring) * self.cores + c


def _remote(src, dst, send, recv, dev):
    return pltpu.make_async_remote_copy(
        src_ref=src, dst_ref=dst, send_sem=send, recv_sem=recv, device_id=dev, device_id_type=MESH
    )


def _enter(devices):
    barrier = pltpu.get_barrier_semaphore()
    for dev in devices:
        pl.semaphore_signal(barrier, inc=1, device_id=dev, device_id_type=MESH)
    pl.semaphore_wait(barrier, len(devices))


OWN, MINUS, PLUS, FAR = range(4)
STEP = (0, -1, 1, 2)


class Gather:
    def __init__(self, at, src, full, send, recv, mate_recv):
        self.at, self.src, self.full = at, src, full
        self.send, self.recv, self.mate_recv = send, recv, mate_recv
        self.rows = src.shape[0]
        self.next_send = 0
        self.sent = []
        c = at.c
        self.first = {s: at.dev(at.y + c * s, at.x + (1 - c) * s, c) for s in (1, -1)}
        self.second = {s: at.dev(at.y + (1 - c) * s, at.x + c * s, c) for s in (1, -1)}
        self.mate = at.dev(at.y, at.x, 1 - c)

    def ref(self, d1, d2, core, half=None):
        at = self.at
        o1, o2 = STEP[d1], STEP[d2]
        x = at.x + (1 - core) * o1 + core * o2
        y = at.y + core * o1 + (1 - core) * o2
        n = self.rows if half is None else self.rows // 2
        r0 = at.dev(y, x, core)["tp"] * self.rows + (0 if half is None else half * n)
        return self.full.at[pl.ds(pl.multiple_of(r0, n), n), :]

    def push(self, src, dst, recv, dev):
        k = self.next_send
        self.next_send += 1
        self.sent.append(dst.shape[0])
        return _remote(src, dst, self.send.at[k], recv, dev)

    def out(self, d1, d2, half=None):
        if d1 == OWN and d2 == OWN:
            n = self.rows if half is None else self.rows // 2
            return self.src.at[pl.ds(0 if half is None else half * n, n), :]
        return self.ref(d1, d2, self.at.c, half)

    def to_mate(self, d1, d2):
        ref = self.ref(d1, d2, self.at.c)
        self.push(self.out(d1, d2), ref, self.mate_recv.at[d1, d2], self.mate).start()

    def arrived(self, d1, d2, half=None):
        ref = self.ref(d1, d2, self.at.c, half)
        _remote(ref, ref, self.send.at[0], self.recv.at[d1, d2, half or 0], self.mate).wait_recv()

    def second_full(self, d1):
        ref = self.ref(d1, OWN, self.at.c)
        return [self.push(self.out(d1, OWN), ref, self.recv.at[d1, to, 0], self.second[s]) for s, to in ((1, MINUS), (-1, PLUS))]

    def prepare(self):
        self.fulls = {d: self.second_full(d) for d in range(4)}

    def start(self):
        ref = self.ref(OWN, OWN, self.at.c)
        for s, to in ((1, MINUS), (-1, PLUS)):
            self.push(self.src, ref, self.recv.at[to, OWN, 0], self.first[s]).start()
        self.go(OWN)
        self.to_mate(OWN, OWN)

    def go(self, d1):
        for cp in self.fulls[d1]:
            cp.start()

    def relay_first(self):
        for d, s, half in ((MINUS, 1, 0), (PLUS, -1, 1)):
            self.arrived(d, OWN)
            ref = self.ref(d, OWN, self.at.c, half)
            self.push(ref, ref, self.recv.at[FAR, OWN, half], self.first[s]).start()
            self.to_mate(d, OWN)

    def far_first(self):
        for half in (0, 1):
            self.arrived(FAR, OWN, half)
        self.to_mate(FAR, OWN)

    def relay_second(self, d1):
        for d, s, half in ((MINUS, 1, 0), (PLUS, -1, 1)):
            self.arrived(d1, d)
            ref = self.ref(d1, d, self.at.c, half)
            self.push(ref, ref, self.recv.at[d1, FAR, half], self.second[s]).start()
            self.to_mate(d1, d)

    def far_second(self, d1):
        for half in (0, 1):
            self.arrived(d1, FAR, half)
        self.to_mate(d1, FAR)

    def await_mate_row(self, t):
        at = self.at
        for j in range(4):
            i1 = (1 - at.c) * t + at.c * j
            i2 = at.c * t + (1 - at.c) * j
            ref = self.full.at[pl.ds(0, self.rows), :]
            _remote(ref, ref, self.send.at[0], self.mate_recv.at[i1, i2], self.mate).wait_recv()

    def drain(self):
        for k, n in enumerate(self.sent):
            ref = self.full.at[pl.ds(0, n), :]
            _remote(ref, ref, self.send.at[k], self.send.at[k], self.mate).wait_send()


def _front_kernel(ring, cores, heads, scale, bq, bs, x_ref, dy_ref, w_ref, wk_ref, wv_ref, wo_ref,
                  xf_ref, dyf_ref, g_ref, dqt_ref, ot_ref, wrow_ref, hop_ref,
                  w_v, wo_v, xblk, qkvt_ref, dot_ref, s_ref, dp_ref, dk_ref, dv_ref, w_buf,
                  send, recv, mate_recv, w_send, w_recv, hop_recv, ld_sem, blk_sem):
    at = Place(ring, cores)
    n_row = at.n_row
    hd = wo_ref.shape[0]
    e = hd // heads
    tokens, width = xf_ref.shape
    tb = tokens // ring
    cw = width // n_row
    c = at.c
    gx = Gather(at, x_ref, xf_ref, send.at[0], recv.at[0], mate_recv.at[0])
    gy = Gather(at, dy_ref, dyf_ref, send.at[1], recv.at[1], mate_recv.at[1])

    kv = (at.y * n_row + at.r) // (n_row * ring // wk_ref.shape[0])
    loads = [
        pltpu.make_async_copy(w_ref, w_v.at[pl.ds(0, hd), :], ld_sem.at[0]),
        pltpu.make_async_copy(wo_ref, wo_v, ld_sem.at[1]),
        pltpu.make_async_copy(wk_ref.at[kv], w_v.at[pl.ds(hd, e), :], ld_sem.at[6]),
        pltpu.make_async_copy(wv_ref.at[kv], w_v.at[pl.ds(hd + e, e), :], ld_sem.at[7]),
    ]
    rows = x_ref.shape[0]
    own_rows = pl.ds(pl.multiple_of((at.y * n_row + at.r) * rows, rows), rows)
    ins = [pltpu.make_async_copy(src, xblk.at[i, pl.ds(0, rows), :], ld_sem.at[2 + i]) for i, src in enumerate((x_ref, dy_ref))]
    outs = [pltpu.make_async_copy(xblk.at[i, pl.ds(0, rows), :], dst.at[own_rows, :], ld_sem.at[4 + i]) for i, dst in enumerate((xf_ref, dyf_ref))]
    for cp in ins:
        cp.start()
    row_peers = [lax.rem(at.r + d, n_row) for d in range(1, n_row)]
    up, down = at.dev(at.y + 1, at.x, c), at.dev(at.y - 1, at.x, c)
    _enter([up, down] + [at.row_dev(r) for r in row_peers])
    gx.prepare()
    gx.start()
    for cp in loads:
        cp.start()
    for cp in ins:
        cp.wait()
    for cp in outs:
        cp.start()

    dk_ref[...] = jnp.zeros_like(dk_ref)
    dv_ref[...] = jnp.zeros_like(dv_ref)

    def project(full, w, out, b):
        def load(i):
            r0 = pl.multiple_of(b * tb + i * bq, bq)
            return pltpu.make_async_copy(full.at[pl.ds(r0, bq), :], xblk.at[i], blk_sem.at[i])

        for i in range(tb // bq):
            load(i).start()

        def block(i, _):
            load(i).wait()
            out[:, pl.ds(pl.multiple_of(b * tb + i * bq, bq), bq)] = _nt(w[...], xblk[i]).astype(BF16)
            return 0

        lax.fori_loop(0, tb // bq, block, 0)

    def row_at(t):
        off = jnp.where(t == 1, ring - 1, jnp.where(t == 2, 1, jnp.where(t == 3, 2, 0)))
        return lax.rem(at.y + off, ring)

    for cp in loads + outs:
        cp.wait()

    def x_turn(t, _):
        @pl.when(t == 0)
        def _():
            gx.relay_first()
            gx.go(MINUS)

            @pl.when(c == 0)
            def _():
                gx.go(PLUS)

            gx.far_first()

            @pl.when(c == 0)
            def _():
                gx.go(FAR)

            gx.relay_second(OWN)

            @pl.when(c == 1)
            def _():
                gx.go(PLUS)

            gx.relay_second(MINUS)

            @pl.when(c == 1)
            def _():
                gx.go(FAR)

            gx.relay_second(PLUS)
            gx.far_second(OWN)

        @pl.when(t == 1)
        def _():
            gx.relay_second(FAR)
            gy.start()
            gx.far_second(MINUS)

        @pl.when(t == 2)
        def _():
            gx.far_second(PLUS)
            gx.far_second(FAR)

        gx.await_mate_row(t)
        project(xf_ref, w_v, qkvt_ref, row_at(t))
        return 0

    gy.prepare()
    lax.fori_loop(0, ring, x_turn, 0)

    krow, vrow = heads * e, (heads + 1) * e
    keys_k, keys_v = slice(krow, krow + e), slice(vrow, vrow + e)
    m4 = heads * bs
    row = lax.broadcasted_iota(jnp.int32, (m4, bq), 0) & (bs - 1)
    col = lax.broadcasted_iota(jnp.int32, (m4, bq), 1)

    def lanes(v):
        parts = [v[:, t:t + 128] for t in range(0, v.shape[1], 128)]
        return parts

    def attend(k):
        base = k * tb
        chunks = [slice(t, t + bq) for t in range(0, base + tb, bq)]

        def queries(j, _):
            q0 = pl.multiple_of(base + j * bs, bs)
            qs = pl.ds(q0, bs)
            qt = jnp.concatenate([qkvt_ref[h * e:(h + 1) * e, qs] for h in range(heads)], axis=1)
            dot = jnp.concatenate([dot_ref[h * e:(h + 1) * e, qs] for h in range(heads)], axis=1)
            q = qt.T
            do = dot.T
            m = None
            for ks in chunks:
                s = _nn(q, qkvt_ref[keys_k, ks])
                if ks.start >= base:
                    s = jnp.where(col + (ks.start - base) <= row + j * bs, s, -jnp.inf)
                s_ref[:, ks] = s
                for part in lanes(s):
                    m = part if m is None else jnp.maximum(m, part)
            m = jnp.max(m, axis=1, keepdims=True)
            total = None
            for ks in chunks:
                p = jnp.exp2((s_ref[:, ks] - m) * (scale * LOG2E))
                s_ref[:, ks] = p
                for part in lanes(p):
                    total = part if total is None else total + part
                dp_ref[:, ks] = _nn(do, qkvt_ref[keys_v, ks])
            inv = 1.0 / jnp.sum(total, axis=1, keepdims=True)
            out = None
            for ks in chunks:
                p = s_ref[:, ks] * inv
                s_ref[:, ks] = p
                pb = p.astype(BF16)
                part = _nt(qkvt_ref[keys_v, ks], pb)
                out = part if out is None else out + part
                dv_ref[:, ks] += _nn(dot, pb)
            out = out.astype(BF16)
            delta = jnp.sum(dot.astype(F32) * out.astype(F32), axis=0, keepdims=True)
            delta = jnp.broadcast_to(delta, (128, m4)).T[:, :1]
            dq = None
            for ks in chunks:
                ds = (s_ref[:, ks] * (dp_ref[:, ks] - delta)).astype(BF16)
                part = _nt(qkvt_ref[keys_k, ks], ds)
                dq = part if dq is None else dq + part
                dk_ref[:, ks] += _nn(qt, ds)
            dq = (dq * scale).astype(BF16)
            for h in range(heads):
                ot_ref[h * e:(h + 1) * e, qs] = out[:, h * bs:(h + 1) * bs]
                dqt_ref[h * e:(h + 1) * e, qs] = dq[:, h * bs:(h + 1) * bs]
            for h in range(0, heads, 2):
                pair = jnp.concatenate([dq[:, h * bs:(h + 1) * bs], dq[:, (h + 1) * bs:(h + 2) * bs]], axis=0)
                g_ref[qs, h * e:(h + 2) * e] = pair.T
            return 0

        lax.fori_loop(0, tb // bs, queries, 0)

    hh = hd // 2

    def w_push(k, src, dst, rsem, dev):
        _remote(src, dst, w_send.at[k], rsem, dev).start()

    def wcols(slot):
        return pl.ds(pl.multiple_of(slot * cw, cw), cw)

    right, left, mate = at.dev(at.y, at.x + 1, c), at.dev(at.y, at.x - 1, c), at.dev(at.y, at.x, 1 - c)

    def w_start():
        for half, dev in ((0, right), (1, left)):
            for k in range(cores):
                w_push(half * 2 + k, w_ref.at[pl.ds(half * hh, hh), wcols(at.slot(at.x + 2, k))], hop_ref.at[half * 2 + k], hop_recv.at[half * 2 + k], dev)
        w_push(4, w_ref.at[pl.ds(0, hd), wcols(at.slot(at.x, 1 - c))], wrow_ref.at[at.r], w_recv.at[0], mate)
        for i, s in enumerate((1, -1)):
            for k in range(cores):
                dst_core = c if k == 0 else 1 - c
                w_push(5 + 2 * i + k, w_ref.at[pl.ds(0, hd), wcols(at.slot(at.x + s, dst_core))], wrow_ref.at[at.r], w_recv.at[1 + 2 * i + k], at.dev(at.y, at.x + s, dst_core))

    def w_relay():
        for half, s in ((0, 1), (1, -1)):
            for n in (half * 2, half * 2 + 1):
                _remote(hop_ref.at[n], hop_ref.at[n], w_send.at[0], hop_recv.at[n], mate).wait_recv()
            for k in range(cores):
                n = half * 2 + k
                src_slot = at.slot(at.x - s, c)
                same = k == 0
                dst_core = c if same else 1 - c
                w_push(9 + n, hop_ref.at[half * 2 + dst_core], wrow_ref.at[src_slot, pl.ds(half * hh, hh), :], w_recv.at[5 + n], at.dev(at.y, at.x + s, dst_core))

    def w_finish():
        whole = wrow_ref.at[0]
        part = wrow_ref.at[0, pl.ds(0, hh), :]
        for n in range(9):
            ref = whole if n < 5 else part
            _remote(ref, ref, w_send.at[0], w_recv.at[n], mate).wait_recv()
        for k in range(13):
            ref = whole if 4 <= k < 9 else part
            _remote(ref, ref, w_send.at[k], w_send.at[k], mate).wait_send()

    own_in = pltpu.make_async_copy(w_ref.at[pl.ds(0, hd), wcols(at.r)], w_buf, ld_sem.at[0])
    own_in.start()
    own_in.wait()
    own_out = pltpu.make_async_copy(w_buf, wrow_ref.at[at.r], ld_sem.at[1])
    own_out.start()

    def turn(t, _):
        @pl.when(t == 0)
        def _():
            gy.relay_first()
            gy.go(MINUS)

            @pl.when(c == 0)
            def _():
                gy.go(PLUS)

            gy.far_first()

            @pl.when(c == 0)
            def _():
                gy.go(FAR)

            gy.relay_second(OWN)

            @pl.when(c == 1)
            def _():
                gy.go(PLUS)

            gy.relay_second(MINUS)

            @pl.when(c == 1)
            def _():
                gy.go(FAR)
                far_step(OWN)

        @pl.when(t == 1)
        def _():
            gy.relay_second(PLUS)

            @pl.when(c == 1)
            def _():
                far_step(MINUS)

            gy.relay_second(FAR)

        @pl.when(t == 2)
        def _():
            w_start()

            @pl.when(c == 1)
            def _():
                far_step(PLUS)

            @pl.when(c == 0)
            def _():
                far_step(OWN)
                far_step(MINUS)

        @pl.when(t == 3)
        def _():
            @pl.when(c == 0)
            def _():
                far_step(PLUS)

            far_step(FAR)
            w_relay()

        gy.await_mate_row(t)
        b = row_at(t)
        project(dyf_ref, wo_v, dot_ref, b)
        for k in range(ring):
            @pl.when(b == k)
            def _(k=k):
                attend(k)
        return 0

    far_cp = {d: gy.push(gy.ref(d, FAR, c), gy.ref(d, FAR, c), gy.mate_recv.at[d, FAR], gy.mate) for d in range(4)}

    def far_step(d):
        for half in (0, 1):
            gy.arrived(d, FAR, half)
        far_cp[d].start()

    lax.fori_loop(0, ring, turn, 0)

    for k in range(0, tokens, bq):
        ks = slice(k, k + bq)
        g_ref[ks, heads * e:(heads + 1) * e] = (dk_ref[:, ks] * scale).astype(BF16).T
        g_ref[ks, (heads + 1) * e:(heads + 2) * e] = dv_ref[:, ks].astype(BF16).T
    own_out.wait()
    w_finish()
    gx.drain()
    gy.drain()


def _front(ring, cores, heads, scale, x, dy, wq, wk, wv, wo):
    rows, width = x.shape
    tokens = rows * ring * ring * cores
    hd = wo.shape[0]
    e = hd // heads
    n_row = ring * cores
    cw = width // n_row
    bq = min(256, tokens // ring)
    bs = min(128, tokens // ring)
    dma = pltpu.SemaphoreType.DMA
    return pl.pallas_call(
        functools.partial(_front_kernel, ring, cores, heads, scale, bq, bs),
        name="front",
        in_specs=[ANY] * 6,
        out_specs=[ANY, ANY, VMEM, VMEM, VMEM, ANY, ANY],
        out_shape=[
            jax.ShapeDtypeStruct((tokens, width), BF16),
            jax.ShapeDtypeStruct((tokens, width), BF16),
            jax.ShapeDtypeStruct((tokens, (heads + 2) * e), BF16),
            jax.ShapeDtypeStruct((hd, tokens), BF16),
            jax.ShapeDtypeStruct((hd, tokens), BF16),
            jax.ShapeDtypeStruct((n_row, hd, cw), BF16),
            jax.ShapeDtypeStruct((4, hd // 2, cw), BF16),
        ],
        scratch_shapes=[
            pltpu.VMEM((hd + 2 * e, width), BF16),
            pltpu.VMEM(wo.shape, BF16),
            pltpu.VMEM((2, bq, width), BF16),
            pltpu.VMEM((hd + 2 * e, tokens), BF16),
            pltpu.VMEM((hd, tokens), BF16),
            pltpu.VMEM((heads * bs, tokens), F32),
            pltpu.VMEM((heads * bs, tokens), F32),
            pltpu.VMEM((e, tokens), F32),
            pltpu.VMEM((e, tokens), F32),
            pltpu.VMEM((hd, cw), BF16),
            dma((2, 40)),
            dma((2, 4, 4, 2)),
            dma((2, 4, 4)),
            dma((13,)),
            dma((9,)),
            dma((4,)),
            dma((8,)),
            dma((2,)),
        ],
        compiler_params=pltpu.CompilerParams(collective_id=0, has_side_effects=True, vmem_limit_bytes=56 << 20),
        cost_estimate=pl.CostEstimate(flops=12 * heads * tokens * tokens * e, bytes_accessed=200 << 20, transcendentals=heads * tokens * tokens // 2),
    )(x, dy, wq, wk, wv, wo)


def _grads_kernel(ring, cores, heads, g_ref, wrow_ref, wk_ref, wv_ref, dqt_ref, ot_ref, x_ref, dy_ref,
                  dx_ref, dwq_ref, dwo_ref, dwk_ref, dwv_ref,
                  gq, w_all, part, rs_half, rs_full, stage, xbuf, obuf, kvt,
                  ag_send, ag_recv, rs_send, rs_recv, out_send, out_recv, in_sem, o_sem, ld_sem):
    at = Place(ring, cores)
    n_row = at.n_row
    tokens, width = x_ref.shape
    gw = g_ref.shape[1]
    hd = dqt_ref.shape[0]
    e = hd // heads
    tb = tokens // ring
    th = tb // 2
    tl = tb // n_row
    cw = w_all.shape[1]
    hw = cw // 2
    half_a, half_b = pl.ds(0, hw), pl.ds(hw, hw)

    def gcols(slot):
        return pl.ds(pl.multiple_of(slot * gw, gw), gw)

    loads = [pltpu.make_async_copy(g_ref, gq.at[:, gcols(at.r)], ld_sem.at[0])]
    n_kv = wk_ref.shape[0] // ring
    per_kv = n_row // n_kv
    own_cols = pl.ds(pl.multiple_of(at.r * cw, cw), cw)
    for r in range(n_row):
        kv = at.y * n_kv + r // per_kv
        loads.append(pltpu.make_async_copy(wrow_ref.at[r], w_all.at[pl.ds(r * gw, hd), :], ld_sem.at[1 + 3 * r]))
        loads.append(pltpu.make_async_copy(wk_ref.at[kv, :, own_cols], w_all.at[pl.ds(r * gw + hd, e), :], ld_sem.at[2 + 3 * r]))
        loads.append(pltpu.make_async_copy(wv_ref.at[kv, :, own_cols], w_all.at[pl.ds(r * gw + hd + e, e), :], ld_sem.at[3 + 3 * r]))
    for cp in loads:
        cp.start()

    up, down = at.dev(at.y + 1, at.x, at.c), at.dev(at.y - 1, at.x, at.c)
    right, left = at.dev(at.y, at.x + 1, at.c), at.dev(at.y, at.x - 1, at.c)
    mate = at.dev(at.y, at.x, 1 - at.c)
    peers = [lax.rem(at.r + d, n_row) for d in range(n_row)]
    _enter([up, down] + [at.row_dev(r) for r in peers[1:]])
    loads[0].wait()

    s_own, s_left, s_right, s_far = at.r, at.slot(at.x - 1, at.c), at.slot(at.x + 1, at.c), at.slot(at.x + 2, at.c)
    m_own, m_left, m_right, m_far = at.slot(at.x, 1 - at.c), at.slot(at.x - 1, 1 - at.c), at.slot(at.x + 1, 1 - at.c), at.slot(at.x + 2, 1 - at.c)
    blocks = [lax.rem(at.y + o, ring) for o in ORDER]
    sends = []

    def piece(k, slot, half=None):
        r0 = pl.multiple_of(blocks[k] * tb, tb)
        rows = pl.ds(r0, tb) if half is None else pl.ds(pl.multiple_of(r0 + half * th, th), th)
        return gq.at[rows, gcols(slot)]

    def ag_send_piece(k, n, slot, dev, half=None):
        ref = piece(k, slot, half)
        cp = _remote(ref, ref, ag_send.at[k, n], ag_recv.at[k, n], dev)
        cp.start()
        sends.append(cp)

    def ag_wait(k, n, slot, half=None):
        ref = piece(k, slot, half)
        _remote(ref, ref, ag_send.at[k, n], ag_recv.at[k, n], mate).wait_recv()

    def ag_own(k):
        ag_send_piece(k, 0, s_own, right)
        ag_send_piece(k, 1, s_own, left)
        ag_send_piece(k, 2, s_own, mate)

    def ag_relay(k):
        ag_wait(k, 0, s_left)
        ag_send_piece(k, 3, s_left, right, 0)
        ag_send_piece(k, 4, s_left, mate)
        ag_wait(k, 1, s_right)
        ag_send_piece(k, 5, s_right, left, 1)
        ag_send_piece(k, 6, s_right, mate)

    def ag_finish(k):
        ag_wait(k, 3, s_far, 0)
        ag_send_piece(k, 7, s_far, mate, 0)
        ag_wait(k, 5, s_far, 1)
        ag_send_piece(k, 8, s_far, mate, 1)
        ag_wait(k, 2, m_own)
        ag_wait(k, 4, m_left)
        ag_wait(k, 6, m_right)
        ag_wait(k, 7, m_far, 0)
        ag_wait(k, 8, m_far, 1)

    nt = min(256, cw)

    def partial(k):
        rows = pl.ds(pl.multiple_of(blocks[k] * tb, tb), tb)

        def tile(j, _):
            cs = pl.ds(pl.multiple_of(j * nt, nt), nt)
            part[k, :, cs] = _nn(gq[rows, :], w_all[:, cs])
            return 0

        lax.fori_loop(0, cw // nt, tile, 0)

    def rs_send_piece(n, src, dst, dev):
        cp = _remote(src, dst, rs_send.at[n], rs_recv.at[n], dev)
        cp.start()
        sends.append(cp)

    def rs_wait(n, ref):
        _remote(ref, ref, rs_send.at[n], rs_recv.at[n], mate).wait_recv()

    bc = xbuf.shape[2]
    n_steps = width // bc

    def stream(src, lhs, out, j0, j1):
        def load(j, slot):
            return pltpu.make_async_copy(src.at[:, pl.ds(pl.multiple_of(j * bc, bc), bc)], xbuf.at[slot], in_sem.at[slot])

        def store(j, slot):
            return pltpu.make_async_copy(obuf.at[slot], out.at[:, pl.ds(pl.multiple_of(j * bc, bc), bc)], o_sem.at[slot])

        if j0 == 0:
            load(0, 0).start()

        def step(j, _):
            slot = lax.rem(j, 2)

            @pl.when(j + 1 < n_steps)
            def _():
                load(j + 1, 1 - slot).start()

            load(j, slot).wait()

            @pl.when(j >= 2)
            def _():
                store(j - 2, slot).wait()

            obuf[slot] = _nn(lhs[...], xbuf[slot])
            store(j, slot).start()
            return 0

        lax.fori_loop(j0, j1, step, 0)
        if j1 == n_steps:
            for j in range(max(n_steps - 2, 0), n_steps):
                store(j, j % 2).wait()

    cut = [n_steps * q // 4 for q in range(5)]

    ag_own(0)
    stream(dy_ref, ot_ref, dwo_ref, cut[0], cut[2])
    ag_relay(0)
    ag_own(1)
    stream(dy_ref, ot_ref, dwo_ref, cut[2], cut[3])
    ag_finish(0)
    for cp in loads[1:]:
        cp.wait()
    partial(0)
    rs_send_piece(0, part.at[0, :, half_a], rs_half.at[0], up)
    rs_send_piece(1, part.at[0, :, half_b], rs_half.at[1], down)
    stream(dy_ref, ot_ref, dwo_ref, cut[3], cut[4])
    ag_relay(1)
    ag_own(2)
    stream(x_ref, dqt_ref, dwq_ref, cut[0], cut[1])
    ag_finish(1)
    partial(1)
    rs_send_piece(2, part.at[1, :, half_b], rs_full.at[0, :, half_b], up)
    ag_relay(2)
    ag_own(3)
    stream(x_ref, dqt_ref, dwq_ref, cut[1], cut[2])
    ag_finish(2)
    partial(2)
    rs_send_piece(4, part.at[2, :, half_a], rs_full.at[1, :, half_a], down)
    ag_relay(3)
    rs_wait(0, rs_half.at[0])
    part[1, :, half_a] += rs_half[0]
    rs_wait(1, rs_half.at[1])
    part[2, :, half_b] += rs_half[1]
    rs_send_piece(3, part.at[1, :, half_a], rs_full.at[0, :, half_a], up)
    rs_send_piece(5, part.at[2, :, half_b], rs_full.at[1, :, half_b], down)
    ag_finish(3)
    partial(3)
    stream(x_ref, dqt_ref, dwq_ref, cut[2], cut[4])

    first = (at.r // per_kv) * per_kv
    for q in range(per_kv):
        cols = pl.ds(pl.multiple_of((first + q) * gw + hd, 128), gw - hd)
        for t in range(0, tokens, th):
            kvt[q * (gw - hd):(q + 1) * (gw - hd), t:t + th] = gq[t:t + th, cols].T
    share = width // per_kv
    col0 = lax.rem(at.r, per_kv) * share

    def kv_load(j, slot):
        cs = pl.ds(pl.multiple_of(col0 + j * bc, bc), bc)
        return pltpu.make_async_copy(x_ref.at[:, cs], xbuf.at[slot], in_sem.at[slot])

    def kv_step(j, _):
        slot = lax.rem(j, 2)

        @pl.when(j + 1 < share // bc)
        def _():
            kv_load(j + 1, 1 - slot).start()

        kv_load(j, slot).wait()
        prod = _nn(kvt[...], xbuf[slot])
        dk = dv = None
        for q in range(per_kv):
            a = prod[q * 2 * e:q * 2 * e + e]
            b = prod[q * 2 * e + e:(q + 1) * 2 * e]
            dk = a if dk is None else dk + a
            dv = b if dv is None else dv + b
        cs = pl.ds(pl.multiple_of(j * bc, bc), bc)
        dwk_ref[:, cs] = dk
        dwv_ref[:, cs] = dv
        return 0

    kv_load(0, 0).start()
    lax.fori_loop(0, share // bc, kv_step, 0)

    rs_wait(4, rs_full.at[1, :, half_a])
    rs_wait(3, rs_full.at[0, :, half_a])
    rs_wait(2, rs_full.at[0, :, half_b])
    rs_wait(5, rs_full.at[1, :, half_b])
    stage[...] = (part[3] + rs_full[0] + rs_full[1]).astype(BF16)
    my_cols = pl.ds(pl.multiple_of(at.r * cw, cw), cw)
    for d in range(1, n_row):
        rows = pl.ds(pl.multiple_of(peers[d] * tl, tl), tl)
        cp = _remote(stage.at[rows, :], dx_ref.at[:, my_cols], out_send.at[d], out_recv.at[d], at.row_dev(peers[d]))
        cp.start()
        sends.append(cp)
    keep = pltpu.make_async_copy(stage.at[pl.ds(pl.multiple_of(at.r * tl, tl), tl), :], dx_ref.at[:, my_cols], ld_sem.at[0])
    keep.start()
    for d in range(1, n_row):
        src = lax.rem(at.r + n_row - d, n_row)
        ref = dx_ref.at[:, pl.ds(pl.multiple_of(src * cw, cw), cw)]
        _remote(ref, ref, out_send.at[d], out_recv.at[d], mate).wait_recv()
    keep.wait()
    for cp in sends:
        cp.wait_send()


def _grads(ring, cores, heads, g, wrow, wk, wv, dqt, ot, x, dy):
    tokens, width = x.shape
    n_row = ring * cores
    hd = dqt.shape[0]
    e = hd // heads
    gw = g.shape[1]
    tb = tokens // ring
    cw = width // n_row
    per_kv = n_row * ring // wk.shape[0]
    bc = min(512, cw // 2)
    dma = pltpu.SemaphoreType.DMA
    return pl.pallas_call(
        functools.partial(_grads_kernel, ring, cores, heads),
        name="grads",
        in_specs=[ANY, ANY, ANY, ANY, VMEM, VMEM, ANY, ANY],
        out_specs=[ANY, ANY, ANY, VMEM, VMEM],
        out_shape=[
            jax.ShapeDtypeStruct((tb // n_row, width), BF16),
            jax.ShapeDtypeStruct((hd, width), F32),
            jax.ShapeDtypeStruct((hd, width), F32),
            jax.ShapeDtypeStruct((e, width // per_kv), F32),
            jax.ShapeDtypeStruct((e, width // per_kv), F32),
        ],
        scratch_shapes=[
            pltpu.VMEM((tokens, n_row * gw), BF16),
            pltpu.VMEM((n_row * gw, cw), BF16),
            pltpu.VMEM((ring, tb, cw), F32),
            pltpu.VMEM((2, tb, cw // 2), F32),
            pltpu.VMEM((2, tb, cw), F32),
            pltpu.VMEM((tb, cw), BF16),
            pltpu.VMEM((2, tokens, bc), BF16),
            pltpu.VMEM((2, hd, bc), F32),
            pltpu.VMEM((per_kv * (gw - hd), tokens), BF16),
            dma((ring, 9)),
            dma((ring, 9)),
            dma((6,)),
            dma((6,)),
            dma((n_row,)),
            dma((n_row,)),
            dma((2,)),
            dma((2,)),
            dma((3 * n_row + 1,)),
        ],
        compiler_params=pltpu.CompilerParams(collective_id=1, has_side_effects=True, vmem_limit_bytes=60 << 20),
        cost_estimate=pl.CostEstimate(flops=2 * tokens * width * (n_row * gw // n_row + 3 * hd), bytes_accessed=100 << 20, transcendentals=0),
    )(g, wrow, wk, wv, dqt, ot, x, dy)


def solution(mesh):
    n = mesh.shape["tp"]
    ring = math.isqrt(n // 2)
    cores = n // (ring * ring)
    if ring != 4 or cores != 2:
        raise ValueError("needs a 4x4 torus")

    def local_grads(x_blk, dy_blk, wq_loc, w_k, w_v, wo_loc):
        model_dim, kv_heads, e = w_k.shape
        heads = wq_loc.shape[1]
        hd = heads * e
        scale = e ** -0.5
        wq = jnp.transpose(wq_loc, (1, 2, 0)).reshape(hd, model_dim)
        wk = jnp.transpose(w_k, (1, 2, 0))
        wv = jnp.transpose(w_v, (1, 2, 0))
        wo = wo_loc.reshape(hd, model_dim)
        x_full, dy_full, g, dqt, ot, wrow, _ = _front(ring, cores, heads, scale, x_blk, dy_blk, wq, wk, wv, wo)
        dx, dwq, dwo, dwk, dwv = _grads(ring, cores, heads, g, wrow, wk, wv, dqt, ot, x_full, dy_full)
        return (dx, jnp.transpose(dwq.reshape(heads, e, model_dim), (2, 0, 1)), dwo.reshape(heads, e, model_dim), dwk.T, dwv.T)

    tok = P(("dp", "tp"))
    return jax.shard_map(
        local_grads,
        mesh=mesh,
        in_specs=(tok, tok, P(None, "tp", None), P(), P(), P("tp")),
        out_specs=(tok, P("dp", "tp", None), tok, tok, tok),
        check_vma=False,
    )
```

```python
import functools
import math

import jax
import jax.numpy as jnp
from jax import lax
from jax.experimental import pallas as pl
from jax.experimental.pallas import tpu as pltpu
from jax.sharding import PartitionSpec as P

F32 = jnp.float32
BF16 = jnp.bfloat16
MESH = pl.DeviceIdType.MESH
ANY = pl.BlockSpec(memory_space=pl.ANY)
VMEM = pl.BlockSpec(memory_space=pltpu.VMEM)
LOG2E = math.log2(math.e)


def _scoped(fn):
    def run(*args, **kw):
        with jax.named_scope(fn.__name__):
            return fn(*args, **kw)

    return run


def _dot(a, b, dims):
    return lax.dot_general(a, b, (dims, ((), ())), preferred_element_type=F32)


def _nn(a, b):
    return _dot(a, b, ((1,), (0,)))


def _nt(a, b):
    return _dot(a, b, ((1,), (1,)))


class Place:
    def __init__(self, ring, cores):
        me = lax.axis_index("tp")
        self.ring, self.cores = ring, cores
        self.c = lax.rem(me, cores)
        self.x = lax.rem(me // cores, ring)
        self.y = me // (cores * ring)
        self.r = self.x * cores + self.c
        self.n_row = ring * cores

    def dev(self, y, x, c):
        y = lax.rem(y + self.ring, self.ring)
        x = lax.rem(x + self.ring, self.ring)
        return {"tp": (y * self.ring + x) * self.cores + c}

    def row_dev(self, r):
        return {"tp": self.y * self.n_row + r}

    def slot(self, x, c):
        return lax.rem(x + self.ring, self.ring) * self.cores + c


def _remote(src, dst, send, recv, dev):
    return pltpu.make_async_remote_copy(
        src_ref=src, dst_ref=dst, send_sem=send, recv_sem=recv, device_id=dev, device_id_type=MESH
    )


@_scoped
def _enter(devices):
    barrier = pltpu.get_barrier_semaphore()
    for dev in devices:
        pl.semaphore_signal(barrier, inc=1, device_id=dev, device_id_type=MESH)
    pl.semaphore_wait(barrier, len(devices))


OWN, MINUS, PLUS, FAR = range(4)
STEP = (0, -1, 1, 2)


class Gather:
    def __init__(self, at, src, full, send, recv, mate_recv):
        self.at, self.src, self.full = at, src, full
        self.send, self.recv, self.mate_recv = send, recv, mate_recv
        self.rows = src.shape[0]
        self.next_send = 0
        self.sent = []
        c = at.c
        self.first = {s: at.dev(at.y + c * s, at.x + (1 - c) * s, c) for s in (1, -1)}
        self.second = {s: at.dev(at.y + (1 - c) * s, at.x + c * s, c) for s in (1, -1)}
        self.mate = at.dev(at.y, at.x, 1 - c)

    def ref(self, d1, d2, core, half=None):
        at = self.at
        o1, o2 = STEP[d1], STEP[d2]
        x = at.x + (1 - core) * o1 + core * o2
        y = at.y + core * o1 + (1 - core) * o2
        n = self.rows if half is None else self.rows // 2
        r0 = at.dev(y, x, core)["tp"] * self.rows + (0 if half is None else half * n)
        return self.full.at[pl.ds(pl.multiple_of(r0, n), n), :]

    def push(self, src, dst, recv, dev):
        k = self.next_send
        self.next_send += 1
        self.sent.append(dst.shape[0])
        return _remote(src, dst, self.send.at[k], recv, dev)

    def out(self, d1, d2, half=None):
        if d1 == OWN and d2 == OWN:
            n = self.rows if half is None else self.rows // 2
            return self.src.at[pl.ds(0 if half is None else half * n, n), :]
        return self.ref(d1, d2, self.at.c, half)

    def to_mate(self, d1, d2):
        ref = self.ref(d1, d2, self.at.c)
        self.push(self.out(d1, d2), ref, self.mate_recv.at[d1, d2], self.mate).start()

    def arrived(self, d1, d2, half=None):
        ref = self.ref(d1, d2, self.at.c, half)
        _remote(ref, ref, self.send.at[0], self.recv.at[d1, d2, half or 0], self.mate).wait_recv()

    def second_full(self, d1):
        ref = self.ref(d1, OWN, self.at.c)
        return [self.push(self.out(d1, OWN), ref, self.recv.at[d1, to, 0], self.second[s]) for s, to in ((1, MINUS), (-1, PLUS))]

    def prepare(self):
        self.fulls = {d: self.second_full(d) for d in range(4)}

    @_scoped
    def start(self):
        ref = self.ref(OWN, OWN, self.at.c)
        for s, to in ((1, MINUS), (-1, PLUS)):
            self.push(self.src, ref, self.recv.at[to, OWN, 0], self.first[s]).start()
        self.go(OWN)
        self.to_mate(OWN, OWN)

    def go(self, d1):
        for cp in self.fulls[d1]:
            cp.start()

    @_scoped
    def relay_first(self):
        for d, s, half in ((MINUS, 1, 0), (PLUS, -1, 1)):
            self.arrived(d, OWN)
            ref = self.ref(d, OWN, self.at.c, half)
            self.push(ref, ref, self.recv.at[FAR, OWN, half], self.first[s]).start()
            self.to_mate(d, OWN)

    @_scoped
    def far_first(self):
        for half in (0, 1):
            self.arrived(FAR, OWN, half)
        self.to_mate(FAR, OWN)

    @_scoped
    def relay_second(self, d1):
        for d, s, half in ((MINUS, 1, 0), (PLUS, -1, 1)):
            self.arrived(d1, d)
            ref = self.ref(d1, d, self.at.c, half)
            self.push(ref, ref, self.recv.at[d1, FAR, half], self.second[s]).start()
            self.to_mate(d1, d)

    @_scoped
    def far_second(self, d1):
        for half in (0, 1):
            self.arrived(d1, FAR, half)
        self.to_mate(d1, FAR)

    @_scoped
    def await_mate_row(self, t):
        at = self.at
        for j in range(4):
            i1 = (1 - at.c) * t + at.c * j
            i2 = at.c * t + (1 - at.c) * j
            ref = self.full.at[pl.ds(0, self.rows), :]
            _remote(ref, ref, self.send.at[0], self.mate_recv.at[i1, i2], self.mate).wait_recv()

    @_scoped
    def drain(self):
        for k, n in enumerate(self.sent):
            ref = self.full.at[pl.ds(0, n), :]
            _remote(ref, ref, self.send.at[k], self.send.at[k], self.mate).wait_send()


def _kernel(ring, cores, heads, scale, bq, bs, bc, x_ref, dy_ref, w_ref, wk_ref, wv_ref, wo_ref,
            dx_ref, dwq_ref, dwo_ref, dwk_ref, dwv_ref, xf_ref, dyf_ref,
            gq, w_all, part, rs_half, rs_full, stage, hop_ref, qkvt_ref, dot_ref, dqt_ref, ot_ref, dk_ref, dv_ref,
            send, recv, mate_recv, w_send, w_recv, hop_recv, ld_sem, blk_sem,
            ag_send, ag_recv, rs_send, rs_recv, out_send, out_recv, in_sem, o_sem):
    at = Place(ring, cores)
    n_row = at.n_row
    hd = wo_ref.shape[0]
    e = hd // heads
    tokens, width = xf_ref.shape
    tb = tokens // ring
    cw = width // n_row
    gw = gq.shape[1] // n_row
    c = at.c
    gx = Gather(at, x_ref, xf_ref, send.at[0], recv.at[0], mate_recv.at[0])
    gy = Gather(at, dy_ref, dyf_ref, send.at[1], recv.at[1], mate_recv.at[1])
    n_kv = wk_ref.shape[0] // ring
    per_kv = n_row // n_kv
    row_peers = [lax.rem(at.r + d, n_row) for d in range(1, n_row)]
    up, down = at.dev(at.y + 1, at.x, c), at.dev(at.y - 1, at.x, c)

    hh = hd // 2

    def w_push(k, src, dst, rsem, dev):
        _remote(src, dst, w_send.at[k], rsem, dev).start()

    def wq_slot(slot, half=None):
        r0 = slot * gw + (0 if half is None else half * hh)
        return w_all.at[pl.ds(r0 if isinstance(r0, int) else pl.multiple_of(r0, hh), hd if half is None else hh), :]

    def wcols(slot):
        return pl.ds(pl.multiple_of(slot * cw, cw), cw)

    right, left, mate = at.dev(at.y, at.x + 1, c), at.dev(at.y, at.x - 1, c), at.dev(at.y, at.x, 1 - c)

    @_scoped
    def w_start():
        for half, dev in ((0, right), (1, left)):
            for k in range(cores):
                w_push(half * 2 + k, w_ref.at[pl.ds(half * hh, hh), wcols(at.slot(at.x + 2, k))], hop_ref.at[half * 2 + k], hop_recv.at[half * 2 + k], dev)
        w_push(4, w_ref.at[pl.ds(0, hd), wcols(at.slot(at.x, 1 - c))], wq_slot(at.r), w_recv.at[0], mate)
        for i, s in enumerate((1, -1)):
            for k in range(cores):
                dst_core = c if k == 0 else 1 - c
                w_push(5 + 2 * i + k, w_ref.at[pl.ds(0, hd), wcols(at.slot(at.x + s, dst_core))], wq_slot(at.r), w_recv.at[1 + 2 * i + k], at.dev(at.y, at.x + s, dst_core))

    @_scoped
    def w_relay():
        for half, s in ((0, 1), (1, -1)):
            for n in (half * 2, half * 2 + 1):
                _remote(hop_ref.at[n], hop_ref.at[n], w_send.at[0], hop_recv.at[n], mate).wait_recv()
            for k in range(cores):
                n = half * 2 + k
                src_slot = at.slot(at.x - s, c)
                same = k == 0
                dst_core = c if same else 1 - c
                w_push(9 + n, hop_ref.at[half * 2 + dst_core], wq_slot(src_slot, half), w_recv.at[5 + n], at.dev(at.y, at.x + s, dst_core))

    @_scoped
    def w_finish():
        whole = wq_slot(0)
        piece = wq_slot(0, 0)
        for n in range(9):
            ref = whole if n < 5 else piece
            _remote(ref, ref, w_send.at[0], w_recv.at[n], mate).wait_recv()

    def w_drain():
        whole = wq_slot(0)
        piece = wq_slot(0, 0)
        for k in range(13):
            ref = whole if 4 <= k < 9 else piece
            _remote(ref, ref, w_send.at[k], w_send.at[k], mate).wait_send()

    own_cols = wcols(at.r)
    rows = x_ref.shape[0]
    own_rows = pl.ds(pl.multiple_of((at.y * n_row + at.r) * rows, rows), rows)

    keep = [pltpu.make_async_copy(w_ref.at[:, own_cols], wq_slot(at.r), ld_sem.at[8])]
    for r in range(n_row):
        kv_r = at.y * n_kv + r // per_kv
        for i, w in enumerate((wk_ref, wv_ref)):
            keep.append(pltpu.make_async_copy(w.at[kv_r, :, own_cols], w_all.at[pl.ds(r * gw + hd + i * e, e), :], ld_sem.at[9 + 2 * r + i]))

    def front(w_v, wo_v, xblk):
        kv = (at.y * n_row + at.r) // (n_row * ring // wk_ref.shape[0])
        loads = [
            pltpu.make_async_copy(w_ref, w_v.at[pl.ds(0, hd), :], ld_sem.at[0]),
            pltpu.make_async_copy(wo_ref, wo_v, ld_sem.at[1]),
            pltpu.make_async_copy(wk_ref.at[kv], w_v.at[pl.ds(hd, e), :], ld_sem.at[6]),
            pltpu.make_async_copy(wv_ref.at[kv], w_v.at[pl.ds(hd + e, e), :], ld_sem.at[7]),
        ]
        ins = [pltpu.make_async_copy(src, xblk.at[i, pl.ds(0, rows), :], ld_sem.at[2 + i]) for i, src in enumerate((x_ref, dy_ref))]
        outs = [pltpu.make_async_copy(xblk.at[i, pl.ds(0, rows), :], dst.at[own_rows, :], ld_sem.at[4 + i]) for i, dst in enumerate((xf_ref, dyf_ref))]
        for cp in ins:
            cp.start()
        _enter([up, down] + [at.row_dev(r) for r in row_peers])
        gx.prepare()
        gx.start()
        for cp in loads + keep:
            cp.start()
        for cp in ins:
            cp.wait()
        for cp in outs:
            cp.start()

        dk_ref[...] = jnp.zeros_like(dk_ref)
        dv_ref[...] = jnp.zeros_like(dv_ref)

        @_scoped
        def project(full, w, out, b):
            def load(i):
                r0 = pl.multiple_of(b * tb + i * bq, bq)
                return pltpu.make_async_copy(full.at[pl.ds(r0, bq), :], xblk.at[i], blk_sem.at[i])

            for i in range(tb // bq):
                load(i).start()

            def block(i, _):
                load(i).wait()
                out[:, pl.ds(pl.multiple_of(b * tb + i * bq, bq), bq)] = _nt(w[...], xblk[i]).astype(BF16)
                return 0

            lax.fori_loop(0, tb // bq, block, 0)

        def row_at(t):
            off = jnp.where(t == 1, ring - 1, jnp.where(t == 2, 1, jnp.where(t == 3, 2, 0)))
            return lax.rem(at.y + off, ring)

        for cp in loads + outs:
            cp.wait()

        def x_turn(t, _):
            @pl.when(t == 0)
            def _():
                gx.relay_first()
                gx.go(MINUS)

                @pl.when(c == 0)
                def _():
                    gx.go(PLUS)

                gx.far_first()

                @pl.when(c == 0)
                def _():
                    gx.go(FAR)

                gx.relay_second(OWN)

                @pl.when(c == 1)
                def _():
                    gx.go(PLUS)

                gx.relay_second(MINUS)

                @pl.when(c == 1)
                def _():
                    gx.go(FAR)

                gx.relay_second(PLUS)
                gx.far_second(OWN)

            @pl.when(t == 1)
            def _():
                gx.relay_second(FAR)
                gy.start()
                gx.far_second(MINUS)

            @pl.when(t == 2)
            def _():
                gx.far_second(PLUS)
                gx.far_second(FAR)

            gx.await_mate_row(t)
            project(xf_ref, w_v, qkvt_ref, row_at(t))
            return 0

        gy.prepare()
        lax.fori_loop(0, ring, x_turn, 0)

        krow, vrow = heads * e, (heads + 1) * e
        keys_k, keys_v = slice(krow, krow + e), slice(vrow, vrow + e)
        m4 = heads * bs
        row = lax.broadcasted_iota(jnp.int32, (m4, bq), 0) & (bs - 1)
        col = lax.broadcasted_iota(jnp.int32, (m4, bq), 1)

        def put(which, ks, value):
            n = ks.start // cw
            part[which * 2 + n, :, ks.start - n * cw:ks.stop - n * cw] = value

        def got(which, ks):
            n = ks.start // cw
            return part[which * 2 + n, :, ks.start - n * cw:ks.stop - n * cw]

        def lanes(v):
            parts = [v[:, t:t + 128] for t in range(0, v.shape[1], 128)]
            return parts

        @_scoped
        def attend(k):
            base = k * tb
            chunks = [slice(t, t + bq) for t in range(0, base + tb, bq)]

            def queries(j, _):
                q0 = pl.multiple_of(base + j * bs, bs)
                qs = pl.ds(q0, bs)
                qt = jnp.concatenate([qkvt_ref[h * e:(h + 1) * e, qs] for h in range(heads)], axis=1)
                dot = jnp.concatenate([dot_ref[h * e:(h + 1) * e, qs] for h in range(heads)], axis=1)
                q = qt.T
                do = dot.T
                m = None
                for ks in chunks:
                    s = _nn(q, qkvt_ref[keys_k, ks])
                    if ks.start >= base:
                        s = jnp.where(col + (ks.start - base) <= row + j * bs, s, -jnp.inf)
                    put(0, ks, s)
                    for part in lanes(s):
                        m = part if m is None else jnp.maximum(m, part)
                m = jnp.max(m, axis=1, keepdims=True)
                total = None
                for ks in chunks:
                    p = jnp.exp2((got(0, ks) - m) * (scale * LOG2E))
                    put(0, ks, p)
                    for part in lanes(p):
                        total = part if total is None else total + part
                    put(1, ks, _nn(do, qkvt_ref[keys_v, ks]))
                inv = 1.0 / jnp.sum(total, axis=1, keepdims=True)
                out = None
                for ks in chunks:
                    p = got(0, ks) * inv
                    put(0, ks, p)
                    pb = p.astype(BF16)
                    part = _nt(qkvt_ref[keys_v, ks], pb)
                    out = part if out is None else out + part
                    dv_ref[:, ks] += _nn(dot, pb)
                out = out.astype(BF16)
                delta = jnp.sum(dot.astype(F32) * out.astype(F32), axis=0, keepdims=True)
                delta = jnp.broadcast_to(delta, (128, m4)).T[:, :1]
                dq = None
                for ks in chunks:
                    ds = (got(0, ks) * (got(1, ks) - delta)).astype(BF16)
                    part = _nt(qkvt_ref[keys_k, ks], ds)
                    dq = part if dq is None else dq + part
                    dk_ref[:, ks] += _nn(qt, ds)
                dq = (dq * scale).astype(BF16)
                for h in range(heads):
                    ot_ref[h * e:(h + 1) * e, qs] = out[:, h * bs:(h + 1) * bs]
                    dqt_ref[h * e:(h + 1) * e, qs] = dq[:, h * bs:(h + 1) * bs]
                for h in range(0, heads, 2):
                    pair = jnp.concatenate([dq[:, h * bs:(h + 1) * bs], dq[:, (h + 1) * bs:(h + 2) * bs]], axis=0)
                    gq[qs, pl.ds(pl.multiple_of(at.r * gw + h * e, 128), 2 * e)] = pair.T
                return 0

            lax.fori_loop(0, tb // bs, queries, 0)

        def turn(t, _):
            @pl.when(t == 0)
            def _():
                gy.relay_first()
                gy.go(MINUS)

                @pl.when(c == 0)
                def _():
                    gy.go(PLUS)

                gy.far_first()

                @pl.when(c == 0)
                def _():
                    gy.go(FAR)

                gy.relay_second(OWN)

                @pl.when(c == 1)
                def _():
                    gy.go(PLUS)

                gy.relay_second(MINUS)

                @pl.when(c == 1)
                def _():
                    gy.go(FAR)
                    far_step(OWN)

            @pl.when(t == 1)
            def _():
                gy.relay_second(PLUS)

                @pl.when(c == 1)
                def _():
                    far_step(MINUS)

                gy.relay_second(FAR)

            @pl.when(t == 2)
            def _():
                w_start()

                @pl.when(c == 1)
                def _():
                    far_step(PLUS)

                @pl.when(c == 0)
                def _():
                    far_step(OWN)
                    far_step(MINUS)

            @pl.when(t == 3)
            def _():
                @pl.when(c == 0)
                def _():
                    far_step(PLUS)

                far_step(FAR)
                w_relay()

            gy.await_mate_row(t)
            b = row_at(t)
            project(dyf_ref, wo_v, dot_ref, b)
            for k in range(ring):
                @pl.when(b == k)
                def _(k=k):
                    attend(k)
            return 0

        far_cp = {d: gy.push(gy.ref(d, FAR, c), gy.ref(d, FAR, c), gy.mate_recv.at[d, FAR], gy.mate) for d in range(4)}

        @_scoped
        def far_step(d):
            for half in (0, 1):
                gy.arrived(d, FAR, half)
            far_cp[d].start()

        lax.fori_loop(0, ring, turn, 0)


    pl.run_scoped(front, pltpu.VMEM((hd + 2 * e, width), BF16), pltpu.VMEM((hd, width), BF16), pltpu.VMEM((2, bq, width), BF16))

    own_g = at.r * gw
    for k in range(0, tokens, bq):
        ks = slice(k, k + bq)
        kv = jnp.concatenate([(dk_ref[:, ks] * scale).astype(BF16), dv_ref[:, ks].astype(BF16)], axis=0)
        gq[ks, pl.ds(pl.multiple_of(own_g + hd, 128), 2 * e)] = kv.T

    def back(xbuf, obuf, kvt):
        th = tb // 2
        tq = th // 2
        tl = tb // n_row
        hw = cw // 2
        half_a, half_b = pl.ds(0, hw), pl.ds(hw, hw)
        units = [(FAR, 0), (FAR, 1), (PLUS, 0), (MINUS, 0), (PLUS, 1), (MINUS, 1), (OWN, 0), (OWN, 1)]
        place = {u: i for i, u in enumerate(units)}
        s_own, s_left, s_right, s_far = (at.slot(at.x + o, c) for o in (0, -1, 1, 2))
        m_own, m_left, m_right, m_far = (at.slot(at.x + o, 1 - c) for o in (0, -1, 1, 2))

        def unit_row(u):
            d, s = units[u]
            return pl.multiple_of(lax.rem(at.y + STEP[d] + ring, ring) * tb + s * th, th)

        def gcols(slot):
            return pl.ds(pl.multiple_of(slot * gw, gw), gw)

        def piece(u, slot, half=None):
            r0 = unit_row(u)
            rows = pl.ds(r0, th) if half is None else pl.ds(pl.multiple_of(r0 + half * tq, tq), tq)
            return gq.at[rows, gcols(slot)]

        sends = []

        def ag_push(u, n, slot, dev, half=None):
            ref = piece(u, slot, half)
            cp = _remote(ref, ref, ag_send.at[u, n], ag_recv.at[u, n], dev)
            cp.start()
            sends.append(cp)

        def ag_wait(u, n, slot, half=None):
            ref = piece(u, slot, half)
            _remote(ref, ref, ag_send.at[u, n], ag_recv.at[u, n], mate).wait_recv()

        def ag_own(u):
            ag_push(u, 0, s_own, right)
            ag_push(u, 1, s_own, left)
            ag_push(u, 2, s_own, mate)

        @_scoped
        def ag_relay(u):
            ag_wait(u, 0, s_left)
            ag_push(u, 3, s_left, right, 0)
            ag_push(u, 4, s_left, mate)
            ag_wait(u, 1, s_right)
            ag_push(u, 5, s_right, left, 1)
            ag_push(u, 6, s_right, mate)

        @_scoped
        def ag_finish(u):
            ag_wait(u, 3, s_far, 0)
            ag_push(u, 7, s_far, mate, 0)
            ag_wait(u, 5, s_far, 1)
            ag_push(u, 8, s_far, mate, 1)
            ag_wait(u, 2, m_own)
            ag_wait(u, 4, m_left)
            ag_wait(u, 6, m_right)
            ag_wait(u, 7, m_far, 0)
            ag_wait(u, 8, m_far, 1)

        nt = min(256, cw)

        def mine(u):
            d, s = units[u]
            return part.at[d, pl.ds(s * th, th), :]

        @_scoped
        def partial(u):
            rows = pl.ds(unit_row(u), th)
            dst = mine(u)

            def tile(j, _):
                cs = pl.ds(pl.multiple_of(j * nt, nt), nt)
                dst[:, cs] = _nn(gq[rows, :], w_all[:, cs])
                return 0

            lax.fori_loop(0, cw // nt, tile, 0)

        def rs_push(n, s, src, dst, dev):
            cp = _remote(src, dst, rs_send.at[n, s], rs_recv.at[n, s], dev)
            cp.start()
            sends.append(cp)

        def rs_wait(n, s):
            ref = rs_half.at[0, s]
            _remote(ref, ref, rs_send.at[n, s], rs_recv.at[n, s], mate).wait_recv()

        def block(d, s, half):
            return part.at[d, pl.ds(s * th, th), half]

        def send_far(s):
            rs_push(0, s, block(FAR, s, half_a), rs_half.at[0, s], up)
            rs_push(1, s, block(FAR, s, half_b), rs_half.at[1, s], down)

        def send_near_a(s):
            rs_push(4, s, block(MINUS, s, half_a), rs_full.at[1, s, 0], down)

        @_scoped
        def send_up_a(s):
            rs_wait(0, s)
            block(PLUS, s, half_a)[...] += rs_half[0, s]
            rs_push(2, s, block(PLUS, s, half_a), rs_full.at[0, s, 0], up)

        def send_up_b(s):
            rs_push(3, s, block(PLUS, s, half_b), rs_full.at[0, s, 1], up)

        @_scoped
        def send_down_b(s):
            rs_wait(1, s)
            block(MINUS, s, half_b)[...] += rs_half[1, s]
            rs_push(5, s, block(MINUS, s, half_b), rs_full.at[1, s, 1], down)

        n_steps = width // bc

        @_scoped
        def stream(src, lhs, out, j0, j1):
            def load(j, slot):
                return pltpu.make_async_copy(src.at[:, pl.ds(pl.multiple_of(j * bc, bc), bc)], xbuf.at[slot], in_sem.at[slot])

            def store(j, slot):
                return pltpu.make_async_copy(obuf.at[slot], out.at[:, pl.ds(pl.multiple_of(j * bc, bc), bc)], o_sem.at[slot])

            if j0 == 0:
                load(0, 0).start()

            def step(j, _):
                slot = lax.rem(j, 2)

                @pl.when(j + 1 < n_steps)
                def _():
                    load(j + 1, 1 - slot).start()

                load(j, slot).wait()

                @pl.when(j >= 2)
                def _():
                    store(j - 2, slot).wait()

                obuf[slot] = _nn(lhs[...], xbuf[slot])
                store(j, slot).start()
                return 0

            lax.fori_loop(j0, j1, step, 0)
            if j1 == n_steps:
                for j in range(max(n_steps - 2, 0), n_steps):
                    store(j, j % 2).wait()

        def wo_steps(a, b):
            stream(dyf_ref, ot_ref, dwo_ref, n_steps * a // 16, n_steps * b // 16)

        def wq_steps(a, b):
            stream(xf_ref, dqt_ref, dwq_ref, n_steps * a // 16, n_steps * b // 16)

        first = (at.r // per_kv) * per_kv
        share = width // per_kv
        col0 = lax.rem(at.r, per_kv) * share

        def kv_load(j, slot):
            cs = pl.ds(pl.multiple_of(col0 + j * bc, bc), bc)
            return pltpu.make_async_copy(xf_ref.at[:, cs], xbuf.at[slot], in_sem.at[slot])

        def kv_step(j, _):
            slot = lax.rem(j, 2)

            @pl.when(j + 1 < share // bc)
            def _():
                kv_load(j + 1, 1 - slot).start()

            kv_load(j, slot).wait()
            prod = _nn(kvt[...], xbuf[slot])
            dk = dv = None
            for q in range(per_kv):
                a = prod[q * 2 * e:q * 2 * e + e]
                b = prod[q * 2 * e + e:(q + 1) * 2 * e]
                dk = a if dk is None else dk + a
                dv = b if dv is None else dv + b
            cs = pl.ds(pl.multiple_of(j * bc, bc), bc)
            dwk_ref[:, cs] = dk
            dwv_ref[:, cs] = dv
            return 0

        @_scoped
        def kv_grads():
            kv_load(0, 0).start()
            for q in range(per_kv):
                cols = pl.ds(pl.multiple_of((first + q) * gw + hd, 128), gw - hd)
                for t in range(0, tokens, bq):
                    kvt[q * (gw - hd):(q + 1) * (gw - hd), t:t + bq] = gq[t:t + bq, cols].T
            lax.fori_loop(0, share // bc, kv_step, 0)

        def hand(i, d, half):
            peer = lax.rem(at.r + d, n_row)
            rows = pl.ds(pl.multiple_of(peer * tl, tl), tl)
            cols = pl.ds(pl.multiple_of(at.r * cw + i * hw, hw), hw)
            return stage.at[rows, half], dx_ref.at[:, cols], at.row_dev(peer)

        @_scoped
        def finish(i, half):
            for s in (0, 1):
                rs_wait(2 + i, s)
                rs_wait(4 + i, s)
                stage[s * th:(s + 1) * th, half] = (block(OWN, s, half)[...] + rs_full[0, s, i] + rs_full[1, s, i]).astype(BF16)
            for d in range(1, n_row):
                src, dst, dev = hand(i, d, half)
                cp = _remote(src, dst, out_send.at[i, d], out_recv.at[i, d], dev)
                cp.start()
                sends.append(cp)
            src, dst, _ = hand(i, 0, half)
            pltpu.make_async_copy(src, dst, out_send.at[i, 0]).start()

        @_scoped
        def received(i, half):
            for d in range(1, n_row):
                src = lax.rem(at.r + n_row - d, n_row)
                ref = dx_ref.at[:, pl.ds(pl.multiple_of(src * cw + i * hw, hw), hw)]
                _remote(ref, ref, out_send.at[i, d], out_recv.at[i, d], mate).wait_recv()
            src, dst, _ = hand(i, 0, half)
            pltpu.make_async_copy(src, dst, out_send.at[i, 0]).wait()

        ag_own(0)
        wo_steps(0, 4)
        ag_relay(0)
        ag_own(1)
        ag_own(2)
        wo_steps(4, 6)
        ag_finish(0)
        for cp in keep:
            cp.wait()
        w_finish()
        partial(0)
        ag_relay(1)
        ag_own(3)
        send_far(0)
        wo_steps(6, 8)
        ag_finish(1)
        partial(1)
        ag_relay(2)
        ag_own(4)
        send_far(1)
        wo_steps(8, 11)
        ag_finish(2)
        partial(2)
        ag_relay(3)
        ag_own(5)
        send_up_a(0)
        wo_steps(11, 14)
        ag_finish(3)
        partial(3)
        ag_relay(4)
        ag_own(6)
        send_near_a(0)
        wo_steps(14, 16)
        ag_finish(4)
        partial(4)
        ag_relay(5)
        ag_own(7)
        send_up_a(1)
        wq_steps(0, 3)
        ag_finish(5)
        partial(5)
        ag_relay(6)
        send_near_a(1)
        send_down_b(0)
        send_up_b(0)
        wq_steps(3, 5)
        send_down_b(1)
        send_up_b(1)
        ag_finish(6)
        partial(6)
        ag_relay(7)
        wq_steps(5, 9)
        ag_finish(7)
        partial(7)
        wq_steps(9, 12)
        finish(0, half_a)
        wq_steps(12, 16)
        kv_grads()
        received(0, half_a)
        finish(1, half_b)
        received(1, half_b)
        for cp in sends:
            cp.wait_send()
        w_drain()
        gx.drain()
        gy.drain()

    pl.run_scoped(back, pltpu.VMEM((2, tokens, bc), BF16), pltpu.VMEM((2, hd, bc), F32), pltpu.VMEM((per_kv * 2 * e, tokens), BF16))


def _layer(ring, cores, heads, scale, x, dy, wq, wk, wv, wo):
    rows, width = x.shape
    tokens = rows * ring * ring * cores
    hd = wo.shape[0]
    e = hd // heads
    n_row = ring * cores
    cw = width // n_row
    gw = hd + 2 * e
    tb = tokens // ring
    th, hw = tb // 2, cw // 2
    per_kv = n_row * ring // wk.shape[0]
    bq = min(256, tb)
    bs = tb // heads
    bc = min(512, cw // 2)
    dma = pltpu.SemaphoreType.DMA
    shape = jax.ShapeDtypeStruct
    return pl.pallas_call(
        functools.partial(_kernel, ring, cores, heads, scale, bq, bs, bc),
        name="layer",
        in_specs=[ANY] * 6,
        out_specs=[ANY, ANY, ANY, VMEM, VMEM, ANY, ANY],
        out_shape=[
            shape((rows, width), BF16),
            shape((hd, width), F32),
            shape((hd, width), F32),
            shape((e, width // per_kv), F32),
            shape((e, width // per_kv), F32),
            shape((tokens, width), BF16),
            shape((tokens, width), BF16),
        ],
        scratch_shapes=[
            pltpu.VMEM((tokens, n_row * gw), BF16),
            pltpu.VMEM((n_row * gw, cw), BF16),
            pltpu.VMEM((4, tb, cw), F32),
            pltpu.VMEM((2, 2, th, hw), F32),
            pltpu.VMEM((2, 2, 2, th, hw), F32),
            pltpu.VMEM((tb, cw), BF16),
            pltpu.VMEM((4, hd // 2, cw), BF16),
            pltpu.VMEM((gw, tokens), BF16),
            pltpu.VMEM((hd, tokens), BF16),
            pltpu.VMEM((hd, tokens), BF16),
            pltpu.VMEM((hd, tokens), BF16),
            pltpu.VMEM((e, tokens), F32),
            pltpu.VMEM((e, tokens), F32),
            dma((2, 40)),
            dma((2, 4, 4, 2)),
            dma((2, 4, 4)),
            dma((13,)),
            dma((9,)),
            dma((4,)),
            dma((9 + 2 * n_row,)),
            dma((2,)),
            dma((8, 9)),
            dma((8, 9)),
            dma((6, 2)),
            dma((6, 2)),
            dma((2, n_row)),
            dma((2, n_row)),
            dma((2,)),
            dma((2,)),
        ],
        compiler_params=pltpu.CompilerParams(collective_id=0, has_side_effects=True, vmem_limit_bytes=67043328),
        cost_estimate=pl.CostEstimate(flops=70 * 10**9, bytes_accessed=300 << 20, transcendentals=heads * tokens * tokens // 2),
    )(x, dy, wq, wk, wv, wo)


def solution(mesh):
    n = mesh.shape["tp"]
    ring = math.isqrt(n // 2)
    cores = n // (ring * ring)
    if ring != 4 or cores != 2:
        raise ValueError("needs a 4x4 torus")

    def local_grads(x_blk, dy_blk, wq_loc, w_k, w_v, wo_loc):
        model_dim, kv_heads, e = w_k.shape
        heads = wq_loc.shape[1]
        hd = heads * e
        scale = e ** -0.5
        wq = jnp.transpose(wq_loc, (1, 2, 0)).reshape(hd, model_dim)
        wk = jnp.transpose(w_k, (1, 2, 0))
        wv = jnp.transpose(w_v, (1, 2, 0))
        wo = wo_loc.reshape(hd, model_dim)
        dx, dwq, dwo, dwk, dwv, _, _ = _layer(ring, cores, heads, scale, x_blk, dy_blk, wq, wk, wv, wo)
        return (dx, jnp.transpose(dwq.reshape(heads, e, model_dim), (2, 0, 1)), dwo.reshape(heads, e, model_dim), dwk.T, dwv.T)

    tok = P(("dp", "tp"))
    return jax.shard_map(
        local_grads,
        mesh=mesh,
        in_specs=(tok, tok, P(None, "tp", None), P(), P(), P("tp")),
        out_specs=(tok, P("dp", "tp", None), tok, tok, tok),
        check_vma=False,
    )
```

```python
import functools
import math

import jax
import jax.numpy as jnp
from jax import lax
from jax.experimental import pallas as pl
from jax.experimental.pallas import tpu as pltpu
from jax.sharding import PartitionSpec as P

F32 = jnp.float32
BF16 = jnp.bfloat16
MESH = pl.DeviceIdType.MESH
ANY = pl.BlockSpec(memory_space=pl.ANY)
VMEM = pl.BlockSpec(memory_space=pltpu.VMEM)
LOG2E = math.log2(math.e)


def _scoped(fn):
    def run(*args, **kw):
        with jax.named_scope(fn.__name__):
            return fn(*args, **kw)

    return run


def _dot(a, b, dims):
    return lax.dot_general(a, b, (dims, ((), ())), preferred_element_type=F32)


def _nn(a, b):
    return _dot(a, b, ((1,), (0,)))


def _nt(a, b):
    return _dot(a, b, ((1,), (1,)))


class Place:
    def __init__(self, ring, cores):
        me = lax.axis_index("tp")
        self.ring, self.cores = ring, cores
        self.c = lax.rem(me, cores)
        self.x = lax.rem(me // cores, ring)
        self.y = me // (cores * ring)
        self.r = self.x * cores + self.c
        self.n_row = ring * cores

    def dev(self, y, x, c):
        y = lax.rem(y + self.ring, self.ring)
        x = lax.rem(x + self.ring, self.ring)
        return {"tp": (y * self.ring + x) * self.cores + c}

    def row_dev(self, r):
        return {"tp": self.y * self.n_row + r}

    def slot(self, x, c):
        return lax.rem(x + self.ring, self.ring) * self.cores + c


def _remote(src, dst, send, recv, dev):
    return pltpu.make_async_remote_copy(
        src_ref=src, dst_ref=dst, send_sem=send, recv_sem=recv, device_id=dev, device_id_type=MESH
    )


@_scoped
def _enter(devices):
    barrier = pltpu.get_barrier_semaphore()
    for dev in devices:
        pl.semaphore_signal(barrier, inc=1, device_id=dev, device_id_type=MESH)
    pl.semaphore_wait(barrier, len(devices))


OWN, MINUS, PLUS, FAR = range(4)
STEP = (0, -1, 1, 2)


class Gather:
    def __init__(self, at, src, full, send, recv, mate_recv):
        self.at, self.src, self.full = at, src, full
        self.send, self.recv, self.mate_recv = send, recv, mate_recv
        self.rows = src.shape[0]
        self.sent = []
        c = at.c
        self.first = {s: at.dev(at.y + c * s, at.x + (1 - c) * s, c) for s in (1, -1)}
        self.second = {s: at.dev(at.y + (1 - c) * s, at.x + c * s, c) for s in (1, -1)}
        self.mate = at.dev(at.y, at.x, 1 - c)
        self.fulls = {d: self.both_ways(self.second, d, lambda to, d=d: (d, to)) for d in range(4)}

    def place(self, d1, d2, core):
        at = self.at
        o1, o2 = STEP[d1], STEP[d2]
        return at.y + core * o1 + (1 - core) * o2, at.x + (1 - core) * o1 + core * o2

    def ref(self, d1, d2, core, half=None):
        y, x = self.place(d1, d2, core)
        n = self.rows if half is None else self.rows // 2
        r0 = self.at.dev(y, x, core)["tp"] * self.rows + (0 if half is None else half * n)
        return self.full.at[pl.ds(pl.multiple_of(r0, n), n), :]

    def push(self, src, dst, recv, dev):
        k = len(self.sent)
        self.sent.append(dst.shape[0])
        return _remote(src, dst, self.send.at[k], recv, dev)

    def out(self, d1, d2, half=None):
        if d1 == OWN and d2 == OWN:
            n = self.rows if half is None else self.rows // 2
            return self.src.at[pl.ds(0 if half is None else half * n, n), :]
        return self.ref(d1, d2, self.at.c, half)

    def both_ways(self, devs, d1, name):
        copies = []
        for step in (0, 1):
            for s, to in ((1, MINUS), (-1, PLUS)):
                half = step if s == 1 else 1 - step
                copies.append(self.push(self.out(d1, OWN, half), self.ref(d1, OWN, self.at.c, half), self.recv.at[*name(to), half], devs[s]))
        return copies

    def to_mate(self, d1, d2):
        ref = self.ref(d1, d2, self.at.c)
        self.push(self.out(d1, d2), ref, self.mate_recv.at[d1, d2], self.mate).start()

    def arrived(self, d1, d2, half):
        ref = self.ref(d1, d2, self.at.c, half)
        _remote(ref, ref, self.send.at[0], self.recv.at[d1, d2, half], self.mate).wait_recv()

    @_scoped
    def start(self):
        for cp in self.both_ways(self.first, OWN, lambda to: (to, OWN)):
            cp.start()
        self.go(OWN)
        self.to_mate(OWN, OWN)

    def go(self, d1):
        for cp in self.fulls[d1]:
            cp.start()

    @_scoped
    def relay_first(self):
        for d, s, half in ((MINUS, 1, 0), (PLUS, -1, 1)):
            self.arrived(d, OWN, half)
            ref = self.ref(d, OWN, self.at.c, half)
            self.push(ref, ref, self.recv.at[FAR, OWN, half], self.first[s]).start()

    @_scoped
    def near_first(self):
        for d, half in ((MINUS, 1), (PLUS, 0)):
            self.arrived(d, OWN, half)
            self.to_mate(d, OWN)

    @_scoped
    def far_first(self):
        for half in (0, 1):
            self.arrived(FAR, OWN, half)
        self.to_mate(FAR, OWN)

    @_scoped
    def relay_second(self, d1):
        for d, s, half in ((MINUS, 1, 0), (PLUS, -1, 1)):
            self.arrived(d1, d, half)
            ref = self.ref(d1, d, self.at.c, half)
            self.push(ref, ref, self.recv.at[d1, FAR, half], self.second[s]).start()

    @_scoped
    def near_second(self, d1):
        for d, half in ((MINUS, 1), (PLUS, 0)):
            self.arrived(d1, d, half)
            self.to_mate(d1, d)

    @_scoped
    def far_second(self, d1):
        for half in (0, 1):
            self.arrived(d1, FAR, half)
        self.to_mate(d1, FAR)

    def load(self, y, x, core, block, sem):
        at = self.at
        r0 = at.dev(y, x, core)["tp"] * self.rows
        b0 = at.slot(x, core) * self.rows
        src = self.full.at[pl.ds(pl.multiple_of(r0, self.rows), self.rows), :]
        return pltpu.make_async_copy(src, block.at[pl.ds(pl.multiple_of(b0, self.rows), self.rows), :], sem)

    @_scoped
    def take_row(self, t, y, block, sem):
        at = self.at
        for j in range(4):
            self.load(y, at.x + STEP[j], at.c, block, sem).start()
        for j in range(4):
            i1 = (1 - at.c) * t + at.c * j
            i2 = at.c * t + (1 - at.c) * j
            ref = self.full.at[pl.ds(0, self.rows), :]
            _remote(ref, ref, self.send.at[0], self.mate_recv.at[i1, i2], self.mate).wait_recv()
            self.load(y, at.x + STEP[j], 1 - at.c, block, sem).start()

    @_scoped
    def drain(self):
        for k, n in enumerate(self.sent):
            ref = self.full.at[pl.ds(0, n), :]
            _remote(ref, ref, self.send.at[k], self.send.at[k], self.mate).wait_send()


def _kernel(ring, cores, heads, scale, bq, bs, bc, x_ref, dy_ref, w_ref, wk_ref, wv_ref, wo_ref,
            dx_ref, dwq_ref, dwo_ref, dwk_ref, dwv_ref, xf_ref, dyf_ref,
            gq, w_all, part, rs_half, rs_full, stage, hop_ref, qkvt_ref, dot_ref, dqt_ref, ot_ref, dk_ref, dv_ref, kn_ref, vn_ref,
            send, recv, mate_recv, w_send, w_recv, hop_recv, ld_sem, blk_sem,
            ag_send, ag_recv, rs_send, rs_recv, out_send, out_recv, in_sem, o_sem):
    at = Place(ring, cores)
    n_row = at.n_row
    hd = wo_ref.shape[0]
    e = hd // heads
    tokens, width = xf_ref.shape
    tb = tokens // ring
    cw = width // n_row
    gw = gq.shape[1] // n_row
    c = at.c
    gx = Gather(at, x_ref, xf_ref, send.at[0], recv.at[0], mate_recv.at[0])
    gy = Gather(at, dy_ref, dyf_ref, send.at[1], recv.at[1], mate_recv.at[1])
    n_kv = wk_ref.shape[0] // ring
    per_kv = n_row // n_kv
    row_peers = [lax.rem(at.r + d, n_row) for d in range(1, n_row)]
    up, down = at.dev(at.y + 1, at.x, c), at.dev(at.y - 1, at.x, c)

    hh = hd // 2
    hw = cw // 2

    def wcols(slot, i=None):
        c0 = slot * cw + (0 if i is None else i * hw)
        n = cw if i is None else hw
        return pl.ds(pl.multiple_of(c0, n), n)

    def wq_slot(slot, half=None, i=None):
        r0 = slot * gw + (0 if half is None else half * hh)
        rows = pl.ds(r0 if isinstance(r0, int) else pl.multiple_of(r0, hh), hd if half is None else hh)
        return w_all.at[rows, pl.ds(0, cw) if i is None else pl.ds(i * hw, hw)]

    def hop(n, i):
        return hop_ref.at[n, :, pl.ds(i * hw, hw)]

    right, left, mate = at.dev(at.y, at.x + 1, c), at.dev(at.y, at.x - 1, c), at.dev(at.y, at.x, 1 - c)

    def w_push(i, k, src, dst, rsem, dev):
        _remote(src, dst, w_send.at[i, k], rsem, dev).start()

    @_scoped
    def w_start(i):
        for half, dev in ((0, right), (1, left)):
            for k in range(cores):
                n = half * 2 + k
                w_push(i, n, w_ref.at[pl.ds(half * hh, hh), wcols(at.slot(at.x + 2, k), i)], hop(n, i), hop_recv.at[i, n], dev)
        w_push(i, 4, w_ref.at[:, wcols(at.slot(at.x, 1 - c), i)], wq_slot(at.r, None, i), w_recv.at[i, 0], mate)
        for n, s in enumerate((1, -1)):
            for k in range(cores):
                core = c if k == 0 else 1 - c
                w_push(i, 5 + 2 * n + k, w_ref.at[:, wcols(at.slot(at.x + s, core), i)], wq_slot(at.r, None, i), w_recv.at[i, 1 + 2 * n + k], at.dev(at.y, at.x + s, core))

    @_scoped
    def w_relay(i):
        for half, s in ((0, 1), (1, -1)):
            for n in (half * 2, half * 2 + 1):
                _remote(hop(n, i), hop(n, i), w_send.at[i, 0], hop_recv.at[i, n], mate).wait_recv()
            for k in range(cores):
                core = c if k == 0 else 1 - c
                n = half * 2 + k
                w_push(i, 9 + n, hop(half * 2 + core, i), wq_slot(at.slot(at.x - s, c), half, i), w_recv.at[i, 5 + n], at.dev(at.y, at.x + s, core))

    @_scoped
    def w_finish(i):
        for n in range(9):
            ref = wq_slot(0, None if n < 5 else 0, i)
            _remote(ref, ref, w_send.at[i, 0], w_recv.at[i, n], mate).wait_recv()

    def w_drain(i):
        for k in range(13):
            ref = wq_slot(0, None if 4 <= k < 9 else 0, i)
            _remote(ref, ref, w_send.at[i, k], w_send.at[i, k], mate).wait_send()

    own_cols = wcols(at.r)
    rows = x_ref.shape[0]
    own_rows = pl.ds(pl.multiple_of((at.y * n_row + at.r) * rows, rows), rows)

    keep = [pltpu.make_async_copy(w_ref.at[:, own_cols], wq_slot(at.r), ld_sem.at[8])]
    for r in range(n_row):
        kv_r = at.y * n_kv + r // per_kv
        for i, w in enumerate((wk_ref, wv_ref)):
            keep.append(pltpu.make_async_copy(w.at[kv_r, :, own_cols], w_all.at[pl.ds(r * gw + hd + i * e, e), :], ld_sem.at[9 + 2 * r + i]))

    def front(w_v, wo_v, xblk):
        kv = (at.y * n_row + at.r) // (n_row * ring // wk_ref.shape[0])
        loads = [
            pltpu.make_async_copy(w_ref, w_v.at[pl.ds(0, hd), :], ld_sem.at[0]),
            pltpu.make_async_copy(wo_ref, wo_v, ld_sem.at[1]),
            pltpu.make_async_copy(wk_ref.at[kv], w_v.at[pl.ds(hd, e), :], ld_sem.at[6]),
            pltpu.make_async_copy(wv_ref.at[kv], w_v.at[pl.ds(hd + e, e), :], ld_sem.at[7]),
        ]
        ins = [pltpu.make_async_copy(src, xblk.at[pl.ds(i * rows, rows), :], ld_sem.at[2 + i]) for i, src in enumerate((x_ref, dy_ref))]
        outs = [pltpu.make_async_copy(xblk.at[pl.ds(i * rows, rows), :], dst.at[own_rows, :], ld_sem.at[4 + i]) for i, dst in enumerate((xf_ref, dyf_ref))]
        for cp in ins:
            cp.start()
        _enter([up, down] + [at.row_dev(r) for r in row_peers])
        gx.start()
        for cp in loads + keep:
            cp.start()
        for cp in ins:
            cp.wait()
        for cp in outs:
            cp.start()

        dk_ref[...] = jnp.zeros_like(dk_ref)
        dv_ref[...] = jnp.zeros_like(dv_ref)

        @_scoped
        def project(w, out, b):
            pltpu.make_async_copy(xf_ref.at[pl.ds(0, tb), :], xblk, blk_sem.at[0]).wait()

            def block(i, _):
                r0 = pl.multiple_of(i * bq, bq)
                out[:, pl.ds(pl.multiple_of(b * tb + i * bq, bq), bq)] = _nt(w[...], xblk[pl.ds(r0, bq), :]).astype(BF16)
                return 0

            lax.fori_loop(0, tb // bq, block, 0)

        def row_at(t):
            off = jnp.where(t == 1, ring - 1, jnp.where(t == 2, 1, jnp.where(t == 3, 2, 0)))
            return lax.rem(at.y + off, ring)

        for cp in loads + outs:
            cp.wait()

        def begin(g):
            g.relay_first()
            g.near_first()
            g.go(MINUS)

            @pl.when(c == 0)
            def _():
                g.go(PLUS)

            g.far_first()

            @pl.when(c == 0)
            def _():
                g.go(FAR)

            g.relay_second(OWN)

            @pl.when(c == 1)
            def _():
                g.go(PLUS)

            g.near_second(OWN)

        def x_turn(t, _):
            @pl.when(t == 0)
            def _():
                begin(gx)
                gx.relay_second(MINUS)

                @pl.when(c == 1)
                def _():
                    gx.go(FAR)

                gx.near_second(MINUS)
                gx.relay_second(PLUS)
                gx.near_second(PLUS)
                gx.relay_second(FAR)
                gy.start()
                gx.far_second(OWN)

            @pl.when(t == 1)
            def _():
                gx.near_second(FAR)
                gx.far_second(MINUS)

            @pl.when(t == 2)
            def _():
                gx.far_second(PLUS)
                gx.far_second(FAR)

            b = row_at(t)
            gx.take_row(t, b, xblk, blk_sem.at[0])
            project(w_v, qkvt_ref, b)
            return 0

        lax.fori_loop(0, ring, x_turn, 0)
        for t in range(0, tokens, bq):
            kn_ref[t:t + bq, :] = qkvt_ref[hd:hd + e, t:t + bq].T
            vn_ref[t:t + bq, :] = qkvt_ref[hd + e:hd + 2 * e, t:t + bq].T

        krow, vrow = heads * e, (heads + 1) * e
        keys_k, keys_v = slice(krow, krow + e), slice(vrow, vrow + e)
        m4 = heads * bs
        row = lax.broadcasted_iota(jnp.int32, (m4, bq), 0) & (bs - 1)
        col = lax.broadcasted_iota(jnp.int32, (m4, bq), 1)

        def put(which, ks, value):
            n = ks.start // cw
            part[which * 2 + n, :, ks.start - n * cw:ks.stop - n * cw] = value

        def got(which, ks):
            n = ks.start // cw
            return part[which * 2 + n, :, ks.start - n * cw:ks.stop - n * cw]

        def lanes(v):
            parts = [v[:, t:t + 128] for t in range(0, v.shape[1], 128)]
            return parts

        @_scoped
        def attend(k):
            base = k * tb
            chunks = [slice(t, t + bq) for t in range(0, base + tb, bq)]

            def queries(j, _):
                q0 = pl.multiple_of(base + j * bs, bs)
                qs = pl.ds(q0, bs)
                qt = jnp.concatenate([qkvt_ref[h * e:(h + 1) * e, qs] for h in range(heads)], axis=1)
                dot = jnp.concatenate([dot_ref[h * e:(h + 1) * e, qs] for h in range(heads)], axis=1)
                q = qt.T
                do = dot.T
                m = None
                for ks in chunks:
                    s = _nn(q, qkvt_ref[keys_k, ks])
                    if ks.start >= base:
                        s = jnp.where(col + (ks.start - base) <= row + j * bs, s, -jnp.inf)
                    put(0, ks, s)
                    for piece in lanes(s):
                        m = piece if m is None else jnp.maximum(m, piece)
                m = jnp.max(m, axis=1, keepdims=True)
                total = None
                for ks in chunks:
                    p = jnp.exp2((got(0, ks) - m) * (scale * LOG2E))
                    put(0, ks, p)
                    for piece in lanes(p):
                        total = piece if total is None else total + piece
                    put(1, ks, _nn(do, qkvt_ref[keys_v, ks]))
                inv = 1.0 / jnp.sum(total, axis=1, keepdims=True)
                out = None
                for ks in chunks:
                    p = got(0, ks) * inv
                    put(0, ks, p)
                    pb = p.astype(BF16)
                    piece = _nn(pb, vn_ref[ks, :])
                    out = piece if out is None else out + piece
                    dv_ref[:, ks] += _nn(dot, pb)
                out = out.astype(BF16)
                delta = jnp.sum(do.astype(F32) * out.astype(F32), axis=1, keepdims=True)
                out = out.T
                dq = None
                for ks in chunks:
                    ds = (got(0, ks) * (got(1, ks) - delta)).astype(BF16)
                    piece = _nn(ds, kn_ref[ks, :])
                    dq = piece if dq is None else dq + piece
                    dk_ref[:, ks] += _nn(qt, ds)
                dq = (dq * scale).astype(BF16).T
                for h in range(heads):
                    ot_ref[h * e:(h + 1) * e, qs] = out[:, h * bs:(h + 1) * bs]
                    dqt_ref[h * e:(h + 1) * e, qs] = dq[:, h * bs:(h + 1) * bs]
                for h in range(0, heads, 2):
                    pair = jnp.concatenate([dq[:, h * bs:(h + 1) * bs], dq[:, (h + 1) * bs:(h + 2) * bs]], axis=0)
                    gq[qs, pl.ds(pl.multiple_of(at.r * gw + h * e, 128), 2 * e)] = pair.T
                return 0

            lax.fori_loop(0, tb // bs, queries, 0)

        def turn(t, _):
            @pl.when(t == 0)
            def _():
                begin(gy)

                @pl.when(c == 1)
                def _():
                    far_step(OWN)

            @pl.when(t == 1)
            def _():
                gy.relay_second(MINUS)

                @pl.when(c == 1)
                def _():
                    gy.go(FAR)

                gy.near_second(MINUS)
                gy.relay_second(PLUS)
                gy.near_second(PLUS)

                @pl.when(c == 1)
                def _():
                    far_step(MINUS)

                gy.relay_second(FAR)
                gy.near_second(FAR)

            @pl.when(t == 2)
            def _():
                w_start(0)

                @pl.when(c == 1)
                def _():
                    far_step(PLUS)

                @pl.when(c == 0)
                def _():
                    far_step(OWN)
                    far_step(MINUS)

            @pl.when(t == 3)
            def _():
                @pl.when(c == 0)
                def _():
                    far_step(PLUS)

                far_step(FAR)

            b = row_at(t)
            gy.take_row(t, b, xblk, blk_sem.at[0])

            @pl.when(t == 3)
            def _():
                w_relay(0)

            project(wo_v, dot_ref, b)
            for k in range(ring):
                @pl.when(b == k)
                def _(k=k):
                    attend(k)
            return 0

        far_cp = {d: gy.push(gy.ref(d, FAR, c), gy.ref(d, FAR, c), gy.mate_recv.at[d, FAR], gy.mate) for d in range(4)}

        @_scoped
        def far_step(d):
            for half in (0, 1):
                gy.arrived(d, FAR, half)
            far_cp[d].start()

        lax.fori_loop(0, ring, turn, 0)


    pl.run_scoped(front, pltpu.VMEM((hd + 2 * e, width), BF16), pltpu.VMEM((hd, width), BF16), pltpu.VMEM((tb, width), BF16))

    own_g = at.r * gw
    for k in range(0, tokens, bq):
        ks = slice(k, k + bq)
        kv = jnp.concatenate([(dk_ref[:, ks] * scale).astype(BF16), dv_ref[:, ks].astype(BF16)], axis=0)
        gq[ks, pl.ds(pl.multiple_of(own_g + hd, 128), 2 * e)] = kv.T

    def back(xbuf, obuf, kvt):
        th = tb // 2
        tq = th // 2
        tl = tb // n_row
        half_a, half_b = pl.ds(0, hw), pl.ds(hw, hw)
        units = [(FAR, 0), (MINUS, 0), (FAR, 1), (MINUS, 1), (PLUS, 0), (PLUS, 1), (OWN, 0), (OWN, 1)]
        s_own, s_left, s_right, s_far = (at.slot(at.x + o, c) for o in (0, -1, 1, 2))
        m_own, m_left, m_right, m_far = (at.slot(at.x + o, 1 - c) for o in (0, -1, 1, 2))

        def unit_row(u):
            d, s = units[u]
            return pl.multiple_of(lax.rem(at.y + STEP[d] + ring, ring) * tb + s * th, th)

        def gcols(slot):
            return pl.ds(pl.multiple_of(slot * gw, gw), gw)

        def piece(u, slot, half=None):
            r0 = unit_row(u)
            rows = pl.ds(r0, th) if half is None else pl.ds(pl.multiple_of(r0 + half * tq, tq), tq)
            return gq.at[rows, gcols(slot)]

        sends = []

        def ag_push(u, n, slot, dev, half=None):
            ref = piece(u, slot, half)
            cp = _remote(ref, ref, ag_send.at[u, n], ag_recv.at[u, n], dev)
            cp.start()
            sends.append(cp)

        def ag_wait(u, n, slot, half=None):
            ref = piece(u, slot, half)
            _remote(ref, ref, ag_send.at[u, n], ag_recv.at[u, n], mate).wait_recv()

        def ag_own(u):
            ag_push(u, 0, s_own, right)
            ag_push(u, 1, s_own, left)
            ag_push(u, 2, s_own, mate)

        @_scoped
        def ag_relay(u):
            ag_wait(u, 0, s_left)
            ag_push(u, 3, s_left, right, 0)
            ag_push(u, 4, s_left, mate)
            ag_wait(u, 1, s_right)
            ag_push(u, 5, s_right, left, 1)
            ag_push(u, 6, s_right, mate)

        @_scoped
        def ag_finish(u):
            ag_wait(u, 3, s_far, 0)
            ag_push(u, 7, s_far, mate, 0)
            ag_wait(u, 5, s_far, 1)
            ag_push(u, 8, s_far, mate, 1)
            ag_wait(u, 2, m_own)
            ag_wait(u, 4, m_left)
            ag_wait(u, 6, m_right)
            ag_wait(u, 7, m_far, 0)
            ag_wait(u, 8, m_far, 1)

        nt = min(256, hw)

        @_scoped
        def partial(u, i):
            rows = pl.ds(unit_row(u), th)
            d, s = units[u]
            dst = part.at[d, pl.ds(s * th, th), :]

            def tile(j, _):
                cs = pl.ds(pl.multiple_of(i * hw + j * nt, nt), nt)
                dst[:, cs] = _nn(gq[rows, :], w_all[:, cs])
                return 0

            lax.fori_loop(0, hw // nt, tile, 0)

        def rs_push(n, s, src, dst, dev):
            cp = _remote(src, dst, rs_send.at[n, s], rs_recv.at[n, s], dev)
            cp.start()
            sends.append(cp)

        def rs_wait(n, s):
            ref = rs_half.at[0, s]
            _remote(ref, ref, rs_send.at[n, s], rs_recv.at[n, s], mate).wait_recv()

        def block(d, s, half):
            return part.at[d, pl.ds(s * th, th), half]

        def far_a(s):
            rs_push(0, s, block(FAR, s, half_a), rs_half.at[0, s], up)

        def far_b(s):
            rs_push(1, s, block(FAR, s, half_b), rs_half.at[1, s], down)

        def minus_a(s):
            rs_push(4, s, block(MINUS, s, half_a), rs_full.at[1, s, 0], down)

        def plus_b(s):
            rs_push(3, s, block(PLUS, s, half_b), rs_full.at[0, s, 1], up)

        @_scoped
        def plus_a(s):
            rs_wait(0, s)
            block(PLUS, s, half_a)[...] += rs_half[0, s]
            rs_push(2, s, block(PLUS, s, half_a), rs_full.at[0, s, 0], up)

        @_scoped
        def minus_b(s):
            rs_wait(1, s)
            block(MINUS, s, half_b)[...] += rs_half[1, s]
            rs_push(5, s, block(MINUS, s, half_b), rs_full.at[1, s, 1], down)

        n_steps = width // bc

        @_scoped
        def stream(src, lhs, out, j0, j1):
            def load(j, slot):
                return pltpu.make_async_copy(src.at[:, pl.ds(pl.multiple_of(j * bc, bc), bc)], xbuf.at[slot], in_sem.at[slot])

            def store(j, slot):
                return pltpu.make_async_copy(obuf.at[slot], out.at[:, pl.ds(pl.multiple_of(j * bc, bc), bc)], o_sem.at[slot])

            if j0 == 0:
                load(0, 0).start()

            def step(j, _):
                slot = lax.rem(j, 2)

                @pl.when(j + 1 < n_steps)
                def _():
                    load(j + 1, 1 - slot).start()

                load(j, slot).wait()

                @pl.when(j >= 2)
                def _():
                    store(j - 2, slot).wait()

                obuf[slot] = _nn(lhs[...], xbuf[slot])
                store(j, slot).start()
                return 0

            lax.fori_loop(j0, j1, step, 0)
            if j1 == n_steps:
                for j in range(max(n_steps - 2, 0), n_steps):
                    store(j, j % 2).wait()

        def wo_steps(a, b):
            stream(dyf_ref, ot_ref, dwo_ref, n_steps * a // 16, n_steps * b // 16)

        def wq_steps(a, b):
            stream(xf_ref, dqt_ref, dwq_ref, n_steps * a // 16, n_steps * b // 16)

        first = (at.r // per_kv) * per_kv
        share = width // per_kv
        col0 = lax.rem(at.r, per_kv) * share

        def kv_load(j, slot):
            cs = pl.ds(pl.multiple_of(col0 + j * bc, bc), bc)
            return pltpu.make_async_copy(xf_ref.at[:, cs], xbuf.at[slot], in_sem.at[slot])

        def kv_step(j, _):
            slot = lax.rem(j, 2)

            @pl.when(j + 1 < share // bc)
            def _():
                kv_load(j + 1, 1 - slot).start()

            kv_load(j, slot).wait()
            prod = _nn(kvt[...], xbuf[slot])
            dk = dv = None
            for q in range(per_kv):
                a = prod[q * 2 * e:q * 2 * e + e]
                b = prod[q * 2 * e + e:(q + 1) * 2 * e]
                dk = a if dk is None else dk + a
                dv = b if dv is None else dv + b
            cs = pl.ds(pl.multiple_of(j * bc, bc), bc)
            dwk_ref[:, cs] = dk
            dwv_ref[:, cs] = dv
            return 0

        @_scoped
        def kv_grads():
            kv_load(0, 0).start()
            for q in range(per_kv):
                cols = pl.ds(pl.multiple_of((first + q) * gw + hd, 128), gw - hd)
                for t in range(0, tokens, bq):
                    kvt[q * (gw - hd):(q + 1) * (gw - hd), t:t + bq] = gq[t:t + bq, cols].T
            lax.fori_loop(0, share // bc, kv_step, 0)

        def hand(i, d, half):
            peer = lax.rem(at.r + d, n_row)
            rows = pl.ds(pl.multiple_of(peer * tl, tl), tl)
            cols = pl.ds(pl.multiple_of(at.r * cw + i * hw, hw), hw)
            return stage.at[rows, half], dx_ref.at[:, cols], at.row_dev(peer)

        @_scoped
        def finish(i, half):
            for s in (0, 1):
                rs_wait(2 + i, s)
                rs_wait(4 + i, s)
                stage[s * th:(s + 1) * th, half] = (block(OWN, s, half)[...] + rs_full[0, s, i] + rs_full[1, s, i]).astype(BF16)
            for d in range(1, n_row):
                src, dst, dev = hand(i, d, half)
                cp = _remote(src, dst, out_send.at[i, d], out_recv.at[i, d], dev)
                cp.start()
                sends.append(cp)
            src, dst, _ = hand(i, 0, half)
            pltpu.make_async_copy(src, dst, out_send.at[i, 0]).start()

        @_scoped
        def received(i, half):
            for d in range(1, n_row):
                src = lax.rem(at.r + n_row - d, n_row)
                ref = dx_ref.at[:, pl.ds(pl.multiple_of(src * cw + i * hw, hw), hw)]
                _remote(ref, ref, out_send.at[i, d], out_recv.at[i, d], mate).wait_recv()
            src, dst, _ = hand(i, 0, half)
            pltpu.make_async_copy(src, dst, out_send.at[i, 0]).wait()

        ag_own(0)
        ag_own(1)
        wo_steps(0, 3)
        ag_relay(0)
        ag_own(2)
        ag_finish(0)
        for cp in keep:
            cp.wait()
        w_finish(0)
        partial(0, 0)
        ag_relay(1)
        far_a(0)
        ag_own(3)
        w_start(1)
        ag_finish(1)
        partial(1, 0)
        ag_relay(2)
        minus_a(0)
        ag_own(4)
        wo_steps(3, 5)
        ag_finish(2)
        partial(2, 0)
        ag_relay(3)
        far_a(1)
        w_relay(1)
        ag_own(5)
        wo_steps(5, 7)
        ag_finish(3)
        partial(3, 0)
        ag_relay(4)
        minus_a(1)
        ag_own(6)
        wo_steps(7, 9)
        ag_finish(4)
        partial(4, 0)
        ag_relay(5)
        plus_a(0)
        ag_own(7)
        w_finish(1)
        partial(0, 1)
        far_b(0)
        partial(2, 1)
        far_b(1)
        ag_finish(5)
        partial(5, 0)
        ag_relay(6)
        plus_a(1)
        partial(4, 1)
        plus_b(0)
        partial(5, 1)
        plus_b(1)
        ag_relay(7)
        partial(1, 1)
        minus_b(0)
        partial(3, 1)
        minus_b(1)
        ag_finish(6)
        ag_finish(7)
        wo_steps(9, 16)
        partial(6, 0)
        partial(7, 0)
        wq_steps(0, 2)
        finish(0, half_a)
        partial(6, 1)
        partial(7, 1)
        wq_steps(2, 16)
        kv_grads()
        received(0, half_a)
        finish(1, half_b)
        received(1, half_b)
        for cp in sends:
            cp.wait_send()
        w_drain(0)
        w_drain(1)
        gx.drain()
        gy.drain()

    pl.run_scoped(back, pltpu.VMEM((2, tokens, bc), BF16), pltpu.VMEM((2, hd, bc), F32), pltpu.VMEM((per_kv * 2 * e, tokens), BF16))


def _layer(ring, cores, heads, scale, x, dy, wq, wk, wv, wo):
    rows, width = x.shape
    tokens = rows * ring * ring * cores
    hd = wo.shape[0]
    e = hd // heads
    n_row = ring * cores
    cw = width // n_row
    gw = hd + 2 * e
    tb = tokens // ring
    th, hw = tb // 2, cw // 2
    per_kv = n_row * ring // wk.shape[0]
    bq = min(256, tb)
    bs = tb // heads
    bc = min(512, cw // 2)
    dma = pltpu.SemaphoreType.DMA
    shape = jax.ShapeDtypeStruct
    return pl.pallas_call(
        functools.partial(_kernel, ring, cores, heads, scale, bq, bs, bc),
        name="layer",
        in_specs=[ANY] * 6,
        out_specs=[ANY, ANY, ANY, VMEM, VMEM, ANY, ANY],
        out_shape=[
            shape((rows, width), BF16),
            shape((hd, width), F32),
            shape((hd, width), F32),
            shape((e, width // per_kv), F32),
            shape((e, width // per_kv), F32),
            shape((tokens, width), BF16),
            shape((tokens, width), BF16),
        ],
        scratch_shapes=[
            pltpu.VMEM((tokens, n_row * gw), BF16),
            pltpu.VMEM((n_row * gw, cw), BF16),
            pltpu.VMEM((4, tb, cw), F32),
            pltpu.VMEM((2, 2, th, hw), F32),
            pltpu.VMEM((2, 2, 2, th, hw), F32),
            pltpu.VMEM((tb, cw), BF16),
            pltpu.VMEM((4, hd // 2, cw), BF16),
            pltpu.VMEM((gw, tokens), BF16),
            pltpu.VMEM((hd, tokens), BF16),
            pltpu.VMEM((hd, tokens), BF16),
            pltpu.VMEM((hd, tokens), BF16),
            pltpu.VMEM((e, tokens), F32),
            pltpu.VMEM((e, tokens), F32),
            pltpu.VMEM((tokens, e), BF16),
            pltpu.VMEM((tokens, e), BF16),
            dma((2, 48)),
            dma((2, 4, 4, 2)),
            dma((2, 4, 4)),
            dma((2, 13)),
            dma((2, 9)),
            dma((2, 4)),
            dma((9 + 2 * n_row,)),
            dma((1,)),
            dma((8, 9)),
            dma((8, 9)),
            dma((6, 2)),
            dma((6, 2)),
            dma((2, n_row)),
            dma((2, n_row)),
            dma((2,)),
            dma((2,)),
        ],
        compiler_params=pltpu.CompilerParams(collective_id=0, has_side_effects=True, vmem_limit_bytes=67043328),
        cost_estimate=pl.CostEstimate(flops=70 * 10**9, bytes_accessed=300 << 20, transcendentals=heads * tokens * tokens // 2),
    )(x, dy, wq, wk, wv, wo)


def _emit_kernel(n, *refs):
    copies = [pltpu.make_async_copy(refs[i], refs[n + i], refs[2 * n].at[i]) for i in range(n)]
    for cp in copies:
        cp.start()
    for cp in copies:
        cp.wait()


def _emit(*arrays):
    n = len(arrays)
    return pl.pallas_call(
        functools.partial(_emit_kernel, n),
        name="emit",
        in_specs=[ANY] * n,
        out_specs=[ANY] * n,
        out_shape=[jax.ShapeDtypeStruct(a.shape, a.dtype) for a in arrays],
        scratch_shapes=[pltpu.SemaphoreType.DMA((n,))],
        cost_estimate=pl.CostEstimate(flops=10**6, bytes_accessed=2 * sum(a.size * a.dtype.itemsize for a in arrays), transcendentals=0),
    )(*arrays)


def solution(mesh):
    n = mesh.shape["tp"]
    ring = math.isqrt(n // 2)
    cores = n // (ring * ring)
    if ring != 4 or cores != 2:
        raise ValueError("needs a 4x4 torus")

    def local_grads(x_blk, dy_blk, wq_loc, w_k, w_v, wo_loc):
        model_dim, kv_heads, e = w_k.shape
        heads = wq_loc.shape[1]
        hd = heads * e
        scale = e ** -0.5
        wq = jnp.transpose(wq_loc, (1, 2, 0)).reshape(hd, model_dim)
        wk = jnp.transpose(w_k, (1, 2, 0))
        wv = jnp.transpose(w_v, (1, 2, 0))
        wo = wo_loc.reshape(hd, model_dim)
        dx, dwq, dwo, dwk, dwv, _, _ = _layer(ring, cores, heads, scale, x_blk, dy_blk, wq, wk, wv, wo)
        dx, dwq, dwo, dwk, dwv = _emit(dx, dwq, dwo, dwk, dwv)
        return (dx, jnp.transpose(dwq.reshape(heads, e, model_dim), (2, 0, 1)), dwo.reshape(heads, e, model_dim), dwk.T, dwv.T)

    tok = P(("dp", "tp"))
    return jax.shard_map(
        local_grads,
        mesh=mesh,
        in_specs=(tok, tok, P(None, "tp", None), P(), P(), P("tp")),
        out_specs=(tok, P("dp", "tp", None), tok, tok, tok),
        check_vma=False,
    )
```

```python
import functools
import math

import jax
import jax.numpy as jnp
from jax import lax
from jax.experimental import pallas as pl
from jax.experimental.pallas import tpu as pltpu
from jax.sharding import PartitionSpec as P

F32 = jnp.float32
BF16 = jnp.bfloat16
MESH = pl.DeviceIdType.MESH
ANY = pl.BlockSpec(memory_space=pl.ANY)
VMEM = pl.BlockSpec(memory_space=pltpu.VMEM)
LOG2E = math.log2(math.e)


def _scoped(fn):
    def run(*args, **kw):
        with jax.named_scope(fn.__name__):
            return fn(*args, **kw)

    return run


def _dot(a, b, dims):
    return lax.dot_general(a, b, (dims, ((), ())), preferred_element_type=F32)


def _nn(a, b):
    return _dot(a, b, ((1,), (0,)))


def _nt(a, b):
    return _dot(a, b, ((1,), (1,)))


class Place:
    def __init__(self, ring, cores):
        me = lax.axis_index("tp")
        self.ring, self.cores = ring, cores
        self.c = lax.rem(me, cores)
        self.x = lax.rem(me // cores, ring)
        self.y = me // (cores * ring)
        self.r = self.x * cores + self.c
        self.n_row = ring * cores

    def dev(self, y, x, c):
        y = lax.rem(y + self.ring, self.ring)
        x = lax.rem(x + self.ring, self.ring)
        return {"tp": (y * self.ring + x) * self.cores + c}

    def row_dev(self, r):
        return {"tp": self.y * self.n_row + r}

    def slot(self, x, c):
        return lax.rem(x + self.ring, self.ring) * self.cores + c


def _remote(src, dst, send, recv, dev):
    return pltpu.make_async_remote_copy(
        src_ref=src, dst_ref=dst, send_sem=send, recv_sem=recv, device_id=dev, device_id_type=MESH
    )


@_scoped
def _enter(devices):
    barrier = pltpu.get_barrier_semaphore()
    for dev in devices:
        pl.semaphore_signal(barrier, inc=1, device_id=dev, device_id_type=MESH)
    pl.semaphore_wait(barrier, len(devices))


OWN, MINUS, PLUS, FAR = range(4)
STEP = (0, -1, 1, 2)


class Gather:
    def __init__(self, at, src, full, send, recv, mate_recv):
        self.at, self.src, self.full = at, src, full
        self.send, self.recv, self.mate_recv = send, recv, mate_recv
        self.rows = src.shape[0]
        self.sent = []
        c = at.c
        self.first = {s: at.dev(at.y + c * s, at.x + (1 - c) * s, c) for s in (1, -1)}
        self.second = {s: at.dev(at.y + (1 - c) * s, at.x + c * s, c) for s in (1, -1)}
        self.mate = at.dev(at.y, at.x, 1 - c)
        self.fulls = {d: self.both_ways(self.second, d, lambda to, d=d: (d, to)) for d in range(4)}

    def place(self, d1, d2, core):
        at = self.at
        o1, o2 = STEP[d1], STEP[d2]
        return at.y + core * o1 + (1 - core) * o2, at.x + (1 - core) * o1 + core * o2

    def ref(self, d1, d2, core, half=None):
        y, x = self.place(d1, d2, core)
        n = self.rows if half is None else self.rows // 2
        r0 = self.at.dev(y, x, core)["tp"] * self.rows + (0 if half is None else half * n)
        return self.full.at[pl.ds(pl.multiple_of(r0, n), n), :]

    def push(self, src, dst, recv, dev):
        k = len(self.sent)
        self.sent.append(dst.shape[0])
        return _remote(src, dst, self.send.at[k], recv, dev)

    def out(self, d1, d2, half=None):
        if d1 == OWN and d2 == OWN:
            n = self.rows if half is None else self.rows // 2
            return self.src.at[pl.ds(0 if half is None else half * n, n), :]
        return self.ref(d1, d2, self.at.c, half)

    def both_ways(self, devs, d1, name):
        copies = []
        for step in (0, 1):
            for s, to in ((1, MINUS), (-1, PLUS)):
                half = step if s == 1 else 1 - step
                copies.append(self.push(self.out(d1, OWN, half), self.ref(d1, OWN, self.at.c, half), self.recv.at[*name(to), half], devs[s]))
        return copies

    def to_mate(self, d1, d2):
        ref = self.ref(d1, d2, self.at.c)
        self.push(self.out(d1, d2), ref, self.mate_recv.at[d1, d2], self.mate).start()

    def arrived(self, d1, d2, half):
        ref = self.ref(d1, d2, self.at.c, half)
        _remote(ref, ref, self.send.at[0], self.recv.at[d1, d2, half], self.mate).wait_recv()

    @_scoped
    def start(self):
        for cp in self.both_ways(self.first, OWN, lambda to: (to, OWN)):
            cp.start()
        self.go(OWN)
        self.to_mate(OWN, OWN)

    def go(self, d1):
        for cp in self.fulls[d1]:
            cp.start()

    @_scoped
    def relay_first(self):
        for d, s, half in ((MINUS, 1, 0), (PLUS, -1, 1)):
            self.arrived(d, OWN, half)
            ref = self.ref(d, OWN, self.at.c, half)
            self.push(ref, ref, self.recv.at[FAR, OWN, half], self.first[s]).start()

    @_scoped
    def near_first(self):
        for d, half in ((MINUS, 1), (PLUS, 0)):
            self.arrived(d, OWN, half)
            self.to_mate(d, OWN)

    @_scoped
    def far_first(self):
        for half in (0, 1):
            self.arrived(FAR, OWN, half)
        self.to_mate(FAR, OWN)

    @_scoped
    def relay_second(self, d1):
        for d, s, half in ((MINUS, 1, 0), (PLUS, -1, 1)):
            self.arrived(d1, d, half)
            ref = self.ref(d1, d, self.at.c, half)
            self.push(ref, ref, self.recv.at[d1, FAR, half], self.second[s]).start()

    @_scoped
    def near_second(self, d1):
        for d, half in ((MINUS, 1), (PLUS, 0)):
            self.arrived(d1, d, half)
            self.to_mate(d1, d)

    @_scoped
    def far_second(self, d1):
        for half in (0, 1):
            self.arrived(d1, FAR, half)
        self.to_mate(d1, FAR)

    def load(self, y, x, core, block, sem):
        at = self.at
        r0 = at.dev(y, x, core)["tp"] * self.rows
        b0 = at.slot(x, core) * self.rows
        src = self.full.at[pl.ds(pl.multiple_of(r0, self.rows), self.rows), :]
        return pltpu.make_async_copy(src, block.at[pl.ds(pl.multiple_of(b0, self.rows), self.rows), :], sem)

    @_scoped
    def take_row(self, t, y, block, sem):
        at = self.at
        for j in range(4):
            self.load(y, at.x + STEP[j], at.c, block, sem).start()
        for j in range(4):
            i1 = (1 - at.c) * t + at.c * j
            i2 = at.c * t + (1 - at.c) * j
            ref = self.full.at[pl.ds(0, self.rows), :]
            _remote(ref, ref, self.send.at[0], self.mate_recv.at[i1, i2], self.mate).wait_recv()
            self.load(y, at.x + STEP[j], 1 - at.c, block, sem).start()

    @_scoped
    def drain(self):
        for k, n in enumerate(self.sent):
            ref = self.full.at[pl.ds(0, n), :]
            _remote(ref, ref, self.send.at[k], self.send.at[k], self.mate).wait_send()


def _kernel(ring, cores, heads, scale, bq, bs, bc, x_ref, dy_ref, w_ref, wk_ref, wv_ref, wo_ref,
            dx_ref, dwq_ref, dwo_ref, dwk_ref, dwv_ref, xf_ref, dyf_ref,
            gq, w_all, part, rs_half, rs_full, stage, hop_ref, qkvt_ref, dot_ref, dqt_ref, ot_ref, dk_ref, dv_ref, kn_ref, vn_ref,
            send, recv, mate_recv, w_send, w_recv, hop_recv, ld_sem, blk_sem,
            ag_send, ag_recv, rs_send, rs_recv, out_send, out_recv, in_sem, o_sem):
    at = Place(ring, cores)
    n_row = at.n_row
    hd = wo_ref.shape[0]
    e = hd // heads
    tokens, width = xf_ref.shape
    tb = tokens // ring
    cw = width // n_row
    gw = gq.shape[1] // n_row
    c = at.c
    gx = Gather(at, x_ref, xf_ref, send.at[0], recv.at[0], mate_recv.at[0])
    gy = Gather(at, dy_ref, dyf_ref, send.at[1], recv.at[1], mate_recv.at[1])
    n_kv = wk_ref.shape[0] // ring
    per_kv = n_row // n_kv
    row_peers = [lax.rem(at.r + d, n_row) for d in range(1, n_row)]
    up, down = at.dev(at.y + 1, at.x, c), at.dev(at.y - 1, at.x, c)

    hh = hd // 2

    def w_push(k, src, dst, rsem, dev):
        _remote(src, dst, w_send.at[k], rsem, dev).start()

    def wq_slot(slot, half=None):
        r0 = slot * gw + (0 if half is None else half * hh)
        return w_all.at[pl.ds(r0 if isinstance(r0, int) else pl.multiple_of(r0, hh), hd if half is None else hh), :]

    def wcols(slot):
        return pl.ds(pl.multiple_of(slot * cw, cw), cw)

    right, left, mate = at.dev(at.y, at.x + 1, c), at.dev(at.y, at.x - 1, c), at.dev(at.y, at.x, 1 - c)

    @_scoped
    def w_start():
        for half, dev in ((0, right), (1, left)):
            for k in range(cores):
                w_push(half * 2 + k, w_ref.at[pl.ds(half * hh, hh), wcols(at.slot(at.x + 2, k))], hop_ref.at[half * 2 + k], hop_recv.at[half * 2 + k], dev)
        w_push(4, w_ref.at[pl.ds(0, hd), wcols(at.slot(at.x, 1 - c))], wq_slot(at.r), w_recv.at[0], mate)
        for i, s in enumerate((1, -1)):
            for k in range(cores):
                dst_core = c if k == 0 else 1 - c
                w_push(5 + 2 * i + k, w_ref.at[pl.ds(0, hd), wcols(at.slot(at.x + s, dst_core))], wq_slot(at.r), w_recv.at[1 + 2 * i + k], at.dev(at.y, at.x + s, dst_core))

    @_scoped
    def w_relay():
        for half, s in ((0, 1), (1, -1)):
            for n in (half * 2, half * 2 + 1):
                _remote(hop_ref.at[n], hop_ref.at[n], w_send.at[0], hop_recv.at[n], mate).wait_recv()
            for k in range(cores):
                n = half * 2 + k
                src_slot = at.slot(at.x - s, c)
                same = k == 0
                dst_core = c if same else 1 - c
                w_push(9 + n, hop_ref.at[half * 2 + dst_core], wq_slot(src_slot, half), w_recv.at[5 + n], at.dev(at.y, at.x + s, dst_core))

    @_scoped
    def w_finish():
        whole = wq_slot(0)
        piece = wq_slot(0, 0)
        for n in range(9):
            ref = whole if n < 5 else piece
            _remote(ref, ref, w_send.at[0], w_recv.at[n], mate).wait_recv()

    def w_drain():
        whole = wq_slot(0)
        piece = wq_slot(0, 0)
        for k in range(13):
            ref = whole if 4 <= k < 9 else piece
            _remote(ref, ref, w_send.at[k], w_send.at[k], mate).wait_send()

    own_cols = wcols(at.r)
    rows = x_ref.shape[0]
    own_rows = pl.ds(pl.multiple_of((at.y * n_row + at.r) * rows, rows), rows)

    keep = [pltpu.make_async_copy(w_ref.at[:, own_cols], wq_slot(at.r), ld_sem.at[8])]
    for r in range(n_row):
        kv_r = at.y * n_kv + r // per_kv
        for i, w in enumerate((wk_ref, wv_ref)):
            keep.append(pltpu.make_async_copy(w.at[kv_r, :, own_cols], w_all.at[pl.ds(r * gw + hd + i * e, e), :], ld_sem.at[9 + 2 * r + i]))

    def front(w_v, wo_v, xblk):
        kv = (at.y * n_row + at.r) // (n_row * ring // wk_ref.shape[0])
        loads = [
            pltpu.make_async_copy(w_ref, w_v.at[pl.ds(0, hd), :], ld_sem.at[0]),
            pltpu.make_async_copy(wo_ref, wo_v, ld_sem.at[1]),
            pltpu.make_async_copy(wk_ref.at[kv], w_v.at[pl.ds(hd, e), :], ld_sem.at[6]),
            pltpu.make_async_copy(wv_ref.at[kv], w_v.at[pl.ds(hd + e, e), :], ld_sem.at[7]),
        ]
        ins = [pltpu.make_async_copy(src, xblk.at[pl.ds(i * rows, rows), :], ld_sem.at[2 + i]) for i, src in enumerate((x_ref, dy_ref))]
        outs = [pltpu.make_async_copy(xblk.at[pl.ds(i * rows, rows), :], dst.at[own_rows, :], ld_sem.at[4 + i]) for i, dst in enumerate((xf_ref, dyf_ref))]
        for cp in ins:
            cp.start()
        _enter([up, down] + [at.row_dev(r) for r in row_peers])
        gx.start()
        for cp in loads + keep:
            cp.start()
        for cp in ins:
            cp.wait()
        for cp in outs:
            cp.start()

        dk_ref[...] = jnp.zeros_like(dk_ref)
        dv_ref[...] = jnp.zeros_like(dv_ref)

        @_scoped
        def project(w, out, b):
            pltpu.make_async_copy(xf_ref.at[pl.ds(0, tb), :], xblk, blk_sem.at[0]).wait()

            def block(i, _):
                r0 = pl.multiple_of(i * bq, bq)
                out[:, pl.ds(pl.multiple_of(b * tb + i * bq, bq), bq)] = _nt(w[...], xblk[pl.ds(r0, bq), :]).astype(BF16)
                return 0

            lax.fori_loop(0, tb // bq, block, 0)

        def row_at(t):
            off = jnp.where(t == 1, ring - 1, jnp.where(t == 2, 1, jnp.where(t == 3, 2, 0)))
            return lax.rem(at.y + off, ring)

        for cp in loads + outs:
            cp.wait()

        def begin(g):
            g.relay_first()
            g.near_first()
            g.go(MINUS)

            @pl.when(c == 0)
            def _():
                g.go(PLUS)

        def begin_far(g):
            g.far_first()

            @pl.when(c == 0)
            def _():
                g.go(FAR)

        def begin_second(g):
            g.relay_second(OWN)

            @pl.when(c == 1)
            def _():
                g.go(PLUS)

            g.near_second(OWN)

        def x_turn(t, _):
            @pl.when(t == 0)
            def _():
                begin(gx)
                begin_far(gx)
                begin_second(gx)
                gx.relay_second(MINUS)

                @pl.when(c == 1)
                def _():
                    gx.go(FAR)

                gx.near_second(MINUS)
                gx.relay_second(PLUS)
                gx.near_second(PLUS)
                gx.relay_second(FAR)
                gy.start()
                gx.far_second(OWN)

            @pl.when(t == 1)
            def _():
                gx.near_second(FAR)
                gx.far_second(MINUS)

            @pl.when(t == 2)
            def _():
                gx.far_second(PLUS)
                gx.far_second(FAR)

            @pl.when(t == 3)
            def _():
                begin(gy)

            b = row_at(t)
            gx.take_row(t, b, xblk, blk_sem.at[0])
            project(w_v, qkvt_ref, b)
            return 0

        lax.fori_loop(0, ring, x_turn, 0)
        for t in range(0, tokens, bq):
            kn_ref[t:t + bq, :] = qkvt_ref[hd:hd + e, t:t + bq].T
            vn_ref[t:t + bq, :] = qkvt_ref[hd + e:hd + 2 * e, t:t + bq].T

        keys_k, keys_v = slice(hd, hd + e), slice(hd + e, hd + 2 * e)
        m4 = heads * bs
        factor = scale * LOG2E

        def row_chunks(k):
            return [slice(t, t + bq) for t in range(0, (k + 1) * tb, bq)]

        def stacked(ref, qs):
            return jnp.concatenate([ref[h * e:(h + 1) * e, qs] for h in range(heads)], axis=1)

        def unstack(ref, qs, value):
            for h in range(heads):
                ref[h * e:(h + 1) * e, qs] = value[:, h * bs:(h + 1) * bs]

        def scores(q, ks, k, j):
            s = _nn(q, qkvt_ref[keys_k, ks])
            if ks.start < k * tb:
                return s
            row = lax.broadcasted_iota(jnp.int32, (m4, bq), 0) & (bs - 1)
            col = lax.broadcasted_iota(jnp.int32, (m4, bq), 1)
            return jnp.where(col + (ks.start - k * tb) <= row + j * bs, s, -jnp.inf)

        def folded(op, total, value):
            for t in range(0, value.shape[1], 128):
                piece = value[:, t:t + 128]
                total = piece if total is None else op(total, piece)
            return total

        def score_buf(ks):
            n = ks.start // cw
            return part.at[n, :, ks.start - n * cw:ks.stop - n * cw]

        def stats_buf(k, j):
            per = cw // 128
            n = k * (tb // bs)
            return part.at[2 + n // per, :, pl.ds(pl.multiple_of((n % per + j) * 128, 128), 128)]

        @_scoped
        def forward(k):
            chunks = row_chunks(k)

            def queries(j, _):
                qs = pl.ds(pl.multiple_of(k * tb + j * bs, bs), bs)
                q = stacked(qkvt_ref, qs).T
                m = None
                for ks in chunks:
                    s = scores(q, ks, k, j)
                    score_buf(ks)[...] = s
                    m = folded(jnp.maximum, m, s)
                m = jnp.max(m, axis=1, keepdims=True)
                total = None
                for ks in chunks:
                    p = jnp.exp2((score_buf(ks)[...] - m) * factor)
                    score_buf(ks)[...] = p
                    total = folded(jnp.add, total, p)
                inv = 1.0 / jnp.sum(total, axis=1, keepdims=True)
                lane = lax.broadcasted_iota(jnp.int32, (m4, 128), 1)
                stats_buf(k, j)[...] = jnp.where(lane == 0, m, inv)
                out = None
                for ks in chunks:
                    piece = _nn((score_buf(ks)[...] * inv).astype(BF16), vn_ref[ks, :])
                    out = piece if out is None else out + piece
                unstack(ot_ref, qs, out.astype(BF16).T)
                return 0

            lax.fori_loop(0, tb // bs, queries, 0)

        @_scoped
        def backward(k):
            chunks = row_chunks(k)

            def queries(j, _):
                qs = pl.ds(pl.multiple_of(k * tb + j * bs, bs), bs)
                qt = stacked(qkvt_ref, qs)
                dot = stacked(dot_ref, qs)
                q, do = qt.T, dot.T
                delta = jnp.sum(dot.astype(F32) * stacked(ot_ref, qs).astype(F32), axis=0, keepdims=True)
                delta = jnp.broadcast_to(delta, (128, m4)).T[:, :1]
                stats = stats_buf(k, j)[...]
                m, inv = stats[:, 0:1], stats[:, 1:2]
                dq = None
                for ks in chunks:
                    p = jnp.exp2((scores(q, ks, k, j) - m) * factor) * inv
                    dp = _nn(do, qkvt_ref[keys_v, ks])
                    ds = (p * (dp - delta)).astype(BF16)
                    dv_ref[:, ks] += _nn(dot, p.astype(BF16))
                    dk_ref[:, ks] += _nn(qt, ds)
                    piece = _nn(ds, kn_ref[ks, :])
                    dq = piece if dq is None else dq + piece
                dq = (dq * scale).astype(BF16).T
                unstack(dqt_ref, qs, dq)
                for h in range(0, heads, 2):
                    pair = jnp.concatenate([dq[:, h * bs:(h + 1) * bs], dq[:, (h + 1) * bs:(h + 2) * bs]], axis=0)
                    gq[qs, pl.ds(pl.multiple_of(at.r * gw + h * e, 128), 2 * e)] = pair.T
                return 0

            lax.fori_loop(0, tb // bs, queries, 0)

        begin_far(gy)
        for k in range(ring):
            forward(k)
            if k == 0:
                begin_second(gy)

        def turn(t, _):
            @pl.when(t == 0)
            def _():
                gy.relay_second(MINUS)

                @pl.when(c == 1)
                def _():
                    gy.go(FAR)
                    far_step(OWN)

            @pl.when(t == 1)
            def _():
                gy.near_second(MINUS)
                gy.relay_second(PLUS)
                gy.near_second(PLUS)

                @pl.when(c == 1)
                def _():
                    far_step(MINUS)

                gy.relay_second(FAR)
                gy.near_second(FAR)
                w_start()

            @pl.when(t == 2)
            def _():
                @pl.when(c == 1)
                def _():
                    far_step(PLUS)

                @pl.when(c == 0)
                def _():
                    far_step(OWN)
                    far_step(MINUS)

            @pl.when(t == 3)
            def _():
                @pl.when(c == 0)
                def _():
                    far_step(PLUS)

                far_step(FAR)

            b = row_at(t)
            gy.take_row(t, b, xblk, blk_sem.at[0])
            project(wo_v, dot_ref, b)

            @pl.when(t == 3)
            def _():
                w_relay()

            for k in range(ring):
                @pl.when(b == k)
                def _(k=k):
                    backward(k)
            return 0

        far_cp = {d: gy.push(gy.ref(d, FAR, c), gy.ref(d, FAR, c), gy.mate_recv.at[d, FAR], gy.mate) for d in range(4)}

        @_scoped
        def far_step(d):
            for half in (0, 1):
                gy.arrived(d, FAR, half)
            far_cp[d].start()

        lax.fori_loop(0, ring, turn, 0)


    pl.run_scoped(front, pltpu.VMEM((hd + 2 * e, width), BF16), pltpu.VMEM((hd, width), BF16), pltpu.VMEM((tb, width), BF16))

    own_g = at.r * gw
    for k in range(0, tokens, bq):
        ks = slice(k, k + bq)
        kv = jnp.concatenate([(dk_ref[:, ks] * scale).astype(BF16), dv_ref[:, ks].astype(BF16)], axis=0)
        gq[ks, pl.ds(pl.multiple_of(own_g + hd, 128), 2 * e)] = kv.T

    def back(xbuf, obuf, kvt):
        th = tb // 2
        tq = th // 2
        tl = tb // n_row
        hw = cw // 2
        half_a, half_b = pl.ds(0, hw), pl.ds(hw, hw)
        units = [(FAR, 0), (FAR, 1), (PLUS, 0), (MINUS, 0), (PLUS, 1), (MINUS, 1), (OWN, 0), (OWN, 1)]
        s_own, s_left, s_right, s_far = (at.slot(at.x + o, c) for o in (0, -1, 1, 2))
        m_own, m_left, m_right, m_far = (at.slot(at.x + o, 1 - c) for o in (0, -1, 1, 2))

        def unit_row(u):
            d, s = units[u]
            return pl.multiple_of(lax.rem(at.y + STEP[d] + ring, ring) * tb + s * th, th)

        def gcols(slot):
            return pl.ds(pl.multiple_of(slot * gw, gw), gw)

        def piece(u, slot, half=None):
            r0 = unit_row(u)
            rows = pl.ds(r0, th) if half is None else pl.ds(pl.multiple_of(r0 + half * tq, tq), tq)
            return gq.at[rows, gcols(slot)]

        sends = []

        def ag_push(u, n, slot, dev, half=None):
            ref = piece(u, slot, half)
            cp = _remote(ref, ref, ag_send.at[u, n], ag_recv.at[u, n], dev)
            cp.start()
            sends.append(cp)

        def ag_wait(u, n, slot, half=None):
            ref = piece(u, slot, half)
            _remote(ref, ref, ag_send.at[u, n], ag_recv.at[u, n], mate).wait_recv()

        def ag_own(u):
            ag_push(u, 0, s_own, right)
            ag_push(u, 1, s_own, left)
            ag_push(u, 2, s_own, mate)

        @_scoped
        def ag_relay(u):
            ag_wait(u, 0, s_left)
            ag_push(u, 3, s_left, right, 0)
            ag_push(u, 4, s_left, mate)
            ag_wait(u, 1, s_right)
            ag_push(u, 5, s_right, left, 1)
            ag_push(u, 6, s_right, mate)

        @_scoped
        def ag_finish(u):
            ag_wait(u, 3, s_far, 0)
            ag_push(u, 7, s_far, mate, 0)
            ag_wait(u, 5, s_far, 1)
            ag_push(u, 8, s_far, mate, 1)
            ag_wait(u, 2, m_own)
            ag_wait(u, 4, m_left)
            ag_wait(u, 6, m_right)
            ag_wait(u, 7, m_far, 0)
            ag_wait(u, 8, m_far, 1)

        nt = min(256, hw)

        @_scoped
        def partial(u):
            rows = pl.ds(unit_row(u), th)
            d, s = units[u]
            dst = part.at[d, pl.ds(s * th, th), :]

            def tile(j, _):
                cs = pl.ds(pl.multiple_of(j * nt, nt), nt)
                dst[:, cs] = _nn(gq[rows, :], w_all[:, cs])
                return 0

            lax.fori_loop(0, cw // nt, tile, 0)

        def rs_push(n, s, src, dst, dev):
            cp = _remote(src, dst, rs_send.at[n, s], rs_recv.at[n, s], dev)
            cp.start()
            sends.append(cp)

        def rs_wait(n, s):
            ref = rs_half.at[0, s]
            _remote(ref, ref, rs_send.at[n, s], rs_recv.at[n, s], mate).wait_recv()

        def block(d, s, half):
            return part.at[d, pl.ds(s * th, th), half]

        def far_a(s):
            rs_push(0, s, block(FAR, s, half_a), rs_half.at[0, s], up)

        def far_b(s):
            rs_push(1, s, block(FAR, s, half_b), rs_half.at[1, s], down)

        def minus_a(s):
            rs_push(4, s, block(MINUS, s, half_a), rs_full.at[1, s, 0], down)

        def plus_b(s):
            rs_push(3, s, block(PLUS, s, half_b), rs_full.at[0, s, 1], up)

        @_scoped
        def plus_a(s):
            rs_wait(0, s)
            block(PLUS, s, half_a)[...] += rs_half[0, s]
            rs_push(2, s, block(PLUS, s, half_a), rs_full.at[0, s, 0], up)

        @_scoped
        def minus_b(s):
            rs_wait(1, s)
            block(MINUS, s, half_b)[...] += rs_half[1, s]
            rs_push(5, s, block(MINUS, s, half_b), rs_full.at[1, s, 1], down)

        n_steps = width // bc

        @_scoped
        def stream(src, lhs, out, j0, j1):
            def load(j, slot):
                return pltpu.make_async_copy(src.at[:, pl.ds(pl.multiple_of(j * bc, bc), bc)], xbuf.at[slot], in_sem.at[slot])

            def store(j, slot):
                return pltpu.make_async_copy(obuf.at[slot], out.at[:, pl.ds(pl.multiple_of(j * bc, bc), bc)], o_sem.at[slot])

            if j0 == 0:
                load(0, 0).start()

            def step(j, _):
                slot = lax.rem(j, 2)

                @pl.when(j + 1 < n_steps)
                def _():
                    load(j + 1, 1 - slot).start()

                load(j, slot).wait()

                @pl.when(j >= 2)
                def _():
                    store(j - 2, slot).wait()

                obuf[slot] = _nn(lhs[...], xbuf[slot])
                store(j, slot).start()
                return 0

            lax.fori_loop(j0, j1, step, 0)
            if j1 == n_steps:
                for j in range(max(n_steps - 2, 0), n_steps):
                    store(j, j % 2).wait()

        def wo_steps(a, b):
            stream(dyf_ref, ot_ref, dwo_ref, n_steps * a // 16, n_steps * b // 16)

        def wq_steps(a, b):
            stream(xf_ref, dqt_ref, dwq_ref, n_steps * a // 16, n_steps * b // 16)

        first = (at.r // per_kv) * per_kv
        share = width // per_kv
        col0 = lax.rem(at.r, per_kv) * share

        def kv_load(j, slot):
            cs = pl.ds(pl.multiple_of(col0 + j * bc, bc), bc)
            return pltpu.make_async_copy(xf_ref.at[:, cs], xbuf.at[slot], in_sem.at[slot])

        def kv_step(j, _):
            slot = lax.rem(j, 2)

            @pl.when(j + 1 < share // bc)
            def _():
                kv_load(j + 1, 1 - slot).start()

            kv_load(j, slot).wait()
            prod = _nn(kvt[...], xbuf[slot])
            dk = dv = None
            for q in range(per_kv):
                a = prod[q * 2 * e:q * 2 * e + e]
                b = prod[q * 2 * e + e:(q + 1) * 2 * e]
                dk = a if dk is None else dk + a
                dv = b if dv is None else dv + b
            cs = pl.ds(pl.multiple_of(j * bc, bc), bc)
            dwk_ref[:, cs] = dk
            dwv_ref[:, cs] = dv
            return 0

        @_scoped
        def kv_grads():
            kv_load(0, 0).start()
            for q in range(per_kv):
                cols = pl.ds(pl.multiple_of((first + q) * gw + hd, 128), gw - hd)
                for t in range(0, tokens, bq):
                    kvt[q * (gw - hd):(q + 1) * (gw - hd), t:t + bq] = gq[t:t + bq, cols].T
            lax.fori_loop(0, share // bc, kv_step, 0)

        def hand(i, d, half):
            peer = lax.rem(at.r + d, n_row)
            rows = pl.ds(pl.multiple_of(peer * tl, tl), tl)
            cols = pl.ds(pl.multiple_of(at.r * cw + i * hw, hw), hw)
            return stage.at[rows, half], dx_ref.at[:, cols], at.row_dev(peer)

        @_scoped
        def finish(i, half):
            for s in (0, 1):
                rs_wait(2 + i, s)
                rs_wait(4 + i, s)
                stage[s * th:(s + 1) * th, half] = (block(OWN, s, half)[...] + rs_full[0, s, i] + rs_full[1, s, i]).astype(BF16)
            for d in range(1, n_row):
                src, dst, dev = hand(i, d, half)
                cp = _remote(src, dst, out_send.at[i, d], out_recv.at[i, d], dev)
                cp.start()
                sends.append(cp)
            src, dst, _ = hand(i, 0, half)
            pltpu.make_async_copy(src, dst, out_send.at[i, 0]).start()

        @_scoped
        def received(i, half):
            for d in range(1, n_row):
                src = lax.rem(at.r + n_row - d, n_row)
                ref = dx_ref.at[:, pl.ds(pl.multiple_of(src * cw + i * hw, hw), hw)]
                _remote(ref, ref, out_send.at[i, d], out_recv.at[i, d], mate).wait_recv()
            src, dst, _ = hand(i, 0, half)
            pltpu.make_async_copy(src, dst, out_send.at[i, 0]).wait()

        ag_own(0)
        ag_own(1)
        wo_steps(0, 3)
        ag_relay(0)
        ag_own(2)
        ag_finish(0)
        for cp in keep:
            cp.wait()
        w_finish()
        partial(0)
        ag_relay(1)
        far_a(0)
        far_b(0)
        ag_own(3)
        wo_steps(3, 5)
        ag_finish(1)
        partial(1)
        ag_relay(2)
        far_a(1)
        far_b(1)
        ag_own(4)
        wo_steps(5, 7)
        ag_finish(2)
        partial(2)
        ag_relay(3)
        ag_own(5)
        plus_a(0)
        wo_steps(7, 9)
        ag_finish(3)
        partial(3)
        ag_relay(4)
        minus_a(0)
        ag_own(6)
        wo_steps(9, 11)
        ag_finish(4)
        partial(4)
        ag_relay(5)
        ag_own(7)
        plus_a(1)
        plus_b(0)
        wo_steps(11, 12)
        ag_finish(5)
        partial(5)
        ag_relay(6)
        minus_a(1)
        minus_b(0)
        plus_b(1)
        minus_b(1)
        wo_steps(12, 14)
        ag_finish(6)
        partial(6)
        ag_relay(7)
        wo_steps(14, 16)
        ag_finish(7)
        partial(7)
        wq_steps(0, 3)
        finish(0, half_a)
        wq_steps(3, 16)
        kv_grads()
        received(0, half_a)
        finish(1, half_b)
        received(1, half_b)
        for cp in sends:
            cp.wait_send()
        w_drain()
        gx.drain()
        gy.drain()

    pl.run_scoped(back, pltpu.VMEM((2, tokens, bc), BF16), pltpu.VMEM((2, hd, bc), F32), pltpu.VMEM((per_kv * 2 * e, tokens), BF16))


def _layer(ring, cores, heads, scale, x, dy, wq, wk, wv, wo):
    rows, width = x.shape
    tokens = rows * ring * ring * cores
    hd = wo.shape[0]
    e = hd // heads
    n_row = ring * cores
    cw = width // n_row
    gw = hd + 2 * e
    tb = tokens // ring
    th, hw = tb // 2, cw // 2
    per_kv = n_row * ring // wk.shape[0]
    bq = min(256, tb)
    bs = tb // heads
    bc = min(512, cw // 2)
    dma = pltpu.SemaphoreType.DMA
    shape = jax.ShapeDtypeStruct
    return pl.pallas_call(
        functools.partial(_kernel, ring, cores, heads, scale, bq, bs, bc),
        name="layer",
        in_specs=[ANY] * 6,
        out_specs=[ANY, ANY, ANY, VMEM, VMEM, ANY, ANY],
        out_shape=[
            shape((rows, width), BF16),
            shape((hd, width), F32),
            shape((hd, width), F32),
            shape((e, width // per_kv), F32),
            shape((e, width // per_kv), F32),
            shape((tokens, width), BF16),
            shape((tokens, width), BF16),
        ],
        scratch_shapes=[
            pltpu.VMEM((tokens, n_row * gw), BF16),
            pltpu.VMEM((n_row * gw, cw), BF16),
            pltpu.VMEM((4, tb, cw), F32),
            pltpu.VMEM((2, 2, th, hw), F32),
            pltpu.VMEM((2, 2, 2, th, hw), F32),
            pltpu.VMEM((tb, cw), BF16),
            pltpu.VMEM((4, hd // 2, cw), BF16),
            pltpu.VMEM((gw, tokens), BF16),
            pltpu.VMEM((hd, tokens), BF16),
            pltpu.VMEM((hd, tokens), BF16),
            pltpu.VMEM((hd, tokens), BF16),
            pltpu.VMEM((e, tokens), F32),
            pltpu.VMEM((e, tokens), F32),
            pltpu.VMEM((tokens, e), BF16),
            pltpu.VMEM((tokens, e), BF16),
            dma((2, 48)),
            dma((2, 4, 4, 2)),
            dma((2, 4, 4)),
            dma((13,)),
            dma((9,)),
            dma((4,)),
            dma((9 + 2 * n_row,)),
            dma((1,)),
            dma((8, 9)),
            dma((8, 9)),
            dma((6, 2)),
            dma((6, 2)),
            dma((2, n_row)),
            dma((2, n_row)),
            dma((2,)),
            dma((2,)),
        ],
        compiler_params=pltpu.CompilerParams(collective_id=0, has_side_effects=True, vmem_limit_bytes=67043328),
        cost_estimate=pl.CostEstimate(flops=70 * 10**9, bytes_accessed=300 << 20, transcendentals=heads * tokens * tokens // 2),
    )(x, dy, wq, wk, wv, wo)


def _emit_kernel(src, dst, sem):
    n = sem.shape[0]
    rows = src.shape[0] // n
    copies = [pltpu.make_async_copy(src.at[pl.ds(i * rows, rows), :], dst.at[pl.ds(i * rows, rows), :], sem.at[i]) for i in range(n)]
    for cp in copies:
        cp.start()
    for cp in copies:
        cp.wait()


def _emit(array):
    return pl.pallas_call(
        _emit_kernel,
        name="emit",
        in_specs=[VMEM],
        out_specs=ANY,
        out_shape=jax.ShapeDtypeStruct(array.shape, array.dtype),
        scratch_shapes=[pltpu.SemaphoreType.DMA((4,))],
        compiler_params=pltpu.CompilerParams(vmem_limit_bytes=16 << 20),
        cost_estimate=pl.CostEstimate(flops=10**6, bytes_accessed=2 * array.size * array.dtype.itemsize, transcendentals=0),
    )(array)


def solution(mesh):
    n = mesh.shape["tp"]
    ring = math.isqrt(n // 2)
    cores = n // (ring * ring)
    if ring != 4 or cores != 2:
        raise ValueError("needs a 4x4 torus")

    def local_grads(x_blk, dy_blk, wq_loc, w_k, w_v, wo_loc):
        model_dim, kv_heads, e = w_k.shape
        heads = wq_loc.shape[1]
        hd = heads * e
        scale = e ** -0.5
        wq = jnp.transpose(wq_loc, (1, 2, 0)).reshape(hd, model_dim)
        wk = jnp.transpose(w_k, (1, 2, 0))
        wv = jnp.transpose(w_v, (1, 2, 0))
        wo = wo_loc.reshape(hd, model_dim)
        dx, dwq, dwo, dwk, dwv, _, _ = _layer(ring, cores, heads, scale, x_blk, dy_blk, wq, wk, wv, wo)
        dwq = _emit(dwq)
        return (dx, jnp.transpose(dwq.reshape(heads, e, model_dim), (2, 0, 1)), dwo.reshape(heads, e, model_dim), dwk.T, dwv.T)

    tok = P(("dp", "tp"))
    return jax.shard_map(
        local_grads,
        mesh=mesh,
        in_specs=(tok, tok, P(None, "tp", None), P(), P(), P("tp")),
        out_specs=(tok, P("dp", "tp", None), tok, tok, tok),
        check_vma=False,
    )
```

```python
import functools
import math

import jax
import jax.numpy as jnp
from jax import lax
from jax.experimental import pallas as pl
from jax.experimental.pallas import tpu as pltpu
from jax.sharding import PartitionSpec as P

F32 = jnp.float32
BF16 = jnp.bfloat16
MESH = pl.DeviceIdType.MESH
ANY = pl.BlockSpec(memory_space=pl.ANY)
VMEM = pl.BlockSpec(memory_space=pltpu.VMEM)
LOG2E = math.log2(math.e)


def _scoped(fn):
    def run(*args, **kw):
        with jax.named_scope(fn.__name__):
            return fn(*args, **kw)

    return run


def _dot(a, b, dims):
    return lax.dot_general(a, b, (dims, ((), ())), preferred_element_type=F32)


def _nn(a, b):
    return _dot(a, b, ((1,), (0,)))


def _nt(a, b):
    return _dot(a, b, ((1,), (1,)))


class Place:
    def __init__(self, ring, cores):
        me = lax.axis_index("tp")
        self.ring, self.cores = ring, cores
        self.c = lax.rem(me, cores)
        self.x = lax.rem(me // cores, ring)
        self.y = me // (cores * ring)
        self.r = self.x * cores + self.c
        self.n_row = ring * cores

    def dev(self, y, x, c):
        y = lax.rem(y + self.ring, self.ring)
        x = lax.rem(x + self.ring, self.ring)
        return {"tp": (y * self.ring + x) * self.cores + c}

    def row_dev(self, r):
        return {"tp": self.y * self.n_row + r}

    def slot(self, x, c):
        return lax.rem(x + self.ring, self.ring) * self.cores + c


def _remote(src, dst, send, recv, dev):
    return pltpu.make_async_remote_copy(
        src_ref=src, dst_ref=dst, send_sem=send, recv_sem=recv, device_id=dev, device_id_type=MESH
    )


@_scoped
def _enter(devices):
    barrier = pltpu.get_barrier_semaphore()
    for dev in devices:
        pl.semaphore_signal(barrier, inc=1, device_id=dev, device_id_type=MESH)
    pl.semaphore_wait(barrier, len(devices))


OWN, MINUS, PLUS, FAR = range(4)
STEP = (0, -1, 1, 2)


def _load_shard(at, full, n, y, x, core, block, sem):
    r0 = at.dev(y, x, core)["tp"] * n
    b0 = at.slot(x, core) * n
    src = full.at[pl.ds(pl.multiple_of(r0, n), n), :]
    return pltpu.make_async_copy(src, block.at[pl.ds(pl.multiple_of(b0, n), n), :], sem)


@_scoped
def _take_row(lanes, t, y, block, sem):
    at, full, n = lanes[0].at, lanes[0].full, lanes[0].shard
    for j in range(4):
        _load_shard(at, full, n, y, at.x + STEP[j], at.c, block, sem).start()
    for j in range(4):
        for g in lanes:
            g.await_mate(t, j)
        _load_shard(at, full, n, y, at.x + STEP[j], 1 - at.c, block, sem).start()


class Gather:
    def __init__(self, at, src, full, send, recv, mate_recv, orders, row0, rows, tag):
        self.at, self.src, self.full = at, src, full
        self.send, self.recv, self.mate_recv = send.at[tag], recv.at[tag], mate_recv.at[tag]
        self.order, self.mate_order = orders
        self.row0, self.rows, self.shard = row0, rows, src.shape[0]
        self.sent = []
        c, o = at.c, self.order
        self.first = {s: at.dev(at.y + o * s, at.x + (1 - o) * s, c) for s in (1, -1)}
        self.second = {s: at.dev(at.y + (1 - o) * s, at.x + o * s, c) for s in (1, -1)}
        self.mate = at.dev(at.y, at.x, 1 - c)
        self.fulls = {d: self.both_ways(self.second, d, lambda to, d=d: (d, to)) for d in range(4)}

    def span(self, half):
        n = self.rows if half is None else self.rows // 2
        return self.row0 + (0 if half is None else half * n), n

    def ref(self, d1, d2, half=None):
        at, o = self.at, self.order
        o1, o2 = STEP[d1], STEP[d2]
        start, n = self.span(half)
        r0 = at.dev(at.y + o * o1 + (1 - o) * o2, at.x + (1 - o) * o1 + o * o2, at.c)["tp"] * self.shard + start
        return self.full.at[pl.ds(pl.multiple_of(r0, math.gcd(self.shard, self.row0, n)), n), :]

    def push(self, src, dst, recv, dev):
        k = len(self.sent)
        self.sent.append(dst.shape[0])
        return _remote(src, dst, self.send.at[k], recv, dev)

    def out(self, d1, d2, half=None):
        if d1 == OWN and d2 == OWN:
            return self.src.at[pl.ds(*self.span(half)), :]
        return self.ref(d1, d2, half)

    def both_ways(self, devs, d1, name):
        copies = []
        for step in (0, 1):
            for s, to in ((1, MINUS), (-1, PLUS)):
                half = step if s == 1 else 1 - step
                copies.append(self.push(self.out(d1, OWN, half), self.ref(d1, OWN, half), self.recv.at[*name(to), half], devs[s]))
        return copies

    def to_mate(self, d1, d2):
        ref = self.ref(d1, d2)
        self.push(self.out(d1, d2), ref, self.mate_recv.at[d1, d2], self.mate).start()

    def arrived(self, d1, d2, half):
        ref = self.ref(d1, d2, half)
        _remote(ref, ref, self.send.at[0], self.recv.at[d1, d2, half], self.mate).wait_recv()

    @_scoped
    def start(self):
        for cp in self.both_ways(self.first, OWN, lambda to: (to, OWN)):
            cp.start()
        self.go(OWN)
        self.to_mate(OWN, OWN)

    def go(self, d1):
        for cp in self.fulls[d1]:
            cp.start()

    @_scoped
    def relay_first(self):
        for d, s, half in ((MINUS, 1, 0), (PLUS, -1, 1)):
            self.arrived(d, OWN, half)
            ref = self.ref(d, OWN, half)
            self.push(ref, ref, self.recv.at[FAR, OWN, half], self.first[s]).start()

    @_scoped
    def near_first(self):
        for d, half in ((MINUS, 1), (PLUS, 0)):
            self.arrived(d, OWN, half)
            self.to_mate(d, OWN)

    @_scoped
    def far_first(self):
        for half in (0, 1):
            self.arrived(FAR, OWN, half)
        self.to_mate(FAR, OWN)

    @_scoped
    def relay_second(self, d1):
        for d, s, half in ((MINUS, 1, 0), (PLUS, -1, 1)):
            self.arrived(d1, d, half)
            ref = self.ref(d1, d, half)
            self.push(ref, ref, self.recv.at[d1, FAR, half], self.second[s]).start()

    @_scoped
    def near_second(self, d1):
        for d, half in ((MINUS, 1), (PLUS, 0)):
            self.arrived(d1, d, half)
            self.to_mate(d1, d)

    @_scoped
    def far_second(self, d1):
        for half in (0, 1):
            self.arrived(d1, FAR, half)
        self.to_mate(d1, FAR)

    def await_mate(self, t, j):
        o = self.mate_order
        ref = self.full.at[pl.ds(0, self.rows), :]
        _remote(ref, ref, self.send.at[0], self.mate_recv.at[(1 - o) * j + o * t, (1 - o) * t + o * j], self.mate).wait_recv()

    @_scoped
    def drain(self):
        for k, n in enumerate(self.sent):
            ref = self.full.at[pl.ds(0, n), :]
            _remote(ref, ref, self.send.at[k], self.send.at[k], self.mate).wait_send()


def _kernel(ring, cores, heads, scale, bq, bs, bc, x_ref, dy_ref, w_ref, wk_ref, wv_ref, wo_ref,
            dx_ref, dwq_ref, dwo_ref, dwk_ref, dwv_ref, xf_ref, dyf_ref,
            gq, w_all, part, rs_half, rs_full, stage, hop_ref, qkvt_ref, dot_ref, dqt_ref, ot_ref, dk_ref, dv_ref, kn_ref, vn_ref,
            send, recv, mate_recv, w_send, w_recv, hop_recv, ld_sem, blk_sem,
            ag_send, ag_recv, rs_send, rs_recv, out_send, out_recv, in_sem, o_sem):
    at = Place(ring, cores)
    n_row = at.n_row
    hd = wo_ref.shape[0]
    e = hd // heads
    tokens, width = xf_ref.shape
    tb = tokens // ring
    cw = width // n_row
    gw = gq.shape[1] // n_row
    c = at.c
    shard = x_ref.shape[0]
    split = shard * 3 // 4
    gx = Gather(at, x_ref, xf_ref, send, recv, mate_recv, (c, 1 - c), 0, split, 0)
    gz = Gather(at, x_ref, xf_ref, send, recv, mate_recv, (0, 0), split, shard - split, 1)
    gy = Gather(at, dy_ref, dyf_ref, send, recv, mate_recv, (c, 1 - c), 0, shard, 2)
    n_kv = wk_ref.shape[0] // ring
    per_kv = n_row // n_kv
    row_peers = [lax.rem(at.r + d, n_row) for d in range(1, n_row)]
    up, down = at.dev(at.y + 1, at.x, c), at.dev(at.y - 1, at.x, c)

    hh = hd // 2

    def w_push(k, src, dst, rsem, dev):
        _remote(src, dst, w_send.at[k], rsem, dev).start()

    def wq_slot(slot, half=None):
        r0 = slot * gw + (0 if half is None else half * hh)
        return w_all.at[pl.ds(r0 if isinstance(r0, int) else pl.multiple_of(r0, hh), hd if half is None else hh), :]

    def wcols(slot):
        return pl.ds(pl.multiple_of(slot * cw, cw), cw)

    right, left, mate = at.dev(at.y, at.x + 1, c), at.dev(at.y, at.x - 1, c), at.dev(at.y, at.x, 1 - c)

    @_scoped
    def w_start():
        for half, dev in ((0, right), (1, left)):
            for k in range(cores):
                w_push(half * 2 + k, w_ref.at[pl.ds(half * hh, hh), wcols(at.slot(at.x + 2, k))], hop_ref.at[half * 2 + k], hop_recv.at[half * 2 + k], dev)
        w_push(4, w_ref.at[pl.ds(0, hd), wcols(at.slot(at.x, 1 - c))], wq_slot(at.r), w_recv.at[0], mate)
        for i, s in enumerate((1, -1)):
            for k in range(cores):
                dst_core = c if k == 0 else 1 - c
                w_push(5 + 2 * i + k, w_ref.at[pl.ds(0, hd), wcols(at.slot(at.x + s, dst_core))], wq_slot(at.r), w_recv.at[1 + 2 * i + k], at.dev(at.y, at.x + s, dst_core))

    @_scoped
    def w_relay():
        for half, s in ((0, 1), (1, -1)):
            for n in (half * 2, half * 2 + 1):
                _remote(hop_ref.at[n], hop_ref.at[n], w_send.at[0], hop_recv.at[n], mate).wait_recv()
            for k in range(cores):
                n = half * 2 + k
                src_slot = at.slot(at.x - s, c)
                same = k == 0
                dst_core = c if same else 1 - c
                w_push(9 + n, hop_ref.at[half * 2 + dst_core], wq_slot(src_slot, half), w_recv.at[5 + n], at.dev(at.y, at.x + s, dst_core))

    @_scoped
    def w_finish():
        whole = wq_slot(0)
        piece = wq_slot(0, 0)
        for n in range(9):
            ref = whole if n < 5 else piece
            _remote(ref, ref, w_send.at[0], w_recv.at[n], mate).wait_recv()

    def w_drain():
        whole = wq_slot(0)
        piece = wq_slot(0, 0)
        for k in range(13):
            ref = whole if 4 <= k < 9 else piece
            _remote(ref, ref, w_send.at[k], w_send.at[k], mate).wait_send()

    own_cols = wcols(at.r)
    rows = x_ref.shape[0]
    own_rows = pl.ds(pl.multiple_of((at.y * n_row + at.r) * rows, rows), rows)

    keep = [pltpu.make_async_copy(w_ref.at[:, own_cols], wq_slot(at.r), ld_sem.at[8])]
    for r in range(n_row):
        kv_r = at.y * n_kv + r // per_kv
        for i, w in enumerate((wk_ref, wv_ref)):
            keep.append(pltpu.make_async_copy(w.at[kv_r, :, own_cols], w_all.at[pl.ds(r * gw + hd + i * e, e), :], ld_sem.at[9 + 2 * r + i]))

    def front(w_v, wo_v, xblk):
        kv = (at.y * n_row + at.r) // (n_row * ring // wk_ref.shape[0])
        loads = [
            pltpu.make_async_copy(w_ref, w_v.at[pl.ds(0, hd), :], ld_sem.at[0]),
            pltpu.make_async_copy(wo_ref, wo_v, ld_sem.at[1]),
            pltpu.make_async_copy(wk_ref.at[kv], w_v.at[pl.ds(hd, e), :], ld_sem.at[6]),
            pltpu.make_async_copy(wv_ref.at[kv], w_v.at[pl.ds(hd + e, e), :], ld_sem.at[7]),
        ]
        ins = [pltpu.make_async_copy(src, xblk.at[pl.ds(i * rows, rows), :], ld_sem.at[2 + i]) for i, src in enumerate((x_ref, dy_ref))]
        outs = [pltpu.make_async_copy(xblk.at[pl.ds(i * rows, rows), :], dst.at[own_rows, :], ld_sem.at[4 + i]) for i, dst in enumerate((xf_ref, dyf_ref))]
        for cp in ins:
            cp.start()
        _enter([up, down] + [at.row_dev(r) for r in row_peers])
        gx.start()
        gz.start()
        for cp in loads + keep:
            cp.start()
        for cp in ins:
            cp.wait()
        for cp in outs:
            cp.start()

        dk_ref[...] = jnp.zeros_like(dk_ref)
        dv_ref[...] = jnp.zeros_like(dv_ref)

        @_scoped
        def project(w, out, b):
            pltpu.make_async_copy(xf_ref.at[pl.ds(0, tb), :], xblk, blk_sem.at[0]).wait()

            def block(i, _):
                r0 = pl.multiple_of(i * bq, bq)
                out[:, pl.ds(pl.multiple_of(b * tb + i * bq, bq), bq)] = _nt(w[...], xblk[pl.ds(r0, bq), :]).astype(BF16)
                return 0

            lax.fori_loop(0, tb // bq, block, 0)

        def row_at(t):
            off = jnp.where(t == 1, ring - 1, jnp.where(t == 2, 1, jnp.where(t == 3, 2, 0)))
            return lax.rem(at.y + off, ring)

        for cp in loads + outs:
            cp.wait()

        def begin(g):
            g.relay_first()
            g.near_first()
            g.go(MINUS)

            @pl.when(g.order == 0)
            def _():
                g.go(PLUS)

        def begin_far(g):
            g.far_first()

            @pl.when(g.order == 0)
            def _():
                g.go(FAR)

        def begin_second(g):
            g.relay_second(OWN)

            @pl.when(g.order == 1)
            def _():
                g.go(PLUS)

            g.near_second(OWN)

        def second_minus(g):
            g.relay_second(MINUS)

            @pl.when(g.order == 1)
            def _():
                g.go(FAR)

            g.near_second(MINUS)

        def x_turn(t, _):
            @pl.when(t == 0)
            def _():
                for step in (begin, begin_far, begin_second, second_minus):
                    for g in (gx, gz):
                        step(g)
                for d in (PLUS, FAR):
                    for g in (gx, gz):
                        g.relay_second(d)
                        g.near_second(d)
                gy.start()
                gx.far_second(OWN)

            @pl.when(t == 1)
            def _():
                gx.far_second(MINUS)

            @pl.when(t == 2)
            def _():
                for d in (PLUS, FAR):
                    gx.far_second(d)

            @pl.when(t == 3)
            def _():
                for d in range(4):
                    gz.far_second(d)
                begin(gy)

            b = row_at(t)
            _take_row((gx, gz), t, b, xblk, blk_sem.at[0])
            project(w_v, qkvt_ref, b)
            return 0

        lax.fori_loop(0, ring, x_turn, 0)
        for t in range(0, tokens, bq):
            kn_ref[t:t + bq, :] = qkvt_ref[hd:hd + e, t:t + bq].T
            vn_ref[t:t + bq, :] = qkvt_ref[hd + e:hd + 2 * e, t:t + bq].T

        keys_k, keys_v = slice(hd, hd + e), slice(hd + e, hd + 2 * e)
        m4 = heads * bs
        factor = scale * LOG2E

        def row_chunks(k):
            return [slice(t, t + bq) for t in range(0, (k + 1) * tb, bq)]

        def stacked(ref, qs):
            return jnp.concatenate([ref[h * e:(h + 1) * e, qs] for h in range(heads)], axis=1)

        def unstack(ref, qs, value):
            for h in range(heads):
                ref[h * e:(h + 1) * e, qs] = value[:, h * bs:(h + 1) * bs]

        def scores(q, ks, k, j):
            s = _nn(q, qkvt_ref[keys_k, ks])
            if ks.start < k * tb:
                return s
            row = lax.broadcasted_iota(jnp.int32, (m4, bq), 0) & (bs - 1)
            col = lax.broadcasted_iota(jnp.int32, (m4, bq), 1)
            return jnp.where(col + (ks.start - k * tb) <= row + j * bs, s, -jnp.inf)

        def folded(op, total, value):
            for t in range(0, value.shape[1], 128):
                piece = value[:, t:t + 128]
                total = piece if total is None else op(total, piece)
            return total

        def score_buf(ks):
            n = ks.start // cw
            return part.at[n, :, ks.start - n * cw:ks.stop - n * cw]

        def stats_buf(k, j):
            per = cw // 128
            n = k * (tb // bs)
            return part.at[2 + n // per, :, pl.ds(pl.multiple_of((n % per + j) * 128, 128), 128)]

        @_scoped
        def forward(k):
            chunks = row_chunks(k)

            def queries(j, _):
                qs = pl.ds(pl.multiple_of(k * tb + j * bs, bs), bs)
                q = stacked(qkvt_ref, qs).T
                m = None
                for ks in chunks:
                    s = scores(q, ks, k, j)
                    score_buf(ks)[...] = s
                    m = folded(jnp.maximum, m, s)
                m = jnp.max(m, axis=1, keepdims=True)
                total = None
                for ks in chunks:
                    p = jnp.exp2((score_buf(ks)[...] - m) * factor)
                    score_buf(ks)[...] = p
                    total = folded(jnp.add, total, p)
                inv = 1.0 / jnp.sum(total, axis=1, keepdims=True)
                lane = lax.broadcasted_iota(jnp.int32, (m4, 128), 1)
                stats_buf(k, j)[...] = jnp.where(lane == 0, m, inv)
                out = None
                for ks in chunks:
                    piece = _nn((score_buf(ks)[...] * inv).astype(BF16), vn_ref[ks, :])
                    out = piece if out is None else out + piece
                unstack(ot_ref, qs, out.astype(BF16).T)
                return 0

            lax.fori_loop(0, tb // bs, queries, 0)

        @_scoped
        def backward(k):
            chunks = row_chunks(k)

            def queries(j, _):
                qs = pl.ds(pl.multiple_of(k * tb + j * bs, bs), bs)
                qt = stacked(qkvt_ref, qs)
                dot = stacked(dot_ref, qs)
                q, do = qt.T, dot.T
                delta = jnp.sum(dot.astype(F32) * stacked(ot_ref, qs).astype(F32), axis=0, keepdims=True)
                delta = jnp.broadcast_to(delta, (128, m4)).T[:, :1]
                stats = stats_buf(k, j)[...]
                m, inv = stats[:, 0:1], stats[:, 1:2]
                dq = None
                for ks in chunks:
                    p = jnp.exp2((scores(q, ks, k, j) - m) * factor) * inv
                    dp = _nn(do, qkvt_ref[keys_v, ks])
                    ds = (p * (dp - delta)).astype(BF16)
                    dv_ref[:, ks] += _nn(dot, p.astype(BF16))
                    dk_ref[:, ks] += _nn(qt, ds)
                    piece = _nn(ds, kn_ref[ks, :])
                    dq = piece if dq is None else dq + piece
                dq = (dq * scale).astype(BF16).T
                unstack(dqt_ref, qs, dq)
                for h in range(0, heads, 2):
                    pair = jnp.concatenate([dq[:, h * bs:(h + 1) * bs], dq[:, (h + 1) * bs:(h + 2) * bs]], axis=0)
                    gq[qs, pl.ds(pl.multiple_of(at.r * gw + h * e, 128), 2 * e)] = pair.T
                return 0

            lax.fori_loop(0, tb // bs, queries, 0)

        forward(0)
        begin_far(gy)
        forward(1)
        begin_second(gy)
        forward(2)
        second_minus(gy)
        forward(3)

        def turn(t, _):
            @pl.when(t == 0)
            def _():
                @pl.when(c == 1)
                def _():
                    far_step(OWN)

            @pl.when(t == 1)
            def _():
                for d in (PLUS, FAR):
                    gy.relay_second(d)
                    gy.near_second(d)

                @pl.when(c == 1)
                def _():
                    far_step(MINUS)

                w_start()

            @pl.when(t == 2)
            def _():
                @pl.when(c == 1)
                def _():
                    far_step(PLUS)

                @pl.when(c == 0)
                def _():
                    far_step(OWN)
                    far_step(MINUS)

            @pl.when(t == 3)
            def _():
                @pl.when(c == 0)
                def _():
                    far_step(PLUS)

                far_step(FAR)
                w_relay()

            b = row_at(t)
            _take_row((gy,), t, b, xblk, blk_sem.at[0])
            project(wo_v, dot_ref, b)
            for k in range(ring):
                @pl.when(b == k)
                def _(k=k):
                    backward(k)
            return 0

        far_cp = {d: gy.push(gy.ref(d, FAR), gy.ref(d, FAR), gy.mate_recv.at[d, FAR], gy.mate) for d in range(4)}

        @_scoped
        def far_step(d):
            for half in (0, 1):
                gy.arrived(d, FAR, half)
            far_cp[d].start()

        lax.fori_loop(0, ring, turn, 0)


    pl.run_scoped(front, pltpu.VMEM((hd + 2 * e, width), BF16), pltpu.VMEM((hd, width), BF16), pltpu.VMEM((tb, width), BF16))

    own_g = at.r * gw
    for k in range(0, tokens, bq):
        ks = slice(k, k + bq)
        kv = jnp.concatenate([(dk_ref[:, ks] * scale).astype(BF16), dv_ref[:, ks].astype(BF16)], axis=0)
        gq[ks, pl.ds(pl.multiple_of(own_g + hd, 128), 2 * e)] = kv.T

    def back(xbuf, obuf, kvt):
        th = tb // 2
        tq = th // 2
        tl = tb // n_row
        hw = cw // 2
        half_a, half_b = pl.ds(0, hw), pl.ds(hw, hw)
        units = [(FAR, 0), (FAR, 1), (PLUS, 0), (MINUS, 0), (PLUS, 1), (MINUS, 1), (OWN, 0), (OWN, 1)]
        s_own, s_left, s_right, s_far = (at.slot(at.x + o, c) for o in (0, -1, 1, 2))
        m_own, m_left, m_right, m_far = (at.slot(at.x + o, 1 - c) for o in (0, -1, 1, 2))

        def unit_row(u):
            d, s = units[u]
            return pl.multiple_of(lax.rem(at.y + STEP[d] + ring, ring) * tb + s * th, th)

        def gcols(slot):
            return pl.ds(pl.multiple_of(slot * gw, gw), gw)

        def piece(u, slot, half=None):
            r0 = unit_row(u)
            rows = pl.ds(r0, th) if half is None else pl.ds(pl.multiple_of(r0 + half * tq, tq), tq)
            return gq.at[rows, gcols(slot)]

        sends = []

        def ag_push(u, n, slot, dev, half=None):
            ref = piece(u, slot, half)
            cp = _remote(ref, ref, ag_send.at[u, n], ag_recv.at[u, n], dev)
            cp.start()
            sends.append(cp)

        def ag_wait(u, n, slot, half=None):
            ref = piece(u, slot, half)
            _remote(ref, ref, ag_send.at[u, n], ag_recv.at[u, n], mate).wait_recv()

        def ag_own(u):
            ag_push(u, 0, s_own, right)
            ag_push(u, 1, s_own, left)
            ag_push(u, 2, s_own, mate)

        @_scoped
        def ag_relay(u):
            ag_wait(u, 0, s_left)
            ag_push(u, 3, s_left, right, 0)
            ag_push(u, 4, s_left, mate)
            ag_wait(u, 1, s_right)
            ag_push(u, 5, s_right, left, 1)
            ag_push(u, 6, s_right, mate)

        @_scoped
        def ag_finish(u):
            ag_wait(u, 3, s_far, 0)
            ag_push(u, 7, s_far, mate, 0)
            ag_wait(u, 5, s_far, 1)
            ag_push(u, 8, s_far, mate, 1)
            ag_wait(u, 2, m_own)
            ag_wait(u, 4, m_left)
            ag_wait(u, 6, m_right)
            ag_wait(u, 7, m_far, 0)
            ag_wait(u, 8, m_far, 1)

        nt = min(256, hw)

        @_scoped
        def partial(u):
            rows = pl.ds(unit_row(u), th)
            d, s = units[u]
            dst = part.at[d, pl.ds(s * th, th), :]

            def tile(j, _):
                cs = pl.ds(pl.multiple_of(j * nt, nt), nt)
                dst[:, cs] = _nn(gq[rows, :], w_all[:, cs])
                return 0

            lax.fori_loop(0, cw // nt, tile, 0)

        def rs_push(n, s, src, dst, dev):
            cp = _remote(src, dst, rs_send.at[n, s], rs_recv.at[n, s], dev)
            cp.start()
            sends.append(cp)

        def rs_wait(n, s):
            ref = rs_half.at[0, s]
            _remote(ref, ref, rs_send.at[n, s], rs_recv.at[n, s], mate).wait_recv()

        def block(d, s, half):
            return part.at[d, pl.ds(s * th, th), half]

        def far_a(s):
            rs_push(0, s, block(FAR, s, half_a), rs_half.at[0, s], up)

        def far_b(s):
            rs_push(1, s, block(FAR, s, half_b), rs_half.at[1, s], down)

        def minus_a(s):
            rs_push(4, s, block(MINUS, s, half_a), rs_full.at[1, s, 0], down)

        def plus_b(s):
            rs_push(3, s, block(PLUS, s, half_b), rs_full.at[0, s, 1], up)

        @_scoped
        def plus_a(s):
            rs_wait(0, s)
            block(PLUS, s, half_a)[...] += rs_half[0, s]
            rs_push(2, s, block(PLUS, s, half_a), rs_full.at[0, s, 0], up)

        @_scoped
        def minus_b(s):
            rs_wait(1, s)
            block(MINUS, s, half_b)[...] += rs_half[1, s]
            rs_push(5, s, block(MINUS, s, half_b), rs_full.at[1, s, 1], down)

        n_steps = width // bc
        depth = xbuf.shape[0]

        def chunk(src, c0, j):
            slot = lax.rem(j, depth)
            return pltpu.make_async_copy(src.at[:, pl.ds(pl.multiple_of(c0 + j * bc, bc), bc)], xbuf.at[slot], in_sem.at[slot])

        def ahead(src, c0, n):
            for j in range(min(depth - 1, n)):
                chunk(src, c0, j).start()

        @_scoped
        def stream(src, lhs, out, j0, j1):
            def store(j):
                slot = lax.rem(j, 2)
                return pltpu.make_async_copy(obuf.at[slot], out.at[:, pl.ds(pl.multiple_of(j * bc, bc), bc)], o_sem.at[slot])

            if j0 == 0:
                ahead(src, 0, n_steps)

            def step(j, _):
                @pl.when(j + depth - 1 < n_steps)
                def _():
                    chunk(src, 0, j + depth - 1).start()

                chunk(src, 0, j).wait()

                @pl.when(j >= 2)
                def _():
                    store(j - 2).wait()

                obuf[lax.rem(j, 2)] = _nn(lhs[...], xbuf[lax.rem(j, depth)])
                store(j).start()
                return 0

            lax.fori_loop(j0, j1, step, 0)
            if j1 == n_steps:
                for j in range(max(n_steps - 2, 0), n_steps):
                    store(j).wait()

        def wo_steps(a, b):
            stream(dyf_ref, ot_ref, dwo_ref, n_steps * a // 16, n_steps * b // 16)

        def wq_steps(a, b):
            stream(xf_ref, dqt_ref, dwq_ref, n_steps * a // 16, n_steps * b // 16)

        first = (at.r // per_kv) * per_kv
        share = width // per_kv
        col0 = lax.rem(at.r, per_kv) * share

        def kv_step(j, _):
            @pl.when(j + depth - 1 < share // bc)
            def _():
                chunk(xf_ref, col0, j + depth - 1).start()

            chunk(xf_ref, col0, j).wait()
            prod = _nn(kvt[...], xbuf[lax.rem(j, depth)])
            dk = dv = None
            for q in range(per_kv):
                a = prod[q * 2 * e:q * 2 * e + e]
                b = prod[q * 2 * e + e:(q + 1) * 2 * e]
                dk = a if dk is None else dk + a
                dv = b if dv is None else dv + b
            cs = pl.ds(pl.multiple_of(j * bc, bc), bc)
            dwk_ref[:, cs] = dk
            dwv_ref[:, cs] = dv
            return 0

        @_scoped
        def kv_grads():
            ahead(xf_ref, col0, share // bc)
            for q in range(per_kv):
                cols = pl.ds(pl.multiple_of((first + q) * gw + hd, 128), gw - hd)
                for t in range(0, tokens, bq):
                    kvt[q * (gw - hd):(q + 1) * (gw - hd), t:t + bq] = gq[t:t + bq, cols].T
            lax.fori_loop(0, share // bc, kv_step, 0)

        def hand(i, d, half):
            peer = lax.rem(at.r + d, n_row)
            rows = pl.ds(pl.multiple_of(peer * tl, tl), tl)
            cols = pl.ds(pl.multiple_of(at.r * cw + i * hw, hw), hw)
            return stage.at[rows, half], dx_ref.at[:, cols], at.row_dev(peer)

        @_scoped
        def finish(i, half):
            for s in (0, 1):
                rs_wait(2 + i, s)
                rs_wait(4 + i, s)
                stage[s * th:(s + 1) * th, half] = (block(OWN, s, half)[...] + rs_full[0, s, i] + rs_full[1, s, i]).astype(BF16)
            for d in range(1, n_row):
                src, dst, dev = hand(i, d, half)
                cp = _remote(src, dst, out_send.at[i, d], out_recv.at[i, d], dev)
                cp.start()
                sends.append(cp)
            src, dst, _ = hand(i, 0, half)
            pltpu.make_async_copy(src, dst, out_send.at[i, 0]).start()

        @_scoped
        def received(i, half):
            for d in range(1, n_row):
                src = lax.rem(at.r + n_row - d, n_row)
                ref = dx_ref.at[:, pl.ds(pl.multiple_of(src * cw + i * hw, hw), hw)]
                _remote(ref, ref, out_send.at[i, d], out_recv.at[i, d], mate).wait_recv()
            src, dst, _ = hand(i, 0, half)
            pltpu.make_async_copy(src, dst, out_send.at[i, 0]).wait()

        ag_own(0)
        ag_own(1)
        wo_steps(0, 3)
        ag_relay(0)
        ag_own(2)
        ag_finish(0)
        for cp in keep:
            cp.wait()
        w_finish()
        partial(0)
        ag_relay(1)
        far_a(0)
        far_b(0)
        ag_own(3)
        wo_steps(3, 5)
        ag_finish(1)
        partial(1)
        ag_relay(2)
        far_a(1)
        far_b(1)
        ag_own(4)
        wo_steps(5, 7)
        ag_finish(2)
        partial(2)
        ag_relay(3)
        ag_own(5)
        plus_a(0)
        wo_steps(7, 9)
        ag_finish(3)
        partial(3)
        ag_relay(4)
        minus_a(0)
        ag_own(6)
        wo_steps(9, 11)
        ag_finish(4)
        partial(4)
        ag_relay(5)
        ag_own(7)
        plus_a(1)
        plus_b(0)
        wo_steps(11, 12)
        ag_finish(5)
        partial(5)
        ag_relay(6)
        minus_a(1)
        minus_b(0)
        plus_b(1)
        minus_b(1)
        wo_steps(12, 14)
        ag_finish(6)
        partial(6)
        ag_relay(7)
        wo_steps(14, 16)
        ag_finish(7)
        partial(7)
        wq_steps(0, 3)
        finish(0, half_a)
        wq_steps(3, 16)
        kv_grads()
        received(0, half_a)
        finish(1, half_b)
        received(1, half_b)
        for cp in sends:
            cp.wait_send()
        w_drain()
        for g in (gx, gz, gy):
            g.drain()

    pl.run_scoped(back, pltpu.VMEM((4, tokens, bc), BF16), pltpu.VMEM((2, hd, bc), F32), pltpu.VMEM((per_kv * 2 * e, tokens), BF16))


def _layer(ring, cores, heads, scale, x, dy, wq, wk, wv, wo):
    rows, width = x.shape
    tokens = rows * ring * ring * cores
    hd = wo.shape[0]
    e = hd // heads
    n_row = ring * cores
    cw = width // n_row
    gw = hd + 2 * e
    tb = tokens // ring
    th, hw = tb // 2, cw // 2
    per_kv = n_row * ring // wk.shape[0]
    bq = min(256, tb)
    bs = tb // heads
    bc = min(512, cw // 2)
    dma = pltpu.SemaphoreType.DMA
    shape = jax.ShapeDtypeStruct
    return pl.pallas_call(
        functools.partial(_kernel, ring, cores, heads, scale, bq, bs, bc),
        name="layer",
        in_specs=[ANY] * 6,
        out_specs=[ANY, ANY, ANY, VMEM, VMEM, ANY, ANY],
        out_shape=[
            shape((rows, width), BF16),
            shape((hd, width), F32),
            shape((hd, width), F32),
            shape((e, width // per_kv), F32),
            shape((e, width // per_kv), F32),
            shape((tokens, width), BF16),
            shape((tokens, width), BF16),
        ],
        scratch_shapes=[
            pltpu.VMEM((tokens, n_row * gw), BF16),
            pltpu.VMEM((n_row * gw, cw), BF16),
            pltpu.VMEM((4, tb, cw), F32),
            pltpu.VMEM((2, 2, th, hw), F32),
            pltpu.VMEM((2, 2, 2, th, hw), F32),
            pltpu.VMEM((tb, cw), BF16),
            pltpu.VMEM((4, hd // 2, cw), BF16),
            pltpu.VMEM((gw, tokens), BF16),
            pltpu.VMEM((hd, tokens), BF16),
            pltpu.VMEM((hd, tokens), BF16),
            pltpu.VMEM((hd, tokens), BF16),
            pltpu.VMEM((e, tokens), F32),
            pltpu.VMEM((e, tokens), F32),
            pltpu.VMEM((tokens, e), BF16),
            pltpu.VMEM((tokens, e), BF16),
            dma((3, 48)),
            dma((3, 4, 4, 2)),
            dma((3, 4, 4)),
            dma((13,)),
            dma((9,)),
            dma((4,)),
            dma((9 + 2 * n_row,)),
            dma((1,)),
            dma((8, 9)),
            dma((8, 9)),
            dma((6, 2)),
            dma((6, 2)),
            dma((2, n_row)),
            dma((2, n_row)),
            dma((4,)),
            dma((2,)),
        ],
        compiler_params=pltpu.CompilerParams(collective_id=0, has_side_effects=True, vmem_limit_bytes=67043328),
        cost_estimate=pl.CostEstimate(flops=70 * 10**9, bytes_accessed=300 << 20, transcendentals=heads * tokens * tokens // 2),
    )(x, dy, wq, wk, wv, wo)


def solution(mesh):
    n = mesh.shape["tp"]
    ring = math.isqrt(n // 2)
    cores = n // (ring * ring)
    if ring != 4 or cores != 2:
        raise ValueError("needs a 4x4 torus")

    def local_grads(x_blk, dy_blk, wq_loc, w_k, w_v, wo_loc):
        model_dim, kv_heads, e = w_k.shape
        heads = wq_loc.shape[1]
        hd = heads * e
        scale = e ** -0.5
        wq = jnp.transpose(wq_loc, (1, 2, 0)).reshape(hd, model_dim)
        wk = jnp.transpose(w_k, (1, 2, 0))
        wv = jnp.transpose(w_v, (1, 2, 0))
        wo = wo_loc.reshape(hd, model_dim)
        dx, dwq, dwo, dwk, dwv, _, _ = _layer(ring, cores, heads, scale, x_blk, dy_blk, wq, wk, wv, wo)
        return (dx, jnp.transpose(dwq.reshape(heads, e, model_dim), (2, 0, 1)), dwo.reshape(heads, e, model_dim), dwk.T, dwv.T)

    tok = P(("dp", "tp"))
    return jax.shard_map(
        local_grads,
        mesh=mesh,
        in_specs=(tok, tok, P(None, "tp", None), P(), P(), P("tp")),
        out_specs=(tok, P("dp", "tp", None), tok, tok, tok),
        check_vma=False,
    )
```

```python
import functools
import math

import jax
import jax.numpy as jnp
from jax import lax
from jax.experimental import pallas as pl
from jax.experimental.pallas import tpu as pltpu
from jax.sharding import PartitionSpec as P

F32 = jnp.float32
BF16 = jnp.bfloat16
MESH = pl.DeviceIdType.MESH
ANY = pl.BlockSpec(memory_space=pl.ANY)
VMEM = pl.BlockSpec(memory_space=pltpu.VMEM)
LOG2E = math.log2(math.e)


def _scoped(fn):
    def run(*args, **kw):
        with jax.named_scope(fn.__name__):
            return fn(*args, **kw)

    return run


def _dot(a, b, dims):
    return lax.dot_general(a, b, (dims, ((), ())), preferred_element_type=F32)


def _nn(a, b):
    return _dot(a, b, ((1,), (0,)))


def _nt(a, b):
    return _dot(a, b, ((1,), (1,)))


class Place:
    def __init__(self, ring, cores):
        me = lax.axis_index("tp")
        self.ring, self.cores = ring, cores
        self.c = lax.rem(me, cores)
        self.x = lax.rem(me // cores, ring)
        self.y = me // (cores * ring)
        self.r = self.x * cores + self.c
        self.n_row = ring * cores

    def dev(self, y, x, c):
        y = lax.rem(y + self.ring, self.ring)
        x = lax.rem(x + self.ring, self.ring)
        return {"tp": (y * self.ring + x) * self.cores + c}

    def row_dev(self, r):
        return {"tp": self.y * self.n_row + r}

    def slot(self, x, c):
        return lax.rem(x + self.ring, self.ring) * self.cores + c


def _remote(src, dst, send, recv, dev):
    return pltpu.make_async_remote_copy(
        src_ref=src, dst_ref=dst, send_sem=send, recv_sem=recv, device_id=dev, device_id_type=MESH
    )


@_scoped
def _enter(devices):
    barrier = pltpu.get_barrier_semaphore()
    for dev in devices:
        pl.semaphore_signal(barrier, inc=1, device_id=dev, device_id_type=MESH)
    pl.semaphore_wait(barrier, len(devices))


OWN, MINUS, PLUS, FAR = range(4)
STEP = (0, -1, 1, 2)


def _load_shard(at, full, n, y, x, core, block, sem):
    r0 = at.dev(y, x, core)["tp"] * n
    b0 = at.slot(x, core) * n
    src = full.at[pl.ds(pl.multiple_of(r0, n), n), :]
    return pltpu.make_async_copy(src, block.at[pl.ds(pl.multiple_of(b0, n), n), :], sem)


@_scoped
def _take_row(lanes, t, y, block, sem):
    at, full, n = lanes[0].at, lanes[0].full, lanes[0].shard
    for j in range(4):
        _load_shard(at, full, n, y, at.x + STEP[j], at.c, block, sem).start()
    for j in range(4):
        for g in lanes:
            g.await_mate(t, j)
        _load_shard(at, full, n, y, at.x + STEP[j], 1 - at.c, block, sem).start()


class Gather:
    def __init__(self, at, src, full, send, recv, mate_recv, orders, row0, rows, tag):
        self.at, self.src, self.full = at, src, full
        self.send, self.recv, self.mate_recv = send.at[tag], recv.at[tag], mate_recv.at[tag]
        self.order, self.mate_order = orders
        self.row0, self.rows, self.shard = row0, rows, src.shape[0]
        self.sent = []
        c, o = at.c, self.order
        self.first = {s: at.dev(at.y + o * s, at.x + (1 - o) * s, c) for s in (1, -1)}
        self.second = {s: at.dev(at.y + (1 - o) * s, at.x + o * s, c) for s in (1, -1)}
        self.mate = at.dev(at.y, at.x, 1 - c)
        self.fulls = {d: self.both_ways(self.second, d, lambda to, d=d: (d, to)) for d in range(4)}

    def span(self, half):
        n = self.rows if half is None else self.rows // 2
        return self.row0 + (0 if half is None else half * n), n

    def ref(self, d1, d2, half=None):
        at, o = self.at, self.order
        o1, o2 = STEP[d1], STEP[d2]
        start, n = self.span(half)
        r0 = at.dev(at.y + o * o1 + (1 - o) * o2, at.x + (1 - o) * o1 + o * o2, at.c)["tp"] * self.shard + start
        return self.full.at[pl.ds(pl.multiple_of(r0, math.gcd(self.shard, self.row0, n)), n), :]

    def push(self, src, dst, recv, dev):
        k = len(self.sent)
        self.sent.append(dst.shape[0])
        return _remote(src, dst, self.send.at[k], recv, dev)

    def out(self, d1, d2, half=None):
        if d1 == OWN and d2 == OWN:
            return self.src.at[pl.ds(*self.span(half)), :]
        return self.ref(d1, d2, half)

    def both_ways(self, devs, d1, name):
        copies = []
        for step in (0, 1):
            for s, to in ((1, MINUS), (-1, PLUS)):
                half = step if s == 1 else 1 - step
                copies.append(self.push(self.out(d1, OWN, half), self.ref(d1, OWN, half), self.recv.at[*name(to), half], devs[s]))
        return copies

    def to_mate(self, d1, d2):
        ref = self.ref(d1, d2)
        self.push(self.out(d1, d2), ref, self.mate_recv.at[d1, d2], self.mate).start()

    def arrived(self, d1, d2, half):
        ref = self.ref(d1, d2, half)
        _remote(ref, ref, self.send.at[0], self.recv.at[d1, d2, half], self.mate).wait_recv()

    @_scoped
    def start(self):
        for cp in self.both_ways(self.first, OWN, lambda to: (to, OWN)):
            cp.start()
        self.go(OWN)
        self.to_mate(OWN, OWN)

    def go(self, d1):
        for cp in self.fulls[d1]:
            cp.start()

    @_scoped
    def relay_first(self):
        for d, s, half in ((MINUS, 1, 0), (PLUS, -1, 1)):
            self.arrived(d, OWN, half)
            ref = self.ref(d, OWN, half)
            self.push(ref, ref, self.recv.at[FAR, OWN, half], self.first[s]).start()

    @_scoped
    def near_first(self):
        for d, half in ((MINUS, 1), (PLUS, 0)):
            self.arrived(d, OWN, half)
            self.to_mate(d, OWN)

    @_scoped
    def far_first(self):
        for half in (0, 1):
            self.arrived(FAR, OWN, half)
        self.to_mate(FAR, OWN)

    @_scoped
    def relay_second(self, d1):
        for d, s, half in ((MINUS, 1, 0), (PLUS, -1, 1)):
            self.arrived(d1, d, half)
            ref = self.ref(d1, d, half)
            self.push(ref, ref, self.recv.at[d1, FAR, half], self.second[s]).start()

    @_scoped
    def near_second(self, d1):
        for d, half in ((MINUS, 1), (PLUS, 0)):
            self.arrived(d1, d, half)
            self.to_mate(d1, d)

    @_scoped
    def far_second(self, d1):
        for half in (0, 1):
            self.arrived(d1, FAR, half)
        self.to_mate(d1, FAR)

    def await_mate(self, t, j):
        o = self.mate_order
        ref = self.full.at[pl.ds(0, self.rows), :]
        _remote(ref, ref, self.send.at[0], self.mate_recv.at[(1 - o) * j + o * t, (1 - o) * t + o * j], self.mate).wait_recv()

    @_scoped
    def drain(self):
        for k, n in enumerate(self.sent):
            ref = self.full.at[pl.ds(0, n), :]
            _remote(ref, ref, self.send.at[k], self.send.at[k], self.mate).wait_send()


def _kernel(ring, cores, heads, scale, bq, bs, bc, x_ref, dy_ref, w_ref, wk_ref, wv_ref, wo_ref,
            dx_ref, dwq_ref, dwo_ref, dwk_ref, dwv_ref, xf_ref, dyf_ref,
            gq, w_all, part, rs_half, rs_full, stage, hop_ref, qkvt_ref, dot_ref, dqt_ref, ot_ref, dk_ref, dv_ref, kn_ref, vn_ref,
            send, recv, mate_recv, w_send, w_recv, hop_recv, ld_sem, blk_sem,
            ag_send, ag_recv, rs_send, rs_recv, out_send, out_recv, in_sem, o_sem):
    at = Place(ring, cores)
    n_row = at.n_row
    hd = wo_ref.shape[0]
    e = hd // heads
    tokens, width = xf_ref.shape
    tb = tokens // ring
    cw = width // n_row
    gw = gq.shape[1] // n_row
    c = at.c
    shard = x_ref.shape[0]
    gx = Gather(at, x_ref, xf_ref, send, recv, mate_recv, (c, 1 - c), 0, shard, 0)
    gy = Gather(at, dy_ref, dyf_ref, send, recv, mate_recv, (c, 1 - c), 0, shard, 1)
    n_kv = wk_ref.shape[0] // ring
    per_kv = n_row // n_kv
    row_peers = [lax.rem(at.r + d, n_row) for d in range(1, n_row)]
    up, down = at.dev(at.y + 1, at.x, c), at.dev(at.y - 1, at.x, c)

    hh = hd // 2

    def w_push(k, src, dst, rsem, dev):
        _remote(src, dst, w_send.at[k], rsem, dev).start()

    def wq_slot(slot, half=None):
        r0 = slot * gw + (0 if half is None else half * hh)
        return w_all.at[pl.ds(r0 if isinstance(r0, int) else pl.multiple_of(r0, hh), hd if half is None else hh), :]

    def wcols(slot):
        return pl.ds(pl.multiple_of(slot * cw, cw), cw)

    right, left, mate = at.dev(at.y, at.x + 1, c), at.dev(at.y, at.x - 1, c), at.dev(at.y, at.x, 1 - c)

    @_scoped
    def w_start():
        for half, dev in ((0, right), (1, left)):
            for k in range(cores):
                w_push(half * 2 + k, w_ref.at[pl.ds(half * hh, hh), wcols(at.slot(at.x + 2, k))], hop_ref.at[half * 2 + k], hop_recv.at[half * 2 + k], dev)
        w_push(4, w_ref.at[pl.ds(0, hd), wcols(at.slot(at.x, 1 - c))], wq_slot(at.r), w_recv.at[0], mate)
        for i, s in enumerate((1, -1)):
            for k in range(cores):
                dst_core = c if k == 0 else 1 - c
                w_push(5 + 2 * i + k, w_ref.at[pl.ds(0, hd), wcols(at.slot(at.x + s, dst_core))], wq_slot(at.r), w_recv.at[1 + 2 * i + k], at.dev(at.y, at.x + s, dst_core))

    @_scoped
    def w_relay():
        for half, s in ((0, 1), (1, -1)):
            for n in (half * 2, half * 2 + 1):
                _remote(hop_ref.at[n], hop_ref.at[n], w_send.at[0], hop_recv.at[n], mate).wait_recv()
            for k in range(cores):
                n = half * 2 + k
                src_slot = at.slot(at.x - s, c)
                same = k == 0
                dst_core = c if same else 1 - c
                w_push(9 + n, hop_ref.at[half * 2 + dst_core], wq_slot(src_slot, half), w_recv.at[5 + n], at.dev(at.y, at.x + s, dst_core))

    @_scoped
    def w_finish():
        whole = wq_slot(0)
        piece = wq_slot(0, 0)
        for n in range(9):
            ref = whole if n < 5 else piece
            _remote(ref, ref, w_send.at[0], w_recv.at[n], mate).wait_recv()

    def w_drain():
        whole = wq_slot(0)
        piece = wq_slot(0, 0)
        for k in range(13):
            ref = whole if 4 <= k < 9 else piece
            _remote(ref, ref, w_send.at[k], w_send.at[k], mate).wait_send()

    own_cols = wcols(at.r)
    rows = x_ref.shape[0]
    own_rows = pl.ds(pl.multiple_of((at.y * n_row + at.r) * rows, rows), rows)

    keep = [pltpu.make_async_copy(w_ref.at[:, own_cols], wq_slot(at.r), ld_sem.at[8])]
    for r in range(n_row):
        kv_r = at.y * n_kv + r // per_kv
        for i, w in enumerate((wk_ref, wv_ref)):
            keep.append(pltpu.make_async_copy(w.at[kv_r, :, own_cols], w_all.at[pl.ds(r * gw + hd + i * e, e), :], ld_sem.at[9 + 2 * r + i]))

    def front(w_v, wo_v, xblk):
        kv = (at.y * n_row + at.r) // (n_row * ring // wk_ref.shape[0])
        loads = [
            pltpu.make_async_copy(w_ref, w_v.at[pl.ds(0, hd), :], ld_sem.at[0]),
            pltpu.make_async_copy(wo_ref, wo_v, ld_sem.at[1]),
            pltpu.make_async_copy(wk_ref.at[kv], w_v.at[pl.ds(hd, e), :], ld_sem.at[6]),
            pltpu.make_async_copy(wv_ref.at[kv], w_v.at[pl.ds(hd + e, e), :], ld_sem.at[7]),
        ]
        ins = [pltpu.make_async_copy(src, xblk.at[pl.ds(i * rows, rows), :], ld_sem.at[2 + i]) for i, src in enumerate((x_ref, dy_ref))]
        outs = [pltpu.make_async_copy(xblk.at[pl.ds(i * rows, rows), :], dst.at[own_rows, :], ld_sem.at[4 + i]) for i, dst in enumerate((xf_ref, dyf_ref))]
        for cp in ins:
            cp.start()
        _enter([up, down] + [at.row_dev(r) for r in row_peers])
        gx.start()
        for cp in loads + keep:
            cp.start()
        for cp in ins:
            cp.wait()
        for cp in outs:
            cp.start()

        dk_ref[...] = jnp.zeros_like(dk_ref)
        dv_ref[...] = jnp.zeros_like(dv_ref)

        @_scoped
        def project(w, out, b):
            pltpu.make_async_copy(xf_ref.at[pl.ds(0, tb), :], xblk, blk_sem.at[0]).wait()

            def block(i, _):
                r0 = pl.multiple_of(i * bq, bq)
                out[:, pl.ds(pl.multiple_of(b * tb + i * bq, bq), bq)] = _nt(w[...], xblk[pl.ds(r0, bq), :]).astype(BF16)
                return 0

            lax.fori_loop(0, tb // bq, block, 0)

        def row_at(t):
            off = jnp.where(t == 1, ring - 1, jnp.where(t == 2, 1, jnp.where(t == 3, 2, 0)))
            return lax.rem(at.y + off, ring)

        for cp in loads + outs:
            cp.wait()

        def begin(g):
            g.relay_first()
            g.near_first()
            g.go(MINUS)

            @pl.when(g.order == 0)
            def _():
                g.go(PLUS)

        def begin_far(g):
            g.far_first()

            @pl.when(g.order == 0)
            def _():
                g.go(FAR)

        def begin_second(g):
            g.relay_second(OWN)

            @pl.when(g.order == 1)
            def _():
                g.go(PLUS)

            g.near_second(OWN)

        def second_minus(g):
            g.relay_second(MINUS)

            @pl.when(g.order == 1)
            def _():
                g.go(FAR)

            g.near_second(MINUS)

        def x_turn(t, _):
            @pl.when(t == 0)
            def _():
                begin(gx)
                begin_far(gx)
                begin_second(gx)
                second_minus(gx)
                gx.relay_second(PLUS)
                gx.near_second(PLUS)
                gx.relay_second(FAR)
                gy.start()
                gx.far_second(OWN)

            @pl.when(t == 1)
            def _():
                gx.near_second(FAR)
                gx.far_second(MINUS)

            @pl.when(t == 2)
            def _():
                for d in (PLUS, FAR):
                    gx.far_second(d)

            @pl.when(t == 3)
            def _():
                begin(gy)

            b = row_at(t)
            _take_row((gx,), t, b, xblk, blk_sem.at[0])
            project(w_v, qkvt_ref, b)
            return 0

        lax.fori_loop(0, ring, x_turn, 0)
        for t in range(0, tokens, bq):
            kn_ref[t:t + bq, :] = qkvt_ref[hd:hd + e, t:t + bq].T
            vn_ref[t:t + bq, :] = qkvt_ref[hd + e:hd + 2 * e, t:t + bq].T

        keys_k, keys_v = slice(hd, hd + e), slice(hd + e, hd + 2 * e)
        m4 = heads * bs
        factor = scale * LOG2E

        def row_chunks(k):
            return [slice(t, t + bq) for t in range(0, (k + 1) * tb, bq)]

        def stacked(ref, qs):
            return jnp.concatenate([ref[h * e:(h + 1) * e, qs] for h in range(heads)], axis=1)

        def unstack(ref, qs, value):
            for h in range(heads):
                ref[h * e:(h + 1) * e, qs] = value[:, h * bs:(h + 1) * bs]

        def scores(q, ks, k, j):
            s = _nn(q, qkvt_ref[keys_k, ks])
            if ks.start < k * tb:
                return s
            row = lax.broadcasted_iota(jnp.int32, (m4, bq), 0) & (bs - 1)
            col = lax.broadcasted_iota(jnp.int32, (m4, bq), 1)
            return jnp.where(col + (ks.start - k * tb) <= row + j * bs, s, -jnp.inf)

        def folded(op, total, value):
            for t in range(0, value.shape[1], 128):
                piece = value[:, t:t + 128]
                total = piece if total is None else op(total, piece)
            return total

        def score_buf(ks):
            n = ks.start // cw
            return part.at[n, :, ks.start - n * cw:ks.stop - n * cw]

        def stats_buf(k, j):
            per = cw // 128
            n = k * (tb // bs)
            return part.at[2 + n // per, :, pl.ds(pl.multiple_of((n % per + j) * 128, 128), 128)]

        @_scoped
        def forward(k):
            chunks = row_chunks(k)

            def queries(j, _):
                qs = pl.ds(pl.multiple_of(k * tb + j * bs, bs), bs)
                q = stacked(qkvt_ref, qs).T
                m = None
                for ks in chunks:
                    s = scores(q, ks, k, j)
                    score_buf(ks)[...] = s
                    m = folded(jnp.maximum, m, s)
                m = jnp.max(m, axis=1, keepdims=True)
                total = None
                for ks in chunks:
                    p = jnp.exp2((score_buf(ks)[...] - m) * factor)
                    score_buf(ks)[...] = p
                    total = folded(jnp.add, total, p)
                inv = 1.0 / jnp.sum(total, axis=1, keepdims=True)
                lane = lax.broadcasted_iota(jnp.int32, (m4, 128), 1)
                stats_buf(k, j)[...] = jnp.where(lane == 0, m, inv)
                out = None
                for ks in chunks:
                    piece = _nn((score_buf(ks)[...] * inv).astype(BF16), vn_ref[ks, :])
                    out = piece if out is None else out + piece
                unstack(ot_ref, qs, out.astype(BF16).T)
                return 0

            lax.fori_loop(0, tb // bs, queries, 0)

        @_scoped
        def backward(k):
            chunks = row_chunks(k)

            def queries(j, _):
                qs = pl.ds(pl.multiple_of(k * tb + j * bs, bs), bs)
                qt = stacked(qkvt_ref, qs)
                dot = stacked(dot_ref, qs)
                q, do = qt.T, dot.T
                delta = jnp.sum(dot.astype(F32) * stacked(ot_ref, qs).astype(F32), axis=0, keepdims=True)
                delta = jnp.broadcast_to(delta, (128, m4)).T[:, :1]
                stats = stats_buf(k, j)[...]
                m, inv = stats[:, 0:1], stats[:, 1:2]
                dq = None
                for ks in chunks:
                    p = jnp.exp2((scores(q, ks, k, j) - m) * factor) * inv
                    dp = _nn(do, qkvt_ref[keys_v, ks])
                    ds = (p * (dp - delta)).astype(BF16)
                    dv_ref[:, ks] += _nn(dot, p.astype(BF16))
                    dk_ref[:, ks] += _nn(qt, ds)
                    piece = _nn(ds, kn_ref[ks, :])
                    dq = piece if dq is None else dq + piece
                dq = (dq * scale).astype(BF16).T
                unstack(dqt_ref, qs, dq)
                for h in range(0, heads, 2):
                    pair = jnp.concatenate([dq[:, h * bs:(h + 1) * bs], dq[:, (h + 1) * bs:(h + 2) * bs]], axis=0)
                    gq[qs, pl.ds(pl.multiple_of(at.r * gw + h * e, 128), 2 * e)] = pair.T
                return 0

            lax.fori_loop(0, tb // bs, queries, 0)

        forward(0)
        begin_far(gy)
        forward(1)
        begin_second(gy)
        forward(2)
        second_minus(gy)
        forward(3)

        def turn(t, _):
            @pl.when(t == 0)
            def _():
                @pl.when(c == 1)
                def _():
                    far_step(OWN)

            @pl.when(t == 1)
            def _():
                for d in (PLUS, FAR):
                    gy.relay_second(d)
                    gy.near_second(d)

                @pl.when(c == 1)
                def _():
                    far_step(MINUS)

                w_start()

            @pl.when(t == 2)
            def _():
                @pl.when(c == 1)
                def _():
                    far_step(PLUS)

                @pl.when(c == 0)
                def _():
                    far_step(OWN)
                    far_step(MINUS)

            @pl.when(t == 3)
            def _():
                @pl.when(c == 0)
                def _():
                    far_step(PLUS)

                far_step(FAR)

            b = row_at(t)
            _take_row((gy,), t, b, xblk, blk_sem.at[0])
            project(wo_v, dot_ref, b)

            @pl.when(t == 3)
            def _():
                w_relay()

            for k in range(ring):
                @pl.when(b == k)
                def _(k=k):
                    backward(k)
            return 0

        far_cp = {d: gy.push(gy.ref(d, FAR), gy.ref(d, FAR), gy.mate_recv.at[d, FAR], gy.mate) for d in range(4)}

        @_scoped
        def far_step(d):
            for half in (0, 1):
                gy.arrived(d, FAR, half)
            far_cp[d].start()

        lax.fori_loop(0, ring, turn, 0)


    pl.run_scoped(front, pltpu.VMEM((hd + 2 * e, width), BF16), pltpu.VMEM((hd, width), BF16), pltpu.VMEM((tb, width), BF16))

    own_g = at.r * gw
    for k in range(0, tokens, bq):
        ks = slice(k, k + bq)
        kv = jnp.concatenate([(dk_ref[:, ks] * scale).astype(BF16), dv_ref[:, ks].astype(BF16)], axis=0)
        gq[ks, pl.ds(pl.multiple_of(own_g + hd, 128), 2 * e)] = kv.T

    def back(xbuf, obuf, kvt):
        th = tb // 2
        tq = th // 2
        tl = tb // n_row
        hw = cw // 2
        half_a, half_b = pl.ds(0, hw), pl.ds(hw, hw)
        units = [(FAR, 0), (FAR, 1), (PLUS, 0), (MINUS, 0), (PLUS, 1), (MINUS, 1), (OWN, 0), (OWN, 1)]
        s_own, s_left, s_right, s_far = (at.slot(at.x + o, c) for o in (0, -1, 1, 2))
        m_own, m_left, m_right, m_far = (at.slot(at.x + o, 1 - c) for o in (0, -1, 1, 2))

        def unit_row(u):
            d, s = units[u]
            return pl.multiple_of(lax.rem(at.y + STEP[d] + ring, ring) * tb + s * th, th)

        def gcols(slot):
            return pl.ds(pl.multiple_of(slot * gw, gw), gw)

        def piece(u, slot, half=None):
            r0 = unit_row(u)
            rows = pl.ds(r0, th) if half is None else pl.ds(pl.multiple_of(r0 + half * tq, tq), tq)
            return gq.at[rows, gcols(slot)]

        sends = []

        def ag_push(u, n, slot, dev, half=None):
            ref = piece(u, slot, half)
            cp = _remote(ref, ref, ag_send.at[u, n], ag_recv.at[u, n], dev)
            cp.start()
            sends.append(cp)

        def ag_wait(u, n, slot, half=None):
            ref = piece(u, slot, half)
            _remote(ref, ref, ag_send.at[u, n], ag_recv.at[u, n], mate).wait_recv()

        def ag_own(u):
            ag_push(u, 0, s_own, right)
            ag_push(u, 1, s_own, left)
            ag_push(u, 2, s_own, mate)

        @_scoped
        def ag_relay(u):
            ag_wait(u, 0, s_left)
            ag_push(u, 3, s_left, right, 0)
            ag_push(u, 4, s_left, mate)
            ag_wait(u, 1, s_right)
            ag_push(u, 5, s_right, left, 1)
            ag_push(u, 6, s_right, mate)

        @_scoped
        def ag_finish(u):
            ag_wait(u, 3, s_far, 0)
            ag_push(u, 7, s_far, mate, 0)
            ag_wait(u, 5, s_far, 1)
            ag_push(u, 8, s_far, mate, 1)
            ag_wait(u, 2, m_own)
            ag_wait(u, 4, m_left)
            ag_wait(u, 6, m_right)
            ag_wait(u, 7, m_far, 0)
            ag_wait(u, 8, m_far, 1)

        nt = min(256, hw)

        @_scoped
        def partial(u):
            rows = pl.ds(unit_row(u), th)
            d, s = units[u]
            dst = part.at[d, pl.ds(s * th, th), :]

            def tile(j, _):
                cs = pl.ds(pl.multiple_of(j * nt, nt), nt)
                dst[:, cs] = _nn(gq[rows, :], w_all[:, cs])
                return 0

            lax.fori_loop(0, cw // nt, tile, 0)

        def rs_push(n, s, src, dst, dev):
            cp = _remote(src, dst, rs_send.at[n, s], rs_recv.at[n, s], dev)
            cp.start()
            sends.append(cp)

        def rs_wait(n, s):
            ref = rs_half.at[0, s]
            _remote(ref, ref, rs_send.at[n, s], rs_recv.at[n, s], mate).wait_recv()

        def block(d, s, half):
            return part.at[d, pl.ds(s * th, th), half]

        def far_a(s):
            rs_push(0, s, block(FAR, s, half_a), rs_half.at[0, s], up)

        def far_b(s):
            rs_push(1, s, block(FAR, s, half_b), rs_half.at[1, s], down)

        def minus_a(s):
            rs_push(4, s, block(MINUS, s, half_a), rs_full.at[1, s, 0], down)

        def plus_b(s):
            rs_push(3, s, block(PLUS, s, half_b), rs_full.at[0, s, 1], up)

        @_scoped
        def plus_a(s):
            rs_wait(0, s)
            block(PLUS, s, half_a)[...] += rs_half[0, s]
            rs_push(2, s, block(PLUS, s, half_a), rs_full.at[0, s, 0], up)

        @_scoped
        def minus_b(s):
            rs_wait(1, s)
            block(MINUS, s, half_b)[...] += rs_half[1, s]
            rs_push(5, s, block(MINUS, s, half_b), rs_full.at[1, s, 1], down)

        n_steps = width // bc
        depth = xbuf.shape[0]

        def chunk(src, c0, j):
            slot = lax.rem(j, depth)
            return pltpu.make_async_copy(src.at[:, pl.ds(pl.multiple_of(c0 + j * bc, bc), bc)], xbuf.at[slot], in_sem.at[slot])

        def ahead(src, c0, n):
            for j in range(min(depth - 1, n)):
                chunk(src, c0, j).start()

        @_scoped
        def stream(src, lhs, out, j0, j1):
            def store(j):
                slot = lax.rem(j, 2)
                return pltpu.make_async_copy(obuf.at[slot], out.at[:, pl.ds(pl.multiple_of(j * bc, bc), bc)], o_sem.at[slot])

            if j0 == 0:
                ahead(src, 0, n_steps)

            def step(j, _):
                @pl.when(j + depth - 1 < n_steps)
                def _():
                    chunk(src, 0, j + depth - 1).start()

                chunk(src, 0, j).wait()

                @pl.when(j >= 2)
                def _():
                    store(j - 2).wait()

                obuf[lax.rem(j, 2)] = _nn(lhs[...], xbuf[lax.rem(j, depth)])
                store(j).start()
                return 0

            lax.fori_loop(j0, j1, step, 0)
            if j1 == n_steps:
                for j in range(max(n_steps - 2, 0), n_steps):
                    store(j).wait()

        def wo_steps(a, b):
            stream(dyf_ref, ot_ref, dwo_ref, n_steps * a // 16, n_steps * b // 16)

        def wq_steps(a, b):
            stream(xf_ref, dqt_ref, dwq_ref, n_steps * a // 16, n_steps * b // 16)

        first = (at.r // per_kv) * per_kv
        share = width // per_kv
        col0 = lax.rem(at.r, per_kv) * share

        def kv_step(j, _):
            @pl.when(j + depth - 1 < share // bc)
            def _():
                chunk(xf_ref, col0, j + depth - 1).start()

            chunk(xf_ref, col0, j).wait()
            prod = _nn(kvt[...], xbuf[lax.rem(j, depth)])
            dk = dv = None
            for q in range(per_kv):
                a = prod[q * 2 * e:q * 2 * e + e]
                b = prod[q * 2 * e + e:(q + 1) * 2 * e]
                dk = a if dk is None else dk + a
                dv = b if dv is None else dv + b
            cs = pl.ds(pl.multiple_of(j * bc, bc), bc)
            dwk_ref[:, cs] = dk
            dwv_ref[:, cs] = dv
            return 0

        @_scoped
        def kv_grads():
            ahead(xf_ref, col0, share // bc)
            for q in range(per_kv):
                cols = pl.ds(pl.multiple_of((first + q) * gw + hd, 128), gw - hd)
                for t in range(0, tokens, bq):
                    kvt[q * (gw - hd):(q + 1) * (gw - hd), t:t + bq] = gq[t:t + bq, cols].T
            lax.fori_loop(0, share // bc, kv_step, 0)

        def hand(i, d, half):
            peer = lax.rem(at.r + d, n_row)
            rows = pl.ds(pl.multiple_of(peer * tl, tl), tl)
            cols = pl.ds(pl.multiple_of(at.r * cw + i * hw, hw), hw)
            return stage.at[rows, half], dx_ref.at[:, cols], at.row_dev(peer)

        @_scoped
        def finish(i, half):
            for s in (0, 1):
                rs_wait(2 + i, s)
                rs_wait(4 + i, s)
                stage[s * th:(s + 1) * th, half] = (block(OWN, s, half)[...] + rs_full[0, s, i] + rs_full[1, s, i]).astype(BF16)
            for d in range(1, n_row):
                src, dst, dev = hand(i, d, half)
                cp = _remote(src, dst, out_send.at[i, d], out_recv.at[i, d], dev)
                cp.start()
                sends.append(cp)
            src, dst, _ = hand(i, 0, half)
            pltpu.make_async_copy(src, dst, out_send.at[i, 0]).start()

        @_scoped
        def received(i, half):
            for d in range(1, n_row):
                src = lax.rem(at.r + n_row - d, n_row)
                ref = dx_ref.at[:, pl.ds(pl.multiple_of(src * cw + i * hw, hw), hw)]
                _remote(ref, ref, out_send.at[i, d], out_recv.at[i, d], mate).wait_recv()
            src, dst, _ = hand(i, 0, half)
            pltpu.make_async_copy(src, dst, out_send.at[i, 0]).wait()

        ag_own(0)
        wo_steps(0, 8)
        ag_relay(0)
        ag_own(1)
        ag_own(2)
        wo_steps(8, 10)
        ag_finish(0)
        for cp in keep:
            cp.wait()
        w_finish()
        partial(0)
        ag_relay(1)
        far_a(0)
        far_b(0)
        ag_own(3)
        wo_steps(10, 11)
        ag_finish(1)
        partial(1)
        ag_relay(2)
        far_a(1)
        far_b(1)
        ag_own(4)
        wo_steps(11, 12)
        ag_finish(2)
        partial(2)
        ag_relay(3)
        ag_own(5)
        wo_steps(12, 13)
        ag_finish(3)
        partial(3)
        minus_a(0)
        plus_a(0)
        ag_relay(4)
        ag_own(6)
        wo_steps(13, 14)
        ag_finish(4)
        partial(4)
        ag_relay(5)
        ag_own(7)
        wo_steps(14, 15)
        ag_finish(5)
        partial(5)
        minus_a(1)
        plus_a(1)
        plus_b(0)
        minus_b(0)
        plus_b(1)
        minus_b(1)
        ag_relay(6)
        wo_steps(15, 16)
        ag_finish(6)
        partial(6)
        ag_relay(7)
        wq_steps(0, 4)
        ag_finish(7)
        partial(7)
        finish(0, half_a)
        wq_steps(4, 16)
        kv_grads()
        received(0, half_a)
        finish(1, half_b)
        received(1, half_b)
        for cp in sends:
            cp.wait_send()
        w_drain()
        for g in (gx, gy):
            g.drain()

    pl.run_scoped(back, pltpu.VMEM((4, tokens, bc), BF16), pltpu.VMEM((2, hd, bc), F32), pltpu.VMEM((per_kv * 2 * e, tokens), BF16))


def _layer(ring, cores, heads, scale, x, dy, wq, wk, wv, wo):
    rows, width = x.shape
    tokens = rows * ring * ring * cores
    hd = wo.shape[0]
    e = hd // heads
    n_row = ring * cores
    cw = width // n_row
    gw = hd + 2 * e
    tb = tokens // ring
    th, hw = tb // 2, cw // 2
    per_kv = n_row * ring // wk.shape[0]
    bq = min(256, tb)
    bs = tb // heads
    bc = min(512, cw // 2)
    dma = pltpu.SemaphoreType.DMA
    shape = jax.ShapeDtypeStruct
    return pl.pallas_call(
        functools.partial(_kernel, ring, cores, heads, scale, bq, bs, bc),
        name="layer",
        in_specs=[ANY] * 6,
        out_specs=[ANY, ANY, ANY, VMEM, VMEM, ANY, ANY],
        out_shape=[
            shape((rows, width), BF16),
            shape((hd, width), F32),
            shape((hd, width), F32),
            shape((e, width // per_kv), F32),
            shape((e, width // per_kv), F32),
            shape((tokens, width), BF16),
            shape((tokens, width), BF16),
        ],
        scratch_shapes=[
            pltpu.VMEM((tokens, n_row * gw), BF16),
            pltpu.VMEM((n_row * gw, cw), BF16),
            pltpu.VMEM((4, tb, cw), F32),
            pltpu.VMEM((2, 2, th, hw), F32),
            pltpu.VMEM((2, 2, 2, th, hw), F32),
            pltpu.VMEM((tb, cw), BF16),
            pltpu.VMEM((4, hd // 2, cw), BF16),
            pltpu.VMEM((gw, tokens), BF16),
            pltpu.VMEM((hd, tokens), BF16),
            pltpu.VMEM((hd, tokens), BF16),
            pltpu.VMEM((hd, tokens), BF16),
            pltpu.VMEM((e, tokens), F32),
            pltpu.VMEM((e, tokens), F32),
            pltpu.VMEM((tokens, e), BF16),
            pltpu.VMEM((tokens, e), BF16),
            dma((2, 48)),
            dma((2, 4, 4, 2)),
            dma((2, 4, 4)),
            dma((13,)),
            dma((9,)),
            dma((4,)),
            dma((9 + 2 * n_row,)),
            dma((1,)),
            dma((8, 9)),
            dma((8, 9)),
            dma((6, 2)),
            dma((6, 2)),
            dma((2, n_row)),
            dma((2, n_row)),
            dma((4,)),
            dma((2,)),
        ],
        compiler_params=pltpu.CompilerParams(collective_id=0, has_side_effects=True, vmem_limit_bytes=67043328),
        cost_estimate=pl.CostEstimate(flops=70 * 10**9, bytes_accessed=300 << 20, transcendentals=heads * tokens * tokens // 2),
    )(x, dy, wq, wk, wv, wo)


def solution(mesh):
    n = mesh.shape["tp"]
    ring = math.isqrt(n // 2)
    cores = n // (ring * ring)
    if ring != 4 or cores != 2:
        raise ValueError("needs a 4x4 torus")

    def local_grads(x_blk, dy_blk, wq_loc, w_k, w_v, wo_loc):
        model_dim, kv_heads, e = w_k.shape
        heads = wq_loc.shape[1]
        hd = heads * e
        scale = e ** -0.5
        wq = jnp.transpose(wq_loc, (1, 2, 0)).reshape(hd, model_dim)
        wk = jnp.transpose(w_k, (1, 2, 0))
        wv = jnp.transpose(w_v, (1, 2, 0))
        wo = wo_loc.reshape(hd, model_dim)
        dx, dwq, dwo, dwk, dwv, _, _ = _layer(ring, cores, heads, scale, x_blk, dy_blk, wq, wk, wv, wo)
        return (dx, jnp.transpose(dwq.reshape(heads, e, model_dim), (2, 0, 1)), dwo.reshape(heads, e, model_dim), dwk.T, dwv.T)

    tok = P(("dp", "tp"))
    return jax.shard_map(
        local_grads,
        mesh=mesh,
        in_specs=(tok, tok, P(None, "tp", None), P(), P(), P("tp")),
        out_specs=(tok, P("dp", "tp", None), tok, tok, tok),
        check_vma=False,
    )
```

```python
import functools
import math

import jax
import jax.numpy as jnp
from jax import lax
from jax.experimental import pallas as pl
from jax.experimental.pallas import tpu as pltpu
from jax.sharding import PartitionSpec as P

F32 = jnp.float32
BF16 = jnp.bfloat16
MESH = pl.DeviceIdType.MESH
ANY = pl.BlockSpec(memory_space=pl.ANY)
VMEM = pl.BlockSpec(memory_space=pltpu.VMEM)
LOG2E = math.log2(math.e)


def _scoped(fn):
    def run(*args, **kw):
        with jax.named_scope(fn.__name__):
            return fn(*args, **kw)

    return run


def _dot(a, b, dims):
    return lax.dot_general(a, b, (dims, ((), ())), preferred_element_type=F32)


def _nn(a, b):
    return _dot(a, b, ((1,), (0,)))


def _nt(a, b):
    return _dot(a, b, ((1,), (1,)))


class Place:
    def __init__(self, ring, cores):
        me = lax.axis_index("tp")
        self.ring, self.cores = ring, cores
        self.c = lax.rem(me, cores)
        self.x = lax.rem(me // cores, ring)
        self.y = me // (cores * ring)
        self.r = self.x * cores + self.c
        self.n_row = ring * cores

    def dev(self, y, x, c):
        y = lax.rem(y + self.ring, self.ring)
        x = lax.rem(x + self.ring, self.ring)
        return {"tp": (y * self.ring + x) * self.cores + c}

    def row_dev(self, r):
        return {"tp": self.y * self.n_row + r}

    def slot(self, x, c):
        return lax.rem(x + self.ring, self.ring) * self.cores + c


def _remote(src, dst, send, recv, dev):
    return pltpu.make_async_remote_copy(
        src_ref=src, dst_ref=dst, send_sem=send, recv_sem=recv, device_id=dev, device_id_type=MESH
    )


@_scoped
def _enter(devices):
    barrier = pltpu.get_barrier_semaphore()
    for dev in devices:
        pl.semaphore_signal(barrier, inc=1, device_id=dev, device_id_type=MESH)
    pl.semaphore_wait(barrier, len(devices))


OWN, MINUS, PLUS, FAR = range(4)
STEP = (0, -1, 1, 2)


def _load_shard(at, full, n, y, x, core, block, sem):
    r0 = at.dev(y, x, core)["tp"] * n
    b0 = at.slot(x, core) * n
    src = full.at[pl.ds(pl.multiple_of(r0, n), n), :]
    return pltpu.make_async_copy(src, block.at[pl.ds(pl.multiple_of(b0, n), n), :], sem)


@_scoped
def _take_row(lanes, t, y, block, sem):
    at, full, n = lanes[0].at, lanes[0].full, lanes[0].shard
    for j in range(4):
        _load_shard(at, full, n, y, at.x + STEP[j], at.c, block, sem).start()
    for j in range(4):
        for g in lanes:
            g.await_mate(t, j)
        _load_shard(at, full, n, y, at.x + STEP[j], 1 - at.c, block, sem).start()


class Gather:
    def __init__(self, at, src, full, send, recv, mate_recv, orders, row0, rows, tag):
        self.at, self.src, self.full = at, src, full
        self.send, self.recv, self.mate_recv = send.at[tag], recv.at[tag], mate_recv.at[tag]
        self.order, self.mate_order = orders
        self.row0, self.rows, self.shard = row0, rows, src.shape[0]
        self.sent = []
        c, o = at.c, self.order
        self.first = {s: at.dev(at.y + o * s, at.x + (1 - o) * s, c) for s in (1, -1)}
        self.second = {s: at.dev(at.y + (1 - o) * s, at.x + o * s, c) for s in (1, -1)}
        self.mate = at.dev(at.y, at.x, 1 - c)
        self.fulls = {d: self.both_ways(self.second, d, lambda to, d=d: (d, to)) for d in range(4)}

    def span(self, half):
        n = self.rows if half is None else self.rows // 2
        return self.row0 + (0 if half is None else half * n), n

    def ref(self, d1, d2, half=None):
        at, o = self.at, self.order
        o1, o2 = STEP[d1], STEP[d2]
        start, n = self.span(half)
        r0 = at.dev(at.y + o * o1 + (1 - o) * o2, at.x + (1 - o) * o1 + o * o2, at.c)["tp"] * self.shard + start
        return self.full.at[pl.ds(pl.multiple_of(r0, math.gcd(self.shard, self.row0, n)), n), :]

    def push(self, src, dst, recv, dev):
        k = len(self.sent)
        self.sent.append(dst.shape[0])
        return _remote(src, dst, self.send.at[k], recv, dev)

    def out(self, d1, d2, half=None):
        if d1 == OWN and d2 == OWN:
            return self.src.at[pl.ds(*self.span(half)), :]
        return self.ref(d1, d2, half)

    def both_ways(self, devs, d1, name):
        copies = []
        for step in (0, 1):
            for s, to in ((1, MINUS), (-1, PLUS)):
                half = step if s == 1 else 1 - step
                copies.append(self.push(self.out(d1, OWN, half), self.ref(d1, OWN, half), self.recv.at[*name(to), half], devs[s]))
        return copies

    def to_mate(self, d1, d2):
        ref = self.ref(d1, d2)
        self.push(self.out(d1, d2), ref, self.mate_recv.at[d1, d2], self.mate).start()

    def arrived(self, d1, d2, half):
        ref = self.ref(d1, d2, half)
        _remote(ref, ref, self.send.at[0], self.recv.at[d1, d2, half], self.mate).wait_recv()

    @_scoped
    def start(self):
        for cp in self.both_ways(self.first, OWN, lambda to: (to, OWN)):
            cp.start()
        self.go(OWN)
        self.to_mate(OWN, OWN)

    def go(self, d1):
        for cp in self.fulls[d1]:
            cp.start()

    @_scoped
    def relay_first(self):
        for d, s, half in ((MINUS, 1, 0), (PLUS, -1, 1)):
            self.arrived(d, OWN, half)
            ref = self.ref(d, OWN, half)
            self.push(ref, ref, self.recv.at[FAR, OWN, half], self.first[s]).start()

    @_scoped
    def near_first(self):
        for d, half in ((MINUS, 1), (PLUS, 0)):
            self.arrived(d, OWN, half)
            self.to_mate(d, OWN)

    @_scoped
    def far_first(self):
        for half in (0, 1):
            self.arrived(FAR, OWN, half)
        self.to_mate(FAR, OWN)

    @_scoped
    def relay_second(self, d1):
        for d, s, half in ((MINUS, 1, 0), (PLUS, -1, 1)):
            self.arrived(d1, d, half)
            ref = self.ref(d1, d, half)
            self.push(ref, ref, self.recv.at[d1, FAR, half], self.second[s]).start()

    @_scoped
    def near_second(self, d1):
        for d, half in ((MINUS, 1), (PLUS, 0)):
            self.arrived(d1, d, half)
            self.to_mate(d1, d)

    @_scoped
    def far_second(self, d1):
        for half in (0, 1):
            self.arrived(d1, FAR, half)
        self.to_mate(d1, FAR)

    def await_mate(self, t, j):
        o = self.mate_order
        ref = self.full.at[pl.ds(0, self.rows), :]
        _remote(ref, ref, self.send.at[0], self.mate_recv.at[(1 - o) * j + o * t, (1 - o) * t + o * j], self.mate).wait_recv()

    @_scoped
    def drain(self):
        for k, n in enumerate(self.sent):
            ref = self.full.at[pl.ds(0, n), :]
            _remote(ref, ref, self.send.at[k], self.send.at[k], self.mate).wait_send()


def _kernel(ring, cores, heads, scale, bq, bs, bc, x_ref, dy_ref, w_ref, wk_ref, wv_ref, wo_ref,
            dx_ref, dwq_ref, dwo_ref, dwk_ref, dwv_ref, xf_ref, dyf_ref,
            gq, w_all, part, rs_half, rs_full, stage, hop_ref, qkvt_ref, dot_ref, dqt_ref, ot_ref, dk_ref, dv_ref, kn_ref, vn_ref,
            send, recv, mate_recv, w_send, w_recv, hop_recv, ld_sem, blk_sem,
            ag_send, ag_recv, rs_send, rs_recv, out_send, out_recv, in_sem, o_sem):
    at = Place(ring, cores)
    n_row = at.n_row
    hd = wo_ref.shape[0]
    e = hd // heads
    tokens, width = xf_ref.shape
    tb = tokens // ring
    cw = width // n_row
    gw = gq.shape[1] // n_row
    c = at.c
    shard = x_ref.shape[0]
    gx = Gather(at, x_ref, xf_ref, send, recv, mate_recv, (c, 1 - c), 0, shard, 0)
    gy = Gather(at, dy_ref, dyf_ref, send, recv, mate_recv, (c, 1 - c), 0, shard, 1)
    n_kv = wk_ref.shape[0] // ring
    per_kv = n_row // n_kv
    row_peers = [lax.rem(at.r + d, n_row) for d in range(1, n_row)]
    up, down = at.dev(at.y + 1, at.x, c), at.dev(at.y - 1, at.x, c)

    hh = hd // 2

    def w_push(k, src, dst, rsem, dev):
        _remote(src, dst, w_send.at[k], rsem, dev).start()

    def wq_slot(slot, half=None):
        r0 = slot * gw + (0 if half is None else half * hh)
        return w_all.at[pl.ds(r0 if isinstance(r0, int) else pl.multiple_of(r0, hh), hd if half is None else hh), :]

    def wcols(slot):
        return pl.ds(pl.multiple_of(slot * cw, cw), cw)

    right, left, mate = at.dev(at.y, at.x + 1, c), at.dev(at.y, at.x - 1, c), at.dev(at.y, at.x, 1 - c)

    @_scoped
    def w_start():
        for half, dev in ((0, right), (1, left)):
            for k in range(cores):
                w_push(half * 2 + k, w_ref.at[pl.ds(half * hh, hh), wcols(at.slot(at.x + 2, k))], hop_ref.at[half * 2 + k], hop_recv.at[half * 2 + k], dev)
        w_push(4, w_ref.at[pl.ds(0, hd), wcols(at.slot(at.x, 1 - c))], wq_slot(at.r), w_recv.at[0], mate)
        for i, s in enumerate((1, -1)):
            for k in range(cores):
                dst_core = c if k == 0 else 1 - c
                w_push(5 + 2 * i + k, w_ref.at[pl.ds(0, hd), wcols(at.slot(at.x + s, dst_core))], wq_slot(at.r), w_recv.at[1 + 2 * i + k], at.dev(at.y, at.x + s, dst_core))

    @_scoped
    def w_relay():
        for half, s in ((0, 1), (1, -1)):
            for n in (half * 2, half * 2 + 1):
                _remote(hop_ref.at[n], hop_ref.at[n], w_send.at[0], hop_recv.at[n], mate).wait_recv()
            for k in range(cores):
                n = half * 2 + k
                src_slot = at.slot(at.x - s, c)
                same = k == 0
                dst_core = c if same else 1 - c
                w_push(9 + n, hop_ref.at[half * 2 + dst_core], wq_slot(src_slot, half), w_recv.at[5 + n], at.dev(at.y, at.x + s, dst_core))

    @_scoped
    def w_finish():
        whole = wq_slot(0)
        piece = wq_slot(0, 0)
        for n in range(9):
            ref = whole if n < 5 else piece
            _remote(ref, ref, w_send.at[0], w_recv.at[n], mate).wait_recv()

    def w_drain():
        whole = wq_slot(0)
        piece = wq_slot(0, 0)
        for k in range(13):
            ref = whole if 4 <= k < 9 else piece
            _remote(ref, ref, w_send.at[k], w_send.at[k], mate).wait_send()

    own_cols = wcols(at.r)
    rows = x_ref.shape[0]
    own_rows = pl.ds(pl.multiple_of((at.y * n_row + at.r) * rows, rows), rows)

    keep = [pltpu.make_async_copy(w_ref.at[:, own_cols], wq_slot(at.r), ld_sem.at[8])]
    for r in range(n_row):
        kv_r = at.y * n_kv + r // per_kv
        for i, w in enumerate((wk_ref, wv_ref)):
            keep.append(pltpu.make_async_copy(w.at[kv_r, :, own_cols], w_all.at[pl.ds(r * gw + hd + i * e, e), :], ld_sem.at[9 + 2 * r + i]))

    def front(w_v, wo_v, xblk):
        kv = (at.y * n_row + at.r) // (n_row * ring // wk_ref.shape[0])
        loads = [
            pltpu.make_async_copy(w_ref, w_v.at[pl.ds(0, hd), :], ld_sem.at[0]),
            pltpu.make_async_copy(wo_ref, wo_v, ld_sem.at[1]),
            pltpu.make_async_copy(wk_ref.at[kv], w_v.at[pl.ds(hd, e), :], ld_sem.at[6]),
            pltpu.make_async_copy(wv_ref.at[kv], w_v.at[pl.ds(hd + e, e), :], ld_sem.at[7]),
        ]
        ins = [pltpu.make_async_copy(src, xblk.at[pl.ds(i * rows, rows), :], ld_sem.at[2 + i]) for i, src in enumerate((x_ref, dy_ref))]
        outs = [pltpu.make_async_copy(xblk.at[pl.ds(i * rows, rows), :], dst.at[own_rows, :], ld_sem.at[4 + i]) for i, dst in enumerate((xf_ref, dyf_ref))]
        for cp in ins:
            cp.start()
        _enter([up, down] + [at.row_dev(r) for r in row_peers])
        gx.start()
        for cp in loads + keep:
            cp.start()
        for cp in ins:
            cp.wait()
        for cp in outs:
            cp.start()

        dk_ref[...] = jnp.zeros_like(dk_ref)
        dv_ref[...] = jnp.zeros_like(dv_ref)

        @_scoped
        def project(w, out, b):
            pltpu.make_async_copy(xf_ref.at[pl.ds(0, tb), :], xblk, blk_sem.at[0]).wait()

            def block(i, _):
                r0 = pl.multiple_of(i * bq, bq)
                out[:, pl.ds(pl.multiple_of(b * tb + i * bq, bq), bq)] = _nt(w[...], xblk[pl.ds(r0, bq), :]).astype(BF16)
                return 0

            lax.fori_loop(0, tb // bq, block, 0)

        def row_at(t):
            if isinstance(t, int):
                return lax.rem(at.y + STEP[t] + ring, ring)
            off = jnp.where(t == 1, ring - 1, jnp.where(t == 2, 1, jnp.where(t == 3, 2, 0)))
            return lax.rem(at.y + off, ring)

        for cp in loads + outs:
            cp.wait()

        def begin(g):
            g.relay_first()
            g.near_first()
            g.go(MINUS)

            @pl.when(g.order == 0)
            def _():
                g.go(PLUS)

        def begin_far(g):
            g.far_first()

            @pl.when(g.order == 0)
            def _():
                g.go(FAR)

        def begin_second(g):
            g.relay_second(OWN)

            @pl.when(g.order == 1)
            def _():
                g.go(PLUS)

            g.near_second(OWN)

        def second_minus(g):
            g.relay_second(MINUS)

            @pl.when(g.order == 1)
            def _():
                g.go(FAR)

            g.near_second(MINUS)

        def x_turn(t, _):
            @pl.when(t == 0)
            def _():
                begin(gx)
                begin_far(gx)
                begin_second(gx)
                second_minus(gx)
                gx.relay_second(PLUS)
                gx.near_second(PLUS)
                gx.relay_second(FAR)
                gy.start()
                gx.far_second(OWN)

            @pl.when(t == 1)
            def _():
                gx.near_second(FAR)
                gx.far_second(MINUS)

            @pl.when(t == 2)
            def _():
                for d in (PLUS, FAR):
                    gx.far_second(d)

            @pl.when(t == 3)
            def _():
                begin(gy)

            b = row_at(t)
            _take_row((gx,), t, b, xblk, blk_sem.at[0])
            project(w_v, qkvt_ref, b)
            return 0

        lax.fori_loop(0, ring, x_turn, 0)
        for t in range(0, tokens, bq):
            kn_ref[t:t + bq, :] = qkvt_ref[hd:hd + e, t:t + bq].T
            vn_ref[t:t + bq, :] = qkvt_ref[hd + e:hd + 2 * e, t:t + bq].T

        keys_k, keys_v = slice(hd, hd + e), slice(hd + e, hd + 2 * e)
        m4 = heads * bs
        factor = scale * LOG2E

        def row_chunks(k):
            return [slice(t, t + bq) for t in range(0, (k + 1) * tb, bq)]

        def stacked(ref, qs):
            return jnp.concatenate([ref[h * e:(h + 1) * e, qs] for h in range(heads)], axis=1)

        def unstack(ref, qs, value):
            for h in range(heads):
                ref[h * e:(h + 1) * e, qs] = value[:, h * bs:(h + 1) * bs]

        def scores(q, ks, k, j):
            s = _nn(q, qkvt_ref[keys_k, ks])
            if ks.start < k * tb:
                return s
            row = lax.broadcasted_iota(jnp.int32, (m4, bq), 0) & (bs - 1)
            col = lax.broadcasted_iota(jnp.int32, (m4, bq), 1)
            return jnp.where(col + (ks.start - k * tb) <= row + j * bs, s, -jnp.inf)

        def folded(op, total, value):
            for t in range(0, value.shape[1], 128):
                piece = value[:, t:t + 128]
                total = piece if total is None else op(total, piece)
            return total

        def score_buf(ks):
            n = ks.start // cw
            return part.at[n, :, ks.start - n * cw:ks.stop - n * cw]

        def stats_buf(k, j):
            per = cw // 128
            n = k * (tb // bs)
            return part.at[2 + n // per, :, pl.ds(pl.multiple_of((n % per + j) * 128, 128), 128)]

        @_scoped
        def forward(k):
            chunks = row_chunks(k)

            def queries(j, _):
                qs = pl.ds(pl.multiple_of(k * tb + j * bs, bs), bs)
                q = stacked(qkvt_ref, qs).T
                m = None
                for ks in chunks:
                    s = scores(q, ks, k, j)
                    score_buf(ks)[...] = s
                    m = folded(jnp.maximum, m, s)
                m = jnp.max(m, axis=1, keepdims=True)
                total = None
                for ks in chunks:
                    p = jnp.exp2((score_buf(ks)[...] - m) * factor)
                    score_buf(ks)[...] = p
                    total = folded(jnp.add, total, p)
                inv = 1.0 / jnp.sum(total, axis=1, keepdims=True)
                lane = lax.broadcasted_iota(jnp.int32, (m4, 128), 1)
                stats_buf(k, j)[...] = jnp.where(lane == 0, m, inv)
                out = None
                for ks in chunks:
                    piece = _nn((score_buf(ks)[...] * inv).astype(BF16), vn_ref[ks, :])
                    out = piece if out is None else out + piece
                unstack(ot_ref, qs, out.astype(BF16).T)
                return 0

            lax.fori_loop(0, tb // bs, queries, 0)

        @_scoped
        def backward(k):
            chunks = row_chunks(k)

            def queries(j, _):
                qs = pl.ds(pl.multiple_of(k * tb + j * bs, bs), bs)
                qt = stacked(qkvt_ref, qs)
                dot = stacked(dot_ref, qs)
                q, do = qt.T, dot.T
                delta = jnp.sum(dot.astype(F32) * stacked(ot_ref, qs).astype(F32), axis=0, keepdims=True)
                delta = jnp.broadcast_to(delta, (128, m4)).T[:, :1]
                stats = stats_buf(k, j)[...]
                m, inv = stats[:, 0:1], stats[:, 1:2]
                dq = None
                for ks in chunks:
                    p = jnp.exp2((scores(q, ks, k, j) - m) * factor) * inv
                    dp = _nn(do, qkvt_ref[keys_v, ks])
                    ds = (p * (dp - delta)).astype(BF16)
                    dv_ref[:, ks] += _nn(dot, p.astype(BF16))
                    dk_ref[:, ks] += _nn(qt, ds)
                    piece = _nn(ds, kn_ref[ks, :])
                    dq = piece if dq is None else dq + piece
                dq = (dq * scale).astype(BF16).T
                unstack(dqt_ref, qs, dq)
                for h in range(0, heads, 2):
                    pair = jnp.concatenate([dq[:, h * bs:(h + 1) * bs], dq[:, (h + 1) * bs:(h + 2) * bs]], axis=0)
                    gq[qs, pl.ds(pl.multiple_of(at.r * gw + h * e, 128), 2 * e)] = pair.T
                return 0

            lax.fori_loop(0, tb // bs, queries, 0)

        forward(0)
        begin_far(gy)
        forward(1)
        begin_second(gy)
        forward(2)
        second_minus(gy)
        forward(3)

        def turn(t, _):
            @pl.when(t == 0)
            def _():
                @pl.when(c == 1)
                def _():
                    far_step(OWN)

            @pl.when(t == 1)
            def _():
                for d in (PLUS, FAR):
                    gy.relay_second(d)
                    gy.near_second(d)

                @pl.when(c == 1)
                def _():
                    far_step(MINUS)

                w_start()

            @pl.when(t == 2)
            def _():
                @pl.when(c == 1)
                def _():
                    far_step(PLUS)

                @pl.when(c == 0)
                def _():
                    far_step(OWN)
                    far_step(MINUS)

            b = row_at(t)

            @pl.when(t != 3)
            def _():
                _take_row((gy,), t, b, xblk, blk_sem.at[0])

            project(wo_v, dot_ref, b)

            @pl.when(t == 2)
            def _():
                @pl.when(c == 0)
                def _():
                    far_step(PLUS)

                far_step(FAR)
                w_relay()
                _take_row((gy,), FAR, row_at(FAR), xblk, blk_sem.at[0])

            for k in range(ring):
                @pl.when(b == k)
                def _(k=k):
                    backward(k)
            return 0

        far_cp = {d: gy.push(gy.ref(d, FAR), gy.ref(d, FAR), gy.mate_recv.at[d, FAR], gy.mate) for d in range(4)}

        @_scoped
        def far_step(d):
            for half in (0, 1):
                gy.arrived(d, FAR, half)
            far_cp[d].start()

        lax.fori_loop(0, ring, turn, 0)


    pl.run_scoped(front, pltpu.VMEM((hd + 2 * e, width), BF16), pltpu.VMEM((hd, width), BF16), pltpu.VMEM((tb, width), BF16))

    own_g = at.r * gw
    for k in range(0, tokens, bq):
        ks = slice(k, k + bq)
        kv = jnp.concatenate([(dk_ref[:, ks] * scale).astype(BF16), dv_ref[:, ks].astype(BF16)], axis=0)
        gq[ks, pl.ds(pl.multiple_of(own_g + hd, 128), 2 * e)] = kv.T

    def back(xbuf, obuf, kvt):
        th = tb // 2
        tq = th // 2
        tl = tb // n_row
        hw = cw // 2
        half_a, half_b = pl.ds(0, hw), pl.ds(hw, hw)
        units = [(FAR, 0), (FAR, 1), (PLUS, 0), (MINUS, 0), (PLUS, 1), (MINUS, 1), (OWN, 0), (OWN, 1)]
        s_own, s_left, s_right, s_far = (at.slot(at.x + o, c) for o in (0, -1, 1, 2))
        m_own, m_left, m_right, m_far = (at.slot(at.x + o, 1 - c) for o in (0, -1, 1, 2))

        def unit_row(u):
            d, s = units[u]
            return pl.multiple_of(lax.rem(at.y + STEP[d] + ring, ring) * tb + s * th, th)

        def gcols(slot):
            return pl.ds(pl.multiple_of(slot * gw, gw), gw)

        def piece(u, slot, half=None):
            r0 = unit_row(u)
            rows = pl.ds(r0, th) if half is None else pl.ds(pl.multiple_of(r0 + half * tq, tq), tq)
            return gq.at[rows, gcols(slot)]

        sends = []

        def ag_push(u, n, slot, dev, half=None):
            ref = piece(u, slot, half)
            cp = _remote(ref, ref, ag_send.at[u, n], ag_recv.at[u, n], dev)
            cp.start()
            sends.append(cp)

        def ag_wait(u, n, slot, half=None):
            ref = piece(u, slot, half)
            _remote(ref, ref, ag_send.at[u, n], ag_recv.at[u, n], mate).wait_recv()

        def ag_own(u):
            ag_push(u, 0, s_own, right)
            ag_push(u, 1, s_own, left)
            ag_push(u, 2, s_own, mate)

        @_scoped
        def ag_relay(u):
            ag_wait(u, 0, s_left)
            ag_push(u, 3, s_left, right, 0)
            ag_push(u, 4, s_left, mate)
            ag_wait(u, 1, s_right)
            ag_push(u, 5, s_right, left, 1)
            ag_push(u, 6, s_right, mate)

        @_scoped
        def ag_finish(u):
            ag_wait(u, 3, s_far, 0)
            ag_push(u, 7, s_far, mate, 0)
            ag_wait(u, 5, s_far, 1)
            ag_push(u, 8, s_far, mate, 1)
            ag_wait(u, 2, m_own)
            ag_wait(u, 4, m_left)
            ag_wait(u, 6, m_right)
            ag_wait(u, 7, m_far, 0)
            ag_wait(u, 8, m_far, 1)

        nt = min(256, hw)

        @_scoped
        def partial(u):
            rows = pl.ds(unit_row(u), th)
            d, s = units[u]
            dst = part.at[d, pl.ds(s * th, th), :]

            def tile(j, _):
                cs = pl.ds(pl.multiple_of(j * nt, nt), nt)
                dst[:, cs] = _nn(gq[rows, :], w_all[:, cs])
                return 0

            lax.fori_loop(0, cw // nt, tile, 0)

        def rs_push(n, s, src, dst, dev):
            cp = _remote(src, dst, rs_send.at[n, s], rs_recv.at[n, s], dev)
            cp.start()
            sends.append(cp)

        def rs_wait(n, s):
            ref = rs_half.at[0, s]
            _remote(ref, ref, rs_send.at[n, s], rs_recv.at[n, s], mate).wait_recv()

        def block(d, s, half):
            return part.at[d, pl.ds(s * th, th), half]

        def far_a(s):
            rs_push(0, s, block(FAR, s, half_a), rs_half.at[0, s], up)

        def far_b(s):
            rs_push(1, s, block(FAR, s, half_b), rs_half.at[1, s], down)

        def minus_a(s):
            rs_push(4, s, block(MINUS, s, half_a), rs_full.at[1, s, 0], down)

        def plus_b(s):
            rs_push(3, s, block(PLUS, s, half_b), rs_full.at[0, s, 1], up)

        @_scoped
        def plus_a(s):
            rs_wait(0, s)
            block(PLUS, s, half_a)[...] += rs_half[0, s]
            rs_push(2, s, block(PLUS, s, half_a), rs_full.at[0, s, 0], up)

        @_scoped
        def minus_b(s):
            rs_wait(1, s)
            block(MINUS, s, half_b)[...] += rs_half[1, s]
            rs_push(5, s, block(MINUS, s, half_b), rs_full.at[1, s, 1], down)

        n_steps = width // bc
        depth = xbuf.shape[0]

        def chunk(src, c0, j):
            slot = lax.rem(j, depth)
            return pltpu.make_async_copy(src.at[:, pl.ds(pl.multiple_of(c0 + j * bc, bc), bc)], xbuf.at[slot], in_sem.at[slot])

        def ahead(src, c0, n):
            for j in range(min(depth - 1, n)):
                chunk(src, c0, j).start()

        @_scoped
        def stream(src, lhs, out, j0, j1):
            def store(j):
                slot = lax.rem(j, 2)
                return pltpu.make_async_copy(obuf.at[slot], out.at[:, pl.ds(pl.multiple_of(j * bc, bc), bc)], o_sem.at[slot])

            if j0 == 0:
                ahead(src, 0, n_steps)

            def step(j, _):
                @pl.when(j + depth - 1 < n_steps)
                def _():
                    chunk(src, 0, j + depth - 1).start()

                chunk(src, 0, j).wait()

                @pl.when(j >= 2)
                def _():
                    store(j - 2).wait()

                obuf[lax.rem(j, 2)] = _nn(lhs[...], xbuf[lax.rem(j, depth)])
                store(j).start()
                return 0

            lax.fori_loop(j0, j1, step, 0)
            if j1 == n_steps:
                for j in range(max(n_steps - 2, 0), n_steps):
                    store(j).wait()

        def wo_steps(a, b):
            stream(dyf_ref, ot_ref, dwo_ref, n_steps * a // 16, n_steps * b // 16)

        def wq_steps(a, b):
            stream(xf_ref, dqt_ref, dwq_ref, n_steps * a // 16, n_steps * b // 16)

        first = (at.r // per_kv) * per_kv
        share = width // per_kv
        col0 = lax.rem(at.r, per_kv) * share

        def kv_step(j, _):
            @pl.when(j + depth - 1 < share // bc)
            def _():
                chunk(xf_ref, col0, j + depth - 1).start()

            chunk(xf_ref, col0, j).wait()
            prod = _nn(kvt[...], xbuf[lax.rem(j, depth)])
            dk = dv = None
            for q in range(per_kv):
                a = prod[q * 2 * e:q * 2 * e + e]
                b = prod[q * 2 * e + e:(q + 1) * 2 * e]
                dk = a if dk is None else dk + a
                dv = b if dv is None else dv + b
            cs = pl.ds(pl.multiple_of(j * bc, bc), bc)
            dwk_ref[:, cs] = dk
            dwv_ref[:, cs] = dv
            return 0

        @_scoped
        def kv_grads():
            ahead(xf_ref, col0, share // bc)
            for q in range(per_kv):
                cols = pl.ds(pl.multiple_of((first + q) * gw + hd, 128), gw - hd)
                for t in range(0, tokens, bq):
                    kvt[q * (gw - hd):(q + 1) * (gw - hd), t:t + bq] = gq[t:t + bq, cols].T
            lax.fori_loop(0, share // bc, kv_step, 0)

        per_half = n_row // 2

        def hand(i, r):
            half = (half_a, half_b)[i]
            rows = pl.ds(r * tl, tl)
            cols = pl.ds(pl.multiple_of(at.r * cw + i * hw, hw), hw)
            return stage.at[rows, half], dx_ref.at[:, cols]

        def hand_remote(i, r):
            src, dst = hand(i, r)
            d = lax.rem(r - at.r + n_row, n_row)
            return _remote(src, dst, out_send.at[i, r], out_recv.at[i, d], at.row_dev(r))

        def hand_local(i, r):
            src, dst = hand(i, r)
            return pltpu.make_async_copy(src, dst, out_send.at[i, r])

        @_scoped
        def finish(i, s):
            half = (half_a, half_b)[i]
            rs_wait(2 + i, s)
            rs_wait(4 + i, s)
            stage[s * th:(s + 1) * th, half] = (block(OWN, s, half)[...] + rs_full[0, s, i] + rs_full[1, s, i]).astype(BF16)
            for r in range(s * per_half, (s + 1) * per_half):
                @pl.when(at.r != r)
                def _(r=r):
                    hand_remote(i, r).start()

                @pl.when(at.r == r)
                def _(r=r):
                    hand_local(i, r).start()

        @_scoped
        def received(i):
            for d in range(1, n_row):
                src = lax.rem(at.r + n_row - d, n_row)
                ref = dx_ref.at[:, pl.ds(pl.multiple_of(src * cw + i * hw, hw), hw)]
                _remote(ref, ref, out_send.at[i, 0], out_recv.at[i, d], mate).wait_recv()
            for r in range(n_row):
                @pl.when(at.r != r)
                def _(r=r):
                    hand_remote(i, r).wait_send()

                @pl.when(at.r == r)
                def _(r=r):
                    hand_local(i, r).wait()

        ag_own(0)
        wo_steps(0, 6)
        ag_relay(0)
        ag_own(1)
        ag_own(2)
        wo_steps(6, 9)
        ag_relay(1)
        ag_own(3)
        ag_finish(0)
        for cp in keep:
            cp.wait()
        w_finish()
        partial(0)
        far_a(0)
        far_b(0)
        ag_relay(2)
        ag_own(4)
        wo_steps(9, 10)
        ag_finish(1)
        partial(1)
        far_a(1)
        far_b(1)
        ag_relay(3)
        ag_own(5)
        wo_steps(10, 11)
        ag_finish(2)
        partial(2)
        ag_relay(4)
        ag_own(6)
        plus_a(0)
        wo_steps(11, 12)
        ag_finish(3)
        partial(3)
        minus_a(0)
        ag_relay(5)
        ag_own(7)
        wo_steps(12, 13)
        ag_finish(4)
        partial(4)
        plus_a(1)
        plus_b(0)
        ag_relay(6)
        wo_steps(13, 14)
        ag_finish(5)
        partial(5)
        minus_a(1)
        minus_b(0)
        plus_b(1)
        minus_b(1)
        ag_relay(7)
        wo_steps(14, 16)
        ag_finish(6)
        partial(6)
        wq_steps(0, 2)
        ag_finish(7)
        partial(7)
        wq_steps(2, 5)
        finish(0, 0)
        wq_steps(5, 12)
        finish(0, 1)
        wq_steps(12, 16)
        kv_grads()
        finish(1, 0)
        received(0)
        finish(1, 1)
        received(1)
        for cp in sends:
            cp.wait_send()
        w_drain()
        for g in (gx, gy):
            g.drain()

    pl.run_scoped(back, pltpu.VMEM((4, tokens, bc), BF16), pltpu.VMEM((2, hd, bc), F32), pltpu.VMEM((per_kv * 2 * e, tokens), BF16))


def _layer(ring, cores, heads, scale, x, dy, wq, wk, wv, wo):
    rows, width = x.shape
    tokens = rows * ring * ring * cores
    hd = wo.shape[0]
    e = hd // heads
    n_row = ring * cores
    cw = width // n_row
    gw = hd + 2 * e
    tb = tokens // ring
    th, hw = tb // 2, cw // 2
    per_kv = n_row * ring // wk.shape[0]
    bq = min(256, tb)
    bs = tb // heads
    bc = min(512, cw // 2)
    dma = pltpu.SemaphoreType.DMA
    shape = jax.ShapeDtypeStruct
    return pl.pallas_call(
        functools.partial(_kernel, ring, cores, heads, scale, bq, bs, bc),
        name="layer",
        in_specs=[ANY] * 6,
        out_specs=[ANY, ANY, ANY, VMEM, VMEM, ANY, ANY],
        out_shape=[
            shape((rows, width), BF16),
            shape((hd, width), F32),
            shape((hd, width), F32),
            shape((e, width // per_kv), F32),
            shape((e, width // per_kv), F32),
            shape((tokens, width), BF16),
            shape((tokens, width), BF16),
        ],
        scratch_shapes=[
            pltpu.VMEM((tokens, n_row * gw), BF16),
            pltpu.VMEM((n_row * gw, cw), BF16),
            pltpu.VMEM((4, tb, cw), F32),
            pltpu.VMEM((2, 2, th, hw), F32),
            pltpu.VMEM((2, 2, 2, th, hw), F32),
            pltpu.VMEM((tb, cw), BF16),
            pltpu.VMEM((4, hd // 2, cw), BF16),
            pltpu.VMEM((gw, tokens), BF16),
            pltpu.VMEM((hd, tokens), BF16),
            pltpu.VMEM((hd, tokens), BF16),
            pltpu.VMEM((hd, tokens), BF16),
            pltpu.VMEM((e, tokens), F32),
            pltpu.VMEM((e, tokens), F32),
            pltpu.VMEM((tokens, e), BF16),
            pltpu.VMEM((tokens, e), BF16),
            dma((2, 48)),
            dma((2, 4, 4, 2)),
            dma((2, 4, 4)),
            dma((13,)),
            dma((9,)),
            dma((4,)),
            dma((9 + 2 * n_row,)),
            dma((1,)),
            dma((8, 9)),
            dma((8, 9)),
            dma((6, 2)),
            dma((6, 2)),
            dma((2, n_row)),
            dma((2, n_row)),
            dma((4,)),
            dma((2,)),
        ],
        compiler_params=pltpu.CompilerParams(collective_id=0, has_side_effects=True, vmem_limit_bytes=67043328),
        cost_estimate=pl.CostEstimate(flops=70 * 10**9, bytes_accessed=300 << 20, transcendentals=heads * tokens * tokens // 2),
    )(x, dy, wq, wk, wv, wo)


def solution(mesh):
    n = mesh.shape["tp"]
    ring = math.isqrt(n // 2)
    cores = n // (ring * ring)
    if ring != 4 or cores != 2:
        raise ValueError("needs a 4x4 torus")

    def local_grads(x_blk, dy_blk, wq_loc, w_k, w_v, wo_loc):
        model_dim, kv_heads, e = w_k.shape
        heads = wq_loc.shape[1]
        hd = heads * e
        scale = e ** -0.5
        wq = jnp.transpose(wq_loc, (1, 2, 0)).reshape(hd, model_dim)
        wk = jnp.transpose(w_k, (1, 2, 0))
        wv = jnp.transpose(w_v, (1, 2, 0))
        wo = wo_loc.reshape(hd, model_dim)
        dx, dwq, dwo, dwk, dwv, _, _ = _layer(ring, cores, heads, scale, x_blk, dy_blk, wq, wk, wv, wo)
        return (dx, jnp.transpose(dwq.reshape(heads, e, model_dim), (2, 0, 1)), dwo.reshape(heads, e, model_dim), dwk.T, dwv.T)

    tok = P(("dp", "tp"))
    return jax.shard_map(
        local_grads,
        mesh=mesh,
        in_specs=(tok, tok, P(None, "tp", None), P(), P(), P("tp")),
        out_specs=(tok, P("dp", "tp", None), tok, tok, tok),
        check_vma=False,
    )
```

```python
import functools
import math

import jax
import jax.numpy as jnp
from jax import lax
from jax.experimental import pallas as pl
from jax.experimental.pallas import tpu as pltpu
from jax.sharding import PartitionSpec as P

F32 = jnp.float32
BF16 = jnp.bfloat16
MESH = pl.DeviceIdType.MESH
ANY = pl.BlockSpec(memory_space=pl.ANY)
VMEM = pl.BlockSpec(memory_space=pltpu.VMEM)
LOG2E = math.log2(math.e)


def _scoped(fn):
    def run(*args, **kw):
        with jax.named_scope(fn.__name__):
            return fn(*args, **kw)

    return run


def _dot(a, b, dims):
    return lax.dot_general(a, b, (dims, ((), ())), preferred_element_type=F32)


def _nn(a, b):
    return _dot(a, b, ((1,), (0,)))


def _nt(a, b):
    return _dot(a, b, ((1,), (1,)))


class Place:
    def __init__(self, ring, cores):
        me = lax.axis_index("tp")
        self.ring, self.cores = ring, cores
        self.c = lax.rem(me, cores)
        self.x = lax.rem(me // cores, ring)
        self.y = me // (cores * ring)
        self.r = self.x * cores + self.c
        self.n_row = ring * cores

    def dev(self, y, x, c):
        y = lax.rem(y + self.ring, self.ring)
        x = lax.rem(x + self.ring, self.ring)
        return {"tp": (y * self.ring + x) * self.cores + c}

    def row_dev(self, r):
        return {"tp": self.y * self.n_row + r}

    def slot(self, x, c):
        return lax.rem(x + self.ring, self.ring) * self.cores + c


def _remote(src, dst, send, recv, dev):
    return pltpu.make_async_remote_copy(
        src_ref=src, dst_ref=dst, send_sem=send, recv_sem=recv, device_id=dev, device_id_type=MESH
    )


@_scoped
def _enter(devices):
    barrier = pltpu.get_barrier_semaphore()
    for dev in devices:
        pl.semaphore_signal(barrier, inc=1, device_id=dev, device_id_type=MESH)
    pl.semaphore_wait(barrier, len(devices))


OWN, MINUS, PLUS, FAR = range(4)
STEP = (0, -1, 1, 2)


def _load_shard(at, full, n, y, x, core, block, sem):
    r0 = at.dev(y, x, core)["tp"] * n
    b0 = at.slot(x, core) * n
    src = full.at[pl.ds(pl.multiple_of(r0, n), n), :]
    return pltpu.make_async_copy(src, block.at[pl.ds(pl.multiple_of(b0, n), n), :], sem)


@_scoped
def _take_row(lanes, t, y, block, sem):
    at, full, n = lanes[0].at, lanes[0].full, lanes[0].shard
    for j in range(4):
        _load_shard(at, full, n, y, at.x + STEP[j], at.c, block, sem).start()
    for j in range(4):
        for g in lanes:
            g.await_mate(t, j)
        _load_shard(at, full, n, y, at.x + STEP[j], 1 - at.c, block, sem).start()


class Gather:
    def __init__(self, at, src, full, send, recv, mate_recv, orders, row0, rows, tag):
        self.at, self.src, self.full = at, src, full
        self.send, self.recv, self.mate_recv = send.at[tag], recv.at[tag], mate_recv.at[tag]
        self.order, self.mate_order = orders
        self.row0, self.rows, self.shard = row0, rows, src.shape[0]
        self.sent = []
        c, o = at.c, self.order
        self.first = {s: at.dev(at.y + o * s, at.x + (1 - o) * s, c) for s in (1, -1)}
        self.second = {s: at.dev(at.y + (1 - o) * s, at.x + o * s, c) for s in (1, -1)}
        self.mate = at.dev(at.y, at.x, 1 - c)
        self.fulls = {d: self.both_ways(self.second, d, lambda to, d=d: (d, to)) for d in range(4)}

    def span(self, half):
        n = self.rows if half is None else self.rows // 2
        return self.row0 + (0 if half is None else half * n), n

    def ref(self, d1, d2, half=None):
        at, o = self.at, self.order
        o1, o2 = STEP[d1], STEP[d2]
        start, n = self.span(half)
        r0 = at.dev(at.y + o * o1 + (1 - o) * o2, at.x + (1 - o) * o1 + o * o2, at.c)["tp"] * self.shard + start
        return self.full.at[pl.ds(pl.multiple_of(r0, math.gcd(self.shard, self.row0, n)), n), :]

    def push(self, src, dst, recv, dev):
        k = len(self.sent)
        self.sent.append(dst.shape[0])
        return _remote(src, dst, self.send.at[k], recv, dev)

    def out(self, d1, d2, half=None):
        if d1 == OWN and d2 == OWN:
            return self.src.at[pl.ds(*self.span(half)), :]
        return self.ref(d1, d2, half)

    def both_ways(self, devs, d1, name):
        copies = []
        for step in (0, 1):
            for s, to in ((1, MINUS), (-1, PLUS)):
                half = step if s == 1 else 1 - step
                copies.append(self.push(self.out(d1, OWN, half), self.ref(d1, OWN, half), self.recv.at[*name(to), half], devs[s]))
        return copies

    def to_mate(self, d1, d2):
        ref = self.ref(d1, d2)
        self.push(self.out(d1, d2), ref, self.mate_recv.at[d1, d2], self.mate).start()

    def arrived(self, d1, d2, half):
        ref = self.ref(d1, d2, half)
        _remote(ref, ref, self.send.at[0], self.recv.at[d1, d2, half], self.mate).wait_recv()

    @_scoped
    def start(self):
        for cp in self.both_ways(self.first, OWN, lambda to: (to, OWN)):
            cp.start()
        self.go(OWN)
        self.to_mate(OWN, OWN)

    def go(self, d1):
        for cp in self.fulls[d1]:
            cp.start()

    @_scoped
    def relay_first(self):
        for d, s, half in ((MINUS, 1, 0), (PLUS, -1, 1)):
            self.arrived(d, OWN, half)
            ref = self.ref(d, OWN, half)
            self.push(ref, ref, self.recv.at[FAR, OWN, half], self.first[s]).start()

    @_scoped
    def near_first(self):
        for d, half in ((MINUS, 1), (PLUS, 0)):
            self.arrived(d, OWN, half)
            self.to_mate(d, OWN)

    @_scoped
    def far_first(self):
        for half in (0, 1):
            self.arrived(FAR, OWN, half)
        self.to_mate(FAR, OWN)

    @_scoped
    def relay_second(self, d1):
        for d, s, half in ((MINUS, 1, 0), (PLUS, -1, 1)):
            self.arrived(d1, d, half)
            ref = self.ref(d1, d, half)
            self.push(ref, ref, self.recv.at[d1, FAR, half], self.second[s]).start()

    @_scoped
    def near_second(self, d1):
        for d, half in ((MINUS, 1), (PLUS, 0)):
            self.arrived(d1, d, half)
            self.to_mate(d1, d)

    @_scoped
    def far_second(self, d1):
        for half in (0, 1):
            self.arrived(d1, FAR, half)
        self.to_mate(d1, FAR)

    def await_mate(self, t, j):
        o = self.mate_order
        ref = self.full.at[pl.ds(0, self.rows), :]
        _remote(ref, ref, self.send.at[0], self.mate_recv.at[(1 - o) * j + o * t, (1 - o) * t + o * j], self.mate).wait_recv()

    @_scoped
    def drain(self):
        for k, n in enumerate(self.sent):
            ref = self.full.at[pl.ds(0, n), :]
            _remote(ref, ref, self.send.at[k], self.send.at[k], self.mate).wait_send()


def _kernel(ring, cores, heads, scale, bq, bs, bc, x_ref, dy_ref, w_ref, wk_ref, wv_ref, wo_ref,
            dx_ref, dwq_ref, dwo_ref, dwk_ref, dwv_ref, xf_ref, dyf_ref,
            gq, w_all, part, rs_half, rs_full, stage, hop_ref, qkvt_ref, dot_ref, dqt_ref, ot_ref, dk_ref, dv_ref, kn_ref, vn_ref,
            send, recv, mate_recv, w_send, w_recv, hop_recv, ld_sem, blk_sem,
            ag_send, ag_recv, rs_send, rs_recv, out_send, out_recv, in_sem, o_sem):
    at = Place(ring, cores)
    n_row = at.n_row
    hd = wo_ref.shape[0]
    e = hd // heads
    tokens, width = xf_ref.shape
    tb = tokens // ring
    cw = width // n_row
    gw = gq.shape[1] // n_row
    c = at.c
    shard = x_ref.shape[0]
    gx = Gather(at, x_ref, xf_ref, send, recv, mate_recv, (c, 1 - c), 0, shard, 0)
    split = shard * 3 // 4
    gy = Gather(at, dy_ref, dyf_ref, send, recv, mate_recv, (c, 1 - c), 0, split, 1)
    gz = Gather(at, dy_ref, dyf_ref, send, recv, mate_recv, (0, 0), split, shard - split, 2)
    n_kv = wk_ref.shape[0] // ring
    per_kv = n_row // n_kv
    row_peers = [lax.rem(at.r + d, n_row) for d in range(1, n_row)]
    up, down = at.dev(at.y + 1, at.x, c), at.dev(at.y - 1, at.x, c)

    hh = hd // 2

    def w_push(k, src, dst, rsem, dev):
        _remote(src, dst, w_send.at[k], rsem, dev).start()

    def wq_slot(slot, half=None):
        r0 = slot * gw + (0 if half is None else half * hh)
        return w_all.at[pl.ds(r0 if isinstance(r0, int) else pl.multiple_of(r0, hh), hd if half is None else hh), :]

    def wcols(slot):
        return pl.ds(pl.multiple_of(slot * cw, cw), cw)

    right, left, mate = at.dev(at.y, at.x + 1, c), at.dev(at.y, at.x - 1, c), at.dev(at.y, at.x, 1 - c)

    @_scoped
    def w_start():
        for half, dev in ((0, right), (1, left)):
            for k in range(cores):
                w_push(half * 2 + k, w_ref.at[pl.ds(half * hh, hh), wcols(at.slot(at.x + 2, k))], hop_ref.at[half * 2 + k], hop_recv.at[half * 2 + k], dev)
        w_push(4, w_ref.at[pl.ds(0, hd), wcols(at.slot(at.x, 1 - c))], wq_slot(at.r), w_recv.at[0], mate)
        for i, s in enumerate((1, -1)):
            for k in range(cores):
                dst_core = c if k == 0 else 1 - c
                w_push(5 + 2 * i + k, w_ref.at[pl.ds(0, hd), wcols(at.slot(at.x + s, dst_core))], wq_slot(at.r), w_recv.at[1 + 2 * i + k], at.dev(at.y, at.x + s, dst_core))

    @_scoped
    def w_relay():
        for half, s in ((0, 1), (1, -1)):
            for n in (half * 2, half * 2 + 1):
                _remote(hop_ref.at[n], hop_ref.at[n], w_send.at[0], hop_recv.at[n], mate).wait_recv()
            for k in range(cores):
                n = half * 2 + k
                src_slot = at.slot(at.x - s, c)
                same = k == 0
                dst_core = c if same else 1 - c
                w_push(9 + n, hop_ref.at[half * 2 + dst_core], wq_slot(src_slot, half), w_recv.at[5 + n], at.dev(at.y, at.x + s, dst_core))

    @_scoped
    def w_finish():
        whole = wq_slot(0)
        piece = wq_slot(0, 0)
        for n in range(9):
            ref = whole if n < 5 else piece
            _remote(ref, ref, w_send.at[0], w_recv.at[n], mate).wait_recv()

    def w_drain():
        whole = wq_slot(0)
        piece = wq_slot(0, 0)
        for k in range(13):
            ref = whole if 4 <= k < 9 else piece
            _remote(ref, ref, w_send.at[k], w_send.at[k], mate).wait_send()

    own_cols = wcols(at.r)
    rows = x_ref.shape[0]
    own_rows = pl.ds(pl.multiple_of((at.y * n_row + at.r) * rows, rows), rows)

    keep = [pltpu.make_async_copy(w_ref.at[:, own_cols], wq_slot(at.r), ld_sem.at[8])]
    for r in range(n_row):
        kv_r = at.y * n_kv + r // per_kv
        for i, w in enumerate((wk_ref, wv_ref)):
            keep.append(pltpu.make_async_copy(w.at[kv_r, :, own_cols], w_all.at[pl.ds(r * gw + hd + i * e, e), :], ld_sem.at[9 + 2 * r + i]))

    def front(w_v, wo_v, xblk):
        kv = (at.y * n_row + at.r) // (n_row * ring // wk_ref.shape[0])
        loads = [
            pltpu.make_async_copy(w_ref, w_v.at[pl.ds(0, hd), :], ld_sem.at[0]),
            pltpu.make_async_copy(wo_ref, wo_v, ld_sem.at[1]),
            pltpu.make_async_copy(wk_ref.at[kv], w_v.at[pl.ds(hd, e), :], ld_sem.at[6]),
            pltpu.make_async_copy(wv_ref.at[kv], w_v.at[pl.ds(hd + e, e), :], ld_sem.at[7]),
        ]
        ins = [pltpu.make_async_copy(src, xblk.at[pl.ds(i * rows, rows), :], ld_sem.at[2 + i]) for i, src in enumerate((x_ref, dy_ref))]
        outs = [pltpu.make_async_copy(xblk.at[pl.ds(i * rows, rows), :], dst.at[own_rows, :], ld_sem.at[4 + i]) for i, dst in enumerate((xf_ref, dyf_ref))]
        for cp in ins:
            cp.start()
        _enter([up, down] + [at.row_dev(r) for r in row_peers])
        gx.start()
        for cp in loads + keep:
            cp.start()
        for cp in ins:
            cp.wait()
        for cp in outs:
            cp.start()

        dk_ref[...] = jnp.zeros_like(dk_ref)
        dv_ref[...] = jnp.zeros_like(dv_ref)

        @_scoped
        def project(w, out, b):
            pltpu.make_async_copy(xf_ref.at[pl.ds(0, tb), :], xblk, blk_sem.at[0]).wait()

            def block(i, _):
                r0 = pl.multiple_of(i * bq, bq)
                out[:, pl.ds(pl.multiple_of(b * tb + i * bq, bq), bq)] = _nt(w[...], xblk[pl.ds(r0, bq), :]).astype(BF16)
                return 0

            lax.fori_loop(0, tb // bq, block, 0)

        def row_at(t):
            if isinstance(t, int):
                return lax.rem(at.y + STEP[t] + ring, ring)
            off = jnp.where(t == 1, ring - 1, jnp.where(t == 2, 1, jnp.where(t == 3, 2, 0)))
            return lax.rem(at.y + off, ring)

        for cp in loads + outs:
            cp.wait()

        def begin(g):
            g.relay_first()
            g.near_first()
            g.go(MINUS)

            @pl.when(g.order == 0)
            def _():
                g.go(PLUS)

        def begin_far(g):
            g.far_first()

            @pl.when(g.order == 0)
            def _():
                g.go(FAR)

        def begin_second(g):
            g.relay_second(OWN)

            @pl.when(g.order == 1)
            def _():
                g.go(PLUS)

            g.near_second(OWN)

        def second_minus(g):
            g.relay_second(MINUS)

            @pl.when(g.order == 1)
            def _():
                g.go(FAR)

            g.near_second(MINUS)

        def x_turn(t, _):
            @pl.when(t == 0)
            def _():
                begin(gx)
                begin_far(gx)
                begin_second(gx)
                second_minus(gx)
                gx.relay_second(PLUS)
                gx.near_second(PLUS)
                gx.relay_second(FAR)
                gy.start()
                gz.start()
                gx.far_second(OWN)

            @pl.when(t == 1)
            def _():
                gx.near_second(FAR)
                gx.far_second(MINUS)

            @pl.when(t == 2)
            def _():
                for d in (PLUS, FAR):
                    gx.far_second(d)

            @pl.when(t == 3)
            def _():
                begin(gy)
                begin(gz)

            b = row_at(t)
            _take_row((gx,), t, b, xblk, blk_sem.at[0])
            project(w_v, qkvt_ref, b)
            return 0

        lax.fori_loop(0, ring, x_turn, 0)
        for t in range(0, tokens, bq):
            kn_ref[t:t + bq, :] = qkvt_ref[hd:hd + e, t:t + bq].T
            vn_ref[t:t + bq, :] = qkvt_ref[hd + e:hd + 2 * e, t:t + bq].T

        keys_k, keys_v = slice(hd, hd + e), slice(hd + e, hd + 2 * e)
        m4 = heads * bs
        factor = scale * LOG2E

        def row_chunks(k):
            return [slice(t, t + bq) for t in range(0, (k + 1) * tb, bq)]

        def stacked(ref, qs):
            return jnp.concatenate([ref[h * e:(h + 1) * e, qs] for h in range(heads)], axis=1)

        def unstack(ref, qs, value):
            for h in range(heads):
                ref[h * e:(h + 1) * e, qs] = value[:, h * bs:(h + 1) * bs]

        def scores(q, ks, k, j):
            s = _nn(q, qkvt_ref[keys_k, ks])
            if ks.start < k * tb:
                return s
            row = lax.broadcasted_iota(jnp.int32, (m4, bq), 0) & (bs - 1)
            col = lax.broadcasted_iota(jnp.int32, (m4, bq), 1)
            return jnp.where(col + (ks.start - k * tb) <= row + j * bs, s, -jnp.inf)

        def folded(op, total, value):
            for t in range(0, value.shape[1], 128):
                piece = value[:, t:t + 128]
                total = piece if total is None else op(total, piece)
            return total

        def score_buf(ks):
            n = ks.start // cw
            return part.at[n, :, ks.start - n * cw:ks.stop - n * cw]

        def stats_buf(k, j):
            per = cw // 128
            n = k * (tb // bs)
            return part.at[2 + n // per, :, pl.ds(pl.multiple_of((n % per + j) * 128, 128), 128)]

        @_scoped
        def forward(k):
            chunks = row_chunks(k)

            def queries(j, _):
                qs = pl.ds(pl.multiple_of(k * tb + j * bs, bs), bs)
                q = stacked(qkvt_ref, qs).T
                m = None
                for ks in chunks:
                    s = scores(q, ks, k, j)
                    score_buf(ks)[...] = s
                    m = folded(jnp.maximum, m, s)
                m = jnp.max(m, axis=1, keepdims=True)
                total = None
                for ks in chunks:
                    p = jnp.exp2((score_buf(ks)[...] - m) * factor)
                    score_buf(ks)[...] = p
                    total = folded(jnp.add, total, p)
                inv = 1.0 / jnp.sum(total, axis=1, keepdims=True)
                lane = lax.broadcasted_iota(jnp.int32, (m4, 128), 1)
                stats_buf(k, j)[...] = jnp.where(lane == 0, m, inv)
                out = None
                for ks in chunks:
                    piece = _nn((score_buf(ks)[...] * inv).astype(BF16), vn_ref[ks, :])
                    out = piece if out is None else out + piece
                unstack(ot_ref, qs, out.astype(BF16).T)
                return 0

            lax.fori_loop(0, tb // bs, queries, 0)

        @_scoped
        def backward(k):
            chunks = row_chunks(k)

            def queries(j, _):
                qs = pl.ds(pl.multiple_of(k * tb + j * bs, bs), bs)
                qt = stacked(qkvt_ref, qs)
                dot = stacked(dot_ref, qs)
                q, do = qt.T, dot.T
                delta = jnp.sum(dot.astype(F32) * stacked(ot_ref, qs).astype(F32), axis=0, keepdims=True)
                delta = jnp.broadcast_to(delta, (128, m4)).T[:, :1]
                stats = stats_buf(k, j)[...]
                m, inv = stats[:, 0:1], stats[:, 1:2]
                dq = None
                for ks in chunks:
                    p = jnp.exp2((scores(q, ks, k, j) - m) * factor) * inv
                    dp = _nn(do, qkvt_ref[keys_v, ks])
                    ds = (p * (dp - delta)).astype(BF16)
                    dv_ref[:, ks] += _nn(dot, p.astype(BF16))
                    dk_ref[:, ks] += _nn(qt, ds)
                    piece = _nn(ds, kn_ref[ks, :])
                    dq = piece if dq is None else dq + piece
                dq = (dq * scale).astype(BF16).T
                unstack(dqt_ref, qs, dq)
                for h in range(0, heads, 2):
                    pair = jnp.concatenate([dq[:, h * bs:(h + 1) * bs], dq[:, (h + 1) * bs:(h + 2) * bs]], axis=0)
                    gq[qs, pl.ds(pl.multiple_of(at.r * gw + h * e, 128), 2 * e)] = pair.T
                return 0

            lax.fori_loop(0, tb // bs, queries, 0)

        forward(0)
        begin_far(gy)
        begin_far(gz)
        forward(1)
        begin_second(gy)
        begin_second(gz)
        forward(2)
        second_minus(gy)
        second_minus(gz)
        forward(3)

        def turn(t, _):
            @pl.when(t == 0)
            def _():
                @pl.when(c == 1)
                def _():
                    far_step(OWN)

            @pl.when(t == 1)
            def _():
                for d in (PLUS, FAR):
                    for g in (gy, gz):
                        g.relay_second(d)
                        g.near_second(d)

                @pl.when(c == 1)
                def _():
                    far_step(MINUS)

                w_start()

            @pl.when(t == 2)
            def _():
                @pl.when(c == 1)
                def _():
                    far_step(PLUS)

                @pl.when(c == 0)
                def _():
                    far_step(OWN)
                    far_step(MINUS)

            b = row_at(t)

            @pl.when(t != 3)
            def _():
                _take_row((gy, gz), t, b, xblk, blk_sem.at[0])

            project(wo_v, dot_ref, b)

            @pl.when(t == 2)
            def _():
                @pl.when(c == 0)
                def _():
                    far_step(PLUS)

                far_step(FAR)
                for d in range(4):
                    gz.far_second(d)
                w_relay()
                _take_row((gy, gz), FAR, row_at(FAR), xblk, blk_sem.at[0])

            for k in range(ring):
                @pl.when(b == k)
                def _(k=k):
                    backward(k)
            return 0

        far_cp = {d: gy.push(gy.ref(d, FAR), gy.ref(d, FAR), gy.mate_recv.at[d, FAR], gy.mate) for d in range(4)}

        @_scoped
        def far_step(d):
            for half in (0, 1):
                gy.arrived(d, FAR, half)
            far_cp[d].start()

        lax.fori_loop(0, ring, turn, 0)


    pl.run_scoped(front, pltpu.VMEM((hd + 2 * e, width), BF16), pltpu.VMEM((hd, width), BF16), pltpu.VMEM((tb, width), BF16))

    own_g = at.r * gw
    for k in range(0, tokens, bq):
        ks = slice(k, k + bq)
        kv = jnp.concatenate([(dk_ref[:, ks] * scale).astype(BF16), dv_ref[:, ks].astype(BF16)], axis=0)
        gq[ks, pl.ds(pl.multiple_of(own_g + hd, 128), 2 * e)] = kv.T

    def back(xbuf, obuf, kvt):
        th = tb // 2
        tq = th // 2
        tl = tb // n_row
        hw = cw // 2
        half_a, half_b = pl.ds(0, hw), pl.ds(hw, hw)
        units = [(FAR, 0), (FAR, 1), (PLUS, 0), (MINUS, 0), (PLUS, 1), (MINUS, 1), (OWN, 0), (OWN, 1)]
        s_own, s_left, s_right, s_far = (at.slot(at.x + o, c) for o in (0, -1, 1, 2))
        m_own, m_left, m_right, m_far = (at.slot(at.x + o, 1 - c) for o in (0, -1, 1, 2))

        def unit_row(u):
            d, s = units[u]
            return pl.multiple_of(lax.rem(at.y + STEP[d] + ring, ring) * tb + s * th, th)

        def gcols(slot):
            return pl.ds(pl.multiple_of(slot * gw, gw), gw)

        def piece(u, slot, half=None):
            r0 = unit_row(u)
            rows = pl.ds(r0, th) if half is None else pl.ds(pl.multiple_of(r0 + half * tq, tq), tq)
            return gq.at[rows, gcols(slot)]

        sends = []

        def ag_push(u, n, slot, dev, half=None):
            ref = piece(u, slot, half)
            cp = _remote(ref, ref, ag_send.at[u, n], ag_recv.at[u, n], dev)
            cp.start()
            sends.append(cp)

        def ag_wait(u, n, slot, half=None):
            ref = piece(u, slot, half)
            _remote(ref, ref, ag_send.at[u, n], ag_recv.at[u, n], mate).wait_recv()

        def ag_own(u):
            ag_push(u, 0, s_own, right)
            ag_push(u, 1, s_own, left)
            ag_push(u, 2, s_own, mate)

        @_scoped
        def ag_relay(u):
            ag_wait(u, 0, s_left)
            ag_push(u, 3, s_left, right, 0)
            ag_push(u, 4, s_left, mate)
            ag_wait(u, 1, s_right)
            ag_push(u, 5, s_right, left, 1)
            ag_push(u, 6, s_right, mate)

        @_scoped
        def ag_finish(u):
            ag_wait(u, 3, s_far, 0)
            ag_push(u, 7, s_far, mate, 0)
            ag_wait(u, 5, s_far, 1)
            ag_push(u, 8, s_far, mate, 1)
            ag_wait(u, 2, m_own)
            ag_wait(u, 4, m_left)
            ag_wait(u, 6, m_right)
            ag_wait(u, 7, m_far, 0)
            ag_wait(u, 8, m_far, 1)

        nt = min(256, hw)

        @_scoped
        def partial(u):
            rows = pl.ds(unit_row(u), th)
            d, s = units[u]
            dst = part.at[d, pl.ds(s * th, th), :]

            def tile(j, _):
                cs = pl.ds(pl.multiple_of(j * nt, nt), nt)
                dst[:, cs] = _nn(gq[rows, :], w_all[:, cs])
                return 0

            lax.fori_loop(0, cw // nt, tile, 0)

        def rs_push(n, s, src, dst, dev):
            cp = _remote(src, dst, rs_send.at[n, s], rs_recv.at[n, s], dev)
            cp.start()
            sends.append(cp)

        def rs_wait(n, s):
            ref = rs_half.at[0, s]
            _remote(ref, ref, rs_send.at[n, s], rs_recv.at[n, s], mate).wait_recv()

        def block(d, s, half):
            return part.at[d, pl.ds(s * th, th), half]

        def far_a(s):
            rs_push(0, s, block(FAR, s, half_a), rs_half.at[0, s], up)

        def far_b(s):
            rs_push(1, s, block(FAR, s, half_b), rs_half.at[1, s], down)

        def minus_a(s):
            rs_push(4, s, block(MINUS, s, half_a), rs_full.at[1, s, 0], down)

        def plus_b(s):
            rs_push(3, s, block(PLUS, s, half_b), rs_full.at[0, s, 1], up)

        @_scoped
        def plus_a(s):
            rs_wait(0, s)
            block(PLUS, s, half_a)[...] += rs_half[0, s]
            rs_push(2, s, block(PLUS, s, half_a), rs_full.at[0, s, 0], up)

        @_scoped
        def minus_b(s):
            rs_wait(1, s)
            block(MINUS, s, half_b)[...] += rs_half[1, s]
            rs_push(5, s, block(MINUS, s, half_b), rs_full.at[1, s, 1], down)

        n_steps = width // bc
        depth = xbuf.shape[0]

        def chunk(src, c0, j):
            slot = lax.rem(j, depth)
            return pltpu.make_async_copy(src.at[:, pl.ds(pl.multiple_of(c0 + j * bc, bc), bc)], xbuf.at[slot], in_sem.at[slot])

        def ahead(src, c0, n):
            for j in range(min(depth - 1, n)):
                chunk(src, c0, j).start()

        @_scoped
        def stream(src, lhs, out, j0, j1):
            def store(j):
                slot = lax.rem(j, 2)
                return pltpu.make_async_copy(obuf.at[slot], out.at[:, pl.ds(pl.multiple_of(j * bc, bc), bc)], o_sem.at[slot])

            if j0 == 0:
                ahead(src, 0, n_steps)

            def step(j, _):
                @pl.when(j + depth - 1 < n_steps)
                def _():
                    chunk(src, 0, j + depth - 1).start()

                chunk(src, 0, j).wait()

                @pl.when(j >= 2)
                def _():
                    store(j - 2).wait()

                obuf[lax.rem(j, 2)] = _nn(lhs[...], xbuf[lax.rem(j, depth)])
                store(j).start()
                return 0

            lax.fori_loop(j0, j1, step, 0)
            if j1 == n_steps:
                for j in range(max(n_steps - 2, 0), n_steps):
                    store(j).wait()

        def wo_steps(a, b):
            stream(dyf_ref, ot_ref, dwo_ref, n_steps * a // 16, n_steps * b // 16)

        def wq_steps(a, b):
            stream(xf_ref, dqt_ref, dwq_ref, n_steps * a // 16, n_steps * b // 16)

        first = (at.r // per_kv) * per_kv
        share = width // per_kv
        col0 = lax.rem(at.r, per_kv) * share

        def kv_step(j, _):
            @pl.when(j + depth - 1 < share // bc)
            def _():
                chunk(xf_ref, col0, j + depth - 1).start()

            chunk(xf_ref, col0, j).wait()
            prod = _nn(kvt[...], xbuf[lax.rem(j, depth)])
            dk = dv = None
            for q in range(per_kv):
                a = prod[q * 2 * e:q * 2 * e + e]
                b = prod[q * 2 * e + e:(q + 1) * 2 * e]
                dk = a if dk is None else dk + a
                dv = b if dv is None else dv + b
            cs = pl.ds(pl.multiple_of(j * bc, bc), bc)
            dwk_ref[:, cs] = dk
            dwv_ref[:, cs] = dv
            return 0

        @_scoped
        def kv_grads():
            ahead(xf_ref, col0, share // bc)
            for q in range(per_kv):
                cols = pl.ds(pl.multiple_of((first + q) * gw + hd, 128), gw - hd)
                for t in range(0, tokens, bq):
                    kvt[q * (gw - hd):(q + 1) * (gw - hd), t:t + bq] = gq[t:t + bq, cols].T
            lax.fori_loop(0, share // bc, kv_step, 0)

        per_half = n_row // 2

        def hand(i, r):
            half = (half_a, half_b)[i]
            rows = pl.ds(r * tl, tl)
            cols = pl.ds(pl.multiple_of(at.r * cw + i * hw, hw), hw)
            return stage.at[rows, half], dx_ref.at[:, cols]

        def hand_remote(i, r):
            src, dst = hand(i, r)
            d = lax.rem(r - at.r + n_row, n_row)
            return _remote(src, dst, out_send.at[i, r], out_recv.at[i, d], at.row_dev(r))

        def hand_local(i, r):
            src, dst = hand(i, r)
            return pltpu.make_async_copy(src, dst, out_send.at[i, r])

        @_scoped
        def finish(i, s):
            half = (half_a, half_b)[i]
            rs_wait(2 + i, s)
            rs_wait(4 + i, s)
            stage[s * th:(s + 1) * th, half] = (block(OWN, s, half)[...] + rs_full[0, s, i] + rs_full[1, s, i]).astype(BF16)
            for r in range(s * per_half, (s + 1) * per_half):
                @pl.when(at.r != r)
                def _(r=r):
                    hand_remote(i, r).start()

                @pl.when(at.r == r)
                def _(r=r):
                    hand_local(i, r).start()

        @_scoped
        def received(i):
            for d in range(1, n_row):
                src = lax.rem(at.r + n_row - d, n_row)
                ref = dx_ref.at[:, pl.ds(pl.multiple_of(src * cw + i * hw, hw), hw)]
                _remote(ref, ref, out_send.at[i, 0], out_recv.at[i, d], mate).wait_recv()
            for r in range(n_row):
                @pl.when(at.r != r)
                def _(r=r):
                    hand_remote(i, r).wait_send()

                @pl.when(at.r == r)
                def _(r=r):
                    hand_local(i, r).wait()

        ag_own(0)
        wo_steps(0, 6)
        ag_relay(0)
        ag_own(1)
        ag_own(2)
        wo_steps(6, 9)
        ag_relay(1)
        ag_own(3)
        ag_finish(0)
        for cp in keep:
            cp.wait()
        w_finish()
        partial(0)
        far_a(0)
        far_b(0)
        ag_relay(2)
        ag_own(4)
        wo_steps(9, 10)
        ag_finish(1)
        partial(1)
        far_a(1)
        far_b(1)
        ag_relay(3)
        ag_own(5)
        wo_steps(10, 11)
        ag_finish(2)
        partial(2)
        ag_relay(4)
        ag_own(6)
        plus_a(0)
        wo_steps(11, 12)
        ag_finish(3)
        partial(3)
        minus_a(0)
        ag_relay(5)
        ag_own(7)
        wo_steps(12, 13)
        ag_finish(4)
        partial(4)
        plus_a(1)
        plus_b(0)
        ag_relay(6)
        wo_steps(13, 14)
        ag_finish(5)
        partial(5)
        minus_a(1)
        minus_b(0)
        plus_b(1)
        minus_b(1)
        ag_relay(7)
        wo_steps(14, 16)
        ag_finish(6)
        partial(6)
        wq_steps(0, 2)
        ag_finish(7)
        partial(7)
        wq_steps(2, 5)
        finish(0, 0)
        wq_steps(5, 12)
        finish(0, 1)
        wq_steps(12, 16)
        kv_grads()
        finish(1, 0)
        received(0)
        finish(1, 1)
        received(1)
        for cp in sends:
            cp.wait_send()
        w_drain()
        for g in (gx, gy, gz):
            g.drain()

    pl.run_scoped(back, pltpu.VMEM((4, tokens, bc), BF16), pltpu.VMEM((2, hd, bc), F32), pltpu.VMEM((per_kv * 2 * e, tokens), BF16))


def _layer(ring, cores, heads, scale, x, dy, wq, wk, wv, wo):
    rows, width = x.shape
    tokens = rows * ring * ring * cores
    hd = wo.shape[0]
    e = hd // heads
    n_row = ring * cores
    cw = width // n_row
    gw = hd + 2 * e
    tb = tokens // ring
    th, hw = tb // 2, cw // 2
    per_kv = n_row * ring // wk.shape[0]
    bq = min(256, tb)
    bs = tb // heads
    bc = min(512, cw // 2)
    dma = pltpu.SemaphoreType.DMA
    shape = jax.ShapeDtypeStruct
    return pl.pallas_call(
        functools.partial(_kernel, ring, cores, heads, scale, bq, bs, bc),
        name="layer",
        in_specs=[ANY] * 6,
        out_specs=[ANY, ANY, ANY, VMEM, VMEM, ANY, ANY],
        out_shape=[
            shape((rows, width), BF16),
            shape((hd, width), F32),
            shape((hd, width), F32),
            shape((e, width // per_kv), F32),
            shape((e, width // per_kv), F32),
            shape((tokens, width), BF16),
            shape((tokens, width), BF16),
        ],
        scratch_shapes=[
            pltpu.VMEM((tokens, n_row * gw), BF16),
            pltpu.VMEM((n_row * gw, cw), BF16),
            pltpu.VMEM((4, tb, cw), F32),
            pltpu.VMEM((2, 2, th, hw), F32),
            pltpu.VMEM((2, 2, 2, th, hw), F32),
            pltpu.VMEM((tb, cw), BF16),
            pltpu.VMEM((4, hd // 2, cw), BF16),
            pltpu.VMEM((gw, tokens), BF16),
            pltpu.VMEM((hd, tokens), BF16),
            pltpu.VMEM((hd, tokens), BF16),
            pltpu.VMEM((hd, tokens), BF16),
            pltpu.VMEM((e, tokens), F32),
            pltpu.VMEM((e, tokens), F32),
            pltpu.VMEM((tokens, e), BF16),
            pltpu.VMEM((tokens, e), BF16),
            dma((3, 48)),
            dma((3, 4, 4, 2)),
            dma((3, 4, 4)),
            dma((13,)),
            dma((9,)),
            dma((4,)),
            dma((9 + 2 * n_row,)),
            dma((1,)),
            dma((8, 9)),
            dma((8, 9)),
            dma((6, 2)),
            dma((6, 2)),
            dma((2, n_row)),
            dma((2, n_row)),
            dma((4,)),
            dma((2,)),
        ],
        compiler_params=pltpu.CompilerParams(collective_id=0, has_side_effects=True, vmem_limit_bytes=67043328),
        cost_estimate=pl.CostEstimate(flops=70 * 10**9, bytes_accessed=300 << 20, transcendentals=heads * tokens * tokens // 2),
    )(x, dy, wq, wk, wv, wo)


def solution(mesh):
    n = mesh.shape["tp"]
    ring = math.isqrt(n // 2)
    cores = n // (ring * ring)
    if ring != 4 or cores != 2:
        raise ValueError("needs a 4x4 torus")

    def local_grads(x_blk, dy_blk, wq_loc, w_k, w_v, wo_loc):
        model_dim, kv_heads, e = w_k.shape
        heads = wq_loc.shape[1]
        hd = heads * e
        scale = e ** -0.5
        wq = jnp.transpose(wq_loc, (1, 2, 0)).reshape(hd, model_dim)
        wk = jnp.transpose(w_k, (1, 2, 0))
        wv = jnp.transpose(w_v, (1, 2, 0))
        wo = wo_loc.reshape(hd, model_dim)
        dx, dwq, dwo, dwk, dwv, _, _ = _layer(ring, cores, heads, scale, x_blk, dy_blk, wq, wk, wv, wo)
        return (dx, jnp.transpose(dwq.reshape(heads, e, model_dim), (2, 0, 1)), dwo.reshape(heads, e, model_dim), dwk.T, dwv.T)

    tok = P(("dp", "tp"))
    return jax.shard_map(
        local_grads,
        mesh=mesh,
        in_specs=(tok, tok, P(None, "tp", None), P(), P(), P("tp")),
        out_specs=(tok, P("dp", "tp", None), tok, tok, tok),
        check_vma=False,
    )
```

```python
import functools
import math

import jax
import jax.numpy as jnp
from jax import lax
from jax.experimental import pallas as pl
from jax.experimental.pallas import tpu as pltpu
from jax.sharding import PartitionSpec as P

F32 = jnp.float32
BF16 = jnp.bfloat16
MESH = pl.DeviceIdType.MESH
ANY = pl.BlockSpec(memory_space=pl.ANY)
VMEM = pl.BlockSpec(memory_space=pltpu.VMEM)
LOG2E = math.log2(math.e)


def _scoped(fn):
    def run(*args, **kw):
        with jax.named_scope(fn.__name__):
            return fn(*args, **kw)

    return run


def _dot(a, b, dims):
    return lax.dot_general(a, b, (dims, ((), ())), preferred_element_type=F32)


def _nn(a, b):
    return _dot(a, b, ((1,), (0,)))


def _nt(a, b):
    return _dot(a, b, ((1,), (1,)))


class Place:
    def __init__(self, ring, cores):
        me = lax.axis_index("tp")
        self.ring, self.cores = ring, cores
        self.c = lax.rem(me, cores)
        self.x = lax.rem(me // cores, ring)
        self.y = me // (cores * ring)
        self.r = self.x * cores + self.c
        self.n_row = ring * cores

    def dev(self, y, x, c):
        y = lax.rem(y + self.ring, self.ring)
        x = lax.rem(x + self.ring, self.ring)
        return {"tp": (y * self.ring + x) * self.cores + c}

    def row_dev(self, r):
        return {"tp": self.y * self.n_row + r}

    def slot(self, x, c):
        return lax.rem(x + self.ring, self.ring) * self.cores + c


def _remote(src, dst, send, recv, dev):
    return pltpu.make_async_remote_copy(
        src_ref=src, dst_ref=dst, send_sem=send, recv_sem=recv, device_id=dev, device_id_type=MESH
    )


@_scoped
def _enter(devices):
    barrier = pltpu.get_barrier_semaphore()
    for dev in devices:
        pl.semaphore_signal(barrier, inc=1, device_id=dev, device_id_type=MESH)
    pl.semaphore_wait(barrier, len(devices))


OWN, MINUS, PLUS, FAR = range(4)
STEP = (0, -1, 1, 2)


def _load_shard(at, full, n, y, x, core, block, sem):
    r0 = at.dev(y, x, core)["tp"] * n
    b0 = at.slot(x, core) * n
    src = full.at[pl.ds(pl.multiple_of(r0, n), n), :]
    return pltpu.make_async_copy(src, block.at[pl.ds(pl.multiple_of(b0, n), n), :], sem)


@_scoped
def _take_row(lanes, t, y, block, sem):
    at, full, n = lanes[0].at, lanes[0].full, lanes[0].shard
    for j in range(4):
        _load_shard(at, full, n, y, at.x + STEP[j], at.c, block, sem).start()
    for j in range(4):
        for g in lanes:
            g.await_mate(t, j)
        _load_shard(at, full, n, y, at.x + STEP[j], 1 - at.c, block, sem).start()


class Gather:
    def __init__(self, at, src, full, send, recv, mate_recv, orders, row0, rows, tag):
        self.at, self.src, self.full = at, src, full
        self.send, self.recv, self.mate_recv = send.at[tag], recv.at[tag], mate_recv.at[tag]
        self.order, self.mate_order = orders
        self.row0, self.rows, self.shard = row0, rows, src.shape[0]
        self.sent = []
        c, o = at.c, self.order
        self.first = {s: at.dev(at.y + o * s, at.x + (1 - o) * s, c) for s in (1, -1)}
        self.second = {s: at.dev(at.y + (1 - o) * s, at.x + o * s, c) for s in (1, -1)}
        self.mate = at.dev(at.y, at.x, 1 - c)
        self.fulls = {d: self.both_ways(self.second, d, lambda to, d=d: (d, to)) for d in range(4)}

    def span(self, half):
        n = self.rows if half is None else self.rows // 2
        return self.row0 + (0 if half is None else half * n), n

    def ref(self, d1, d2, half=None):
        at, o = self.at, self.order
        o1, o2 = STEP[d1], STEP[d2]
        start, n = self.span(half)
        r0 = at.dev(at.y + o * o1 + (1 - o) * o2, at.x + (1 - o) * o1 + o * o2, at.c)["tp"] * self.shard + start
        return self.full.at[pl.ds(pl.multiple_of(r0, math.gcd(self.shard, self.row0, n)), n), :]

    def push(self, src, dst, recv, dev):
        k = len(self.sent)
        self.sent.append(dst.shape[0])
        return _remote(src, dst, self.send.at[k], recv, dev)

    def out(self, d1, d2, half=None):
        if d1 == OWN and d2 == OWN:
            return self.src.at[pl.ds(*self.span(half)), :]
        return self.ref(d1, d2, half)

    def both_ways(self, devs, d1, name):
        copies = []
        for step in (0, 1):
            for s, to in ((1, MINUS), (-1, PLUS)):
                half = step if s == 1 else 1 - step
                copies.append(self.push(self.out(d1, OWN, half), self.ref(d1, OWN, half), self.recv.at[*name(to), half], devs[s]))
        return copies

    def to_mate(self, d1, d2):
        ref = self.ref(d1, d2)
        self.push(self.out(d1, d2), ref, self.mate_recv.at[d1, d2], self.mate).start()

    def arrived(self, d1, d2, half):
        ref = self.ref(d1, d2, half)
        _remote(ref, ref, self.send.at[0], self.recv.at[d1, d2, half], self.mate).wait_recv()

    @_scoped
    def start(self):
        for cp in self.both_ways(self.first, OWN, lambda to: (to, OWN)):
            cp.start()
        self.go(OWN)
        self.to_mate(OWN, OWN)

    def go(self, d1):
        for cp in self.fulls[d1]:
            cp.start()

    @_scoped
    def relay_first(self):
        for d, s, half in ((MINUS, 1, 0), (PLUS, -1, 1)):
            self.arrived(d, OWN, half)
            ref = self.ref(d, OWN, half)
            self.push(ref, ref, self.recv.at[FAR, OWN, half], self.first[s]).start()

    @_scoped
    def near_first(self):
        for d, half in ((MINUS, 1), (PLUS, 0)):
            self.arrived(d, OWN, half)
            self.to_mate(d, OWN)

    @_scoped
    def far_first(self):
        for half in (0, 1):
            self.arrived(FAR, OWN, half)
        self.to_mate(FAR, OWN)

    @_scoped
    def relay_second(self, d1):
        for d, s, half in ((MINUS, 1, 0), (PLUS, -1, 1)):
            self.arrived(d1, d, half)
            ref = self.ref(d1, d, half)
            self.push(ref, ref, self.recv.at[d1, FAR, half], self.second[s]).start()

    @_scoped
    def near_second(self, d1):
        for d, half in ((MINUS, 1), (PLUS, 0)):
            self.arrived(d1, d, half)
            self.to_mate(d1, d)

    @_scoped
    def far_second(self, d1):
        for half in (0, 1):
            self.arrived(d1, FAR, half)
        self.to_mate(d1, FAR)

    def await_mate(self, t, j):
        o = self.mate_order
        ref = self.full.at[pl.ds(0, self.rows), :]
        _remote(ref, ref, self.send.at[0], self.mate_recv.at[(1 - o) * j + o * t, (1 - o) * t + o * j], self.mate).wait_recv()

    @_scoped
    def drain(self):
        for k, n in enumerate(self.sent):
            ref = self.full.at[pl.ds(0, n), :]
            _remote(ref, ref, self.send.at[k], self.send.at[k], self.mate).wait_send()


def _kernel(ring, cores, heads, scale, bq, bs, bc, x_ref, dy_ref, w_ref, wk_ref, wv_ref, wo_ref,
            dx_ref, dwq_ref, dwo_ref, dwk_ref, dwv_ref, xf_ref, dyf_ref,
            gq, w_all, part, rs_half, rs_full, stage, hop_ref, qkvt_ref, dot_ref, dqt_ref, ot_ref, dk_ref, dv_ref, kn_ref, vn_ref,
            send, recv, mate_recv, w_send, w_recv, hop_recv, ld_sem, blk_sem,
            ag_send, ag_recv, rs_send, rs_recv, out_send, out_recv, in_sem, o_sem):
    at = Place(ring, cores)
    n_row = at.n_row
    hd = wo_ref.shape[0]
    e = hd // heads
    tokens, width = xf_ref.shape
    tb = tokens // ring
    cw = width // n_row
    gw = gq.shape[1] // n_row
    c = at.c
    shard = x_ref.shape[0]
    gx = Gather(at, x_ref, xf_ref, send, recv, mate_recv, (c, 1 - c), 0, shard, 0)
    split = shard * 3 // 4
    gy = Gather(at, dy_ref, dyf_ref, send, recv, mate_recv, (c, 1 - c), 0, split, 1)
    gz = Gather(at, dy_ref, dyf_ref, send, recv, mate_recv, (0, 0), split, shard - split, 2)
    n_kv = wk_ref.shape[0] // ring
    per_kv = n_row // n_kv
    row_peers = [lax.rem(at.r + d, n_row) for d in range(1, n_row)]
    up, down = at.dev(at.y + 1, at.x, c), at.dev(at.y - 1, at.x, c)

    hh = hd // 2

    def w_push(k, src, dst, rsem, dev):
        _remote(src, dst, w_send.at[k], rsem, dev).start()

    def wq_slot(slot, half=None):
        r0 = slot * gw + (0 if half is None else half * hh)
        return w_all.at[pl.ds(r0 if isinstance(r0, int) else pl.multiple_of(r0, hh), hd if half is None else hh), :]

    def wcols(slot):
        return pl.ds(pl.multiple_of(slot * cw, cw), cw)

    right, left, mate = at.dev(at.y, at.x + 1, c), at.dev(at.y, at.x - 1, c), at.dev(at.y, at.x, 1 - c)

    @_scoped
    def w_start():
        for half, dev in ((0, right), (1, left)):
            for k in range(cores):
                w_push(half * 2 + k, w_ref.at[pl.ds(half * hh, hh), wcols(at.slot(at.x + 2, k))], hop_ref.at[half * 2 + k], hop_recv.at[half * 2 + k], dev)
        w_push(4, w_ref.at[pl.ds(0, hd), wcols(at.slot(at.x, 1 - c))], wq_slot(at.r), w_recv.at[0], mate)
        for i, s in enumerate((1, -1)):
            for k in range(cores):
                dst_core = c if k == 0 else 1 - c
                w_push(5 + 2 * i + k, w_ref.at[pl.ds(0, hd), wcols(at.slot(at.x + s, dst_core))], wq_slot(at.r), w_recv.at[1 + 2 * i + k], at.dev(at.y, at.x + s, dst_core))

    @_scoped
    def w_relay():
        for half, s in ((0, 1), (1, -1)):
            for n in (half * 2, half * 2 + 1):
                _remote(hop_ref.at[n], hop_ref.at[n], w_send.at[0], hop_recv.at[n], mate).wait_recv()
            for k in range(cores):
                n = half * 2 + k
                src_slot = at.slot(at.x - s, c)
                same = k == 0
                dst_core = c if same else 1 - c
                w_push(9 + n, hop_ref.at[half * 2 + dst_core], wq_slot(src_slot, half), w_recv.at[5 + n], at.dev(at.y, at.x + s, dst_core))

    @_scoped
    def w_finish():
        whole = wq_slot(0)
        piece = wq_slot(0, 0)
        for n in range(9):
            ref = whole if n < 5 else piece
            _remote(ref, ref, w_send.at[0], w_recv.at[n], mate).wait_recv()

    def w_drain():
        whole = wq_slot(0)
        piece = wq_slot(0, 0)
        for k in range(13):
            ref = whole if 4 <= k < 9 else piece
            _remote(ref, ref, w_send.at[k], w_send.at[k], mate).wait_send()

    own_cols = wcols(at.r)
    rows = x_ref.shape[0]
    own_rows = pl.ds(pl.multiple_of((at.y * n_row + at.r) * rows, rows), rows)

    keep = [pltpu.make_async_copy(w_ref.at[:, own_cols], wq_slot(at.r), ld_sem.at[8])]
    for r in range(n_row):
        kv_r = at.y * n_kv + r // per_kv
        for i, w in enumerate((wk_ref, wv_ref)):
            keep.append(pltpu.make_async_copy(w.at[kv_r, :, own_cols], w_all.at[pl.ds(r * gw + hd + i * e, e), :], ld_sem.at[9 + 2 * r + i]))

    def front(w_v, wo_v, xblk):
        kv = (at.y * n_row + at.r) // (n_row * ring // wk_ref.shape[0])
        loads = [
            pltpu.make_async_copy(w_ref, w_v.at[pl.ds(0, hd), :], ld_sem.at[0]),
            pltpu.make_async_copy(wo_ref, wo_v, ld_sem.at[1]),
            pltpu.make_async_copy(wk_ref.at[kv], w_v.at[pl.ds(hd, e), :], ld_sem.at[6]),
            pltpu.make_async_copy(wv_ref.at[kv], w_v.at[pl.ds(hd + e, e), :], ld_sem.at[7]),
        ]
        ins = [pltpu.make_async_copy(src, xblk.at[pl.ds(i * rows, rows), :], ld_sem.at[2 + i]) for i, src in enumerate((x_ref, dy_ref))]
        outs = [pltpu.make_async_copy(xblk.at[pl.ds(i * rows, rows), :], dst.at[own_rows, :], ld_sem.at[4 + i]) for i, dst in enumerate((xf_ref, dyf_ref))]
        for cp in ins:
            cp.start()
        _enter([up, down] + [at.row_dev(r) for r in row_peers])
        gx.start()
        for cp in loads + keep:
            cp.start()
        for cp in ins:
            cp.wait()
        for cp in outs:
            cp.start()

        dk_ref[...] = jnp.zeros_like(dk_ref)
        dv_ref[...] = jnp.zeros_like(dv_ref)

        @_scoped
        def project(w, out, b):
            pltpu.make_async_copy(xf_ref.at[pl.ds(0, tb), :], xblk, blk_sem.at[0]).wait()

            def block(i, _):
                r0 = pl.multiple_of(i * bq, bq)
                out[:, pl.ds(pl.multiple_of(b * tb + i * bq, bq), bq)] = _nt(w[...], xblk[pl.ds(r0, bq), :]).astype(BF16)
                return 0

            lax.fori_loop(0, tb // bq, block, 0)

        def row_at(t):
            if isinstance(t, int):
                return lax.rem(at.y + STEP[t] + ring, ring)
            off = jnp.where(t == 1, ring - 1, jnp.where(t == 2, 1, jnp.where(t == 3, 2, 0)))
            return lax.rem(at.y + off, ring)

        for cp in loads + outs:
            cp.wait()

        def begin(g):
            g.relay_first()
            g.near_first()
            g.go(MINUS)

            @pl.when(g.order == 0)
            def _():
                g.go(PLUS)

        def begin_far(g):
            g.far_first()

            @pl.when(g.order == 0)
            def _():
                g.go(FAR)

        def begin_second(g):
            g.relay_second(OWN)

            @pl.when(g.order == 1)
            def _():
                g.go(PLUS)

            g.near_second(OWN)

        def second_minus(g):
            g.relay_second(MINUS)

            @pl.when(g.order == 1)
            def _():
                g.go(FAR)

            g.near_second(MINUS)

        def x_turn(t, _):
            @pl.when(t == 0)
            def _():
                begin(gx)
                begin_far(gx)
                begin_second(gx)
                second_minus(gx)
                gx.relay_second(PLUS)
                gx.near_second(PLUS)
                gx.relay_second(FAR)
                gy.start()
                gz.start()
                gx.far_second(OWN)

            @pl.when(t == 1)
            def _():
                gx.near_second(FAR)
                gx.far_second(MINUS)

            @pl.when(t == 2)
            def _():
                for d in (PLUS, FAR):
                    gx.far_second(d)

            @pl.when(t == 3)
            def _():
                begin(gy)
                begin(gz)

            b = row_at(t)
            _take_row((gx,), t, b, xblk, blk_sem.at[0])
            project(w_v, qkvt_ref, b)
            return 0

        lax.fori_loop(0, ring, x_turn, 0)
        for t in range(0, tokens, bq):
            kn_ref[t:t + bq, :] = qkvt_ref[hd:hd + e, t:t + bq].T
            vn_ref[t:t + bq, :] = qkvt_ref[hd + e:hd + 2 * e, t:t + bq].T

        keys_k, keys_v = slice(hd, hd + e), slice(hd + e, hd + 2 * e)
        m4 = heads * bs
        factor = scale * LOG2E

        def row_chunks(k):
            return [slice(t, t + bq) for t in range(0, (k + 1) * tb, bq)]

        def stacked(ref, qs):
            return jnp.concatenate([ref[h * e:(h + 1) * e, qs] for h in range(heads)], axis=1)

        def unstack(ref, qs, value):
            for h in range(heads):
                ref[h * e:(h + 1) * e, qs] = value[:, h * bs:(h + 1) * bs]

        def scores(q, ks, k, j):
            s = _nn(q, qkvt_ref[keys_k, ks])
            if ks.start < k * tb:
                return s
            row = lax.broadcasted_iota(jnp.int32, (m4, bq), 0) & (bs - 1)
            col = lax.broadcasted_iota(jnp.int32, (m4, bq), 1)
            return jnp.where(col + (ks.start - k * tb) <= row + j * bs, s, -jnp.inf)

        def folded(op, total, value):
            for t in range(0, value.shape[1], 128):
                piece = value[:, t:t + 128]
                total = piece if total is None else op(total, piece)
            return total

        def score_buf(ks):
            n = ks.start // cw
            return part.at[n, :, ks.start - n * cw:ks.stop - n * cw]

        def stats_buf(k, j):
            per = cw // 128
            n = k * (tb // bs)
            return part.at[2 + n // per, :, pl.ds(pl.multiple_of((n % per + j) * 128, 128), 128)]

        @_scoped
        def forward(k):
            chunks = row_chunks(k)

            def queries(j, _):
                qs = pl.ds(pl.multiple_of(k * tb + j * bs, bs), bs)
                q = stacked(qkvt_ref, qs).T
                m = None
                for ks in chunks:
                    s = scores(q, ks, k, j)
                    score_buf(ks)[...] = s
                    m = folded(jnp.maximum, m, s)
                m = jnp.max(m, axis=1, keepdims=True)
                total = None
                for ks in chunks:
                    p = jnp.exp2((score_buf(ks)[...] - m) * factor)
                    score_buf(ks)[...] = p
                    total = folded(jnp.add, total, p)
                inv = 1.0 / jnp.sum(total, axis=1, keepdims=True)
                lane = lax.broadcasted_iota(jnp.int32, (m4, 128), 1)
                stats_buf(k, j)[...] = jnp.where(lane == 0, m, inv)
                out = None
                for ks in chunks:
                    piece = _nn((score_buf(ks)[...] * inv).astype(BF16), vn_ref[ks, :])
                    out = piece if out is None else out + piece
                unstack(ot_ref, qs, out.astype(BF16).T)
                return 0

            lax.fori_loop(0, tb // bs, queries, 0)

        @_scoped
        def backward(k):
            chunks = row_chunks(k)

            def queries(j, _):
                qs = pl.ds(pl.multiple_of(k * tb + j * bs, bs), bs)
                qt = stacked(qkvt_ref, qs)
                dot = stacked(dot_ref, qs)
                q, do = qt.T, dot.T
                delta = jnp.sum(dot.astype(F32) * stacked(ot_ref, qs).astype(F32), axis=0, keepdims=True)
                delta = jnp.broadcast_to(delta, (128, m4)).T[:, :1]
                stats = stats_buf(k, j)[...]
                m, inv = stats[:, 0:1], stats[:, 1:2]
                dq = None
                for ks in chunks:
                    p = jnp.exp2((scores(q, ks, k, j) - m) * factor) * inv
                    dp = _nn(do, qkvt_ref[keys_v, ks])
                    ds = (p * (dp - delta)).astype(BF16)
                    dv_ref[:, ks] += _nn(dot, p.astype(BF16))
                    dk_ref[:, ks] += _nn(qt, ds)
                    piece = _nn(ds, kn_ref[ks, :])
                    dq = piece if dq is None else dq + piece
                dq = (dq * scale).astype(BF16).T
                unstack(dqt_ref, qs, dq)
                for h in range(0, heads, 2):
                    pair = jnp.concatenate([dq[:, h * bs:(h + 1) * bs], dq[:, (h + 1) * bs:(h + 2) * bs]], axis=0)
                    gq[qs, pl.ds(pl.multiple_of(at.r * gw + h * e, 128), 2 * e)] = pair.T
                return 0

            lax.fori_loop(0, tb // bs, queries, 0)

        forward(0)
        begin_far(gy)
        begin_far(gz)
        forward(1)
        begin_second(gy)
        begin_second(gz)
        forward(2)
        forward(3)
        second_minus(gy)
        second_minus(gz)

        def turn(t, _):
            @pl.when(t == 0)
            def _():
                @pl.when(c == 1)
                def _():
                    far_step(OWN)

            @pl.when(t == 1)
            def _():
                for d in (PLUS, FAR):
                    for g in (gy, gz):
                        g.relay_second(d)
                        g.near_second(d)

                @pl.when(c == 1)
                def _():
                    far_step(MINUS)

                w_start()

            @pl.when(t == 2)
            def _():
                @pl.when(c == 1)
                def _():
                    far_step(PLUS)

                @pl.when(c == 0)
                def _():
                    far_step(OWN)
                    far_step(MINUS)

            b = row_at(t)

            @pl.when(t != 3)
            def _():
                _take_row((gy, gz), t, b, xblk, blk_sem.at[0])

            project(wo_v, dot_ref, b)

            @pl.when(t == 2)
            def _():
                @pl.when(c == 0)
                def _():
                    far_step(PLUS)

                far_step(FAR)
                for d in range(4):
                    gz.far_second(d)
                w_relay()
                _take_row((gy, gz), FAR, row_at(FAR), xblk, blk_sem.at[0])

            for k in range(ring):
                @pl.when(b == k)
                def _(k=k):
                    backward(k)
            return 0

        far_cp = {d: gy.push(gy.ref(d, FAR), gy.ref(d, FAR), gy.mate_recv.at[d, FAR], gy.mate) for d in range(4)}

        @_scoped
        def far_step(d):
            for half in (0, 1):
                gy.arrived(d, FAR, half)
            far_cp[d].start()

        lax.fori_loop(0, ring, turn, 0)


    pl.run_scoped(front, pltpu.VMEM((hd + 2 * e, width), BF16), pltpu.VMEM((hd, width), BF16), pltpu.VMEM((tb, width), BF16))

    def back(xbuf, obuf, kvt):
        th = tb // 2
        tq = th // 2
        tl = tb // n_row
        hw = cw // 2
        half_a, half_b = pl.ds(0, hw), pl.ds(hw, hw)
        units = [(FAR, 0), (FAR, 1), (PLUS, 0), (MINUS, 0), (PLUS, 1), (MINUS, 1), (OWN, 0), (OWN, 1)]
        s_own, s_left, s_right, s_far = (at.slot(at.x + o, c) for o in (0, -1, 1, 2))
        m_own, m_left, m_right, m_far = (at.slot(at.x + o, 1 - c) for o in (0, -1, 1, 2))

        def unit_row(u):
            d, s = units[u]
            return pl.multiple_of(lax.rem(at.y + STEP[d] + ring, ring) * tb + s * th, th)

        def gcols(slot):
            return pl.ds(pl.multiple_of(slot * gw, gw), gw)

        def piece(u, slot, half=None):
            r0 = unit_row(u)
            rows = pl.ds(r0, th) if half is None else pl.ds(pl.multiple_of(r0 + half * tq, tq), tq)
            return gq.at[rows, gcols(slot)]

        sends = []

        def ag_push(u, n, slot, dev, half=None):
            ref = piece(u, slot, half)
            cp = _remote(ref, ref, ag_send.at[u, n], ag_recv.at[u, n], dev)
            cp.start()
            sends.append(cp)

        def ag_wait(u, n, slot, half=None):
            ref = piece(u, slot, half)
            _remote(ref, ref, ag_send.at[u, n], ag_recv.at[u, n], mate).wait_recv()

        def ag_own(u):
            ag_push(u, 0, s_own, right)
            ag_push(u, 1, s_own, left)
            ag_push(u, 2, s_own, mate)

        @_scoped
        def ag_relay(u):
            ag_wait(u, 0, s_left)
            ag_push(u, 3, s_left, right, 0)
            ag_push(u, 4, s_left, mate)
            ag_wait(u, 1, s_right)
            ag_push(u, 5, s_right, left, 1)
            ag_push(u, 6, s_right, mate)

        @_scoped
        def ag_finish(u):
            ag_wait(u, 3, s_far, 0)
            ag_push(u, 7, s_far, mate, 0)
            ag_wait(u, 5, s_far, 1)
            ag_push(u, 8, s_far, mate, 1)
            ag_wait(u, 2, m_own)
            ag_wait(u, 4, m_left)
            ag_wait(u, 6, m_right)
            ag_wait(u, 7, m_far, 0)
            ag_wait(u, 8, m_far, 1)

        def settle(u):
            rows = pl.ds(unit_row(u), th)
            kv = jnp.concatenate([(dk_ref[:, rows] * scale).astype(BF16), dv_ref[:, rows].astype(BF16)], axis=0)
            gq[rows, pl.ds(pl.multiple_of(at.r * gw + hd, 128), 2 * e)] = kv.T

        nt = min(256, hw)

        @_scoped
        def partial(u):
            rows = pl.ds(unit_row(u), th)
            d, s = units[u]
            dst = part.at[d, pl.ds(s * th, th), :]

            def tile(j, _):
                cs = pl.ds(pl.multiple_of(j * nt, nt), nt)
                dst[:, cs] = _nn(gq[rows, :], w_all[:, cs])
                return 0

            lax.fori_loop(0, cw // nt, tile, 0)

        def rs_push(n, s, src, dst, dev):
            cp = _remote(src, dst, rs_send.at[n, s], rs_recv.at[n, s], dev)
            cp.start()
            sends.append(cp)

        def rs_wait(n, s):
            ref = rs_half.at[0, s]
            _remote(ref, ref, rs_send.at[n, s], rs_recv.at[n, s], mate).wait_recv()

        def block(d, s, half):
            return part.at[d, pl.ds(s * th, th), half]

        def far_a(s):
            rs_push(0, s, block(FAR, s, half_a), rs_half.at[0, s], up)

        def far_b(s):
            rs_push(1, s, block(FAR, s, half_b), rs_half.at[1, s], down)

        def minus_a(s):
            rs_push(4, s, block(MINUS, s, half_a), rs_full.at[1, s, 0], down)

        def plus_b(s):
            rs_push(3, s, block(PLUS, s, half_b), rs_full.at[0, s, 1], up)

        @_scoped
        def plus_a(s):
            rs_wait(0, s)
            block(PLUS, s, half_a)[...] += rs_half[0, s]
            rs_push(2, s, block(PLUS, s, half_a), rs_full.at[0, s, 0], up)

        @_scoped
        def minus_b(s):
            rs_wait(1, s)
            block(MINUS, s, half_b)[...] += rs_half[1, s]
            rs_push(5, s, block(MINUS, s, half_b), rs_full.at[1, s, 1], down)

        n_steps = width // bc
        depth = xbuf.shape[0]

        def chunk(src, c0, j):
            slot = lax.rem(j, depth)
            return pltpu.make_async_copy(src.at[:, pl.ds(pl.multiple_of(c0 + j * bc, bc), bc)], xbuf.at[slot], in_sem.at[slot])

        def ahead(src, c0, n):
            for j in range(min(depth - 1, n)):
                chunk(src, c0, j).start()

        @_scoped
        def stream(src, lhs, out, j0, j1):
            def store(j):
                slot = lax.rem(j, 2)
                return pltpu.make_async_copy(obuf.at[slot], out.at[:, pl.ds(pl.multiple_of(j * bc, bc), bc)], o_sem.at[slot])

            if j0 == 0:
                ahead(src, 0, n_steps)

            def step(j, _):
                @pl.when(j + depth - 1 < n_steps)
                def _():
                    chunk(src, 0, j + depth - 1).start()

                chunk(src, 0, j).wait()

                @pl.when(j >= 2)
                def _():
                    store(j - 2).wait()

                obuf[lax.rem(j, 2)] = _nn(lhs[...], xbuf[lax.rem(j, depth)])
                store(j).start()
                return 0

            lax.fori_loop(j0, j1, step, 0)
            if j1 == n_steps:
                for j in range(max(n_steps - 2, 0), n_steps):
                    store(j).wait()

        def wo_steps(a, b):
            stream(dyf_ref, ot_ref, dwo_ref, n_steps * a // 16, n_steps * b // 16)

        def wq_steps(a, b):
            stream(xf_ref, dqt_ref, dwq_ref, n_steps * a // 16, n_steps * b // 16)

        first = (at.r // per_kv) * per_kv
        share = width // per_kv
        col0 = lax.rem(at.r, per_kv) * share

        def kv_step(j, _):
            @pl.when(j + depth - 1 < share // bc)
            def _():
                chunk(xf_ref, col0, j + depth - 1).start()

            chunk(xf_ref, col0, j).wait()
            prod = _nn(kvt[...], xbuf[lax.rem(j, depth)])
            dk = dv = None
            for q in range(per_kv):
                a = prod[q * 2 * e:q * 2 * e + e]
                b = prod[q * 2 * e + e:(q + 1) * 2 * e]
                dk = a if dk is None else dk + a
                dv = b if dv is None else dv + b
            cs = pl.ds(pl.multiple_of(j * bc, bc), bc)
            dwk_ref[:, cs] = dk
            dwv_ref[:, cs] = dv
            return 0

        @_scoped
        def kv_grads():
            ahead(xf_ref, col0, share // bc)
            for q in range(per_kv):
                cols = pl.ds(pl.multiple_of((first + q) * gw + hd, 128), gw - hd)
                for t in range(0, tokens, bq):
                    kvt[q * (gw - hd):(q + 1) * (gw - hd), t:t + bq] = gq[t:t + bq, cols].T
            lax.fori_loop(0, share // bc, kv_step, 0)

        per_half = n_row // 2

        def hand(i, r):
            half = (half_a, half_b)[i]
            rows = pl.ds(r * tl, tl)
            cols = pl.ds(pl.multiple_of(at.r * cw + i * hw, hw), hw)
            return stage.at[rows, half], dx_ref.at[:, cols]

        def hand_remote(i, r):
            src, dst = hand(i, r)
            d = lax.rem(r - at.r + n_row, n_row)
            return _remote(src, dst, out_send.at[i, r], out_recv.at[i, d], at.row_dev(r))

        def hand_local(i, r):
            src, dst = hand(i, r)
            return pltpu.make_async_copy(src, dst, out_send.at[i, r])

        @_scoped
        def finish(i, s):
            half = (half_a, half_b)[i]
            rs_wait(2 + i, s)
            rs_wait(4 + i, s)
            stage[s * th:(s + 1) * th, half] = (block(OWN, s, half)[...] + rs_full[0, s, i] + rs_full[1, s, i]).astype(BF16)
            for r in range(s * per_half, (s + 1) * per_half):
                @pl.when(at.r != r)
                def _(r=r):
                    hand_remote(i, r).start()

                @pl.when(at.r == r)
                def _(r=r):
                    hand_local(i, r).start()

        @_scoped
        def received(i):
            for d in range(1, n_row):
                src = lax.rem(at.r + n_row - d, n_row)
                ref = dx_ref.at[:, pl.ds(pl.multiple_of(src * cw + i * hw, hw), hw)]
                _remote(ref, ref, out_send.at[i, 0], out_recv.at[i, d], mate).wait_recv()
            for r in range(n_row):
                @pl.when(at.r != r)
                def _(r=r):
                    hand_remote(i, r).wait_send()

                @pl.when(at.r == r)
                def _(r=r):
                    hand_local(i, r).wait()

        settle(0)
        settle(1)
        ag_own(0)
        for u in range(2, 8):
            settle(u)
        wo_steps(0, 4)
        ag_relay(0)
        ag_own(1)
        ag_own(2)
        wo_steps(4, 7)
        ag_finish(0)
        for cp in keep:
            cp.wait()
        w_finish()
        partial(0)
        ag_relay(1)
        far_a(0)
        far_b(0)
        ag_own(3)
        ag_relay(2)
        ag_own(4)
        wo_steps(7, 8)
        ag_finish(1)
        partial(1)
        far_a(1)
        far_b(1)
        ag_relay(3)
        ag_own(5)
        wo_steps(8, 10)
        ag_finish(2)
        partial(2)
        ag_relay(4)
        ag_own(6)
        plus_a(0)
        wo_steps(10, 12)
        ag_finish(3)
        partial(3)
        minus_a(0)
        ag_relay(5)
        ag_own(7)
        wo_steps(12, 13)
        ag_finish(4)
        partial(4)
        plus_a(1)
        plus_b(0)
        ag_relay(6)
        wo_steps(13, 14)
        ag_finish(5)
        partial(5)
        minus_a(1)
        minus_b(0)
        plus_b(1)
        minus_b(1)
        ag_relay(7)
        wo_steps(14, 16)
        ag_finish(6)
        partial(6)
        wq_steps(0, 2)
        ag_finish(7)
        partial(7)
        wq_steps(2, 5)
        finish(0, 0)
        wq_steps(5, 12)
        finish(0, 1)
        wq_steps(12, 16)
        kv_grads()
        finish(1, 0)
        received(0)
        finish(1, 1)
        received(1)
        for cp in sends:
            cp.wait_send()
        w_drain()
        for g in (gx, gy, gz):
            g.drain()

    pl.run_scoped(back, pltpu.VMEM((4, tokens, bc), BF16), pltpu.VMEM((2, hd, bc), F32), pltpu.VMEM((per_kv * 2 * e, tokens), BF16))


def _layer(ring, cores, heads, scale, x, dy, wq, wk, wv, wo):
    rows, width = x.shape
    tokens = rows * ring * ring * cores
    hd = wo.shape[0]
    e = hd // heads
    n_row = ring * cores
    cw = width // n_row
    gw = hd + 2 * e
    tb = tokens // ring
    th, hw = tb // 2, cw // 2
    per_kv = n_row * ring // wk.shape[0]
    bq = min(256, tb)
    bs = tb // heads
    bc = min(512, cw // 2)
    dma = pltpu.SemaphoreType.DMA
    shape = jax.ShapeDtypeStruct
    return pl.pallas_call(
        functools.partial(_kernel, ring, cores, heads, scale, bq, bs, bc),
        name="layer",
        in_specs=[ANY] * 6,
        out_specs=[ANY, ANY, ANY, VMEM, VMEM, ANY, ANY],
        out_shape=[
            shape((rows, width), BF16),
            shape((hd, width), F32),
            shape((hd, width), F32),
            shape((e, width // per_kv), F32),
            shape((e, width // per_kv), F32),
            shape((tokens, width), BF16),
            shape((tokens, width), BF16),
        ],
        scratch_shapes=[
            pltpu.VMEM((tokens, n_row * gw), BF16),
            pltpu.VMEM((n_row * gw, cw), BF16),
            pltpu.VMEM((4, tb, cw), F32),
            pltpu.VMEM((2, 2, th, hw), F32),
            pltpu.VMEM((2, 2, 2, th, hw), F32),
            pltpu.VMEM((tb, cw), BF16),
            pltpu.VMEM((4, hd // 2, cw), BF16),
            pltpu.VMEM((gw, tokens), BF16),
            pltpu.VMEM((hd, tokens), BF16),
            pltpu.VMEM((hd, tokens), BF16),
            pltpu.VMEM((hd, tokens), BF16),
            pltpu.VMEM((e, tokens), F32),
            pltpu.VMEM((e, tokens), F32),
            pltpu.VMEM((tokens, e), BF16),
            pltpu.VMEM((tokens, e), BF16),
            dma((3, 48)),
            dma((3, 4, 4, 2)),
            dma((3, 4, 4)),
            dma((13,)),
            dma((9,)),
            dma((4,)),
            dma((9 + 2 * n_row,)),
            dma((1,)),
            dma((8, 9)),
            dma((8, 9)),
            dma((6, 2)),
            dma((6, 2)),
            dma((2, n_row)),
            dma((2, n_row)),
            dma((4,)),
            dma((2,)),
        ],
        compiler_params=pltpu.CompilerParams(collective_id=0, has_side_effects=True, vmem_limit_bytes=67043328),
        cost_estimate=pl.CostEstimate(flops=70 * 10**9, bytes_accessed=300 << 20, transcendentals=heads * tokens * tokens // 2),
    )(x, dy, wq, wk, wv, wo)


def solution(mesh):
    n = mesh.shape["tp"]
    ring = math.isqrt(n // 2)
    cores = n // (ring * ring)
    if ring != 4 or cores != 2:
        raise ValueError("needs a 4x4 torus")

    def local_grads(x_blk, dy_blk, wq_loc, w_k, w_v, wo_loc):
        model_dim, kv_heads, e = w_k.shape
        heads = wq_loc.shape[1]
        hd = heads * e
        scale = e ** -0.5
        wq = jnp.transpose(wq_loc, (1, 2, 0)).reshape(hd, model_dim)
        wk = jnp.transpose(w_k, (1, 2, 0))
        wv = jnp.transpose(w_v, (1, 2, 0))
        wo = wo_loc.reshape(hd, model_dim)
        dx, dwq, dwo, dwk, dwv, _, _ = _layer(ring, cores, heads, scale, x_blk, dy_blk, wq, wk, wv, wo)
        return (dx, jnp.transpose(dwq.reshape(heads, e, model_dim), (2, 0, 1)), dwo.reshape(heads, e, model_dim), dwk.T, dwv.T)

    tok = P(("dp", "tp"))
    return jax.shard_map(
        local_grads,
        mesh=mesh,
        in_specs=(tok, tok, P(None, "tp", None), P(), P(), P("tp")),
        out_specs=(tok, P("dp", "tp", None), tok, tok, tok),
        check_vma=False,
    )
```

```python
import functools
import math

import jax
import jax.numpy as jnp
from jax import lax
from jax.experimental import pallas as pl
from jax.experimental.pallas import tpu as pltpu
from jax.sharding import PartitionSpec as P

F32 = jnp.float32
BF16 = jnp.bfloat16
MESH = pl.DeviceIdType.MESH
ANY = pl.BlockSpec(memory_space=pl.ANY)
VMEM = pl.BlockSpec(memory_space=pltpu.VMEM)
LOG2E = math.log2(math.e)


def _scoped(fn):
    def run(*args, **kw):
        with jax.named_scope(fn.__name__):
            return fn(*args, **kw)

    return run


def _dot(a, b, dims):
    return lax.dot_general(a, b, (dims, ((), ())), preferred_element_type=F32)


def _nn(a, b):
    return _dot(a, b, ((1,), (0,)))


def _nt(a, b):
    return _dot(a, b, ((1,), (1,)))


class Place:
    def __init__(self, ring, cores):
        me = lax.axis_index("tp")
        self.ring, self.cores = ring, cores
        self.c = lax.rem(me, cores)
        self.x = lax.rem(me // cores, ring)
        self.y = me // (cores * ring)
        self.r = self.x * cores + self.c
        self.n_row = ring * cores

    def dev(self, y, x, c):
        y = lax.rem(y + self.ring, self.ring)
        x = lax.rem(x + self.ring, self.ring)
        return {"tp": (y * self.ring + x) * self.cores + c}

    def row_dev(self, r):
        return {"tp": self.y * self.n_row + r}

    def slot(self, x, c):
        return lax.rem(x + self.ring, self.ring) * self.cores + c


def _remote(src, dst, send, recv, dev):
    return pltpu.make_async_remote_copy(
        src_ref=src, dst_ref=dst, send_sem=send, recv_sem=recv, device_id=dev, device_id_type=MESH
    )


@_scoped
def _enter(devices):
    barrier = pltpu.get_barrier_semaphore()
    for dev in devices:
        pl.semaphore_signal(barrier, inc=1, device_id=dev, device_id_type=MESH)
    pl.semaphore_wait(barrier, len(devices))


OWN, MINUS, PLUS, FAR = range(4)
STEP = (0, -1, 1, 2)


def _load_shard(at, full, n, y, x, core, block, sem):
    r0 = at.dev(y, x, core)["tp"] * n
    b0 = at.slot(x, core) * n
    src = full.at[pl.ds(pl.multiple_of(r0, n), n), :]
    return pltpu.make_async_copy(src, block.at[pl.ds(pl.multiple_of(b0, n), n), :], sem)


@_scoped
def _take_row(lanes, t, y, block, sem):
    at, full, n = lanes[0].at, lanes[0].full, lanes[0].shard
    for j in range(4):
        _load_shard(at, full, n, y, at.x + STEP[j], at.c, block, sem).start()
    for j in range(4):
        for g in lanes:
            g.await_mate(t, j)
        _load_shard(at, full, n, y, at.x + STEP[j], 1 - at.c, block, sem).start()


class Gather:
    def __init__(self, at, src, full, send, recv, mate_recv, orders, row0, rows, tag):
        self.at, self.src, self.full = at, src, full
        self.send, self.recv, self.mate_recv = send.at[tag], recv.at[tag], mate_recv.at[tag]
        self.order, self.mate_order = orders
        self.row0, self.rows, self.shard = row0, rows, src.shape[0]
        self.sent = []
        c, o = at.c, self.order
        self.first = {s: at.dev(at.y + o * s, at.x + (1 - o) * s, c) for s in (1, -1)}
        self.second = {s: at.dev(at.y + (1 - o) * s, at.x + o * s, c) for s in (1, -1)}
        self.mate = at.dev(at.y, at.x, 1 - c)
        self.fulls = {d: self.both_ways(self.second, d, lambda to, d=d: (d, to)) for d in range(4)}

    def span(self, half):
        n = self.rows if half is None else self.rows // 2
        return self.row0 + (0 if half is None else half * n), n

    def ref(self, d1, d2, half=None):
        at, o = self.at, self.order
        o1, o2 = STEP[d1], STEP[d2]
        start, n = self.span(half)
        r0 = at.dev(at.y + o * o1 + (1 - o) * o2, at.x + (1 - o) * o1 + o * o2, at.c)["tp"] * self.shard + start
        return self.full.at[pl.ds(pl.multiple_of(r0, math.gcd(self.shard, self.row0, n)), n), :]

    def push(self, src, dst, recv, dev):
        k = len(self.sent)
        self.sent.append(dst.shape[0])
        return _remote(src, dst, self.send.at[k], recv, dev)

    def out(self, d1, d2, half=None):
        if d1 == OWN and d2 == OWN:
            return self.src.at[pl.ds(*self.span(half)), :]
        return self.ref(d1, d2, half)

    def both_ways(self, devs, d1, name):
        copies = []
        for step in (0, 1):
            for s, to in ((1, MINUS), (-1, PLUS)):
                half = step if s == 1 else 1 - step
                copies.append(self.push(self.out(d1, OWN, half), self.ref(d1, OWN, half), self.recv.at[*name(to), half], devs[s]))
        return copies

    def to_mate(self, d1, d2):
        ref = self.ref(d1, d2)
        self.push(self.out(d1, d2), ref, self.mate_recv.at[d1, d2], self.mate).start()

    def arrived(self, d1, d2, half):
        ref = self.ref(d1, d2, half)
        _remote(ref, ref, self.send.at[0], self.recv.at[d1, d2, half], self.mate).wait_recv()

    @_scoped
    def start(self):
        for cp in self.both_ways(self.first, OWN, lambda to: (to, OWN)):
            cp.start()
        self.go(OWN)
        self.to_mate(OWN, OWN)

    def go(self, d1):
        for cp in self.fulls[d1]:
            cp.start()

    @_scoped
    def relay_first(self):
        for d, s, half in ((MINUS, 1, 0), (PLUS, -1, 1)):
            self.arrived(d, OWN, half)
            ref = self.ref(d, OWN, half)
            self.push(ref, ref, self.recv.at[FAR, OWN, half], self.first[s]).start()

    @_scoped
    def near_first(self):
        for d, half in ((MINUS, 1), (PLUS, 0)):
            self.arrived(d, OWN, half)
            self.to_mate(d, OWN)

    @_scoped
    def far_first(self):
        for half in (0, 1):
            self.arrived(FAR, OWN, half)
        self.to_mate(FAR, OWN)

    @_scoped
    def relay_second(self, d1):
        for d, s, half in ((MINUS, 1, 0), (PLUS, -1, 1)):
            self.arrived(d1, d, half)
            ref = self.ref(d1, d, half)
            self.push(ref, ref, self.recv.at[d1, FAR, half], self.second[s]).start()

    @_scoped
    def near_second(self, d1):
        for d, half in ((MINUS, 1), (PLUS, 0)):
            self.arrived(d1, d, half)
            self.to_mate(d1, d)

    @_scoped
    def far_second(self, d1):
        for half in (0, 1):
            self.arrived(d1, FAR, half)
        self.to_mate(d1, FAR)

    def await_mate(self, t, j):
        o = self.mate_order
        ref = self.full.at[pl.ds(0, self.rows), :]
        _remote(ref, ref, self.send.at[0], self.mate_recv.at[(1 - o) * j + o * t, (1 - o) * t + o * j], self.mate).wait_recv()

    @_scoped
    def drain(self):
        for k, n in enumerate(self.sent):
            ref = self.full.at[pl.ds(0, n), :]
            _remote(ref, ref, self.send.at[k], self.send.at[k], self.mate).wait_send()


def _kernel(ring, cores, heads, scale, bq, bs, bc, x_ref, dy_ref, w_ref, wk_ref, wv_ref, wo_ref,
            dx_ref, dwq_ref, dwo_ref, dwk_ref, dwv_ref, xf_ref, dyf_ref,
            gq, w_all, part, rs_half, rs_full, stage, hop_ref, qkvt_ref, dot_ref, dqt_ref, ot_ref, dk_ref, dv_ref, kn_ref, vn_ref,
            send, recv, mate_recv, w_send, w_recv, hop_recv, ld_sem, blk_sem,
            ag_send, ag_recv, rs_send, rs_recv, out_send, out_recv, in_sem, o_sem):
    at = Place(ring, cores)
    n_row = at.n_row
    hd = wo_ref.shape[0]
    e = hd // heads
    tokens, width = xf_ref.shape
    tb = tokens // ring
    cw = width // n_row
    gw = gq.shape[1] // n_row
    c = at.c
    shard = x_ref.shape[0]
    gx = Gather(at, x_ref, xf_ref, send, recv, mate_recv, (c, 1 - c), 0, shard, 0)
    split = shard * 3 // 4
    gy = Gather(at, dy_ref, dyf_ref, send, recv, mate_recv, (c, 1 - c), 0, split, 1)
    gz = Gather(at, dy_ref, dyf_ref, send, recv, mate_recv, (0, 0), split, shard - split, 2)
    n_kv = wk_ref.shape[0] // ring
    per_kv = n_row // n_kv
    row_peers = [lax.rem(at.r + d, n_row) for d in range(1, n_row)]
    up, down = at.dev(at.y + 1, at.x, c), at.dev(at.y - 1, at.x, c)

    hh = hd // 2

    def w_push(k, src, dst, rsem, dev):
        _remote(src, dst, w_send.at[k], rsem, dev).start()

    def wq_slot(slot, half=None):
        r0 = slot * gw + (0 if half is None else half * hh)
        return w_all.at[pl.ds(r0 if isinstance(r0, int) else pl.multiple_of(r0, hh), hd if half is None else hh), :]

    def wcols(slot):
        return pl.ds(pl.multiple_of(slot * cw, cw), cw)

    right, left, mate = at.dev(at.y, at.x + 1, c), at.dev(at.y, at.x - 1, c), at.dev(at.y, at.x, 1 - c)

    @_scoped
    def w_start():
        for half, dev in ((0, right), (1, left)):
            for k in range(cores):
                w_push(half * 2 + k, w_ref.at[pl.ds(half * hh, hh), wcols(at.slot(at.x + 2, k))], hop_ref.at[half * 2 + k], hop_recv.at[half * 2 + k], dev)
        w_push(4, w_ref.at[pl.ds(0, hd), wcols(at.slot(at.x, 1 - c))], wq_slot(at.r), w_recv.at[0], mate)
        for i, s in enumerate((1, -1)):
            for k in range(cores):
                dst_core = c if k == 0 else 1 - c
                w_push(5 + 2 * i + k, w_ref.at[pl.ds(0, hd), wcols(at.slot(at.x + s, dst_core))], wq_slot(at.r), w_recv.at[1 + 2 * i + k], at.dev(at.y, at.x + s, dst_core))

    @_scoped
    def w_relay():
        for half, s in ((0, 1), (1, -1)):
            for n in (half * 2, half * 2 + 1):
                _remote(hop_ref.at[n], hop_ref.at[n], w_send.at[0], hop_recv.at[n], mate).wait_recv()
            for k in range(cores):
                n = half * 2 + k
                src_slot = at.slot(at.x - s, c)
                same = k == 0
                dst_core = c if same else 1 - c
                w_push(9 + n, hop_ref.at[half * 2 + dst_core], wq_slot(src_slot, half), w_recv.at[5 + n], at.dev(at.y, at.x + s, dst_core))

    @_scoped
    def w_finish():
        whole = wq_slot(0)
        piece = wq_slot(0, 0)
        for n in range(9):
            ref = whole if n < 5 else piece
            _remote(ref, ref, w_send.at[0], w_recv.at[n], mate).wait_recv()

    def w_drain():
        whole = wq_slot(0)
        piece = wq_slot(0, 0)
        for k in range(13):
            ref = whole if 4 <= k < 9 else piece
            _remote(ref, ref, w_send.at[k], w_send.at[k], mate).wait_send()

    own_cols = wcols(at.r)
    rows = x_ref.shape[0]
    own_rows = pl.ds(pl.multiple_of((at.y * n_row + at.r) * rows, rows), rows)

    keep = [pltpu.make_async_copy(w_ref.at[:, own_cols], wq_slot(at.r), ld_sem.at[8])]
    for r in range(n_row):
        kv_r = at.y * n_kv + r // per_kv
        for i, w in enumerate((wk_ref, wv_ref)):
            keep.append(pltpu.make_async_copy(w.at[kv_r, :, own_cols], w_all.at[pl.ds(r * gw + hd + i * e, e), :], ld_sem.at[9 + 2 * r + i]))

    th = tb // 2
    tq = th // 2
    tl = tb // n_row
    hw = cw // 2
    half_a, half_b = pl.ds(0, hw), pl.ds(hw, hw)
    units = [(FAR, 0), (FAR, 1), (PLUS, 0), (MINUS, 0), (PLUS, 1), (MINUS, 1), (OWN, 0), (OWN, 1)]
    s_own, s_left, s_right, s_far = (at.slot(at.x + o, c) for o in (0, -1, 1, 2))
    m_own, m_left, m_right, m_far = (at.slot(at.x + o, 1 - c) for o in (0, -1, 1, 2))

    def unit_row(u):
        d, s = units[u % len(units)]
        return pl.multiple_of(lax.rem(at.y + STEP[d] + ring, ring) * tb + s * th, th)

    last = len(units)

    def gcols(u, slot):
        if u == 0:
            return pl.ds(pl.multiple_of(slot * gw, 128), hd)
        if u == last:
            return pl.ds(pl.multiple_of(slot * gw + hd, 128), gw - hd)
        return pl.ds(pl.multiple_of(slot * gw, gw), gw)

    def piece(u, slot, half=None):
        r0 = unit_row(u)
        rows = pl.ds(r0, th) if half is None else pl.ds(pl.multiple_of(r0 + half * tq, tq), tq)
        return gq.at[rows, gcols(u, slot)]

    ag_sent = []

    def ag_push(u, n, slot, dev, half=None):
        ref = piece(u, slot, half)
        _remote(ref, ref, ag_send.at[u, n], ag_recv.at[u, n], dev).start()
        ag_sent.append((u, n, half))

    def ag_drain():
        for u, n, half in ag_sent:
            ref = piece(u, s_own, half)
            _remote(ref, ref, ag_send.at[u, n], ag_recv.at[u, n], mate).wait_send()

    def ag_wait(u, n, slot, half=None):
        ref = piece(u, slot, half)
        _remote(ref, ref, ag_send.at[u, n], ag_recv.at[u, n], mate).wait_recv()

    def ag_own(u):
        ag_push(u, 0, s_own, right)
        ag_push(u, 1, s_own, left)
        ag_push(u, 2, s_own, mate)

    @_scoped
    def ag_relay(u):
        ag_wait(u, 0, s_left)
        ag_push(u, 3, s_left, right, 0)
        ag_push(u, 4, s_left, mate)
        ag_wait(u, 1, s_right)
        ag_push(u, 5, s_right, left, 1)
        ag_push(u, 6, s_right, mate)

    @_scoped
    def ag_finish(u):
        ag_wait(u, 3, s_far, 0)
        ag_push(u, 7, s_far, mate, 0)
        ag_wait(u, 5, s_far, 1)
        ag_push(u, 8, s_far, mate, 1)
        ag_wait(u, 2, m_own)
        ag_wait(u, 4, m_left)
        ag_wait(u, 6, m_right)
        ag_wait(u, 7, m_far, 0)
        ag_wait(u, 8, m_far, 1)

    def settle(u):
        rows = pl.ds(unit_row(u), th)
        kv = jnp.concatenate([(dk_ref[:, rows] * scale).astype(BF16), dv_ref[:, rows].astype(BF16)], axis=0)
        gq[rows, pl.ds(pl.multiple_of(at.r * gw + hd, 128), 2 * e)] = kv.T

    def front(w_v, wo_v, xblk):
        kv = (at.y * n_row + at.r) // (n_row * ring // wk_ref.shape[0])
        loads = [
            pltpu.make_async_copy(w_ref, w_v.at[pl.ds(0, hd), :], ld_sem.at[0]),
            pltpu.make_async_copy(wo_ref, wo_v, ld_sem.at[1]),
            pltpu.make_async_copy(wk_ref.at[kv], w_v.at[pl.ds(hd, e), :], ld_sem.at[6]),
            pltpu.make_async_copy(wv_ref.at[kv], w_v.at[pl.ds(hd + e, e), :], ld_sem.at[7]),
        ]
        ins = [pltpu.make_async_copy(src, xblk.at[pl.ds(i * rows, rows), :], ld_sem.at[2 + i]) for i, src in enumerate((x_ref, dy_ref))]
        outs = [pltpu.make_async_copy(xblk.at[pl.ds(i * rows, rows), :], dst.at[own_rows, :], ld_sem.at[4 + i]) for i, dst in enumerate((xf_ref, dyf_ref))]
        for cp in ins:
            cp.start()
        _enter([up, down] + [at.row_dev(r) for r in row_peers])
        gx.start()
        for cp in loads + keep:
            cp.start()
        for cp in ins:
            cp.wait()
        for cp in outs:
            cp.start()

        dk_ref[...] = jnp.zeros_like(dk_ref)
        dv_ref[...] = jnp.zeros_like(dv_ref)

        @_scoped
        def project(w, out, b):
            pltpu.make_async_copy(xf_ref.at[pl.ds(0, tb), :], xblk, blk_sem.at[0]).wait()

            def block(i, _):
                r0 = pl.multiple_of(i * bq, bq)
                out[:, pl.ds(pl.multiple_of(b * tb + i * bq, bq), bq)] = _nt(w[...], xblk[pl.ds(r0, bq), :]).astype(BF16)
                return 0

            lax.fori_loop(0, tb // bq, block, 0)

        def row_at(t):
            if isinstance(t, int):
                return lax.rem(at.y + STEP[t] + ring, ring)
            off = jnp.where(t == 1, ring - 1, jnp.where(t == 2, 1, jnp.where(t == 3, 2, 0)))
            return lax.rem(at.y + off, ring)

        for cp in loads + outs:
            cp.wait()

        def begin(g):
            g.relay_first()
            g.near_first()
            g.go(MINUS)

            @pl.when(g.order == 0)
            def _():
                g.go(PLUS)

        def begin_far(g):
            g.far_first()

            @pl.when(g.order == 0)
            def _():
                g.go(FAR)

        def begin_second(g):
            g.relay_second(OWN)

            @pl.when(g.order == 1)
            def _():
                g.go(PLUS)

            g.near_second(OWN)

        def second_minus(g):
            g.relay_second(MINUS)

            @pl.when(g.order == 1)
            def _():
                g.go(FAR)

            g.near_second(MINUS)

        def x_turn(t, _):
            @pl.when(t == 0)
            def _():
                begin(gx)
                begin_far(gx)
                begin_second(gx)
                second_minus(gx)
                gx.relay_second(PLUS)
                gx.near_second(PLUS)
                gx.relay_second(FAR)
                gy.start()
                gz.start()
                gx.far_second(OWN)

            @pl.when(t == 1)
            def _():
                gx.near_second(FAR)
                gx.far_second(MINUS)

            @pl.when(t == 2)
            def _():
                for d in (PLUS, FAR):
                    gx.far_second(d)

            @pl.when(t == 3)
            def _():
                begin(gy)
                begin(gz)

            b = row_at(t)
            _take_row((gx,), t, b, xblk, blk_sem.at[0])
            project(w_v, qkvt_ref, b)
            return 0

        lax.fori_loop(0, ring, x_turn, 0)
        for t in range(0, tokens, bq):
            kn_ref[t:t + bq, :] = qkvt_ref[hd:hd + e, t:t + bq].T
            vn_ref[t:t + bq, :] = qkvt_ref[hd + e:hd + 2 * e, t:t + bq].T

        keys_k, keys_v = slice(hd, hd + e), slice(hd + e, hd + 2 * e)
        m4 = heads * bs
        factor = scale * LOG2E

        def row_chunks(k):
            return [slice(t, t + bq) for t in range(0, (k + 1) * tb, bq)]

        def stacked(ref, qs):
            return jnp.concatenate([ref[h * e:(h + 1) * e, qs] for h in range(heads)], axis=1)

        def unstack(ref, qs, value):
            for h in range(heads):
                ref[h * e:(h + 1) * e, qs] = value[:, h * bs:(h + 1) * bs]

        def scores(q, ks, k, j):
            s = _nn(q, qkvt_ref[keys_k, ks])
            if ks.start < k * tb:
                return s
            row = lax.broadcasted_iota(jnp.int32, (m4, bq), 0) & (bs - 1)
            col = lax.broadcasted_iota(jnp.int32, (m4, bq), 1)
            return jnp.where(col + (ks.start - k * tb) <= row + j * bs, s, -jnp.inf)

        def folded(op, total, value):
            for t in range(0, value.shape[1], 128):
                piece = value[:, t:t + 128]
                total = piece if total is None else op(total, piece)
            return total

        def score_buf(ks):
            n = ks.start // cw
            return part.at[n, :, ks.start - n * cw:ks.stop - n * cw]

        def stats_buf(k, j):
            per = cw // 128
            n = k * (tb // bs)
            return part.at[2 + n // per, :, pl.ds(pl.multiple_of((n % per + j) * 128, 128), 128)]

        @_scoped
        def forward(k):
            chunks = row_chunks(k)

            def queries(j, _):
                qs = pl.ds(pl.multiple_of(k * tb + j * bs, bs), bs)
                q = stacked(qkvt_ref, qs).T
                m = None
                for ks in chunks:
                    s = scores(q, ks, k, j)
                    score_buf(ks)[...] = s
                    m = folded(jnp.maximum, m, s)
                m = jnp.max(m, axis=1, keepdims=True)
                total = None
                for ks in chunks:
                    p = jnp.exp2((score_buf(ks)[...] - m) * factor)
                    score_buf(ks)[...] = p
                    total = folded(jnp.add, total, p)
                inv = 1.0 / jnp.sum(total, axis=1, keepdims=True)
                lane = lax.broadcasted_iota(jnp.int32, (m4, 128), 1)
                stats_buf(k, j)[...] = jnp.where(lane == 0, m, inv)
                out = None
                for ks in chunks:
                    piece = _nn((score_buf(ks)[...] * inv).astype(BF16), vn_ref[ks, :])
                    out = piece if out is None else out + piece
                unstack(ot_ref, qs, out.astype(BF16).T)
                return 0

            lax.fori_loop(0, tb // bs, queries, 0)

        @_scoped
        def backward(k, second):
            chunks = row_chunks(k)

            def queries(j, _):
                qs = pl.ds(pl.multiple_of(k * tb + j * bs, bs), bs)
                qt = stacked(qkvt_ref, qs)
                dot = stacked(dot_ref, qs)
                q, do = qt.T, dot.T
                delta = jnp.sum(dot.astype(F32) * stacked(ot_ref, qs).astype(F32), axis=0, keepdims=True)
                delta = jnp.broadcast_to(delta, (128, m4)).T[:, :1]
                stats = stats_buf(k, j)[...]
                m, inv = stats[:, 0:1], stats[:, 1:2]
                dq = None
                for ks in chunks:
                    p = jnp.exp2((scores(q, ks, k, j) - m) * factor) * inv
                    dp = _nn(do, qkvt_ref[keys_v, ks])
                    ds = (p * (dp - delta)).astype(BF16)
                    dv_ref[:, ks] += _nn(dot, p.astype(BF16))
                    dk_ref[:, ks] += _nn(qt, ds)
                    piece = _nn(ds, kn_ref[ks, :])
                    dq = piece if dq is None else dq + piece
                dq = (dq * scale).astype(BF16).T
                unstack(dqt_ref, qs, dq)
                for h in range(0, heads, 2):
                    pair = jnp.concatenate([dq[:, h * bs:(h + 1) * bs], dq[:, (h + 1) * bs:(h + 2) * bs]], axis=0)
                    gq[qs, pl.ds(pl.multiple_of(at.r * gw + h * e, 128), 2 * e)] = pair.T
                return 0

            n = tb // bs // 2
            lax.fori_loop(second * n, (second + 1) * n, queries, 0)

        forward(0)
        begin_far(gy)
        begin_far(gz)
        forward(1)
        begin_second(gy)
        begin_second(gz)
        forward(2)
        forward(3)
        second_minus(gy)
        second_minus(gz)

        def turn(h, _):
            t, second = h // 2, lax.rem(h, 2)

            @pl.when(h == 0)
            def _():
                @pl.when(c == 1)
                def _():
                    far_step(OWN)

            @pl.when(h == 1)
            def _():
                for g in (gy, gz):
                    g.relay_second(PLUS)
                    g.near_second(PLUS)

                @pl.when(c == 1)
                def _():
                    far_step(MINUS)

            @pl.when(h == 2)
            def _():
                for g in (gy, gz):
                    g.relay_second(FAR)
                    g.near_second(FAR)

                w_start()

            @pl.when(h == 3)
            def _():
                @pl.when(c == 1)
                def _():
                    far_step(PLUS)

                @pl.when(c == 0)
                def _():
                    far_step(OWN)
                    far_step(MINUS)

            b = row_at(t)

            @pl.when((second == 0) & (t != 3))
            def _():
                _take_row((gy, gz), t, b, xblk, blk_sem.at[0])

            @pl.when(second == 0)
            def _():
                project(wo_v, dot_ref, b)

            @pl.when(h == 5)
            def _():
                @pl.when(c == 0)
                def _():
                    far_step(PLUS)

                far_step(FAR)
                for d in range(4):
                    gz.far_second(d)
                w_relay()
                _take_row((gy, gz), FAR, row_at(FAR), xblk, blk_sem.at[0])

            @pl.when(h == 7)
            def _():
                ag_own(0)

            for k in range(ring):
                @pl.when(b == k)
                def _(k=k):
                    backward(k, second)
            return 0

        far_cp = {d: gy.push(gy.ref(d, FAR), gy.ref(d, FAR), gy.mate_recv.at[d, FAR], gy.mate) for d in range(4)}

        @_scoped
        def far_step(d):
            for half in (0, 1):
                gy.arrived(d, FAR, half)
            far_cp[d].start()

        lax.fori_loop(0, 2 * ring, turn, 0)


    pl.run_scoped(front, pltpu.VMEM((hd + 2 * e, width), BF16), pltpu.VMEM((hd, width), BF16), pltpu.VMEM((tb, width), BF16))

    def back(xbuf, obuf, kvt):
        sends = []

        nt = min(256, hw)

        @_scoped
        def partial(u):
            rows = pl.ds(unit_row(u), th)
            d, s = units[u]
            dst = part.at[d, pl.ds(s * th, th), :]

            def tile(j, _):
                cs = pl.ds(pl.multiple_of(j * nt, nt), nt)
                dst[:, cs] = _nn(gq[rows, :], w_all[:, cs])
                return 0

            lax.fori_loop(0, cw // nt, tile, 0)

        def rs_push(n, s, src, dst, dev):
            cp = _remote(src, dst, rs_send.at[n, s], rs_recv.at[n, s], dev)
            cp.start()
            sends.append(cp)

        def rs_wait(n, s):
            ref = rs_half.at[0, s]
            _remote(ref, ref, rs_send.at[n, s], rs_recv.at[n, s], mate).wait_recv()

        def block(d, s, half):
            return part.at[d, pl.ds(s * th, th), half]

        def far_a(s):
            rs_push(0, s, block(FAR, s, half_a), rs_half.at[0, s], up)

        def far_b(s):
            rs_push(1, s, block(FAR, s, half_b), rs_half.at[1, s], down)

        def minus_a(s):
            rs_push(4, s, block(MINUS, s, half_a), rs_full.at[1, s, 0], down)

        def plus_b(s):
            rs_push(3, s, block(PLUS, s, half_b), rs_full.at[0, s, 1], up)

        @_scoped
        def plus_a(s):
            rs_wait(0, s)
            block(PLUS, s, half_a)[...] += rs_half[0, s]
            rs_push(2, s, block(PLUS, s, half_a), rs_full.at[0, s, 0], up)

        @_scoped
        def minus_b(s):
            rs_wait(1, s)
            block(MINUS, s, half_b)[...] += rs_half[1, s]
            rs_push(5, s, block(MINUS, s, half_b), rs_full.at[1, s, 1], down)

        n_steps = width // bc
        depth = xbuf.shape[0]

        def chunk(src, c0, j):
            slot = lax.rem(j, depth)
            return pltpu.make_async_copy(src.at[:, pl.ds(pl.multiple_of(c0 + j * bc, bc), bc)], xbuf.at[slot], in_sem.at[slot])

        def ahead(src, c0, n):
            for j in range(min(depth - 1, n)):
                chunk(src, c0, j).start()

        @_scoped
        def stream(src, lhs, out, j0, j1):
            def store(j):
                slot = lax.rem(j, 2)
                return pltpu.make_async_copy(obuf.at[slot], out.at[:, pl.ds(pl.multiple_of(j * bc, bc), bc)], o_sem.at[slot])

            if j0 == 0:
                ahead(src, 0, n_steps)

            def step(j, _):
                @pl.when(j + depth - 1 < n_steps)
                def _():
                    chunk(src, 0, j + depth - 1).start()

                chunk(src, 0, j).wait()

                @pl.when(j >= 2)
                def _():
                    store(j - 2).wait()

                obuf[lax.rem(j, 2)] = _nn(lhs[...], xbuf[lax.rem(j, depth)])
                store(j).start()
                return 0

            lax.fori_loop(j0, j1, step, 0)
            if j1 == n_steps:
                for j in range(max(n_steps - 2, 0), n_steps):
                    store(j).wait()

        def wo_steps(a, b):
            stream(dyf_ref, ot_ref, dwo_ref, n_steps * a // 16, n_steps * b // 16)

        def wq_steps(a, b):
            stream(xf_ref, dqt_ref, dwq_ref, n_steps * a // 16, n_steps * b // 16)

        first = (at.r // per_kv) * per_kv
        share = width // per_kv
        col0 = lax.rem(at.r, per_kv) * share

        def kv_step(j, _):
            @pl.when(j + depth - 1 < share // bc)
            def _():
                chunk(xf_ref, col0, j + depth - 1).start()

            chunk(xf_ref, col0, j).wait()
            prod = _nn(kvt[...], xbuf[lax.rem(j, depth)])
            dk = dv = None
            for q in range(per_kv):
                a = prod[q * 2 * e:q * 2 * e + e]
                b = prod[q * 2 * e + e:(q + 1) * 2 * e]
                dk = a if dk is None else dk + a
                dv = b if dv is None else dv + b
            cs = pl.ds(pl.multiple_of(j * bc, bc), bc)
            dwk_ref[:, cs] = dk
            dwv_ref[:, cs] = dv
            return 0

        @_scoped
        def kv_grads():
            ahead(xf_ref, col0, share // bc)
            for q in range(per_kv):
                cols = pl.ds(pl.multiple_of((first + q) * gw + hd, 128), gw - hd)
                for t in range(0, tokens, bq):
                    kvt[q * (gw - hd):(q + 1) * (gw - hd), t:t + bq] = gq[t:t + bq, cols].T
            lax.fori_loop(0, share // bc, kv_step, 0)

        per_half = n_row // 2

        def hand(i, r):
            half = (half_a, half_b)[i]
            rows = pl.ds(r * tl, tl)
            cols = pl.ds(pl.multiple_of(at.r * cw + i * hw, hw), hw)
            return stage.at[rows, half], dx_ref.at[:, cols]

        def hand_remote(i, r):
            src, dst = hand(i, r)
            d = lax.rem(r - at.r + n_row, n_row)
            return _remote(src, dst, out_send.at[i, r], out_recv.at[i, d], at.row_dev(r))

        def hand_local(i, r):
            src, dst = hand(i, r)
            return pltpu.make_async_copy(src, dst, out_send.at[i, r])

        @_scoped
        def finish(i, s):
            half = (half_a, half_b)[i]
            rs_wait(2 + i, s)
            rs_wait(4 + i, s)
            stage[s * th:(s + 1) * th, half] = (block(OWN, s, half)[...] + rs_full[0, s, i] + rs_full[1, s, i]).astype(BF16)
            for r in range(s * per_half, (s + 1) * per_half):
                @pl.when(at.r != r)
                def _(r=r):
                    hand_remote(i, r).start()

                @pl.when(at.r == r)
                def _(r=r):
                    hand_local(i, r).start()

        @_scoped
        def received(i):
            for d in range(1, n_row):
                src = lax.rem(at.r + n_row - d, n_row)
                ref = dx_ref.at[:, pl.ds(pl.multiple_of(src * cw + i * hw, hw), hw)]
                _remote(ref, ref, out_send.at[i, 0], out_recv.at[i, d], mate).wait_recv()
            for r in range(n_row):
                @pl.when(at.r != r)
                def _(r=r):
                    hand_remote(i, r).wait_send()

                @pl.when(at.r == r)
                def _(r=r):
                    hand_local(i, r).wait()

        settle(0)
        ag_relay(0)
        settle(1)
        ag_own(last)
        for u in range(2, 8):
            settle(u)
        ag_finish(0)
        wo_steps(0, 2)
        ag_relay(last)
        ag_own(1)
        ag_own(2)
        wo_steps(2, 4)
        ag_finish(last)
        for cp in keep:
            cp.wait()
        w_finish()
        partial(0)
        ag_relay(1)
        far_a(0)
        far_b(0)
        ag_own(3)
        ag_relay(2)
        ag_own(4)
        wo_steps(4, 6)
        ag_finish(1)
        partial(1)
        far_a(1)
        far_b(1)
        ag_relay(3)
        ag_own(5)
        wo_steps(6, 8)
        ag_finish(2)
        partial(2)
        ag_relay(4)
        ag_own(6)
        plus_a(0)
        wo_steps(8, 10)
        ag_finish(3)
        partial(3)
        minus_a(0)
        ag_relay(5)
        ag_own(7)
        wo_steps(10, 12)
        ag_finish(4)
        partial(4)
        plus_a(1)
        plus_b(0)
        ag_relay(6)
        wo_steps(12, 14)
        ag_finish(5)
        partial(5)
        minus_a(1)
        minus_b(0)
        plus_b(1)
        minus_b(1)
        ag_relay(7)
        wo_steps(14, 16)
        ag_finish(6)
        partial(6)
        wq_steps(0, 2)
        ag_finish(7)
        partial(7)
        wq_steps(2, 5)
        finish(0, 0)
        wq_steps(5, 12)
        finish(0, 1)
        wq_steps(12, 16)
        kv_grads()
        finish(1, 0)
        received(0)
        finish(1, 1)
        received(1)
        for cp in sends:
            cp.wait_send()
        ag_drain()
        w_drain()
        for g in (gx, gy, gz):
            g.drain()

    pl.run_scoped(back, pltpu.VMEM((4, tokens, bc), BF16), pltpu.VMEM((2, hd, bc), F32), pltpu.VMEM((per_kv * 2 * e, tokens), BF16))


def _layer(ring, cores, heads, scale, x, dy, wq, wk, wv, wo):
    rows, width = x.shape
    tokens = rows * ring * ring * cores
    hd = wo.shape[0]
    e = hd // heads
    n_row = ring * cores
    cw = width // n_row
    gw = hd + 2 * e
    tb = tokens // ring
    th, hw = tb // 2, cw // 2
    per_kv = n_row * ring // wk.shape[0]
    bq = min(256, tb)
    bs = tb // heads
    bc = min(512, cw // 2)
    dma = pltpu.SemaphoreType.DMA
    shape = jax.ShapeDtypeStruct
    return pl.pallas_call(
        functools.partial(_kernel, ring, cores, heads, scale, bq, bs, bc),
        name="layer",
        in_specs=[ANY] * 6,
        out_specs=[ANY, ANY, ANY, VMEM, VMEM, ANY, ANY],
        out_shape=[
            shape((rows, width), BF16),
            shape((hd, width), F32),
            shape((hd, width), F32),
            shape((e, width // per_kv), F32),
            shape((e, width // per_kv), F32),
            shape((tokens, width), BF16),
            shape((tokens, width), BF16),
        ],
        scratch_shapes=[
            pltpu.VMEM((tokens, n_row * gw), BF16),
            pltpu.VMEM((n_row * gw, cw), BF16),
            pltpu.VMEM((4, tb, cw), F32),
            pltpu.VMEM((2, 2, th, hw), F32),
            pltpu.VMEM((2, 2, 2, th, hw), F32),
            pltpu.VMEM((tb, cw), BF16),
            pltpu.VMEM((4, hd // 2, cw), BF16),
            pltpu.VMEM((gw, tokens), BF16),
            pltpu.VMEM((hd, tokens), BF16),
            pltpu.VMEM((hd, tokens), BF16),
            pltpu.VMEM((hd, tokens), BF16),
            pltpu.VMEM((e, tokens), F32),
            pltpu.VMEM((e, tokens), F32),
            pltpu.VMEM((tokens, e), BF16),
            pltpu.VMEM((tokens, e), BF16),
            dma((3, 48)),
            dma((3, 4, 4, 2)),
            dma((3, 4, 4)),
            dma((13,)),
            dma((9,)),
            dma((4,)),
            dma((9 + 2 * n_row,)),
            dma((1,)),
            dma((9, 9)),
            dma((9, 9)),
            dma((6, 2)),
            dma((6, 2)),
            dma((2, n_row)),
            dma((2, n_row)),
            dma((4,)),
            dma((2,)),
        ],
        compiler_params=pltpu.CompilerParams(collective_id=0, has_side_effects=True, vmem_limit_bytes=67043328),
        cost_estimate=pl.CostEstimate(flops=70 * 10**9, bytes_accessed=300 << 20, transcendentals=heads * tokens * tokens // 2),
    )(x, dy, wq, wk, wv, wo)


def solution(mesh):
    n = mesh.shape["tp"]
    ring = math.isqrt(n // 2)
    cores = n // (ring * ring)
    if ring != 4 or cores != 2:
        raise ValueError("needs a 4x4 torus")

    def local_grads(x_blk, dy_blk, wq_loc, w_k, w_v, wo_loc):
        model_dim, kv_heads, e = w_k.shape
        heads = wq_loc.shape[1]
        hd = heads * e
        scale = e ** -0.5
        wq = jnp.transpose(wq_loc, (1, 2, 0)).reshape(hd, model_dim)
        wk = jnp.transpose(w_k, (1, 2, 0))
        wv = jnp.transpose(w_v, (1, 2, 0))
        wo = wo_loc.reshape(hd, model_dim)
        dx, dwq, dwo, dwk, dwv, _, _ = _layer(ring, cores, heads, scale, x_blk, dy_blk, wq, wk, wv, wo)
        return (dx, jnp.transpose(dwq.reshape(heads, e, model_dim), (2, 0, 1)), dwo.reshape(heads, e, model_dim), dwk.T, dwv.T)

    tok = P(("dp", "tp"))
    return jax.shard_map(
        local_grads,
        mesh=mesh,
        in_specs=(tok, tok, P(None, "tp", None), P(), P(), P("tp")),
        out_specs=(tok, P("dp", "tp", None), tok, tok, tok),
        check_vma=False,
    )
```

```python
import functools
import math

import jax
import jax.numpy as jnp
from jax import lax
from jax.experimental import pallas as pl
from jax.experimental.pallas import tpu as pltpu
from jax.sharding import PartitionSpec as P

F32 = jnp.float32
BF16 = jnp.bfloat16
MESH = pl.DeviceIdType.MESH
ANY = pl.BlockSpec(memory_space=pl.ANY)
VMEM = pl.BlockSpec(memory_space=pltpu.VMEM)
LOG2E = math.log2(math.e)


def _scoped(fn):
    def run(*args, **kw):
        with jax.named_scope(fn.__name__):
            return fn(*args, **kw)

    return run


def _dot(a, b, dims):
    return lax.dot_general(a, b, (dims, ((), ())), preferred_element_type=F32)


def _nn(a, b):
    return _dot(a, b, ((1,), (0,)))


def _nt(a, b):
    return _dot(a, b, ((1,), (1,)))


class Place:
    def __init__(self, ring, cores):
        me = lax.axis_index("tp")
        self.ring, self.cores = ring, cores
        self.c = lax.rem(me, cores)
        self.x = lax.rem(me // cores, ring)
        self.y = me // (cores * ring)
        self.r = self.x * cores + self.c
        self.n_row = ring * cores

    def dev(self, y, x, c):
        y = lax.rem(y + self.ring, self.ring)
        x = lax.rem(x + self.ring, self.ring)
        return {"tp": (y * self.ring + x) * self.cores + c}

    def row_dev(self, r):
        return {"tp": self.y * self.n_row + r}

    def slot(self, x, c):
        return lax.rem(x + self.ring, self.ring) * self.cores + c


def _remote(src, dst, send, recv, dev):
    return pltpu.make_async_remote_copy(
        src_ref=src, dst_ref=dst, send_sem=send, recv_sem=recv, device_id=dev, device_id_type=MESH
    )


@_scoped
def _enter(devices):
    barrier = pltpu.get_barrier_semaphore()
    for dev in devices:
        pl.semaphore_signal(barrier, inc=1, device_id=dev, device_id_type=MESH)
    pl.semaphore_wait(barrier, len(devices))


OWN, MINUS, PLUS, FAR = range(4)
STEP = (0, -1, 1, 2)


def _load_shard(at, full, n, y, x, core, block, sem):
    r0 = at.dev(y, x, core)["tp"] * n
    b0 = at.slot(x, core) * n
    src = full.at[pl.ds(pl.multiple_of(r0, n), n), :]
    return pltpu.make_async_copy(src, block.at[pl.ds(pl.multiple_of(b0, n), n), :], sem)


@_scoped
def _take_row(lanes, t, y, block, sem):
    at, full, n = lanes[0].at, lanes[0].full, lanes[0].shard
    for j in range(4):
        _load_shard(at, full, n, y, at.x + STEP[j], at.c, block, sem).start()
    for j in range(4):
        for g in lanes:
            g.await_mate(t, j)
        _load_shard(at, full, n, y, at.x + STEP[j], 1 - at.c, block, sem).start()


class Gather:
    def __init__(self, at, src, full, send, recv, mate_recv, orders, row0, rows, tag):
        self.at, self.src, self.full = at, src, full
        self.send, self.recv, self.mate_recv = send.at[tag], recv.at[tag], mate_recv.at[tag]
        self.order, self.mate_order = orders
        self.row0, self.rows, self.shard = row0, rows, src.shape[0]
        self.sent = []
        c, o = at.c, self.order
        self.first = {s: at.dev(at.y + o * s, at.x + (1 - o) * s, c) for s in (1, -1)}
        self.second = {s: at.dev(at.y + (1 - o) * s, at.x + o * s, c) for s in (1, -1)}
        self.mate = at.dev(at.y, at.x, 1 - c)
        self.fulls = {d: self.both_ways(self.second, d, lambda to, d=d: (d, to)) for d in range(4)}

    def span(self, half):
        n = self.rows if half is None else self.rows // 2
        return self.row0 + (0 if half is None else half * n), n

    def ref(self, d1, d2, half=None):
        at, o = self.at, self.order
        o1, o2 = STEP[d1], STEP[d2]
        start, n = self.span(half)
        r0 = at.dev(at.y + o * o1 + (1 - o) * o2, at.x + (1 - o) * o1 + o * o2, at.c)["tp"] * self.shard + start
        return self.full.at[pl.ds(pl.multiple_of(r0, math.gcd(self.shard, self.row0, n)), n), :]

    def push(self, src, dst, recv, dev):
        k = len(self.sent)
        self.sent.append(dst.shape[0])
        return _remote(src, dst, self.send.at[k], recv, dev)

    def out(self, d1, d2, half=None):
        if d1 == OWN and d2 == OWN:
            return self.src.at[pl.ds(*self.span(half)), :]
        return self.ref(d1, d2, half)

    def both_ways(self, devs, d1, name):
        copies = []
        for step in (0, 1):
            for s, to in ((1, MINUS), (-1, PLUS)):
                half = step if s == 1 else 1 - step
                copies.append(self.push(self.out(d1, OWN, half), self.ref(d1, OWN, half), self.recv.at[*name(to), half], devs[s]))
        return copies

    def to_mate(self, d1, d2):
        ref = self.ref(d1, d2)
        self.push(self.out(d1, d2), ref, self.mate_recv.at[d1, d2], self.mate).start()

    def arrived(self, d1, d2, half):
        ref = self.ref(d1, d2, half)
        _remote(ref, ref, self.send.at[0], self.recv.at[d1, d2, half], self.mate).wait_recv()

    @_scoped
    def start(self):
        for cp in self.both_ways(self.first, OWN, lambda to: (to, OWN)):
            cp.start()
        self.go(OWN)
        self.to_mate(OWN, OWN)

    def go(self, d1):
        for cp in self.fulls[d1]:
            cp.start()

    @_scoped
    def relay_first(self):
        for d, s, half in ((MINUS, 1, 0), (PLUS, -1, 1)):
            self.arrived(d, OWN, half)
            ref = self.ref(d, OWN, half)
            self.push(ref, ref, self.recv.at[FAR, OWN, half], self.first[s]).start()

    @_scoped
    def near_first(self):
        for d, half in ((MINUS, 1), (PLUS, 0)):
            self.arrived(d, OWN, half)
            self.to_mate(d, OWN)

    @_scoped
    def far_first(self):
        for half in (0, 1):
            self.arrived(FAR, OWN, half)
        self.to_mate(FAR, OWN)

    @_scoped
    def relay_second(self, d1):
        for d, s, half in ((MINUS, 1, 0), (PLUS, -1, 1)):
            self.arrived(d1, d, half)
            ref = self.ref(d1, d, half)
            self.push(ref, ref, self.recv.at[d1, FAR, half], self.second[s]).start()

    @_scoped
    def near_second(self, d1):
        for d, half in ((MINUS, 1), (PLUS, 0)):
            self.arrived(d1, d, half)
            self.to_mate(d1, d)

    @_scoped
    def far_second(self, d1):
        for half in (0, 1):
            self.arrived(d1, FAR, half)
        self.to_mate(d1, FAR)

    def await_mate(self, t, j):
        o = self.mate_order
        ref = self.full.at[pl.ds(0, self.rows), :]
        _remote(ref, ref, self.send.at[0], self.mate_recv.at[(1 - o) * j + o * t, (1 - o) * t + o * j], self.mate).wait_recv()

    @_scoped
    def drain(self):
        for k, n in enumerate(self.sent):
            ref = self.full.at[pl.ds(0, n), :]
            _remote(ref, ref, self.send.at[k], self.send.at[k], self.mate).wait_send()


def _kernel(ring, cores, heads, scale, bq, bs, bc, x_ref, dy_ref, w_ref, wk_ref, wv_ref, wo_ref,
            dx_ref, dwq_ref, dwo_ref, dwk_ref, dwv_ref, xf_ref, dyf_ref,
            gq, w_all, part, rs_half, rs_full, stage, hop_ref, qkvt_ref, dot_ref, dqt_ref, ot_ref, dk_ref, dv_ref, kn_ref, vn_ref,
            send, recv, mate_recv, w_send, w_recv, hop_recv, ld_sem, blk_sem,
            ag_send, ag_recv, rs_send, rs_recv, out_send, out_recv, in_sem, o_sem):
    at = Place(ring, cores)
    n_row = at.n_row
    hd = wo_ref.shape[0]
    e = hd // heads
    tokens, width = xf_ref.shape
    tb = tokens // ring
    cw = width // n_row
    gw = gq.shape[1] // n_row
    c = at.c
    shard = x_ref.shape[0]
    gx = Gather(at, x_ref, xf_ref, send, recv, mate_recv, (c, 1 - c), 0, shard, 0)
    split = shard * 3 // 4
    gy = Gather(at, dy_ref, dyf_ref, send, recv, mate_recv, (c, 1 - c), 0, split, 1)
    gz = Gather(at, dy_ref, dyf_ref, send, recv, mate_recv, (0, 0), split, shard - split, 2)
    n_kv = wk_ref.shape[0] // ring
    per_kv = n_row // n_kv
    row_peers = [lax.rem(at.r + d, n_row) for d in range(1, n_row)]
    up, down = at.dev(at.y + 1, at.x, c), at.dev(at.y - 1, at.x, c)

    hh = hd // 2

    def w_push(k, src, dst, rsem, dev):
        _remote(src, dst, w_send.at[k], rsem, dev).start()

    def wq_slot(slot, half=None):
        r0 = slot * gw + (0 if half is None else half * hh)
        return w_all.at[pl.ds(r0 if isinstance(r0, int) else pl.multiple_of(r0, hh), hd if half is None else hh), :]

    def wcols(slot):
        return pl.ds(pl.multiple_of(slot * cw, cw), cw)

    right, left, mate = at.dev(at.y, at.x + 1, c), at.dev(at.y, at.x - 1, c), at.dev(at.y, at.x, 1 - c)

    @_scoped
    def w_start():
        for half, dev in ((0, right), (1, left)):
            for k in range(cores):
                w_push(half * 2 + k, w_ref.at[pl.ds(half * hh, hh), wcols(at.slot(at.x + 2, k))], hop_ref.at[half * 2 + k], hop_recv.at[half * 2 + k], dev)
        w_push(4, w_ref.at[pl.ds(0, hd), wcols(at.slot(at.x, 1 - c))], wq_slot(at.r), w_recv.at[0], mate)
        for i, s in enumerate((1, -1)):
            for k in range(cores):
                dst_core = c if k == 0 else 1 - c
                w_push(5 + 2 * i + k, w_ref.at[pl.ds(0, hd), wcols(at.slot(at.x + s, dst_core))], wq_slot(at.r), w_recv.at[1 + 2 * i + k], at.dev(at.y, at.x + s, dst_core))

    @_scoped
    def w_relay():
        for half, s in ((0, 1), (1, -1)):
            for n in (half * 2, half * 2 + 1):
                _remote(hop_ref.at[n], hop_ref.at[n], w_send.at[0], hop_recv.at[n], mate).wait_recv()
            for k in range(cores):
                n = half * 2 + k
                src_slot = at.slot(at.x - s, c)
                same = k == 0
                dst_core = c if same else 1 - c
                w_push(9 + n, hop_ref.at[half * 2 + dst_core], wq_slot(src_slot, half), w_recv.at[5 + n], at.dev(at.y, at.x + s, dst_core))

    @_scoped
    def w_finish():
        whole = wq_slot(0)
        piece = wq_slot(0, 0)
        for n in range(9):
            ref = whole if n < 5 else piece
            _remote(ref, ref, w_send.at[0], w_recv.at[n], mate).wait_recv()

    def w_drain():
        whole = wq_slot(0)
        piece = wq_slot(0, 0)
        for k in range(13):
            ref = whole if 4 <= k < 9 else piece
            _remote(ref, ref, w_send.at[k], w_send.at[k], mate).wait_send()

    own_cols = wcols(at.r)
    rows = x_ref.shape[0]
    own_rows = pl.ds(pl.multiple_of((at.y * n_row + at.r) * rows, rows), rows)

    keep = [pltpu.make_async_copy(w_ref.at[:, own_cols], wq_slot(at.r), ld_sem.at[8])]
    for r in range(n_row):
        kv_r = at.y * n_kv + r // per_kv
        for i, w in enumerate((wk_ref, wv_ref)):
            keep.append(pltpu.make_async_copy(w.at[kv_r, :, own_cols], w_all.at[pl.ds(r * gw + hd + i * e, e), :], ld_sem.at[9 + 2 * r + i]))

    th = tb // 2
    tq = th // 2
    tl = tb // n_row
    hw = cw // 2
    half_a, half_b = pl.ds(0, hw), pl.ds(hw, hw)
    units = [(FAR, 0), (FAR, 1), (PLUS, 0), (MINUS, 0), (PLUS, 1), (MINUS, 1), (OWN, 0), (OWN, 1)]
    s_own, s_left, s_right, s_far = (at.slot(at.x + o, c) for o in (0, -1, 1, 2))
    m_own, m_left, m_right, m_far = (at.slot(at.x + o, 1 - c) for o in (0, -1, 1, 2))

    def unit_row(u):
        d, s = units[u % len(units)]
        return pl.multiple_of(lax.rem(at.y + STEP[d] + ring, ring) * tb + s * th, th)

    last = len(units)

    def gcols(u, slot):
        if u == 0:
            return pl.ds(pl.multiple_of(slot * gw, 128), hd)
        if u == last:
            return pl.ds(pl.multiple_of(slot * gw + hd, 128), gw - hd)
        return pl.ds(pl.multiple_of(slot * gw, gw), gw)

    def piece(u, slot, half=None):
        r0 = unit_row(u)
        rows = pl.ds(r0, th) if half is None else pl.ds(pl.multiple_of(r0 + half * tq, tq), tq)
        return gq.at[rows, gcols(u, slot)]

    ag_sent = []

    def ag_push(u, n, slot, dev, half=None):
        ref = piece(u, slot, half)
        _remote(ref, ref, ag_send.at[u, n], ag_recv.at[u, n], dev).start()
        ag_sent.append((u, n, half))

    def ag_drain():
        for u, n, half in ag_sent:
            ref = piece(u, s_own, half)
            _remote(ref, ref, ag_send.at[u, n], ag_recv.at[u, n], mate).wait_send()

    def ag_wait(u, n, slot, half=None):
        ref = piece(u, slot, half)
        _remote(ref, ref, ag_send.at[u, n], ag_recv.at[u, n], mate).wait_recv()

    def ag_own(u):
        ag_push(u, 0, s_own, right)
        ag_push(u, 1, s_own, left)
        ag_push(u, 2, s_own, mate)

    @_scoped
    def ag_relay(u):
        ag_wait(u, 0, s_left)
        ag_push(u, 3, s_left, right, 0)
        ag_push(u, 4, s_left, mate)
        ag_wait(u, 1, s_right)
        ag_push(u, 5, s_right, left, 1)
        ag_push(u, 6, s_right, mate)

    @_scoped
    def ag_finish(u):
        ag_wait(u, 3, s_far, 0)
        ag_push(u, 7, s_far, mate, 0)
        ag_wait(u, 5, s_far, 1)
        ag_push(u, 8, s_far, mate, 1)
        ag_wait(u, 2, m_own)
        ag_wait(u, 4, m_left)
        ag_wait(u, 6, m_right)
        ag_wait(u, 7, m_far, 0)
        ag_wait(u, 8, m_far, 1)

    def settle(u):
        rows = pl.ds(unit_row(u), th)
        kv = jnp.concatenate([(dk_ref[:, rows] * scale).astype(BF16), dv_ref[:, rows].astype(BF16)], axis=0)
        gq[rows, pl.ds(pl.multiple_of(at.r * gw + hd, 128), 2 * e)] = kv.T

    def front(w_v, wo_v, xblk):
        kv = (at.y * n_row + at.r) // (n_row * ring // wk_ref.shape[0])
        loads = [
            pltpu.make_async_copy(w_ref, w_v.at[pl.ds(0, hd), :], ld_sem.at[0]),
            pltpu.make_async_copy(wo_ref, wo_v, ld_sem.at[1]),
            pltpu.make_async_copy(wk_ref.at[kv], w_v.at[pl.ds(hd, e), :], ld_sem.at[6]),
            pltpu.make_async_copy(wv_ref.at[kv], w_v.at[pl.ds(hd + e, e), :], ld_sem.at[7]),
        ]
        ins = [pltpu.make_async_copy(src, xblk.at[pl.ds(i * rows, rows), :], ld_sem.at[2 + i]) for i, src in enumerate((x_ref, dy_ref))]
        outs = [pltpu.make_async_copy(xblk.at[pl.ds(i * rows, rows), :], dst.at[own_rows, :], ld_sem.at[4 + i]) for i, dst in enumerate((xf_ref, dyf_ref))]
        for cp in ins:
            cp.start()
        _enter([up, down] + [at.row_dev(r) for r in row_peers])
        gx.start()
        for cp in loads + keep:
            cp.start()
        for cp in ins:
            cp.wait()
        for cp in outs:
            cp.start()

        dk_ref[...] = jnp.zeros_like(dk_ref)
        dv_ref[...] = jnp.zeros_like(dv_ref)

        @_scoped
        def project(w, out, b):
            pltpu.make_async_copy(xf_ref.at[pl.ds(0, tb), :], xblk, blk_sem.at[0]).wait()

            def block(i, _):
                r0 = pl.multiple_of(i * bq, bq)
                out[:, pl.ds(pl.multiple_of(b * tb + i * bq, bq), bq)] = _nt(w[...], xblk[pl.ds(r0, bq), :]).astype(BF16)
                return 0

            lax.fori_loop(0, tb // bq, block, 0)

        def row_at(t):
            if isinstance(t, int):
                return lax.rem(at.y + STEP[t] + ring, ring)
            off = jnp.where(t == 1, ring - 1, jnp.where(t == 2, 1, jnp.where(t == 3, 2, 0)))
            return lax.rem(at.y + off, ring)

        for cp in loads + outs:
            cp.wait()

        def begin(g):
            g.relay_first()
            g.near_first()
            g.go(MINUS)

            @pl.when(g.order == 0)
            def _():
                g.go(PLUS)

        def begin_far(g):
            g.far_first()

            @pl.when(g.order == 0)
            def _():
                g.go(FAR)

        def begin_second(g):
            g.relay_second(OWN)

            @pl.when(g.order == 1)
            def _():
                g.go(PLUS)

            g.near_second(OWN)

        def second_minus(g):
            g.relay_second(MINUS)

            @pl.when(g.order == 1)
            def _():
                g.go(FAR)

            g.near_second(MINUS)

        def x_turn(t, _):
            @pl.when(t == 0)
            def _():
                begin(gx)
                begin_far(gx)
                begin_second(gx)
                second_minus(gx)
                gx.relay_second(PLUS)
                gx.near_second(PLUS)
                gx.relay_second(FAR)
                gy.start()
                gz.start()
                gx.far_second(OWN)

            @pl.when(t == 1)
            def _():
                gx.near_second(FAR)
                gx.far_second(MINUS)

            @pl.when(t == 2)
            def _():
                for d in (PLUS, FAR):
                    gx.far_second(d)

            @pl.when(t == 3)
            def _():
                begin(gy)
                begin(gz)

            b = row_at(t)
            _take_row((gx,), t, b, xblk, blk_sem.at[0])
            project(w_v, qkvt_ref, b)
            return 0

        lax.fori_loop(0, ring, x_turn, 0)
        for t in range(0, tokens, bq):
            kn_ref[t:t + bq, :] = qkvt_ref[hd:hd + e, t:t + bq].T
            vn_ref[t:t + bq, :] = qkvt_ref[hd + e:hd + 2 * e, t:t + bq].T

        keys_k, keys_v = slice(hd, hd + e), slice(hd + e, hd + 2 * e)
        m4 = heads * bs
        factor = scale * LOG2E

        def row_chunks(k):
            return [slice(t, t + bq) for t in range(0, (k + 1) * tb, bq)]

        def stacked(ref, qs):
            return jnp.concatenate([ref[h * e:(h + 1) * e, qs] for h in range(heads)], axis=1)

        def unstack(ref, qs, value):
            for h in range(heads):
                ref[h * e:(h + 1) * e, qs] = value[:, h * bs:(h + 1) * bs]

        def scores(q, ks, k, j):
            s = _nn(q, qkvt_ref[keys_k, ks])
            if ks.start < k * tb:
                return s
            row = lax.broadcasted_iota(jnp.int32, (m4, bq), 0) & (bs - 1)
            col = lax.broadcasted_iota(jnp.int32, (m4, bq), 1)
            return jnp.where(col + (ks.start - k * tb) <= row + j * bs, s, -jnp.inf)

        def folded(op, total, value):
            for t in range(0, value.shape[1], 128):
                piece = value[:, t:t + 128]
                total = piece if total is None else op(total, piece)
            return total

        def score_buf(ks):
            n = ks.start // cw
            return part.at[n, :, ks.start - n * cw:ks.stop - n * cw]

        def stats_buf(k, j):
            per = cw // 128
            n = k * (tb // bs)
            return part.at[2 + n // per, :, pl.ds(pl.multiple_of((n % per + j) * 128, 128), 128)]

        @_scoped
        def forward(k):
            chunks = row_chunks(k)

            def queries(j, _):
                qs = pl.ds(pl.multiple_of(k * tb + j * bs, bs), bs)
                q = stacked(qkvt_ref, qs).T
                m = None
                for ks in chunks:
                    s = scores(q, ks, k, j)
                    score_buf(ks)[...] = s
                    m = folded(jnp.maximum, m, s)
                m = jnp.max(m, axis=1, keepdims=True)
                total = None
                for ks in chunks:
                    p = jnp.exp2((score_buf(ks)[...] - m) * factor)
                    score_buf(ks)[...] = p
                    total = folded(jnp.add, total, p)
                inv = 1.0 / jnp.sum(total, axis=1, keepdims=True)
                lane = lax.broadcasted_iota(jnp.int32, (m4, 128), 1)
                stats_buf(k, j)[...] = jnp.where(lane == 0, m, inv)
                out = None
                for ks in chunks:
                    piece = _nn((score_buf(ks)[...] * inv).astype(BF16), vn_ref[ks, :])
                    out = piece if out is None else out + piece
                unstack(ot_ref, qs, out.astype(BF16).T)
                return 0

            lax.fori_loop(0, tb // bs, queries, 0)

        @_scoped
        def backward(k, second):
            chunks = row_chunks(k)

            def queries(j, _):
                qs = pl.ds(pl.multiple_of(k * tb + j * bs, bs), bs)
                qt = stacked(qkvt_ref, qs)
                dot = stacked(dot_ref, qs)
                q, do = qt.T, dot.T
                delta = jnp.sum(dot.astype(F32) * stacked(ot_ref, qs).astype(F32), axis=0, keepdims=True)
                delta = jnp.broadcast_to(delta, (128, m4)).T[:, :1]
                stats = stats_buf(k, j)[...]
                m, inv = stats[:, 0:1], stats[:, 1:2]
                dq = None
                for ks in chunks:
                    p = jnp.exp2((scores(q, ks, k, j) - m) * factor) * inv
                    dp = _nn(do, qkvt_ref[keys_v, ks])
                    ds = (p * (dp - delta)).astype(BF16)
                    dv_ref[:, ks] += _nn(dot, p.astype(BF16))
                    dk_ref[:, ks] += _nn(qt, ds)
                    piece = _nn(ds, kn_ref[ks, :])
                    dq = piece if dq is None else dq + piece
                dq = (dq * scale).astype(BF16).T
                unstack(dqt_ref, qs, dq)
                for h in range(0, heads, 2):
                    pair = jnp.concatenate([dq[:, h * bs:(h + 1) * bs], dq[:, (h + 1) * bs:(h + 2) * bs]], axis=0)
                    gq[qs, pl.ds(pl.multiple_of(at.r * gw + h * e, 128), 2 * e)] = pair.T
                return 0

            n = tb // bs // 2
            lax.fori_loop(second * n, (second + 1) * n, queries, 0)

        forward(0)
        begin_far(gy)
        begin_far(gz)
        forward(1)
        begin_second(gy)
        begin_second(gz)
        forward(2)

        @pl.when(c == 0)
        def _():
            w_start()

        forward(3)
        second_minus(gy)
        second_minus(gz)

        def turn(h, _):
            t, second = h // 2, lax.rem(h, 2)

            @pl.when(h == 0)
            def _():
                @pl.when(c == 1)
                def _():
                    far_step(OWN)

            @pl.when(h == 1)
            def _():
                for g in (gy, gz):
                    g.relay_second(PLUS)
                    g.near_second(PLUS)

                @pl.when(c == 1)
                def _():
                    far_step(MINUS)

            @pl.when(h == 2)
            def _():
                for g in (gy, gz):
                    g.relay_second(FAR)
                    g.near_second(FAR)

                @pl.when(c == 1)
                def _():
                    w_start()

            @pl.when(h == 3)
            def _():
                @pl.when(c == 1)
                def _():
                    far_step(PLUS)

                @pl.when(c == 0)
                def _():
                    far_step(OWN)
                    far_step(MINUS)
                    w_relay()

            b = row_at(t)

            @pl.when((second == 0) & (t != 3))
            def _():
                _take_row((gy, gz), t, b, xblk, blk_sem.at[0])

            @pl.when(second == 0)
            def _():
                project(wo_v, dot_ref, b)

            @pl.when(h == 5)
            def _():
                @pl.when(c == 0)
                def _():
                    far_step(PLUS)

                far_step(FAR)
                for d in range(4):
                    gz.far_second(d)

                @pl.when(c == 1)
                def _():
                    w_relay()

                _take_row((gy, gz), FAR, row_at(FAR), xblk, blk_sem.at[0])

            @pl.when(h == 7)
            def _():
                ag_own(0)

            for k in range(ring):
                @pl.when(b == k)
                def _(k=k):
                    backward(k, second)
            return 0

        far_cp = {d: gy.push(gy.ref(d, FAR), gy.ref(d, FAR), gy.mate_recv.at[d, FAR], gy.mate) for d in range(4)}

        @_scoped
        def far_step(d):
            for half in (0, 1):
                gy.arrived(d, FAR, half)
            far_cp[d].start()

        lax.fori_loop(0, 2 * ring, turn, 0)


    pl.run_scoped(front, pltpu.VMEM((hd + 2 * e, width), BF16), pltpu.VMEM((hd, width), BF16), pltpu.VMEM((tb, width), BF16))

    def back(xbuf, obuf, kvt):
        sends = []

        nt = min(256, hw)

        @_scoped
        def partial(u):
            rows = pl.ds(unit_row(u), th)
            d, s = units[u]
            dst = part.at[d, pl.ds(s * th, th), :]

            def tile(j, _):
                cs = pl.ds(pl.multiple_of(j * nt, nt), nt)
                dst[:, cs] = _nn(gq[rows, :], w_all[:, cs])
                return 0

            lax.fori_loop(0, cw // nt, tile, 0)

        def rs_push(n, s, src, dst, dev):
            cp = _remote(src, dst, rs_send.at[n, s], rs_recv.at[n, s], dev)
            cp.start()
            sends.append(cp)

        def rs_wait(n, s):
            ref = rs_half.at[0, s]
            _remote(ref, ref, rs_send.at[n, s], rs_recv.at[n, s], mate).wait_recv()

        def block(d, s, half):
            return part.at[d, pl.ds(s * th, th), half]

        def far_a(s):
            rs_push(0, s, block(FAR, s, half_a), rs_half.at[0, s], up)

        def far_b(s):
            rs_push(1, s, block(FAR, s, half_b), rs_half.at[1, s], down)

        def minus_a(s):
            rs_push(4, s, block(MINUS, s, half_a), rs_full.at[1, s, 0], down)

        def plus_b(s):
            rs_push(3, s, block(PLUS, s, half_b), rs_full.at[0, s, 1], up)

        @_scoped
        def plus_a(s):
            rs_wait(0, s)
            block(PLUS, s, half_a)[...] += rs_half[0, s]
            rs_push(2, s, block(PLUS, s, half_a), rs_full.at[0, s, 0], up)

        @_scoped
        def minus_b(s):
            rs_wait(1, s)
            block(MINUS, s, half_b)[...] += rs_half[1, s]
            rs_push(5, s, block(MINUS, s, half_b), rs_full.at[1, s, 1], down)

        n_steps = width // bc
        depth = xbuf.shape[0]

        def chunk(src, c0, j):
            slot = lax.rem(j, depth)
            return pltpu.make_async_copy(src.at[:, pl.ds(pl.multiple_of(c0 + j * bc, bc), bc)], xbuf.at[slot], in_sem.at[slot])

        def ahead(src, c0, n):
            for j in range(min(depth - 1, n)):
                chunk(src, c0, j).start()

        @_scoped
        def stream(src, lhs, out, j0, j1):
            def store(j):
                slot = lax.rem(j, 2)
                return pltpu.make_async_copy(obuf.at[slot], out.at[:, pl.ds(pl.multiple_of(j * bc, bc), bc)], o_sem.at[slot])

            if j0 == 0:
                ahead(src, 0, n_steps)

            def step(j, _):
                @pl.when(j + depth - 1 < n_steps)
                def _():
                    chunk(src, 0, j + depth - 1).start()

                chunk(src, 0, j).wait()

                @pl.when(j >= 2)
                def _():
                    store(j - 2).wait()

                obuf[lax.rem(j, 2)] = _nn(lhs[...], xbuf[lax.rem(j, depth)])
                store(j).start()
                return 0

            lax.fori_loop(j0, j1, step, 0)
            if j1 == n_steps:
                for j in range(max(n_steps - 2, 0), n_steps):
                    store(j).wait()

        def wo_steps(a, b):
            stream(dyf_ref, ot_ref, dwo_ref, n_steps * a // 16, n_steps * b // 16)

        def wq_steps(a, b):
            stream(xf_ref, dqt_ref, dwq_ref, n_steps * a // 16, n_steps * b // 16)

        first = (at.r // per_kv) * per_kv
        share = width // per_kv
        col0 = lax.rem(at.r, per_kv) * share

        def kv_step(j, _):
            @pl.when(j + depth - 1 < share // bc)
            def _():
                chunk(xf_ref, col0, j + depth - 1).start()

            chunk(xf_ref, col0, j).wait()
            prod = _nn(kvt[...], xbuf[lax.rem(j, depth)])
            dk = dv = None
            for q in range(per_kv):
                a = prod[q * 2 * e:q * 2 * e + e]
                b = prod[q * 2 * e + e:(q + 1) * 2 * e]
                dk = a if dk is None else dk + a
                dv = b if dv is None else dv + b
            cs = pl.ds(pl.multiple_of(j * bc, bc), bc)
            dwk_ref[:, cs] = dk
            dwv_ref[:, cs] = dv
            return 0

        @_scoped
        def kv_grads():
            ahead(xf_ref, col0, share // bc)
            for q in range(per_kv):
                cols = pl.ds(pl.multiple_of((first + q) * gw + hd, 128), gw - hd)
                for t in range(0, tokens, bq):
                    kvt[q * (gw - hd):(q + 1) * (gw - hd), t:t + bq] = gq[t:t + bq, cols].T
            lax.fori_loop(0, share // bc, kv_step, 0)

        per_half = n_row // 2

        def hand(i, r):
            half = (half_a, half_b)[i]
            rows = pl.ds(r * tl, tl)
            cols = pl.ds(pl.multiple_of(at.r * cw + i * hw, hw), hw)
            return stage.at[rows, half], dx_ref.at[:, cols]

        def hand_remote(i, r):
            src, dst = hand(i, r)
            d = lax.rem(r - at.r + n_row, n_row)
            return _remote(src, dst, out_send.at[i, r], out_recv.at[i, d], at.row_dev(r))

        def hand_local(i, r):
            src, dst = hand(i, r)
            return pltpu.make_async_copy(src, dst, out_send.at[i, r])

        @_scoped
        def finish(i, s):
            half = (half_a, half_b)[i]
            rs_wait(2 + i, s)
            rs_wait(4 + i, s)
            stage[s * th:(s + 1) * th, half] = (block(OWN, s, half)[...] + rs_full[0, s, i] + rs_full[1, s, i]).astype(BF16)
            for r in range(s * per_half, (s + 1) * per_half):
                @pl.when(at.r != r)
                def _(r=r):
                    hand_remote(i, r).start()

                @pl.when(at.r == r)
                def _(r=r):
                    hand_local(i, r).start()

        @_scoped
        def received(i):
            for d in range(1, n_row):
                src = lax.rem(at.r + n_row - d, n_row)
                ref = dx_ref.at[:, pl.ds(pl.multiple_of(src * cw + i * hw, hw), hw)]
                _remote(ref, ref, out_send.at[i, 0], out_recv.at[i, d], mate).wait_recv()
            for r in range(n_row):
                @pl.when(at.r != r)
                def _(r=r):
                    hand_remote(i, r).wait_send()

                @pl.when(at.r == r)
                def _(r=r):
                    hand_local(i, r).wait()

        settle(0)
        settle(1)
        ag_own(last)
        ag_relay(0)
        for u in range(2, 8):
            settle(u)
        wo_steps(0, 1)
        ag_relay(last)
        ag_own(1)
        ag_own(2)
        wo_steps(1, 4)
        ag_finish(0)
        ag_finish(last)
        for cp in keep:
            cp.wait()
        w_finish()
        partial(0)
        ag_relay(1)
        far_a(0)
        far_b(0)
        ag_own(3)
        ag_relay(2)
        ag_own(4)
        wo_steps(4, 6)
        ag_finish(1)
        partial(1)
        far_a(1)
        far_b(1)
        ag_relay(3)
        ag_own(5)
        wo_steps(6, 8)
        ag_finish(2)
        partial(2)
        ag_relay(4)
        ag_own(6)
        plus_a(0)
        wo_steps(8, 10)
        ag_finish(3)
        partial(3)
        minus_a(0)
        ag_relay(5)
        ag_own(7)
        wo_steps(10, 12)
        ag_finish(4)
        partial(4)
        plus_a(1)
        plus_b(0)
        ag_relay(6)
        wo_steps(12, 14)
        ag_finish(5)
        partial(5)
        minus_a(1)
        minus_b(0)
        plus_b(1)
        minus_b(1)
        ag_relay(7)
        wo_steps(14, 16)
        ag_finish(6)
        partial(6)
        wq_steps(0, 2)
        ag_finish(7)
        partial(7)
        wq_steps(2, 5)
        finish(0, 0)
        wq_steps(5, 12)
        finish(0, 1)
        wq_steps(12, 16)
        kv_grads()
        finish(1, 0)
        received(0)
        finish(1, 1)
        received(1)
        for cp in sends:
            cp.wait_send()
        ag_drain()
        w_drain()
        for g in (gx, gy, gz):
            g.drain()

    pl.run_scoped(back, pltpu.VMEM((4, tokens, bc), BF16), pltpu.VMEM((2, hd, bc), F32), pltpu.VMEM((per_kv * 2 * e, tokens), BF16))


def _layer(ring, cores, heads, scale, x, dy, wq, wk, wv, wo):
    rows, width = x.shape
    tokens = rows * ring * ring * cores
    hd = wo.shape[0]
    e = hd // heads
    n_row = ring * cores
    cw = width // n_row
    gw = hd + 2 * e
    tb = tokens // ring
    th, hw = tb // 2, cw // 2
    per_kv = n_row * ring // wk.shape[0]
    bq = min(256, tb)
    bs = tb // heads
    bc = min(512, cw // 2)
    dma = pltpu.SemaphoreType.DMA
    shape = jax.ShapeDtypeStruct
    return pl.pallas_call(
        functools.partial(_kernel, ring, cores, heads, scale, bq, bs, bc),
        name="layer",
        in_specs=[ANY] * 6,
        out_specs=[ANY, ANY, ANY, VMEM, VMEM, ANY, ANY],
        out_shape=[
            shape((rows, width), BF16),
            shape((hd, width), F32),
            shape((hd, width), F32),
            shape((e, width // per_kv), F32),
            shape((e, width // per_kv), F32),
            shape((tokens, width), BF16),
            shape((tokens, width), BF16),
        ],
        scratch_shapes=[
            pltpu.VMEM((tokens, n_row * gw), BF16),
            pltpu.VMEM((n_row * gw, cw), BF16),
            pltpu.VMEM((4, tb, cw), F32),
            pltpu.VMEM((2, 2, th, hw), F32),
            pltpu.VMEM((2, 2, 2, th, hw), F32),
            pltpu.VMEM((tb, cw), BF16),
            pltpu.VMEM((4, hd // 2, cw), BF16),
            pltpu.VMEM((gw, tokens), BF16),
            pltpu.VMEM((hd, tokens), BF16),
            pltpu.VMEM((hd, tokens), BF16),
            pltpu.VMEM((hd, tokens), BF16),
            pltpu.VMEM((e, tokens), F32),
            pltpu.VMEM((e, tokens), F32),
            pltpu.VMEM((tokens, e), BF16),
            pltpu.VMEM((tokens, e), BF16),
            dma((3, 48)),
            dma((3, 4, 4, 2)),
            dma((3, 4, 4)),
            dma((13,)),
            dma((9,)),
            dma((4,)),
            dma((9 + 2 * n_row,)),
            dma((1,)),
            dma((9, 9)),
            dma((9, 9)),
            dma((6, 2)),
            dma((6, 2)),
            dma((2, n_row)),
            dma((2, n_row)),
            dma((4,)),
            dma((2,)),
        ],
        compiler_params=pltpu.CompilerParams(collective_id=0, has_side_effects=True, vmem_limit_bytes=67043328),
        cost_estimate=pl.CostEstimate(flops=70 * 10**9, bytes_accessed=300 << 20, transcendentals=heads * tokens * tokens // 2),
    )(x, dy, wq, wk, wv, wo)


def solution(mesh):
    n = mesh.shape["tp"]
    ring = math.isqrt(n // 2)
    cores = n // (ring * ring)
    if ring != 4 or cores != 2:
        raise ValueError("needs a 4x4 torus")

    def local_grads(x_blk, dy_blk, wq_loc, w_k, w_v, wo_loc):
        model_dim, kv_heads, e = w_k.shape
        heads = wq_loc.shape[1]
        hd = heads * e
        scale = e ** -0.5
        wq = jnp.transpose(wq_loc, (1, 2, 0)).reshape(hd, model_dim)
        wk = jnp.transpose(w_k, (1, 2, 0))
        wv = jnp.transpose(w_v, (1, 2, 0))
        wo = wo_loc.reshape(hd, model_dim)
        dx, dwq, dwo, dwk, dwv, _, _ = _layer(ring, cores, heads, scale, x_blk, dy_blk, wq, wk, wv, wo)
        return (dx, jnp.transpose(dwq.reshape(heads, e, model_dim), (2, 0, 1)), dwo.reshape(heads, e, model_dim), dwk.T, dwv.T)

    tok = P(("dp", "tp"))
    return jax.shard_map(
        local_grads,
        mesh=mesh,
        in_specs=(tok, tok, P(None, "tp", None), P(), P(), P("tp")),
        out_specs=(tok, P("dp", "tp", None), tok, tok, tok),
        check_vma=False,
    )
```

```python
import functools
import math

import jax
import jax.numpy as jnp
from jax import lax
from jax.experimental import pallas as pl
from jax.experimental.pallas import tpu as pltpu
from jax.sharding import PartitionSpec as P

F32 = jnp.float32
BF16 = jnp.bfloat16
MESH = pl.DeviceIdType.MESH
ANY = pl.BlockSpec(memory_space=pl.ANY)
VMEM = pl.BlockSpec(memory_space=pltpu.VMEM)
LOG2E = math.log2(math.e)


def _scoped(fn):
    def run(*args, **kw):
        with jax.named_scope(fn.__name__):
            return fn(*args, **kw)

    return run


def _dot(a, b, dims):
    return lax.dot_general(a, b, (dims, ((), ())), preferred_element_type=F32)


def _nn(a, b):
    return _dot(a, b, ((1,), (0,)))


def _nt(a, b):
    return _dot(a, b, ((1,), (1,)))


class Place:
    def __init__(self, ring, cores):
        me = lax.axis_index("tp")
        self.ring, self.cores = ring, cores
        self.c = lax.rem(me, cores)
        self.x = lax.rem(me // cores, ring)
        self.y = me // (cores * ring)
        self.r = self.x * cores + self.c
        self.n_row = ring * cores

    def dev(self, y, x, c):
        y = lax.rem(y + self.ring, self.ring)
        x = lax.rem(x + self.ring, self.ring)
        return {"tp": (y * self.ring + x) * self.cores + c}

    def row_dev(self, r):
        return {"tp": self.y * self.n_row + r}

    def slot(self, x, c):
        return lax.rem(x + self.ring, self.ring) * self.cores + c


def _remote(src, dst, send, recv, dev):
    return pltpu.make_async_remote_copy(
        src_ref=src, dst_ref=dst, send_sem=send, recv_sem=recv, device_id=dev, device_id_type=MESH
    )


@_scoped
def _enter(devices):
    barrier = pltpu.get_barrier_semaphore()
    for dev in devices:
        pl.semaphore_signal(barrier, inc=1, device_id=dev, device_id_type=MESH)
    pl.semaphore_wait(barrier, len(devices))


OWN, MINUS, PLUS, FAR = range(4)
STEP = (0, -1, 1, 2)


def _load_shard(at, full, n, y, x, core, block, sem):
    r0 = at.dev(y, x, core)["tp"] * n
    b0 = at.slot(x, core) * n
    src = full.at[pl.ds(pl.multiple_of(r0, n), n), :]
    return pltpu.make_async_copy(src, block.at[pl.ds(pl.multiple_of(b0, n), n), :], sem)


@_scoped
def _take_row(lanes, t, y, block, sem):
    at, full, n = lanes[0].at, lanes[0].full, lanes[0].shard
    for j in range(4):
        _load_shard(at, full, n, y, at.x + STEP[j], at.c, block, sem).start()
    for j in range(4):
        for g in lanes:
            g.await_mate(t, j)
        _load_shard(at, full, n, y, at.x + STEP[j], 1 - at.c, block, sem).start()


class Gather:
    def __init__(self, at, src, full, send, recv, mate_recv, orders, row0, rows, tag):
        self.at, self.src, self.full = at, src, full
        self.send, self.recv, self.mate_recv = send.at[tag], recv.at[tag], mate_recv.at[tag]
        self.order, self.mate_order = orders
        self.row0, self.rows, self.shard = row0, rows, src.shape[0]
        self.sent = []
        c, o = at.c, self.order
        self.first = {s: at.dev(at.y + o * s, at.x + (1 - o) * s, c) for s in (1, -1)}
        self.second = {s: at.dev(at.y + (1 - o) * s, at.x + o * s, c) for s in (1, -1)}
        self.mate = at.dev(at.y, at.x, 1 - c)
        self.fulls = {d: self.both_ways(self.second, d, lambda to, d=d: (d, to)) for d in range(4)}

    def span(self, half):
        n = self.rows if half is None else self.rows // 2
        return self.row0 + (0 if half is None else half * n), n

    def ref(self, d1, d2, half=None):
        at, o = self.at, self.order
        o1, o2 = STEP[d1], STEP[d2]
        start, n = self.span(half)
        r0 = at.dev(at.y + o * o1 + (1 - o) * o2, at.x + (1 - o) * o1 + o * o2, at.c)["tp"] * self.shard + start
        return self.full.at[pl.ds(pl.multiple_of(r0, math.gcd(self.shard, self.row0, n)), n), :]

    def push(self, src, dst, recv, dev):
        k = len(self.sent)
        self.sent.append(dst.shape[0])
        return _remote(src, dst, self.send.at[k], recv, dev)

    def out(self, d1, d2, half=None):
        if d1 == OWN and d2 == OWN:
            return self.src.at[pl.ds(*self.span(half)), :]
        return self.ref(d1, d2, half)

    def both_ways(self, devs, d1, name):
        copies = []
        for step in (0, 1):
            for s, to in ((1, MINUS), (-1, PLUS)):
                half = step if s == 1 else 1 - step
                copies.append(self.push(self.out(d1, OWN, half), self.ref(d1, OWN, half), self.recv.at[*name(to), half], devs[s]))
        return copies

    def to_mate(self, d1, d2):
        ref = self.ref(d1, d2)
        self.push(self.out(d1, d2), ref, self.mate_recv.at[d1, d2], self.mate).start()

    def arrived(self, d1, d2, half):
        ref = self.ref(d1, d2, half)
        _remote(ref, ref, self.send.at[0], self.recv.at[d1, d2, half], self.mate).wait_recv()

    @_scoped
    def start(self):
        for cp in self.both_ways(self.first, OWN, lambda to: (to, OWN)):
            cp.start()
        self.go(OWN)
        self.to_mate(OWN, OWN)

    def go(self, d1):
        for cp in self.fulls[d1]:
            cp.start()

    @_scoped
    def relay_first(self):
        for d, s, half in ((MINUS, 1, 0), (PLUS, -1, 1)):
            self.arrived(d, OWN, half)
            ref = self.ref(d, OWN, half)
            self.push(ref, ref, self.recv.at[FAR, OWN, half], self.first[s]).start()

    @_scoped
    def near_first(self):
        for d, half in ((MINUS, 1), (PLUS, 0)):
            self.arrived(d, OWN, half)
            self.to_mate(d, OWN)

    @_scoped
    def far_first(self):
        for half in (0, 1):
            self.arrived(FAR, OWN, half)
        self.to_mate(FAR, OWN)

    @_scoped
    def relay_second(self, d1):
        for d, s, half in ((MINUS, 1, 0), (PLUS, -1, 1)):
            self.arrived(d1, d, half)
            ref = self.ref(d1, d, half)
            self.push(ref, ref, self.recv.at[d1, FAR, half], self.second[s]).start()

    @_scoped
    def near_second(self, d1):
        for d, half in ((MINUS, 1), (PLUS, 0)):
            self.arrived(d1, d, half)
            self.to_mate(d1, d)

    @_scoped
    def far_second(self, d1):
        for half in (0, 1):
            self.arrived(d1, FAR, half)
        self.to_mate(d1, FAR)

    def await_mate(self, t, j):
        o = self.mate_order
        ref = self.full.at[pl.ds(0, self.rows), :]
        _remote(ref, ref, self.send.at[0], self.mate_recv.at[(1 - o) * j + o * t, (1 - o) * t + o * j], self.mate).wait_recv()

    @_scoped
    def drain(self):
        for k, n in enumerate(self.sent):
            ref = self.full.at[pl.ds(0, n), :]
            _remote(ref, ref, self.send.at[k], self.send.at[k], self.mate).wait_send()


def _kernel(ring, cores, heads, scale, bq, bs, bc, x_ref, dy_ref, w_ref, wk_ref, wv_ref, wo_ref,
            dx_ref, dwq_ref, dwo_ref, dwk_ref, dwv_ref, xf_ref, dyf_ref,
            gq, w_all, part, rs_half, rs_full, stage, hop_ref, qkvt_ref, dot_ref, dqt_ref, ot_ref, dk_ref, dv_ref, kn_ref, vn_ref,
            send, recv, mate_recv, w_send, w_recv, hop_recv, ld_sem, blk_sem,
            ag_send, ag_recv, rs_send, rs_recv, out_send, out_recv, in_sem, o_sem):
    at = Place(ring, cores)
    n_row = at.n_row
    hd = wo_ref.shape[0]
    e = hd // heads
    tokens, width = xf_ref.shape
    tb = tokens // ring
    cw = width // n_row
    gw = gq.shape[1] // n_row
    c = at.c
    shard = x_ref.shape[0]
    gx = Gather(at, x_ref, xf_ref, send, recv, mate_recv, (c, 1 - c), 0, shard, 0)
    split = shard * 3 // 4
    gy = Gather(at, dy_ref, dyf_ref, send, recv, mate_recv, (c, 1 - c), 0, split, 1)
    gz = Gather(at, dy_ref, dyf_ref, send, recv, mate_recv, (0, 0), split, shard - split, 2)
    n_kv = wk_ref.shape[0] // ring
    per_kv = n_row // n_kv
    row_peers = [lax.rem(at.r + d, n_row) for d in range(1, n_row)]
    up, down = at.dev(at.y + 1, at.x, c), at.dev(at.y - 1, at.x, c)

    hh = hd // 2

    def w_push(k, src, dst, rsem, dev):
        _remote(src, dst, w_send.at[k], rsem, dev).start()

    def wq_slot(slot, half=None):
        r0 = slot * gw + (0 if half is None else half * hh)
        return w_all.at[pl.ds(r0 if isinstance(r0, int) else pl.multiple_of(r0, hh), hd if half is None else hh), :]

    def wcols(slot):
        return pl.ds(pl.multiple_of(slot * cw, cw), cw)

    right, left, mate = at.dev(at.y, at.x + 1, c), at.dev(at.y, at.x - 1, c), at.dev(at.y, at.x, 1 - c)

    @_scoped
    def w_start():
        for half, dev in ((0, right), (1, left)):
            for k in range(cores):
                w_push(half * 2 + k, w_ref.at[pl.ds(half * hh, hh), wcols(at.slot(at.x + 2, k))], hop_ref.at[half * 2 + k], hop_recv.at[half * 2 + k], dev)
        w_push(4, w_ref.at[pl.ds(0, hd), wcols(at.slot(at.x, 1 - c))], wq_slot(at.r), w_recv.at[0], mate)
        for i, s in enumerate((1, -1)):
            for k in range(cores):
                dst_core = c if k == 0 else 1 - c
                w_push(5 + 2 * i + k, w_ref.at[pl.ds(0, hd), wcols(at.slot(at.x + s, dst_core))], wq_slot(at.r), w_recv.at[1 + 2 * i + k], at.dev(at.y, at.x + s, dst_core))

    @_scoped
    def w_relay():
        for half, s in ((0, 1), (1, -1)):
            for n in (half * 2, half * 2 + 1):
                _remote(hop_ref.at[n], hop_ref.at[n], w_send.at[0], hop_recv.at[n], mate).wait_recv()
            for k in range(cores):
                n = half * 2 + k
                src_slot = at.slot(at.x - s, c)
                same = k == 0
                dst_core = c if same else 1 - c
                w_push(9 + n, hop_ref.at[half * 2 + dst_core], wq_slot(src_slot, half), w_recv.at[5 + n], at.dev(at.y, at.x + s, dst_core))

    @_scoped
    def w_finish():
        whole = wq_slot(0)
        piece = wq_slot(0, 0)
        for n in range(9):
            ref = whole if n < 5 else piece
            _remote(ref, ref, w_send.at[0], w_recv.at[n], mate).wait_recv()

    def w_drain():
        whole = wq_slot(0)
        piece = wq_slot(0, 0)
        for k in range(13):
            ref = whole if 4 <= k < 9 else piece
            _remote(ref, ref, w_send.at[k], w_send.at[k], mate).wait_send()

    own_cols = wcols(at.r)
    rows = x_ref.shape[0]
    own_rows = pl.ds(pl.multiple_of((at.y * n_row + at.r) * rows, rows), rows)

    keep = [pltpu.make_async_copy(w_ref.at[:, own_cols], wq_slot(at.r), ld_sem.at[8])]
    for r in range(n_row):
        kv_r = at.y * n_kv + r // per_kv
        for i, w in enumerate((wk_ref, wv_ref)):
            keep.append(pltpu.make_async_copy(w.at[kv_r, :, own_cols], w_all.at[pl.ds(r * gw + hd + i * e, e), :], ld_sem.at[9 + 2 * r + i]))

    th = tb // 2
    tq = th // 2
    tl = tb // n_row
    hw = cw // 2
    half_a, half_b = pl.ds(0, hw), pl.ds(hw, hw)
    units = [(FAR, 0), (FAR, 1), (PLUS, 0), (MINUS, 0), (PLUS, 1), (MINUS, 1), (OWN, 0), (OWN, 1)]
    s_own, s_left, s_right, s_far = (at.slot(at.x + o, c) for o in (0, -1, 1, 2))
    m_own, m_left, m_right, m_far = (at.slot(at.x + o, 1 - c) for o in (0, -1, 1, 2))

    def unit_row(u):
        d, s = units[u % len(units)]
        return pl.multiple_of(lax.rem(at.y + STEP[d] + ring, ring) * tb + s * th, th)

    last = len(units)

    def gcols(u, slot):
        if u == 0:
            return pl.ds(pl.multiple_of(slot * gw, 128), hd)
        if u == last:
            return pl.ds(pl.multiple_of(slot * gw + hd, 128), gw - hd)
        return pl.ds(pl.multiple_of(slot * gw, gw), gw)

    def piece(u, slot, half=None):
        r0 = unit_row(u)
        rows = pl.ds(r0, th) if half is None else pl.ds(pl.multiple_of(r0 + half * tq, tq), tq)
        return gq.at[rows, gcols(u, slot)]

    ag_sent = []

    def ag_push(u, n, slot, dev, half=None):
        ref = piece(u, slot, half)
        _remote(ref, ref, ag_send.at[u, n], ag_recv.at[u, n], dev).start()
        ag_sent.append((u, n, half))

    def ag_drain():
        for u, n, half in ag_sent:
            ref = piece(u, s_own, half)
            _remote(ref, ref, ag_send.at[u, n], ag_recv.at[u, n], mate).wait_send()

    def ag_wait(u, n, slot, half=None):
        ref = piece(u, slot, half)
        _remote(ref, ref, ag_send.at[u, n], ag_recv.at[u, n], mate).wait_recv()

    def ag_own(u):
        ag_push(u, 0, s_own, right)
        ag_push(u, 1, s_own, left)
        ag_push(u, 2, s_own, mate)

    @_scoped
    def ag_relay(u):
        ag_wait(u, 0, s_left)
        ag_push(u, 3, s_left, right, 0)
        ag_push(u, 4, s_left, mate)
        ag_wait(u, 1, s_right)
        ag_push(u, 5, s_right, left, 1)
        ag_push(u, 6, s_right, mate)

    @_scoped
    def ag_finish(u):
        ag_wait(u, 3, s_far, 0)
        ag_push(u, 7, s_far, mate, 0)
        ag_wait(u, 5, s_far, 1)
        ag_push(u, 8, s_far, mate, 1)
        ag_wait(u, 2, m_own)
        ag_wait(u, 4, m_left)
        ag_wait(u, 6, m_right)
        ag_wait(u, 7, m_far, 0)
        ag_wait(u, 8, m_far, 1)

    def settle(u):
        rows = pl.ds(unit_row(u), th)
        kv = jnp.concatenate([(dk_ref[:, rows] * scale).astype(BF16), dv_ref[:, rows].astype(BF16)], axis=0)
        gq[rows, pl.ds(pl.multiple_of(at.r * gw + hd, 128), 2 * e)] = kv.T

    def front(w_v, wo_v, xblk):
        kv = (at.y * n_row + at.r) // (n_row * ring // wk_ref.shape[0])
        loads = [
            pltpu.make_async_copy(w_ref, w_v.at[pl.ds(0, hd), :], ld_sem.at[0]),
            pltpu.make_async_copy(wo_ref, wo_v, ld_sem.at[1]),
            pltpu.make_async_copy(wk_ref.at[kv], w_v.at[pl.ds(hd, e), :], ld_sem.at[6]),
            pltpu.make_async_copy(wv_ref.at[kv], w_v.at[pl.ds(hd + e, e), :], ld_sem.at[7]),
        ]
        ins = [pltpu.make_async_copy(src, xblk.at[pl.ds(i * rows, rows), :], ld_sem.at[2 + i]) for i, src in enumerate((x_ref, dy_ref))]
        outs = [pltpu.make_async_copy(xblk.at[pl.ds(i * rows, rows), :], dst.at[own_rows, :], ld_sem.at[4 + i]) for i, dst in enumerate((xf_ref, dyf_ref))]
        for cp in ins:
            cp.start()
        _enter([up, down] + [at.row_dev(r) for r in row_peers])
        gx.start()
        for cp in loads + keep:
            cp.start()
        for cp in ins:
            cp.wait()
        for cp in outs:
            cp.start()

        dk_ref[...] = jnp.zeros_like(dk_ref)
        dv_ref[...] = jnp.zeros_like(dv_ref)

        @_scoped
        def project(w, out, b):
            pltpu.make_async_copy(xf_ref.at[pl.ds(0, tb), :], xblk, blk_sem.at[0]).wait()

            def block(i, _):
                r0 = pl.multiple_of(i * bq, bq)
                out[:, pl.ds(pl.multiple_of(b * tb + i * bq, bq), bq)] = _nt(w[...], xblk[pl.ds(r0, bq), :]).astype(BF16)
                return 0

            lax.fori_loop(0, tb // bq, block, 0)

        def row_at(t):
            if isinstance(t, int):
                return lax.rem(at.y + STEP[t] + ring, ring)
            off = jnp.where(t == 1, ring - 1, jnp.where(t == 2, 1, jnp.where(t == 3, 2, 0)))
            return lax.rem(at.y + off, ring)

        for cp in loads + outs:
            cp.wait()

        def begin(g):
            g.relay_first()
            g.near_first()
            g.go(MINUS)

            @pl.when(g.order == 0)
            def _():
                g.go(PLUS)

        def begin_far(g):
            g.far_first()

            @pl.when(g.order == 0)
            def _():
                g.go(FAR)

        def begin_second(g):
            g.relay_second(OWN)

            @pl.when(g.order == 1)
            def _():
                g.go(PLUS)

            g.near_second(OWN)

        def second_minus(g):
            g.relay_second(MINUS)

            @pl.when(g.order == 1)
            def _():
                g.go(FAR)

            g.near_second(MINUS)

        def x_turn(t, _):
            @pl.when(t == 0)
            def _():
                begin(gx)
                begin_far(gx)
                begin_second(gx)
                second_minus(gx)
                gx.relay_second(PLUS)
                gx.near_second(PLUS)
                gx.relay_second(FAR)
                gy.start()
                gz.start()
                gx.far_second(OWN)

            @pl.when(t == 1)
            def _():
                gx.near_second(FAR)
                gx.far_second(MINUS)

            @pl.when(t == 2)
            def _():
                for d in (PLUS, FAR):
                    gx.far_second(d)

            @pl.when(t == 3)
            def _():
                begin(gy)
                begin(gz)

            b = row_at(t)
            _take_row((gx,), t, b, xblk, blk_sem.at[0])
            project(w_v, qkvt_ref, b)
            return 0

        lax.fori_loop(0, ring, x_turn, 0)
        for t in range(0, tokens, bq):
            kn_ref[t:t + bq, :] = qkvt_ref[hd:hd + e, t:t + bq].T
            vn_ref[t:t + bq, :] = qkvt_ref[hd + e:hd + 2 * e, t:t + bq].T

        keys_k, keys_v = slice(hd, hd + e), slice(hd + e, hd + 2 * e)
        m4 = heads * bs
        factor = scale * LOG2E

        def row_chunks(k):
            return [slice(t, t + bq) for t in range(0, (k + 1) * tb, bq)]

        def stacked(ref, qs):
            return jnp.concatenate([ref[h * e:(h + 1) * e, qs] for h in range(heads)], axis=1)

        def unstack(ref, qs, value):
            for h in range(heads):
                ref[h * e:(h + 1) * e, qs] = value[:, h * bs:(h + 1) * bs]

        def scores(q, ks, k, j):
            s = _nn(q, qkvt_ref[keys_k, ks])
            if ks.start < k * tb:
                return s
            row = lax.broadcasted_iota(jnp.int32, (m4, bq), 0) & (bs - 1)
            col = lax.broadcasted_iota(jnp.int32, (m4, bq), 1)
            return jnp.where(col + (ks.start - k * tb) <= row + j * bs, s, -jnp.inf)

        def folded(op, total, value):
            for t in range(0, value.shape[1], 128):
                piece = value[:, t:t + 128]
                total = piece if total is None else op(total, piece)
            return total

        def score_buf(ks):
            n = ks.start // cw
            return part.at[n, :, ks.start - n * cw:ks.stop - n * cw]

        def stats_buf(k, j):
            per = cw // 128
            n = k * (tb // bs)
            return part.at[2 + n // per, :, pl.ds(pl.multiple_of((n % per + j) * 128, 128), 128)]

        @_scoped
        def forward(k):
            chunks = row_chunks(k)

            def queries(j, _):
                qs = pl.ds(pl.multiple_of(k * tb + j * bs, bs), bs)
                q = stacked(qkvt_ref, qs).T
                m = None
                for ks in chunks:
                    s = scores(q, ks, k, j)
                    score_buf(ks)[...] = s
                    m = folded(jnp.maximum, m, s)
                m = jnp.max(m, axis=1, keepdims=True)
                total = None
                for ks in chunks:
                    p = jnp.exp2((score_buf(ks)[...] - m) * factor)
                    score_buf(ks)[...] = p
                    total = folded(jnp.add, total, p)
                inv = 1.0 / jnp.sum(total, axis=1, keepdims=True)
                lane = lax.broadcasted_iota(jnp.int32, (m4, 128), 1)
                stats_buf(k, j)[...] = jnp.where(lane == 0, m, inv)
                out = None
                for ks in chunks:
                    piece = _nn((score_buf(ks)[...] * inv).astype(BF16), vn_ref[ks, :])
                    out = piece if out is None else out + piece
                unstack(ot_ref, qs, out.astype(BF16).T)
                return 0

            lax.fori_loop(0, tb // bs, queries, 0)

        @_scoped
        def backward(k, second):
            chunks = row_chunks(k)

            def queries(j, _):
                qs = pl.ds(pl.multiple_of(k * tb + j * bs, bs), bs)
                qt = stacked(qkvt_ref, qs)
                dot = stacked(dot_ref, qs)
                q, do = qt.T, dot.T
                delta = jnp.sum(dot.astype(F32) * stacked(ot_ref, qs).astype(F32), axis=0, keepdims=True)
                delta = jnp.broadcast_to(delta, (128, m4)).T[:, :1]
                stats = stats_buf(k, j)[...]
                m, inv = stats[:, 0:1], stats[:, 1:2]
                dq = None
                for ks in chunks:
                    p = jnp.exp2((scores(q, ks, k, j) - m) * factor) * inv
                    dp = _nn(do, qkvt_ref[keys_v, ks])
                    ds = (p * (dp - delta)).astype(BF16)
                    dv_ref[:, ks] += _nn(dot, p.astype(BF16))
                    dk_ref[:, ks] += _nn(qt, ds)
                    piece = _nn(ds, kn_ref[ks, :])
                    dq = piece if dq is None else dq + piece
                dq = (dq * scale).astype(BF16).T
                unstack(dqt_ref, qs, dq)
                for h in range(0, heads, 2):
                    pair = jnp.concatenate([dq[:, h * bs:(h + 1) * bs], dq[:, (h + 1) * bs:(h + 2) * bs]], axis=0)
                    gq[qs, pl.ds(pl.multiple_of(at.r * gw + h * e, 128), 2 * e)] = pair.T
                return 0

            n = tb // bs // 2
            lax.fori_loop(second * n, (second + 1) * n, queries, 0)

        forward(0)
        begin_far(gy)
        begin_far(gz)
        forward(1)
        begin_second(gy)
        begin_second(gz)
        forward(2)
        forward(3)
        second_minus(gy)
        second_minus(gz)

        @pl.when(c == 0)
        def _():
            w_start()


        def turn(h, _):
            t, second = h // 2, lax.rem(h, 2)

            @pl.when(h == 0)
            def _():
                @pl.when(c == 1)
                def _():
                    far_step(OWN)

            @pl.when(h == 1)
            def _():
                for g in (gy, gz):
                    g.relay_second(PLUS)
                    g.near_second(PLUS)

                @pl.when(c == 1)
                def _():
                    far_step(MINUS)

            @pl.when(h == 2)
            def _():
                for g in (gy, gz):
                    g.relay_second(FAR)
                    g.near_second(FAR)

                @pl.when(c == 1)
                def _():
                    w_start()

            @pl.when(h == 3)
            def _():
                @pl.when(c == 1)
                def _():
                    far_step(PLUS)

                @pl.when(c == 0)
                def _():
                    far_step(OWN)
                    far_step(MINUS)
                    w_relay()

            b = row_at(t)

            @pl.when((second == 0) & (t != 3))
            def _():
                _take_row((gy, gz), t, b, xblk, blk_sem.at[0])

            @pl.when(second == 0)
            def _():
                project(wo_v, dot_ref, b)

            @pl.when(h == 5)
            def _():
                @pl.when(c == 0)
                def _():
                    far_step(PLUS)

                far_step(FAR)
                for d in range(4):
                    gz.far_second(d)

                @pl.when(c == 1)
                def _():
                    w_relay()

                _take_row((gy, gz), FAR, row_at(FAR), xblk, blk_sem.at[0])

            @pl.when(h == 7)
            def _():
                ag_own(0)

            for k in range(ring):
                @pl.when(b == k)
                def _(k=k):
                    backward(k, second)
            return 0

        far_cp = {d: gy.push(gy.ref(d, FAR), gy.ref(d, FAR), gy.mate_recv.at[d, FAR], gy.mate) for d in range(4)}

        @_scoped
        def far_step(d):
            for half in (0, 1):
                gy.arrived(d, FAR, half)
            far_cp[d].start()

        lax.fori_loop(0, 2 * ring, turn, 0)


    pl.run_scoped(front, pltpu.VMEM((hd + 2 * e, width), BF16), pltpu.VMEM((hd, width), BF16), pltpu.VMEM((tb, width), BF16))

    def back(xbuf, obuf, kvt):
        sends = []

        nt = min(256, hw)

        @_scoped
        def partial(u):
            rows = pl.ds(unit_row(u), th)
            d, s = units[u]
            dst = part.at[d, pl.ds(s * th, th), :]

            def tile(j, _):
                cs = pl.ds(pl.multiple_of(j * nt, nt), nt)
                dst[:, cs] = _nn(gq[rows, :], w_all[:, cs])
                return 0

            lax.fori_loop(0, cw // nt, tile, 0)

        def rs_push(n, s, src, dst, dev):
            cp = _remote(src, dst, rs_send.at[n, s], rs_recv.at[n, s], dev)
            cp.start()
            sends.append(cp)

        def rs_wait(n, s):
            ref = rs_half.at[0, s]
            _remote(ref, ref, rs_send.at[n, s], rs_recv.at[n, s], mate).wait_recv()

        def block(d, s, half):
            return part.at[d, pl.ds(s * th, th), half]

        def far_a(s):
            rs_push(0, s, block(FAR, s, half_a), rs_half.at[0, s], up)

        def far_b(s):
            rs_push(1, s, block(FAR, s, half_b), rs_half.at[1, s], down)

        def minus_a(s):
            rs_push(4, s, block(MINUS, s, half_a), rs_full.at[1, s, 0], down)

        def plus_b(s):
            rs_push(3, s, block(PLUS, s, half_b), rs_full.at[0, s, 1], up)

        @_scoped
        def plus_a(s):
            rs_wait(0, s)
            block(PLUS, s, half_a)[...] += rs_half[0, s]
            rs_push(2, s, block(PLUS, s, half_a), rs_full.at[0, s, 0], up)

        @_scoped
        def minus_b(s):
            rs_wait(1, s)
            block(MINUS, s, half_b)[...] += rs_half[1, s]
            rs_push(5, s, block(MINUS, s, half_b), rs_full.at[1, s, 1], down)

        n_steps = width // bc
        depth = xbuf.shape[0]

        def chunk(src, c0, j):
            slot = lax.rem(j, depth)
            return pltpu.make_async_copy(src.at[:, pl.ds(pl.multiple_of(c0 + j * bc, bc), bc)], xbuf.at[slot], in_sem.at[slot])

        def ahead(src, c0, n):
            for j in range(min(depth - 1, n)):
                chunk(src, c0, j).start()

        @_scoped
        def stream(src, lhs, out, j0, j1):
            def store(j):
                slot = lax.rem(j, 2)
                return pltpu.make_async_copy(obuf.at[slot], out.at[:, pl.ds(pl.multiple_of(j * bc, bc), bc)], o_sem.at[slot])

            if j0 == 0:
                ahead(src, 0, n_steps)

            def step(j, _):
                @pl.when(j + depth - 1 < n_steps)
                def _():
                    chunk(src, 0, j + depth - 1).start()

                chunk(src, 0, j).wait()

                @pl.when(j >= 2)
                def _():
                    store(j - 2).wait()

                obuf[lax.rem(j, 2)] = _nn(lhs[...], xbuf[lax.rem(j, depth)])
                store(j).start()
                return 0

            lax.fori_loop(j0, j1, step, 0)
            if j1 == n_steps:
                for j in range(max(n_steps - 2, 0), n_steps):
                    store(j).wait()

        def wo_steps(a, b):
            stream(dyf_ref, ot_ref, dwo_ref, n_steps * a // 16, n_steps * b // 16)

        def wq_steps(a, b):
            stream(xf_ref, dqt_ref, dwq_ref, n_steps * a // 16, n_steps * b // 16)

        first = (at.r // per_kv) * per_kv
        share = width // per_kv
        col0 = lax.rem(at.r, per_kv) * share

        def kv_step(j, _):
            @pl.when(j + depth - 1 < share // bc)
            def _():
                chunk(xf_ref, col0, j + depth - 1).start()

            chunk(xf_ref, col0, j).wait()
            prod = _nn(kvt[...], xbuf[lax.rem(j, depth)])
            dk = dv = None
            for q in range(per_kv):
                a = prod[q * 2 * e:q * 2 * e + e]
                b = prod[q * 2 * e + e:(q + 1) * 2 * e]
                dk = a if dk is None else dk + a
                dv = b if dv is None else dv + b
            cs = pl.ds(pl.multiple_of(j * bc, bc), bc)
            dwk_ref[:, cs] = dk
            dwv_ref[:, cs] = dv
            return 0

        @_scoped
        def kv_grads():
            ahead(xf_ref, col0, share // bc)
            for q in range(per_kv):
                cols = pl.ds(pl.multiple_of((first + q) * gw + hd, 128), gw - hd)
                for t in range(0, tokens, bq):
                    kvt[q * (gw - hd):(q + 1) * (gw - hd), t:t + bq] = gq[t:t + bq, cols].T
            lax.fori_loop(0, share // bc, kv_step, 0)

        per_half = n_row // 2

        def hand(i, r):
            half = (half_a, half_b)[i]
            rows = pl.ds(r * tl, tl)
            cols = pl.ds(pl.multiple_of(at.r * cw + i * hw, hw), hw)
            return stage.at[rows, half], dx_ref.at[:, cols]

        def hand_remote(i, r):
            src, dst = hand(i, r)
            d = lax.rem(r - at.r + n_row, n_row)
            return _remote(src, dst, out_send.at[i, r], out_recv.at[i, d], at.row_dev(r))

        def hand_local(i, r):
            src, dst = hand(i, r)
            return pltpu.make_async_copy(src, dst, out_send.at[i, r])

        @_scoped
        def finish(i, s):
            half = (half_a, half_b)[i]
            rs_wait(2 + i, s)
            rs_wait(4 + i, s)
            stage[s * th:(s + 1) * th, half] = (block(OWN, s, half)[...] + rs_full[0, s, i] + rs_full[1, s, i]).astype(BF16)
            for r in range(s * per_half, (s + 1) * per_half):
                @pl.when(at.r != r)
                def _(r=r):
                    hand_remote(i, r).start()

                @pl.when(at.r == r)
                def _(r=r):
                    hand_local(i, r).start()

        @_scoped
        def received(i):
            for d in range(1, n_row):
                src = lax.rem(at.r + n_row - d, n_row)
                ref = dx_ref.at[:, pl.ds(pl.multiple_of(src * cw + i * hw, hw), hw)]
                _remote(ref, ref, out_send.at[i, 0], out_recv.at[i, d], mate).wait_recv()
            for r in range(n_row):
                @pl.when(at.r != r)
                def _(r=r):
                    hand_remote(i, r).wait_send()

                @pl.when(at.r == r)
                def _(r=r):
                    hand_local(i, r).wait()

        settle(0)
        settle(1)
        ag_own(last)
        ag_relay(0)
        for u in range(2, 8):
            settle(u)
        wo_steps(0, 1)
        ag_relay(last)
        ag_own(1)
        ag_own(2)
        wo_steps(1, 4)
        ag_finish(0)
        ag_finish(last)
        for cp in keep:
            cp.wait()
        w_finish()
        partial(0)
        ag_relay(1)
        far_a(0)
        far_b(0)
        ag_own(3)
        ag_relay(2)
        ag_own(4)
        wo_steps(4, 6)
        ag_finish(1)
        partial(1)
        far_a(1)
        far_b(1)
        ag_relay(3)
        ag_own(5)
        wo_steps(6, 8)
        ag_finish(2)
        partial(2)
        ag_relay(4)
        ag_own(6)
        plus_a(0)
        wo_steps(8, 10)
        ag_finish(3)
        partial(3)
        minus_a(0)
        ag_relay(5)
        ag_own(7)
        wo_steps(10, 12)
        ag_finish(4)
        partial(4)
        plus_a(1)
        plus_b(0)
        ag_relay(6)
        wo_steps(12, 14)
        ag_finish(5)
        partial(5)
        minus_a(1)
        minus_b(0)
        plus_b(1)
        minus_b(1)
        ag_relay(7)
        wo_steps(14, 16)
        ag_finish(6)
        partial(6)
        wq_steps(0, 2)
        ag_finish(7)
        partial(7)
        wq_steps(2, 5)
        finish(0, 0)
        wq_steps(5, 12)
        finish(0, 1)
        wq_steps(12, 16)
        kv_grads()
        finish(1, 0)
        received(0)
        finish(1, 1)
        received(1)
        for cp in sends:
            cp.wait_send()
        ag_drain()
        w_drain()
        for g in (gx, gy, gz):
            g.drain()

    pl.run_scoped(back, pltpu.VMEM((4, tokens, bc), BF16), pltpu.VMEM((2, hd, bc), F32), pltpu.VMEM((per_kv * 2 * e, tokens), BF16))


def _layer(ring, cores, heads, scale, x, dy, wq, wk, wv, wo):
    rows, width = x.shape
    tokens = rows * ring * ring * cores
    hd = wo.shape[0]
    e = hd // heads
    n_row = ring * cores
    cw = width // n_row
    gw = hd + 2 * e
    tb = tokens // ring
    th, hw = tb // 2, cw // 2
    per_kv = n_row * ring // wk.shape[0]
    bq = min(256, tb)
    bs = tb // heads
    bc = min(512, cw // 2)
    dma = pltpu.SemaphoreType.DMA
    shape = jax.ShapeDtypeStruct
    return pl.pallas_call(
        functools.partial(_kernel, ring, cores, heads, scale, bq, bs, bc),
        name="layer",
        in_specs=[ANY] * 6,
        out_specs=[ANY, ANY, ANY, VMEM, VMEM, ANY, ANY],
        out_shape=[
            shape((rows, width), BF16),
            shape((hd, width), F32),
            shape((hd, width), F32),
            shape((e, width // per_kv), F32),
            shape((e, width // per_kv), F32),
            shape((tokens, width), BF16),
            shape((tokens, width), BF16),
        ],
        scratch_shapes=[
            pltpu.VMEM((tokens, n_row * gw), BF16),
            pltpu.VMEM((n_row * gw, cw), BF16),
            pltpu.VMEM((4, tb, cw), F32),
            pltpu.VMEM((2, 2, th, hw), F32),
            pltpu.VMEM((2, 2, 2, th, hw), F32),
            pltpu.VMEM((tb, cw), BF16),
            pltpu.VMEM((4, hd // 2, cw), BF16),
            pltpu.VMEM((gw, tokens), BF16),
            pltpu.VMEM((hd, tokens), BF16),
            pltpu.VMEM((hd, tokens), BF16),
            pltpu.VMEM((hd, tokens), BF16),
            pltpu.VMEM((e, tokens), F32),
            pltpu.VMEM((e, tokens), F32),
            pltpu.VMEM((tokens, e), BF16),
            pltpu.VMEM((tokens, e), BF16),
            dma((3, 48)),
            dma((3, 4, 4, 2)),
            dma((3, 4, 4)),
            dma((13,)),
            dma((9,)),
            dma((4,)),
            dma((9 + 2 * n_row,)),
            dma((1,)),
            dma((9, 9)),
            dma((9, 9)),
            dma((6, 2)),
            dma((6, 2)),
            dma((2, n_row)),
            dma((2, n_row)),
            dma((4,)),
            dma((2,)),
        ],
        compiler_params=pltpu.CompilerParams(collective_id=0, has_side_effects=True, vmem_limit_bytes=67043328),
        cost_estimate=pl.CostEstimate(flops=70 * 10**9, bytes_accessed=300 << 20, transcendentals=heads * tokens * tokens // 2),
    )(x, dy, wq, wk, wv, wo)


def solution(mesh):
    n = mesh.shape["tp"]
    ring = math.isqrt(n // 2)
    cores = n // (ring * ring)
    if ring != 4 or cores != 2:
        raise ValueError("needs a 4x4 torus")

    def local_grads(x_blk, dy_blk, wq_loc, w_k, w_v, wo_loc):
        model_dim, kv_heads, e = w_k.shape
        heads = wq_loc.shape[1]
        hd = heads * e
        scale = e ** -0.5
        wq = jnp.transpose(wq_loc, (1, 2, 0)).reshape(hd, model_dim)
        wk = jnp.transpose(w_k, (1, 2, 0))
        wv = jnp.transpose(w_v, (1, 2, 0))
        wo = wo_loc.reshape(hd, model_dim)
        dx, dwq, dwo, dwk, dwv, _, _ = _layer(ring, cores, heads, scale, x_blk, dy_blk, wq, wk, wv, wo)
        return (dx, jnp.transpose(dwq.reshape(heads, e, model_dim), (2, 0, 1)), dwo.reshape(heads, e, model_dim), dwk.T, dwv.T)

    tok = P(("dp", "tp"))
    return jax.shard_map(
        local_grads,
        mesh=mesh,
        in_specs=(tok, tok, P(None, "tp", None), P(), P(), P("tp")),
        out_specs=(tok, P("dp", "tp", None), tok, tok, tok),
        check_vma=False,
    )
```

```python
import functools
import math

import jax
import jax.numpy as jnp
from jax import lax
from jax.experimental import pallas as pl
from jax.experimental.pallas import tpu as pltpu
from jax.sharding import PartitionSpec as P

F32 = jnp.float32
BF16 = jnp.bfloat16
MESH = pl.DeviceIdType.MESH
ANY = pl.BlockSpec(memory_space=pl.ANY)
VMEM = pl.BlockSpec(memory_space=pltpu.VMEM)
LOG2E = math.log2(math.e)


def _scoped(fn):
    def run(*args, **kw):
        with jax.named_scope(fn.__name__):
            return fn(*args, **kw)

    return run


def _dot(a, b, dims):
    return lax.dot_general(a, b, (dims, ((), ())), preferred_element_type=F32)


def _nn(a, b):
    return _dot(a, b, ((1,), (0,)))


def _nt(a, b):
    return _dot(a, b, ((1,), (1,)))


class Place:
    def __init__(self, ring, cores):
        me = lax.axis_index("tp")
        self.ring, self.cores = ring, cores
        self.c = lax.rem(me, cores)
        self.x = lax.rem(me // cores, ring)
        self.y = me // (cores * ring)
        self.r = self.x * cores + self.c
        self.n_row = ring * cores

    def dev(self, y, x, c):
        y = lax.rem(y + self.ring, self.ring)
        x = lax.rem(x + self.ring, self.ring)
        return {"tp": (y * self.ring + x) * self.cores + c}

    def row_dev(self, r):
        return {"tp": self.y * self.n_row + r}

    def slot(self, x, c):
        return lax.rem(x + self.ring, self.ring) * self.cores + c


def _remote(src, dst, send, recv, dev):
    return pltpu.make_async_remote_copy(
        src_ref=src, dst_ref=dst, send_sem=send, recv_sem=recv, device_id=dev, device_id_type=MESH
    )


@_scoped
def _enter(devices):
    barrier = pltpu.get_barrier_semaphore()
    for dev in devices:
        pl.semaphore_signal(barrier, inc=1, device_id=dev, device_id_type=MESH)
    pl.semaphore_wait(barrier, len(devices))


OWN, MINUS, PLUS, FAR = range(4)
STEP = (0, -1, 1, 2)


def _load_shard(at, full, n, y, x, core, block, sem):
    r0 = at.dev(y, x, core)["tp"] * n
    b0 = at.slot(x, core) * n
    src = full.at[pl.ds(pl.multiple_of(r0, n), n), :]
    return pltpu.make_async_copy(src, block.at[pl.ds(pl.multiple_of(b0, n), n), :], sem)


@_scoped
def _take_row(lanes, t, y, block, sem):
    at, full, n = lanes[0].at, lanes[0].full, lanes[0].shard
    for j in range(4):
        _load_shard(at, full, n, y, at.x + STEP[j], at.c, block, sem).start()
    for j in range(4):
        for g in lanes:
            g.await_mate(t, j)
        _load_shard(at, full, n, y, at.x + STEP[j], 1 - at.c, block, sem).start()


class Gather:
    def __init__(self, at, src, full, send, recv, mate_recv, orders, row0, rows, tag):
        self.at, self.src, self.full = at, src, full
        self.send, self.recv, self.mate_recv = send.at[tag], recv.at[tag], mate_recv.at[tag]
        self.order, self.mate_order = orders
        self.row0, self.rows, self.shard = row0, rows, src.shape[0]
        self.sent = []
        c, o = at.c, self.order
        self.first = {s: at.dev(at.y + o * s, at.x + (1 - o) * s, c) for s in (1, -1)}
        self.second = {s: at.dev(at.y + (1 - o) * s, at.x + o * s, c) for s in (1, -1)}
        self.mate = at.dev(at.y, at.x, 1 - c)
        self.fulls = {d: self.both_ways(self.second, d, lambda to, d=d: (d, to)) for d in range(4)}

    def span(self, half):
        n = self.rows if half is None else self.rows // 2
        return self.row0 + (0 if half is None else half * n), n

    def ref(self, d1, d2, half=None):
        at, o = self.at, self.order
        o1, o2 = STEP[d1], STEP[d2]
        start, n = self.span(half)
        r0 = at.dev(at.y + o * o1 + (1 - o) * o2, at.x + (1 - o) * o1 + o * o2, at.c)["tp"] * self.shard + start
        return self.full.at[pl.ds(pl.multiple_of(r0, math.gcd(self.shard, self.row0, n)), n), :]

    def push(self, src, dst, recv, dev):
        k = len(self.sent)
        self.sent.append(dst.shape[0])
        return _remote(src, dst, self.send.at[k], recv, dev)

    def out(self, d1, d2, half=None):
        if d1 == OWN and d2 == OWN:
            return self.src.at[pl.ds(*self.span(half)), :]
        return self.ref(d1, d2, half)

    def both_ways(self, devs, d1, name):
        copies = []
        for step in (0, 1):
            for s, to in ((1, MINUS), (-1, PLUS)):
                half = step if s == 1 else 1 - step
                copies.append(self.push(self.out(d1, OWN, half), self.ref(d1, OWN, half), self.recv.at[*name(to), half], devs[s]))
        return copies

    def to_mate(self, d1, d2):
        ref = self.ref(d1, d2)
        self.push(self.out(d1, d2), ref, self.mate_recv.at[d1, d2], self.mate).start()

    def arrived(self, d1, d2, half):
        ref = self.ref(d1, d2, half)
        _remote(ref, ref, self.send.at[0], self.recv.at[d1, d2, half], self.mate).wait_recv()

    @_scoped
    def start(self):
        for cp in self.both_ways(self.first, OWN, lambda to: (to, OWN)):
            cp.start()
        self.go(OWN)
        self.to_mate(OWN, OWN)

    def go(self, d1):
        for cp in self.fulls[d1]:
            cp.start()

    @_scoped
    def relay_first(self):
        for d, s, half in ((MINUS, 1, 0), (PLUS, -1, 1)):
            self.arrived(d, OWN, half)
            ref = self.ref(d, OWN, half)
            self.push(ref, ref, self.recv.at[FAR, OWN, half], self.first[s]).start()

    @_scoped
    def near_first(self):
        for d, half in ((MINUS, 1), (PLUS, 0)):
            self.arrived(d, OWN, half)
            self.to_mate(d, OWN)

    @_scoped
    def far_first(self):
        for half in (0, 1):
            self.arrived(FAR, OWN, half)
        self.to_mate(FAR, OWN)

    @_scoped
    def relay_second(self, d1):
        for d, s, half in ((MINUS, 1, 0), (PLUS, -1, 1)):
            self.arrived(d1, d, half)
            ref = self.ref(d1, d, half)
            self.push(ref, ref, self.recv.at[d1, FAR, half], self.second[s]).start()

    @_scoped
    def near_second(self, d1):
        for d, half in ((MINUS, 1), (PLUS, 0)):
            self.arrived(d1, d, half)
            self.to_mate(d1, d)

    @_scoped
    def far_second(self, d1):
        for half in (0, 1):
            self.arrived(d1, FAR, half)
        self.to_mate(d1, FAR)

    def await_mate(self, t, j):
        o = self.mate_order
        ref = self.full.at[pl.ds(0, self.rows), :]
        _remote(ref, ref, self.send.at[0], self.mate_recv.at[(1 - o) * j + o * t, (1 - o) * t + o * j], self.mate).wait_recv()

    @_scoped
    def drain(self):
        for k, n in enumerate(self.sent):
            ref = self.full.at[pl.ds(0, n), :]
            _remote(ref, ref, self.send.at[k], self.send.at[k], self.mate).wait_send()


def _kernel(ring, cores, heads, scale, bq, bs, bc, x_ref, dy_ref, w_ref, wk_ref, wv_ref, wo_ref,
            dx_ref, dwq_ref, dwo_ref, dwk_ref, dwv_ref, xf_ref, dyf_ref,
            gq, w_all, part, rs_half, rs_full, stage, hop_ref, qkvt_ref, dot_ref, dqt_ref, ot_ref, dk_ref, dv_ref, kn_ref, vn_ref,
            send, recv, mate_recv, w_send, w_recv, hop_recv, ld_sem, blk_sem,
            ag_send, ag_recv, rs_send, rs_recv, out_send, out_recv, in_sem, o_sem):
    at = Place(ring, cores)
    n_row = at.n_row
    hd = wo_ref.shape[0]
    e = hd // heads
    tokens, width = xf_ref.shape
    tb = tokens // ring
    cw = width // n_row
    gw = gq.shape[1] // n_row
    c = at.c
    shard = x_ref.shape[0]
    gx = Gather(at, x_ref, xf_ref, send, recv, mate_recv, (c, 1 - c), 0, shard, 0)
    split = shard * 3 // 4
    gy = Gather(at, dy_ref, dyf_ref, send, recv, mate_recv, (c, 1 - c), 0, split, 1)
    gz = Gather(at, dy_ref, dyf_ref, send, recv, mate_recv, (0, 0), split, shard - split, 2)
    n_kv = wk_ref.shape[0] // ring
    per_kv = n_row // n_kv
    row_peers = [lax.rem(at.r + d, n_row) for d in range(1, n_row)]
    up, down = at.dev(at.y + 1, at.x, c), at.dev(at.y - 1, at.x, c)

    hh = hd // 2

    def w_push(k, src, dst, rsem, dev):
        _remote(src, dst, w_send.at[k], rsem, dev).start()

    def wq_slot(slot, half=None):
        r0 = slot * gw + (0 if half is None else half * hh)
        return w_all.at[pl.ds(r0 if isinstance(r0, int) else pl.multiple_of(r0, hh), hd if half is None else hh), :]

    def wcols(slot):
        return pl.ds(pl.multiple_of(slot * cw, cw), cw)

    right, left, mate = at.dev(at.y, at.x + 1, c), at.dev(at.y, at.x - 1, c), at.dev(at.y, at.x, 1 - c)

    @_scoped
    def w_start():
        for half, dev in ((0, right), (1, left)):
            for k in range(cores):
                w_push(half * 2 + k, w_ref.at[pl.ds(half * hh, hh), wcols(at.slot(at.x + 2, k))], hop_ref.at[half * 2 + k], hop_recv.at[half * 2 + k], dev)
        w_push(4, w_ref.at[pl.ds(0, hd), wcols(at.slot(at.x, 1 - c))], wq_slot(at.r), w_recv.at[0], mate)
        for i, s in enumerate((1, -1)):
            for k in range(cores):
                dst_core = c if k == 0 else 1 - c
                w_push(5 + 2 * i + k, w_ref.at[pl.ds(0, hd), wcols(at.slot(at.x + s, dst_core))], wq_slot(at.r), w_recv.at[1 + 2 * i + k], at.dev(at.y, at.x + s, dst_core))

    @_scoped
    def w_relay():
        for half, s in ((0, 1), (1, -1)):
            for n in (half * 2, half * 2 + 1):
                _remote(hop_ref.at[n], hop_ref.at[n], w_send.at[0], hop_recv.at[n], mate).wait_recv()
            for k in range(cores):
                n = half * 2 + k
                src_slot = at.slot(at.x - s, c)
                same = k == 0
                dst_core = c if same else 1 - c
                w_push(9 + n, hop_ref.at[half * 2 + dst_core], wq_slot(src_slot, half), w_recv.at[5 + n], at.dev(at.y, at.x + s, dst_core))

    @_scoped
    def w_finish():
        whole = wq_slot(0)
        piece = wq_slot(0, 0)
        for n in range(9):
            ref = whole if n < 5 else piece
            _remote(ref, ref, w_send.at[0], w_recv.at[n], mate).wait_recv()

    def w_drain():
        whole = wq_slot(0)
        piece = wq_slot(0, 0)
        for k in range(13):
            ref = whole if 4 <= k < 9 else piece
            _remote(ref, ref, w_send.at[k], w_send.at[k], mate).wait_send()

    own_cols = wcols(at.r)
    rows = x_ref.shape[0]
    own_rows = pl.ds(pl.multiple_of((at.y * n_row + at.r) * rows, rows), rows)

    keep = [pltpu.make_async_copy(w_ref.at[:, own_cols], wq_slot(at.r), ld_sem.at[8])]
    for r in range(n_row):
        kv_r = at.y * n_kv + r // per_kv
        for i, w in enumerate((wk_ref, wv_ref)):
            keep.append(pltpu.make_async_copy(w.at[kv_r, :, own_cols], w_all.at[pl.ds(r * gw + hd + i * e, e), :], ld_sem.at[9 + 2 * r + i]))

    th = tb // 2
    tq = th // 2
    tl = tb // n_row
    hw = cw // 2
    half_a, half_b = pl.ds(0, hw), pl.ds(hw, hw)
    units = [(FAR, 0), (FAR, 1), (PLUS, 0), (MINUS, 0), (PLUS, 1), (MINUS, 1), (OWN, 0), (OWN, 1)]
    s_own, s_left, s_right, s_far = (at.slot(at.x + o, c) for o in (0, -1, 1, 2))
    m_own, m_left, m_right, m_far = (at.slot(at.x + o, 1 - c) for o in (0, -1, 1, 2))

    def unit_row(u):
        d, s = units[u % len(units)]
        return pl.multiple_of(lax.rem(at.y + STEP[d] + ring, ring) * tb + s * th, th)

    last = len(units)

    def gcols(u, slot):
        if u == 0:
            return pl.ds(pl.multiple_of(slot * gw, 128), hd)
        if u == last:
            return pl.ds(pl.multiple_of(slot * gw + hd, 128), gw - hd)
        return pl.ds(pl.multiple_of(slot * gw, gw), gw)

    def piece(u, slot, half=None):
        r0 = unit_row(u)
        rows = pl.ds(r0, th) if half is None else pl.ds(pl.multiple_of(r0 + half * tq, tq), tq)
        return gq.at[rows, gcols(u, slot)]

    ag_sent = []

    def ag_push(u, n, slot, dev, half=None):
        ref = piece(u, slot, half)
        _remote(ref, ref, ag_send.at[u, n], ag_recv.at[u, n], dev).start()
        ag_sent.append((u, n, half))

    def ag_drain():
        for u, n, half in ag_sent:
            ref = piece(u, s_own, half)
            _remote(ref, ref, ag_send.at[u, n], ag_recv.at[u, n], mate).wait_send()

    def ag_wait(u, n, slot, half=None):
        ref = piece(u, slot, half)
        _remote(ref, ref, ag_send.at[u, n], ag_recv.at[u, n], mate).wait_recv()

    def ag_own(u):
        ag_push(u, 0, s_own, right)
        ag_push(u, 1, s_own, left)
        ag_push(u, 2, s_own, mate)

    @_scoped
    def ag_relay(u):
        ag_wait(u, 0, s_left)
        ag_push(u, 3, s_left, right, 0)
        ag_push(u, 4, s_left, mate)
        ag_wait(u, 1, s_right)
        ag_push(u, 5, s_right, left, 1)
        ag_push(u, 6, s_right, mate)

    @_scoped
    def ag_finish(u):
        ag_wait(u, 3, s_far, 0)
        ag_push(u, 7, s_far, mate, 0)
        ag_wait(u, 5, s_far, 1)
        ag_push(u, 8, s_far, mate, 1)
        ag_wait(u, 2, m_own)
        ag_wait(u, 4, m_left)
        ag_wait(u, 6, m_right)
        ag_wait(u, 7, m_far, 0)
        ag_wait(u, 8, m_far, 1)

    def settle(u):
        rows = pl.ds(unit_row(u), th)
        kv = jnp.concatenate([(dk_ref[:, rows] * scale).astype(BF16), dv_ref[:, rows].astype(BF16)], axis=0)
        gq[rows, pl.ds(pl.multiple_of(at.r * gw + hd, 128), 2 * e)] = kv.T

    def front(w_v, wo_v, xblk):
        kv = (at.y * n_row + at.r) // (n_row * ring // wk_ref.shape[0])
        loads = [
            pltpu.make_async_copy(w_ref, w_v.at[pl.ds(0, hd), :], ld_sem.at[0]),
            pltpu.make_async_copy(wo_ref, wo_v, ld_sem.at[1]),
            pltpu.make_async_copy(wk_ref.at[kv], w_v.at[pl.ds(hd, e), :], ld_sem.at[6]),
            pltpu.make_async_copy(wv_ref.at[kv], w_v.at[pl.ds(hd + e, e), :], ld_sem.at[7]),
        ]
        ins = [pltpu.make_async_copy(src, xblk.at[pl.ds(i * rows, rows), :], ld_sem.at[2 + i]) for i, src in enumerate((x_ref, dy_ref))]
        outs = [pltpu.make_async_copy(xblk.at[pl.ds(i * rows, rows), :], dst.at[own_rows, :], ld_sem.at[4 + i]) for i, dst in enumerate((xf_ref, dyf_ref))]
        for cp in ins:
            cp.start()
        _enter([up, down] + [at.row_dev(r) for r in row_peers])
        gx.start()
        for cp in loads + keep:
            cp.start()
        for cp in ins:
            cp.wait()
        for cp in outs:
            cp.start()

        dk_ref[...] = jnp.zeros_like(dk_ref)
        dv_ref[...] = jnp.zeros_like(dv_ref)

        @_scoped
        def project(w, out, b):
            pltpu.make_async_copy(xf_ref.at[pl.ds(0, tb), :], xblk, blk_sem.at[0]).wait()

            def block(i, _):
                r0 = pl.multiple_of(i * bq, bq)
                out[:, pl.ds(pl.multiple_of(b * tb + i * bq, bq), bq)] = _nt(w[...], xblk[pl.ds(r0, bq), :]).astype(BF16)
                return 0

            lax.fori_loop(0, tb // bq, block, 0)

        def row_at(t):
            if isinstance(t, int):
                return lax.rem(at.y + STEP[t] + ring, ring)
            off = jnp.where(t == 1, ring - 1, jnp.where(t == 2, 1, jnp.where(t == 3, 2, 0)))
            return lax.rem(at.y + off, ring)

        for cp in loads + outs:
            cp.wait()

        def begin(g):
            g.relay_first()
            g.near_first()
            g.go(MINUS)

            @pl.when(g.order == 0)
            def _():
                g.go(PLUS)

        def begin_far(g):
            g.far_first()

            @pl.when(g.order == 0)
            def _():
                g.go(FAR)

        def begin_second(g):
            g.relay_second(OWN)

            @pl.when(g.order == 1)
            def _():
                g.go(PLUS)

            g.near_second(OWN)

        def second_minus(g):
            g.relay_second(MINUS)

            @pl.when(g.order == 1)
            def _():
                g.go(FAR)

            g.near_second(MINUS)

        def x_turn(t, _):
            @pl.when(t == 0)
            def _():
                begin(gx)
                begin_far(gx)
                begin_second(gx)
                second_minus(gx)
                gx.relay_second(PLUS)
                gx.near_second(PLUS)
                gx.relay_second(FAR)
                gy.start()
                gz.start()
                gx.far_second(OWN)

            @pl.when(t == 1)
            def _():
                gx.near_second(FAR)
                gx.far_second(MINUS)

            @pl.when(t == 2)
            def _():
                for d in (PLUS, FAR):
                    gx.far_second(d)

            @pl.when(t == 3)
            def _():
                begin(gy)
                begin(gz)

            b = row_at(t)
            _take_row((gx,), t, b, xblk, blk_sem.at[0])
            project(w_v, qkvt_ref, b)
            return 0

        lax.fori_loop(0, ring, x_turn, 0)
        for t in range(0, tokens, bq):
            kn_ref[t:t + bq, :] = qkvt_ref[hd:hd + e, t:t + bq].T
            vn_ref[t:t + bq, :] = qkvt_ref[hd + e:hd + 2 * e, t:t + bq].T

        keys_k, keys_v = slice(hd, hd + e), slice(hd + e, hd + 2 * e)
        m4 = heads * bs
        factor = scale * LOG2E

        def row_chunks(k):
            return [slice(t, t + bq) for t in range(0, (k + 1) * tb, bq)]

        def stacked(ref, qs):
            return jnp.concatenate([ref[h * e:(h + 1) * e, qs] for h in range(heads)], axis=1)

        def unstack(ref, qs, value):
            for h in range(heads):
                ref[h * e:(h + 1) * e, qs] = value[:, h * bs:(h + 1) * bs]

        def scores(q, ks, k, j):
            s = _nn(q, qkvt_ref[keys_k, ks])
            if ks.start < k * tb:
                return s
            row = lax.broadcasted_iota(jnp.int32, (m4, bq), 0) & (bs - 1)
            col = lax.broadcasted_iota(jnp.int32, (m4, bq), 1)
            return jnp.where(col + (ks.start - k * tb) <= row + j * bs, s, -jnp.inf)

        def folded(op, total, value):
            for t in range(0, value.shape[1], 128):
                piece = value[:, t:t + 128]
                total = piece if total is None else op(total, piece)
            return total

        def score_buf(ks):
            n = ks.start // cw
            return part.at[n, :, ks.start - n * cw:ks.stop - n * cw]

        def stats_buf(k, j):
            per = cw // 128
            n = k * (tb // bs)
            return part.at[2 + n // per, :, pl.ds(pl.multiple_of((n % per + j) * 128, 128), 128)]

        @_scoped
        def forward(k):
            chunks = row_chunks(k)

            def queries(j, _):
                qs = pl.ds(pl.multiple_of(k * tb + j * bs, bs), bs)
                q = stacked(qkvt_ref, qs).T
                m = None
                for ks in chunks:
                    s = scores(q, ks, k, j)
                    score_buf(ks)[...] = s
                    m = folded(jnp.maximum, m, s)
                m = jnp.max(m, axis=1, keepdims=True)
                total = None
                for ks in chunks:
                    p = jnp.exp2((score_buf(ks)[...] - m) * factor)
                    score_buf(ks)[...] = p
                    total = folded(jnp.add, total, p)
                inv = 1.0 / jnp.sum(total, axis=1, keepdims=True)
                lane = lax.broadcasted_iota(jnp.int32, (m4, 128), 1)
                stats_buf(k, j)[...] = jnp.where(lane == 0, m, inv)
                out = None
                for ks in chunks:
                    piece = _nn((score_buf(ks)[...] * inv).astype(BF16), vn_ref[ks, :])
                    out = piece if out is None else out + piece
                unstack(ot_ref, qs, out.astype(BF16).T)
                return 0

            lax.fori_loop(0, tb // bs, queries, 0)

        @_scoped
        def backward(k, second):
            chunks = row_chunks(k)

            def queries(j, _):
                qs = pl.ds(pl.multiple_of(k * tb + j * bs, bs), bs)
                qt = stacked(qkvt_ref, qs)
                dot = stacked(dot_ref, qs)
                q, do = qt.T, dot.T
                delta = jnp.sum(dot.astype(F32) * stacked(ot_ref, qs).astype(F32), axis=0, keepdims=True)
                delta = jnp.broadcast_to(delta, (128, m4)).T[:, :1]
                stats = stats_buf(k, j)[...]
                m, inv = stats[:, 0:1], stats[:, 1:2]
                dq = None
                for ks in chunks:
                    p = jnp.exp2((scores(q, ks, k, j) - m) * factor) * inv
                    dp = _nn(do, qkvt_ref[keys_v, ks])
                    ds = (p * (dp - delta)).astype(BF16)
                    dv_ref[:, ks] += _nn(dot, p.astype(BF16))
                    dk_ref[:, ks] += _nn(qt, ds)
                    piece = _nn(ds, kn_ref[ks, :])
                    dq = piece if dq is None else dq + piece
                dq = (dq * scale).astype(BF16).T
                unstack(dqt_ref, qs, dq)
                for h in range(0, heads, 2):
                    pair = jnp.concatenate([dq[:, h * bs:(h + 1) * bs], dq[:, (h + 1) * bs:(h + 2) * bs]], axis=0)
                    gq[qs, pl.ds(pl.multiple_of(at.r * gw + h * e, 128), 2 * e)] = pair.T
                return 0

            n = tb // bs // 2
            lax.fori_loop(second * n, (second + 1) * n, queries, 0)

        forward(0)
        begin_far(gy)
        begin_far(gz)

        @pl.when(c == 0)
        def _():
            w_start()

        forward(1)
        begin_second(gy)
        begin_second(gz)
        forward(2)

        forward(3)
        second_minus(gy)
        second_minus(gz)

        def turn(h, _):
            t, second = h // 2, lax.rem(h, 2)

            @pl.when(h == 0)
            def _():
                @pl.when(c == 1)
                def _():
                    far_step(OWN)

            @pl.when(h == 1)
            def _():
                for g in (gy, gz):
                    g.relay_second(PLUS)
                    g.near_second(PLUS)

                @pl.when(c == 1)
                def _():
                    far_step(MINUS)

            @pl.when(h == 2)
            def _():
                for g in (gy, gz):
                    g.relay_second(FAR)
                    g.near_second(FAR)

                @pl.when(c == 1)
                def _():
                    w_start()

            @pl.when(h == 3)
            def _():
                @pl.when(c == 1)
                def _():
                    far_step(PLUS)

                @pl.when(c == 0)
                def _():
                    far_step(OWN)
                    far_step(MINUS)
                    w_relay()

            b = row_at(t)

            @pl.when((second == 0) & (t != 3))
            def _():
                _take_row((gy, gz), t, b, xblk, blk_sem.at[0])

            @pl.when(second == 0)
            def _():
                project(wo_v, dot_ref, b)

            @pl.when(h == 5)
            def _():
                @pl.when(c == 0)
                def _():
                    far_step(PLUS)

                far_step(FAR)
                for d in range(4):
                    gz.far_second(d)

                @pl.when(c == 1)
                def _():
                    w_relay()

                _take_row((gy, gz), FAR, row_at(FAR), xblk, blk_sem.at[0])

            @pl.when(h == 7)
            def _():
                ag_own(0)

            for k in range(ring):
                @pl.when(b == k)
                def _(k=k):
                    backward(k, second)
            return 0

        far_cp = {d: gy.push(gy.ref(d, FAR), gy.ref(d, FAR), gy.mate_recv.at[d, FAR], gy.mate) for d in range(4)}

        @_scoped
        def far_step(d):
            for half in (0, 1):
                gy.arrived(d, FAR, half)
            far_cp[d].start()

        lax.fori_loop(0, 2 * ring, turn, 0)


    pl.run_scoped(front, pltpu.VMEM((hd + 2 * e, width), BF16), pltpu.VMEM((hd, width), BF16), pltpu.VMEM((tb, width), BF16))

    def back(xbuf, obuf, kvt):
        sends = []

        nt = min(256, hw)

        @_scoped
        def partial(u):
            rows = pl.ds(unit_row(u), th)
            d, s = units[u]
            dst = part.at[d, pl.ds(s * th, th), :]

            def tile(j, _):
                cs = pl.ds(pl.multiple_of(j * nt, nt), nt)
                dst[:, cs] = _nn(gq[rows, :], w_all[:, cs])
                return 0

            lax.fori_loop(0, cw // nt, tile, 0)

        def rs_push(n, s, src, dst, dev):
            cp = _remote(src, dst, rs_send.at[n, s], rs_recv.at[n, s], dev)
            cp.start()
            sends.append(cp)

        def rs_wait(n, s):
            ref = rs_half.at[0, s]
            _remote(ref, ref, rs_send.at[n, s], rs_recv.at[n, s], mate).wait_recv()

        def block(d, s, half):
            return part.at[d, pl.ds(s * th, th), half]

        def far_a(s):
            rs_push(0, s, block(FAR, s, half_a), rs_half.at[0, s], up)

        def far_b(s):
            rs_push(1, s, block(FAR, s, half_b), rs_half.at[1, s], down)

        def minus_a(s):
            rs_push(4, s, block(MINUS, s, half_a), rs_full.at[1, s, 0], down)

        def plus_b(s):
            rs_push(3, s, block(PLUS, s, half_b), rs_full.at[0, s, 1], up)

        @_scoped
        def plus_a(s):
            rs_wait(0, s)
            block(PLUS, s, half_a)[...] += rs_half[0, s]
            rs_push(2, s, block(PLUS, s, half_a), rs_full.at[0, s, 0], up)

        @_scoped
        def minus_b(s):
            rs_wait(1, s)
            block(MINUS, s, half_b)[...] += rs_half[1, s]
            rs_push(5, s, block(MINUS, s, half_b), rs_full.at[1, s, 1], down)

        n_steps = width // bc
        depth = xbuf.shape[0]

        def chunk(src, c0, j):
            slot = lax.rem(j, depth)
            return pltpu.make_async_copy(src.at[:, pl.ds(pl.multiple_of(c0 + j * bc, bc), bc)], xbuf.at[slot], in_sem.at[slot])

        def ahead(src, c0, n):
            for j in range(min(depth - 1, n)):
                chunk(src, c0, j).start()

        @_scoped
        def stream(src, lhs, out, j0, j1):
            def store(j):
                slot = lax.rem(j, 2)
                return pltpu.make_async_copy(obuf.at[slot], out.at[:, pl.ds(pl.multiple_of(j * bc, bc), bc)], o_sem.at[slot])

            if j0 == 0:
                ahead(src, 0, n_steps)

            def step(j, _):
                @pl.when(j + depth - 1 < n_steps)
                def _():
                    chunk(src, 0, j + depth - 1).start()

                chunk(src, 0, j).wait()

                @pl.when(j >= 2)
                def _():
                    store(j - 2).wait()

                obuf[lax.rem(j, 2)] = _nn(lhs[...], xbuf[lax.rem(j, depth)])
                store(j).start()
                return 0

            lax.fori_loop(j0, j1, step, 0)
            if j1 == n_steps:
                for j in range(max(n_steps - 2, 0), n_steps):
                    store(j).wait()

        def wo_steps(a, b):
            stream(dyf_ref, ot_ref, dwo_ref, n_steps * a // 16, n_steps * b // 16)

        def wq_steps(a, b):
            stream(xf_ref, dqt_ref, dwq_ref, n_steps * a // 16, n_steps * b // 16)

        first = (at.r // per_kv) * per_kv
        share = width // per_kv
        col0 = lax.rem(at.r, per_kv) * share

        def kv_step(j, _):
            @pl.when(j + depth - 1 < share // bc)
            def _():
                chunk(xf_ref, col0, j + depth - 1).start()

            chunk(xf_ref, col0, j).wait()
            prod = _nn(kvt[...], xbuf[lax.rem(j, depth)])
            dk = dv = None
            for q in range(per_kv):
                a = prod[q * 2 * e:q * 2 * e + e]
                b = prod[q * 2 * e + e:(q + 1) * 2 * e]
                dk = a if dk is None else dk + a
                dv = b if dv is None else dv + b
            cs = pl.ds(pl.multiple_of(j * bc, bc), bc)
            dwk_ref[:, cs] = dk
            dwv_ref[:, cs] = dv
            return 0

        @_scoped
        def kv_grads():
            ahead(xf_ref, col0, share // bc)
            for q in range(per_kv):
                cols = pl.ds(pl.multiple_of((first + q) * gw + hd, 128), gw - hd)
                for t in range(0, tokens, bq):
                    kvt[q * (gw - hd):(q + 1) * (gw - hd), t:t + bq] = gq[t:t + bq, cols].T
            lax.fori_loop(0, share // bc, kv_step, 0)

        per_half = n_row // 2

        def hand(i, r):
            half = (half_a, half_b)[i]
            rows = pl.ds(r * tl, tl)
            cols = pl.ds(pl.multiple_of(at.r * cw + i * hw, hw), hw)
            return stage.at[rows, half], dx_ref.at[:, cols]

        def hand_remote(i, r):
            src, dst = hand(i, r)
            d = lax.rem(r - at.r + n_row, n_row)
            return _remote(src, dst, out_send.at[i, r], out_recv.at[i, d], at.row_dev(r))

        def hand_local(i, r):
            src, dst = hand(i, r)
            return pltpu.make_async_copy(src, dst, out_send.at[i, r])

        @_scoped
        def finish(i, s):
            half = (half_a, half_b)[i]
            rs_wait(2 + i, s)
            rs_wait(4 + i, s)
            stage[s * th:(s + 1) * th, half] = (block(OWN, s, half)[...] + rs_full[0, s, i] + rs_full[1, s, i]).astype(BF16)
            for r in range(s * per_half, (s + 1) * per_half):
                @pl.when(at.r != r)
                def _(r=r):
                    hand_remote(i, r).start()

                @pl.when(at.r == r)
                def _(r=r):
                    hand_local(i, r).start()

        @_scoped
        def received(i):
            for d in range(1, n_row):
                src = lax.rem(at.r + n_row - d, n_row)
                ref = dx_ref.at[:, pl.ds(pl.multiple_of(src * cw + i * hw, hw), hw)]
                _remote(ref, ref, out_send.at[i, 0], out_recv.at[i, d], mate).wait_recv()
            for r in range(n_row):
                @pl.when(at.r != r)
                def _(r=r):
                    hand_remote(i, r).wait_send()

                @pl.when(at.r == r)
                def _(r=r):
                    hand_local(i, r).wait()

        settle(0)
        settle(1)
        ag_own(last)
        ag_relay(0)
        for u in range(2, 8):
            settle(u)
        wo_steps(0, 1)
        ag_relay(last)
        ag_own(1)
        ag_own(2)
        wo_steps(1, 4)
        ag_finish(0)
        ag_finish(last)
        for cp in keep:
            cp.wait()
        w_finish()
        partial(0)
        ag_relay(1)
        far_a(0)
        far_b(0)
        ag_own(3)
        ag_relay(2)
        ag_own(4)
        wo_steps(4, 6)
        ag_finish(1)
        partial(1)
        far_a(1)
        far_b(1)
        ag_relay(3)
        ag_own(5)
        wo_steps(6, 8)
        ag_finish(2)
        partial(2)
        ag_relay(4)
        ag_own(6)
        plus_a(0)
        wo_steps(8, 10)
        ag_finish(3)
        partial(3)
        minus_a(0)
        ag_relay(5)
        ag_own(7)
        wo_steps(10, 12)
        ag_finish(4)
        partial(4)
        plus_a(1)
        plus_b(0)
        ag_relay(6)
        wo_steps(12, 14)
        ag_finish(5)
        partial(5)
        minus_a(1)
        minus_b(0)
        plus_b(1)
        minus_b(1)
        ag_relay(7)
        wo_steps(14, 16)
        ag_finish(6)
        partial(6)
        wq_steps(0, 2)
        ag_finish(7)
        partial(7)
        wq_steps(2, 5)
        finish(0, 0)
        wq_steps(5, 12)
        finish(0, 1)
        wq_steps(12, 16)
        kv_grads()
        finish(1, 0)
        received(0)
        finish(1, 1)
        received(1)
        for cp in sends:
            cp.wait_send()
        ag_drain()
        w_drain()
        for g in (gx, gy, gz):
            g.drain()

    pl.run_scoped(back, pltpu.VMEM((4, tokens, bc), BF16), pltpu.VMEM((2, hd, bc), F32), pltpu.VMEM((per_kv * 2 * e, tokens), BF16))


def _layer(ring, cores, heads, scale, x, dy, wq, wk, wv, wo):
    rows, width = x.shape
    tokens = rows * ring * ring * cores
    hd = wo.shape[0]
    e = hd // heads
    n_row = ring * cores
    cw = width // n_row
    gw = hd + 2 * e
    tb = tokens // ring
    th, hw = tb // 2, cw // 2
    per_kv = n_row * ring // wk.shape[0]
    bq = min(256, tb)
    bs = tb // heads
    bc = min(512, cw // 2)
    dma = pltpu.SemaphoreType.DMA
    shape = jax.ShapeDtypeStruct
    return pl.pallas_call(
        functools.partial(_kernel, ring, cores, heads, scale, bq, bs, bc),
        name="layer",
        in_specs=[ANY] * 6,
        out_specs=[ANY, ANY, ANY, VMEM, VMEM, ANY, ANY],
        out_shape=[
            shape((rows, width), BF16),
            shape((hd, width), F32),
            shape((hd, width), F32),
            shape((e, width // per_kv), F32),
            shape((e, width // per_kv), F32),
            shape((tokens, width), BF16),
            shape((tokens, width), BF16),
        ],
        scratch_shapes=[
            pltpu.VMEM((tokens, n_row * gw), BF16),
            pltpu.VMEM((n_row * gw, cw), BF16),
            pltpu.VMEM((4, tb, cw), F32),
            pltpu.VMEM((2, 2, th, hw), F32),
            pltpu.VMEM((2, 2, 2, th, hw), F32),
            pltpu.VMEM((tb, cw), BF16),
            pltpu.VMEM((4, hd // 2, cw), BF16),
            pltpu.VMEM((gw, tokens), BF16),
            pltpu.VMEM((hd, tokens), BF16),
            pltpu.VMEM((hd, tokens), BF16),
            pltpu.VMEM((hd, tokens), BF16),
            pltpu.VMEM((e, tokens), F32),
            pltpu.VMEM((e, tokens), F32),
            pltpu.VMEM((tokens, e), BF16),
            pltpu.VMEM((tokens, e), BF16),
            dma((3, 48)),
            dma((3, 4, 4, 2)),
            dma((3, 4, 4)),
            dma((13,)),
            dma((9,)),
            dma((4,)),
            dma((9 + 2 * n_row,)),
            dma((1,)),
            dma((9, 9)),
            dma((9, 9)),
            dma((6, 2)),
            dma((6, 2)),
            dma((2, n_row)),
            dma((2, n_row)),
            dma((4,)),
            dma((2,)),
        ],
        compiler_params=pltpu.CompilerParams(collective_id=0, has_side_effects=True, vmem_limit_bytes=67043328),
        cost_estimate=pl.CostEstimate(flops=70 * 10**9, bytes_accessed=300 << 20, transcendentals=heads * tokens * tokens // 2),
    )(x, dy, wq, wk, wv, wo)


def solution(mesh):
    n = mesh.shape["tp"]
    ring = math.isqrt(n // 2)
    cores = n // (ring * ring)
    if ring != 4 or cores != 2:
        raise ValueError("needs a 4x4 torus")

    def local_grads(x_blk, dy_blk, wq_loc, w_k, w_v, wo_loc):
        model_dim, kv_heads, e = w_k.shape
        heads = wq_loc.shape[1]
        hd = heads * e
        scale = e ** -0.5
        wq = jnp.transpose(wq_loc, (1, 2, 0)).reshape(hd, model_dim)
        wk = jnp.transpose(w_k, (1, 2, 0))
        wv = jnp.transpose(w_v, (1, 2, 0))
        wo = wo_loc.reshape(hd, model_dim)
        dx, dwq, dwo, dwk, dwv, _, _ = _layer(ring, cores, heads, scale, x_blk, dy_blk, wq, wk, wv, wo)
        return (dx, jnp.transpose(dwq.reshape(heads, e, model_dim), (2, 0, 1)), dwo.reshape(heads, e, model_dim), dwk.T, dwv.T)

    tok = P(("dp", "tp"))
    return jax.shard_map(
        local_grads,
        mesh=mesh,
        in_specs=(tok, tok, P(None, "tp", None), P(), P(), P("tp")),
        out_specs=(tok, P("dp", "tp", None), tok, tok, tok),
        check_vma=False,
    )
```
